32 devices in a mesh: dp: 8 (over z, y), tensor: 4 (over x, core).
Axes of the slice: x: 2, y: 2, z: 4, core: 2. Of those that a mesh axis runs over, the one named last changes fastest.
Arguments:
- inputs: bfloat16 [4096, 2304], P('dp'), may hold values from -6 to 6
- cotangent: bfloat16 [4096, 2304], P('dp'), may hold values from -6 to 6
- segments: int32 [4096], P('dp'), may hold values from 0 to 127, as said below
- positions: int32 [4096], P('dp'), may hold values from 0 to 127, as said below
- w_query: bfloat16 [2304, 2048], P('dp', 'tensor'), may hold values from -0.125 to 0.125
- w_key: bfloat16 [2304, 1024], P('dp', 'tensor'), may hold values from -0.125 to 0.125
- w_value: bfloat16 [2304, 1024], P('dp', 'tensor'), may hold values from -0.125 to 0.125
- w_output: bfloat16 [2048, 2304], P('tensor', 'dp'), may hold values from -0.125 to 0.125
- w_gate: bfloat16 [2304, 9216], P('dp', 'tensor'), may hold values from -0.125 to 0.125
- w_up: bfloat16 [2304, 9216], P('dp', 'tensor'), may hold values from -0.125 to 0.125
- w_down: bfloat16 [9216, 2304], P('tensor', 'dp'), may hold values from -0.0625 to 0.0625
- gain_attn: bfloat16 [2304], P('dp'), may hold values from 0.5 to 1.5
- gain_post_attn: bfloat16 [2304], P('dp'), may hold values from 0.5 to 1.5
- gain_ffw: bfloat16 [2304], P('dp'), may hold values from 0.5 to 1.5
- gain_post_ffw: bfloat16 [2304], P('dp'), may hold values from 0.5 to 1.5
Outputs:
- output: bfloat16 [4096, 2304], P('dp')
- grad_inputs: bfloat16 [4096, 2304], P('dp')
- grad_query: float32 [2304, 2048], P('dp', 'tensor')
- grad_key: float32 [2304, 1024], P('dp', 'tensor')
- grad_value: float32 [2304, 1024], P('dp', 'tensor')
- grad_output: float32 [2048, 2304], P('tensor', 'dp')
- grad_gate: float32 [2304, 9216], P('dp', 'tensor')
- grad_up: float32 [2304, 9216], P('dp', 'tensor')
- grad_down: float32 [9216, 2304], P('tensor', 'dp')
- grad_gain_attn: float32 [2304], P('dp')
- grad_gain_post_attn: float32 [2304], P('dp')
- grad_gain_ffw: float32 [2304], P('dp')
- grad_gain_post_ffw: float32 [2304], P('dp')
The draws below stay inside these ranges and needn't reach their ends.
Inputs may be any that keep to these rules, and one draw needn't show every extreme that they name: `segments`: in every packed row of 128 tokens the document numbers start at 0 and rise by one at each new document. `positions`: positions count from 0 at the first token of each document and rise by one per token.
All inputs are finite; a program needn't handle non-finite values.
Results may differ from the reference program's by a relative error of at most 0.022.
Values may be sent and summed in bfloat16 or wider, within the bound.
A program may use at most 256 MiB of HBM per device.

```python
import math
import jax
import jax.numpy as jnp
from jax import lax

D = 2304
FF = 9216
HEADS = 8
KV = 4
HD = 256
ROW_LEN = 128
TOKENS = 4096


def split_rows(key):
    inner = jax.random.fold_in(key, 7)
    rows = TOKENS // ROW_LEN
    marks = jax.random.randint(inner, (rows, ROW_LEN), 0, 40)
    index = jnp.arange(ROW_LEN, dtype=jnp.int32)
    row_index = jnp.arange(rows, dtype=jnp.int32)[:, None]
    starts = jnp.where(index[None, :] == 0, 1, jnp.where(marks == 0, 1, 0)).astype(jnp.int32)
    starts = jnp.where(row_index == 0, 1, starts).astype(jnp.int32)
    starts = jnp.where(row_index == rows - 1, jnp.where(index[None, :] == 0, 1, 0), starts).astype(jnp.int32)
    seg_ids = jnp.cumsum(starts, axis=1).astype(jnp.int32) - 1
    begin = lax.cummax(jnp.where(starts == 1, index[None, :], 0).astype(jnp.int32), axis=1)
    place = index[None, :] - begin
    return (seg_ids.reshape(TOKENS).astype(jnp.int32), place.reshape(TOKENS).astype(jnp.int32))


def draw_segments(key, part):
    return split_rows(key)[0]


def draw_positions(key, part):
    return split_rows(key)[1]


def strengthened(result, rng, source, target, parts, factor):
    owner, partner = [(jnp.arange(result.shape[position]) // (result.shape[position] // parts)).reshape([-1 if axis == position else 1 for axis in range(result.ndim)]) for position in (source, target)]
    chosen = jax.random.permutation(rng, parts)[partner]
    strong = (owner == chosen) | (owner == (partner + parts // 2) % parts)
    return jnp.where(strong, factor * result, result)


def block_scale(rng, extent, cuts, low, high):
    loudness, own = 1.0, jax.random.fold_in(rng, 6)
    for axis_at, parts in cuts:
        steps = jnp.exp(jax.random.uniform(jax.random.fold_in(own, axis_at), (parts,), jnp.float32, low / len(cuts), high / len(cuts)))
        loudness = loudness * jnp.repeat(steps, extent[axis_at] // parts).reshape([-1 if axis == axis_at else 1 for axis in range(len(extent))])
    return loudness


def normal_values(stream_key, dims, scale, bound, split=(), kind=jnp.bfloat16):
    result = jax.random.normal(stream_key, dims, jnp.float32) * scale
    if len(split) > 0:
        result = block_scale(stream_key, dims, split, -0.22, 0.18) * result
    return jnp.clip(result, min=-bound, max=bound).astype(kind)


def bell_draw_with(key, extent, deviation, most, split, heavy, kind=jnp.bfloat16):
    entries = deviation * jax.random.normal(key, extent, jnp.float32)
    if split:
        entries = entries * block_scale(key, extent, split, -0.22, 0.18)
    return jnp.clip(strengthened(entries, jax.random.fold_in(key, 3), *heavy), -most, most).astype(kind)


def setup_inputs(seed: int = 0) -> dict:
    splits = jax.random.split(jax.random.key(seed), 16)
    return {
        "inputs": normal_values(splits[0], (TOKENS, D), 1.0, 6.0, ((0, 8),)),
        "cotangent": bell_draw_with(splits[1], (TOKENS, D), 1.0, 6.0, ((0, 8),), (0, 1, 8, 2.0)),
        "segments": draw_segments(jax.random.fold_in(splits[15], 71), 0),
        "positions": draw_positions(jax.random.fold_in(splits[15], 71), 0),
        "w_query": normal_values(splits[4], (D, HEADS * HD), D ** -0.5, 0.125, ((0, 8), (1, 4))),
        "w_key": normal_values(splits[5], (D, KV * HD), D ** -0.5, 0.125, ((0, 8), (1, 4))),
        "w_value": normal_values(splits[6], (D, KV * HD), D ** -0.5, 0.125, ((0, 8), (1, 4))),
        "w_output": normal_values(splits[7], (HEADS * HD, D), (HEADS * HD) ** -0.5, 0.125, ((0, 4), (1, 8))),
        "w_gate": normal_values(splits[8], (D, FF), D ** -0.5, 0.125, ((0, 8), (1, 4))),
        "w_up": normal_values(splits[9], (D, FF), D ** -0.5, 0.125, ((0, 8), (1, 4))),
        "w_down": normal_values(splits[10], (FF, D), FF ** -0.5, 0.0625, ((0, 4), (1, 8))),
        "gain_attn": jnp.clip(1.0 + 0.1 * jax.random.normal(splits[11], (D,), jnp.float32), 0.5, 1.5).astype(jnp.bfloat16),
        "gain_post_attn": jnp.clip(1.0 + 0.1 * jax.random.normal(splits[12], (D,), jnp.float32), 0.5, 1.5).astype(jnp.bfloat16),
        "gain_ffw": jnp.clip(1.0 + 0.1 * jax.random.normal(splits[13], (D,), jnp.float32), 0.5, 1.5).astype(jnp.bfloat16),
        "gain_post_ffw": jnp.clip(1.0 + 0.1 * jax.random.normal(splits[14], (D,), jnp.float32), 0.5, 1.5).astype(jnp.bfloat16),
    }


EPS = 1e-06
CAP = 50.0
THETA = 10000.0

def rms_scale(field, gain):
    inverse = lax.rsqrt(lax.optimization_barrier(jnp.mean(field * field, axis=-1, keepdims=True)) + EPS)
    return field * inverse * gain

def rms_back(field, gain, grad):
    value, pull = jax.vjp(rms_scale, field, gain)
    return pull(grad)

def geglu(gate, upward):
    return jax.nn.gelu(gate, approximate=True) * upward

def rotate(field, angles, sign):
    half = field.shape[-1] // 2
    cosine = jnp.cos(angles)
    sine = jnp.sin(angles) * sign
    first = field[..., :half]
    second = field[..., half:]
    return jnp.concatenate([first * cosine - second * sine, second * cosine + first * sine], axis=-1)

def make_angles(positions, head_size):
    half = head_size // 2
    freqs = THETA ** (-(jnp.arange(half).astype(jnp.float32) * 2.0) / head_size)
    return positions.astype(jnp.float32)[:, None, None] * freqs[None, None, :]

def row_mask(segments, rows, length):
    seg_rows = segments.reshape(rows, length)
    same = seg_rows[:, :, None] == seg_rows[:, None, :]
    index = jnp.arange(length)
    causal = index[:, None] >= index[None, :]
    return jnp.logical_and(same, causal[None])

def block_pass(inputs, cotangent, segments, positions, weights, gains):
    w_query, w_key, w_value, w_output, w_gate, w_up, w_down = weights
    gain_one, gain_two, gain_three, gain_four = gains
    count = inputs.shape[0]
    rows = count // ROW_LEN
    group = HEADS // KV
    scale = 1.0 / math.sqrt(HD)
    f32 = jnp.float32
    bf16 = jnp.bfloat16
    source = inputs.astype(f32)
    normed = rms_scale(source, gain_one).astype(bf16)
    angles = make_angles(positions, HD)
    query_raw = jnp.dot(normed, w_query, preferred_element_type=f32).reshape(count, HEADS, HD)
    key_raw = jnp.dot(normed, w_key, preferred_element_type=f32).reshape(count, KV, HD)
    queries = (rotate(query_raw, angles, 1.0) * scale).astype(bf16)
    keys = rotate(key_raw, angles, 1.0).astype(bf16)
    values = jnp.dot(normed, w_value, preferred_element_type=f32).astype(bf16)
    mask = row_mask(segments, rows, ROW_LEN)[:, None, None]
    query_five = queries.reshape(rows, ROW_LEN, KV, group, HD).astype(f32)
    key_four = keys.reshape(rows, ROW_LEN, KV, HD).astype(f32)
    value_four = values.reshape(rows, ROW_LEN, KV, HD).astype(f32)
    capped = CAP * jnp.tanh(jnp.einsum('rqkgd,rskd->rkgqs', query_five, key_four) / CAP)
    expo = jnp.where(mask, jnp.exp(capped), 0.0)
    total = lax.optimization_barrier(jnp.sum(expo, axis=-1, keepdims=True))
    lse = jnp.log(total)
    probs = (expo / total).astype(bf16)
    attended = jnp.einsum('rkgqs,rskd->rqkgd', probs.astype(f32), value_four)
    attended = attended.reshape(count, HEADS * HD).astype(bf16)
    branch_attn = jnp.dot(attended, w_output, preferred_element_type=f32)
    hidden = source + rms_scale(branch_attn, gain_two)
    normed_ffw = rms_scale(hidden, gain_three).astype(bf16)
    gate = jnp.dot(normed_ffw, w_gate, preferred_element_type=f32)
    upward = jnp.dot(normed_ffw, w_up, preferred_element_type=f32)
    mixed = geglu(gate, upward).astype(bf16)
    branch_ffw = jnp.dot(mixed, w_down, preferred_element_type=f32)
    output = (hidden + rms_scale(branch_ffw, gain_four)).astype(bf16)
    d_out = cotangent.astype(f32)
    d_branch_ffw, d_gain_four = rms_back(branch_ffw, gain_four, d_out)
    d_branch_ffw = d_branch_ffw.astype(bf16)
    grad_down = jnp.dot(mixed.T, d_branch_ffw, preferred_element_type=f32)
    d_mixed = jnp.dot(d_branch_ffw, w_down.T, preferred_element_type=f32)
    value_unused, pull = jax.vjp(geglu, gate, upward)
    d_gate, d_up = pull(d_mixed)
    d_gate = d_gate.astype(bf16)
    d_up = d_up.astype(bf16)
    grad_gate = jnp.dot(normed_ffw.T, d_gate, preferred_element_type=f32)
    grad_up = jnp.dot(normed_ffw.T, d_up, preferred_element_type=f32)
    d_normed_ffw = jnp.dot(d_gate, w_gate.T, preferred_element_type=f32) + jnp.dot(d_up, w_up.T, preferred_element_type=f32)
    d_hidden_norm, d_gain_three = rms_back(hidden, gain_three, d_normed_ffw)
    d_hidden = d_out + d_hidden_norm
    d_branch_attn, d_gain_two = rms_back(branch_attn, gain_two, d_hidden)
    d_branch_attn = d_branch_attn.astype(bf16)
    grad_output = jnp.dot(attended.T, d_branch_attn, preferred_element_type=f32)
    d_attended = jnp.dot(d_branch_attn, w_output.T, preferred_element_type=f32).astype(bf16)
    d_att_five = d_attended.reshape(rows, ROW_LEN, KV, group, HD).astype(f32)
    recomputed = jnp.where(mask, jnp.exp(capped - lse), 0.0)
    d_values = jnp.einsum('rkgqs,rqkgd->rskd', recomputed.astype(bf16).astype(f32), d_att_five)
    d_probs = jnp.einsum('rqkgd,rskd->rkgqs', d_att_five, value_four)
    d_soft = recomputed * (d_probs - lax.optimization_barrier(jnp.sum(recomputed * d_probs, axis=-1, keepdims=True)))
    d_capped = (d_soft * (1.0 - (capped / CAP) ** 2)).astype(bf16).astype(f32)
    d_queries = jnp.einsum('rkgqs,rskd->rqkgd', d_capped, key_four).reshape(count, HEADS, HD)
    d_keys = jnp.einsum('rkgqs,rqkgd->rskd', d_capped, query_five).reshape(count, KV, HD)
    d_query_proj = (rotate(d_queries, angles, -1.0) * scale).astype(bf16).reshape(count, HEADS * HD)
    d_key_proj = rotate(d_keys, angles, -1.0).astype(bf16).reshape(count, KV * HD)
    d_value_proj = d_values.reshape(count, KV * HD).astype(bf16)
    grad_query = jnp.dot(normed.T, d_query_proj, preferred_element_type=f32)
    grad_key = jnp.dot(normed.T, d_key_proj, preferred_element_type=f32)
    grad_value = jnp.dot(normed.T, d_value_proj, preferred_element_type=f32)
    d_normed = jnp.dot(d_query_proj, w_query.T, preferred_element_type=f32)
    d_normed = d_normed + jnp.dot(d_key_proj, w_key.T, preferred_element_type=f32)
    d_normed = d_normed + jnp.dot(d_value_proj, w_value.T, preferred_element_type=f32)
    d_source, d_gain_one = rms_back(source, gain_one, d_normed)
    grad_inputs = (d_hidden + d_source).astype(bf16)
    grads = (grad_query, grad_key, grad_value, grad_output, grad_gate, grad_up, grad_down, d_gain_one, d_gain_two, d_gain_three, d_gain_four)
    return (output, grad_inputs, grads)

def reference(inputs, cotangent, segments, positions, w_query, w_key, w_value, w_output, w_gate, w_up, w_down, gain_attn, gain_post_attn, gain_ffw, gain_post_ffw):
    weights = (w_query, w_key, w_value, w_output, w_gate, w_up, w_down)
    gains = (gain_attn.astype(jnp.float32), gain_post_attn.astype(jnp.float32), gain_ffw.astype(jnp.float32), gain_post_ffw.astype(jnp.float32))
    block = math.gcd(TOKENS, 4096)
    blocks = TOKENS // block
    stacked = (inputs.reshape(blocks, block, D), cotangent.reshape(blocks, block, D), segments.reshape(blocks, block), positions.reshape(blocks, block))
    start = tuple((jnp.zeros(w.shape, jnp.float32) for w in weights)) + tuple((jnp.zeros((D,), jnp.float32) for piece in range(4)))

    def step(carry, items):
        output, grad_inputs, grads = block_pass(items[0], items[1], items[2], items[3], weights, gains)
        carry = tuple((left + right for left, right in zip(carry, grads)))
        return (carry, (output, grad_inputs))
    totals, outputs = lax.scan(step, start, stacked)
    output = outputs[0].reshape(TOKENS, D)
    grad_inputs = outputs[1].reshape(TOKENS, D)
    return (output, grad_inputs, totals[0], totals[1], totals[2], totals[3], totals[4], totals[5], totals[6], totals[7], totals[8], totals[9], totals[10])
```

```python
import math

import jax
import jax.numpy as jnp
from jax import lax
from jax.sharding import PartitionSpec as P

HEADS = 8
KV = 4
HD = 256
ROW_LEN = 128
LANE = 128


EPS = 1e-06
CAP = 50.0
THETA = 10000.0

f32 = jnp.float32
bf16 = jnp.bfloat16


def rms_scale(field, gain):
    inverse = lax.rsqrt(jnp.mean(field * field, axis=-1, keepdims=True) + EPS)
    return field * inverse * gain


def rms_back(field, gain, grad):
    inverse = lax.rsqrt(jnp.mean(field * field, axis=-1, keepdims=True) + EPS)
    unit = field * inverse
    d_gain = jnp.sum(grad * unit, axis=0)
    scaled = grad * gain
    d_field = inverse * (scaled - unit * jnp.mean(scaled * unit, axis=-1, keepdims=True))
    return d_field, d_gain


def geglu(gate, upward):
    return jax.nn.gelu(gate, approximate=True) * upward


def rotate(field, cosine, sine):
    half = field.shape[-1] // 2
    first = field[..., :half]
    second = field[..., half:]
    return jnp.concatenate(
        [first * cosine - second * sine, second * cosine + first * sine], axis=-1
    )


def make_angles(positions, head_size):
    half = head_size // 2
    freqs = THETA ** (-(jnp.arange(half).astype(f32) * 2.0) / head_size)
    return positions.astype(f32)[:, None, None] * freqs[None, None, :]


def row_mask(segments, rows, length):
    seg_rows = segments.reshape(rows, length)
    same = seg_rows[:, :, None] == seg_rows[:, None, :]
    index = jnp.arange(length)
    causal = index[:, None] >= index[None, :]
    return jnp.logical_and(same, causal[None])


def dot(left, right):
    return jnp.dot(left, right, preferred_element_type=f32)


def contract_rows(left, right):
    return lax.dot_general(left, right, (((0,), (0,)), ((), ())), preferred_element_type=f32)


def contract_cols(left, right):
    return lax.dot_general(left, right, (((1,), (1,)), ((), ())), preferred_element_type=f32)


class Grid:
    def __init__(self, mesh):
        self.dp = mesh.shape["dp"]
        self.tensor = mesh.shape["tensor"]
        self.depth = 4 if self.dp % 4 == 0 else (2 if self.dp % 2 == 0 else 1)
        self.width = self.dp // self.depth

    def here(self):
        index = lax.axis_index("dp")
        self.deep = index // self.width
        self.wide = lax.rem(index, self.width)
        self.rank = lax.axis_index("tensor")

    def shift(self, value, step):
        pairs = [
            (z * self.width + y, ((z + step) % self.depth) * self.width + y)
            for z in range(self.depth)
            for y in range(self.width)
        ]
        return lax.ppermute(value, "dp", pairs)

    def swap_wide(self, value, bit):
        pairs = [
            (z * self.width + y, z * self.width + (y ^ bit))
            for z in range(self.depth)
            for y in range(self.width)
        ]
        return lax.ppermute(value, "dp", pairs)

    def swap_rank(self, value, bit):
        return lax.ppermute(value, "tensor", [(q, q ^ bit) for q in range(self.tensor)])

    def wide_bits(self):
        return [1 << b for b in range(self.width.bit_length() - 1)]

    def rank_bits(self):
        return [1 << b for b in range(self.tensor.bit_length() - 1)]

    def assemble(self, pieces):
        rows, columns = pieces[0].shape
        out = jnp.zeros((self.dp, rows, columns), pieces[0].dtype)
        for step, piece in enumerate(pieces):
            group = {0: piece}
            for bit in self.wide_bits():
                for key in list(group):
                    group[key ^ bit] = self.swap_wide(group[key], bit)
            source = lax.rem(self.deep + self.depth - step, self.depth)
            for key, part in group.items():
                at = source * self.width + jnp.bitwise_xor(self.wide, key)
                out = lax.dynamic_update_slice(out, part[None], (at, 0, 0))
        return out.reshape(self.dp * rows, columns)

    def gather_rows(self, block):
        return self.assemble([block] + [self.shift(block, s) for s in range(1, self.depth)])

    def exchange_blocks(self, blocks):
        pieces = []
        for step in range(self.depth):
            to = lax.rem(self.deep + step, self.depth)
            part = lax.dynamic_index_in_dim(blocks, to, 0, keepdims=False)
            pieces.append(part if step == 0 else self.shift(part, step))
        return self.assemble(pieces)

    def reduce_width(self, full):
        rows, columns = full.shape[0] // self.dp, full.shape[1]
        held = full.reshape(self.depth, self.width, rows, columns)
        for bit in reversed(self.wide_bits()):
            held = held.reshape(self.depth, 2, bit, rows, columns)
            mine = lax.rem(self.wide // bit, 2)
            other = lax.dynamic_index_in_dim(held, 1 - mine, 1, keepdims=False)
            own = lax.dynamic_index_in_dim(held, mine, 1, keepdims=False)
            held = own + self.swap_wide(other, bit)
        return held.reshape(self.depth, rows, columns)

    def pick(self, held, step):
        to = lax.rem(self.deep + step, self.depth)
        return lax.dynamic_index_in_dim(held, to, 0, keepdims=False)

    def scatter_rows(self, full):
        held = self.reduce_width(full)
        total = self.pick(held, 0).astype(f32)
        for step in range(1, self.depth):
            total = total + self.shift(self.pick(held, step), step).astype(f32)
        return total

    def return_blocks(self, full):
        held = self.reduce_width(full)
        out = jnp.zeros_like(held)
        for step in range(self.depth):
            part = self.pick(held, step)
            part = part if step == 0 else self.shift(part, step)
            source = lax.rem(self.deep + self.depth - step, self.depth)
            out = lax.dynamic_update_slice(out, part[None], (source, 0, 0))
        return out

    def spread_rank(self, block):
        for bit in reversed(self.rank_bits()):
            block = jnp.concatenate([block, self.swap_rank(block, bit)], axis=0)
        return block

    def reduce_rank(self, full):
        for bit in self.rank_bits():
            half = full.shape[0] // 2
            full = full[:half] + self.swap_rank(full[half:], bit)
        return full

    def flips(self):
        order = [0]
        for bit in reversed(self.rank_bits()):
            order = order + [k ^ bit for k in order]
        return order

    def spread_all(self, block):
        parts = [self.spread_rank(block)]
        for step in range(1, self.depth):
            parts.append(self.spread_rank(self.shift(block, step)))
        return jnp.concatenate(parts, axis=0)

    def reduce_all(self, make_part):
        terms = []
        for step in list(range(1, self.depth)) + [0]:
            term = self.reduce_rank(make_part(step))
            terms.append(term if step == 0 else self.shift(term, -step))
        total = terms[-1].astype(f32)
        for term in terms[:-1]:
            total = total + term.astype(f32)
        return total


def unit_cuts(units, parts):
    tiles = units // LANE
    edges = [(tiles * k + parts - 1) // parts for k in range(parts + 1)]
    starts = [e * LANE for e in edges[:-1]]
    sizes = [(b - a) * LANE for a, b in zip(edges[:-1], edges[1:])]
    return starts, sizes, max(sizes)


def cut_units(block, cuts):
    starts, sizes, share = cuts
    return jnp.stack(
        [
            jnp.pad(block[:, a : a + n], ((0, 0), (0, share - n))) if n < share else block[:, a : a + n]
            for a, n in zip(starts, sizes)
        ]
    )


def join_units(blocks, cuts):
    starts, sizes, share = cuts
    return jnp.concatenate([blocks[k, :, :n] for k, n in enumerate(sizes)], axis=1)


def make_body(grid):
    def body(
        inputs,
        cotangent,
        segments,
        positions,
        w_query,
        w_key,
        w_value,
        w_output,
        w_gate,
        w_up,
        w_down,
        gain_attn,
        gain_post_attn,
        gain_ffw,
        gain_post_ffw,
    ):
        grid.here()
        count, width = inputs.shape
        shard = w_query.shape[0]
        group = HEADS // KV
        local_kv = w_key.shape[1] // HD
        local_heads = local_kv * group
        q_cols, k_cols = w_query.shape[1], w_key.shape[1]
        scale = 1.0 / math.sqrt(HD)
        part = count // grid.tensor
        rows = count // ROW_LEN
        cuts = unit_cuts(w_gate.shape[1], grid.depth)
        share = cuts[2]

        gains = jnp.stack([gain_attn, gain_post_attn, gain_ffw, gain_post_ffw])
        gains = grid.gather_rows(gains).reshape(grid.dp, 4, shard)
        gains = gains.transpose(1, 0, 2).reshape(4, width).astype(f32)
        gain_one, gain_two, gain_three, gain_four = gains[0], gains[1], gains[2], gains[3]
        full_qkv = grid.gather_rows(jnp.concatenate([w_query, w_key, w_value], axis=1))
        full_out = grid.gather_rows(w_output.T)
        full_gu = grid.exchange_blocks(
            jnp.concatenate([cut_units(w_gate, cuts), cut_units(w_up, cuts)], axis=2)
        )
        full_dn = grid.exchange_blocks(cut_units(w_down.T, cuts))

        where = [jnp.bitwise_xor(grid.rank, flip) * part for flip in grid.flips()]
        take = lambda a: jnp.concatenate(
            [lax.dynamic_slice_in_dim(a, at, part, 0) for at in where], axis=0
        )
        source = take(inputs).astype(f32)
        segs = take(segments)
        angles = make_angles(take(positions), HD)
        cosine, sine = jnp.cos(angles), jnp.sin(angles)

        normed = rms_scale(source, gain_one).astype(bf16)
        qkv = dot(normed, full_qkv)
        query_raw = qkv[:, :q_cols].reshape(count, local_heads, HD)
        key_raw = qkv[:, q_cols : q_cols + k_cols].reshape(count, local_kv, HD)
        queries = (rotate(query_raw, cosine, sine) * scale).astype(bf16)
        keys = rotate(key_raw, cosine, sine).astype(bf16)
        values = qkv[:, q_cols + k_cols :].astype(bf16)
        mask = row_mask(segs, rows, ROW_LEN)[:, None, None]
        query_five = queries.reshape(rows, ROW_LEN, local_kv, group, HD)
        key_four = keys.reshape(rows, ROW_LEN, local_kv, HD)
        value_four = values.reshape(rows, ROW_LEN, local_kv, HD)
        scores = jnp.einsum("rqkgd,rskd->rkgqs", query_five, key_four, preferred_element_type=f32)
        capped = CAP * jnp.tanh(scores / CAP)
        expo = jnp.where(mask, jnp.exp(capped), 0.0)
        total = jnp.sum(expo, axis=-1, keepdims=True)
        soft = expo / total
        probs = soft.astype(bf16)
        attended = jnp.einsum("rkgqs,rskd->rqkgd", probs, value_four, preferred_element_type=f32)
        attended = attended.reshape(count, local_heads * HD).astype(bf16)
        branch_attn = grid.reduce_rank(contract_cols(attended, full_out).astype(bf16)).astype(f32)

        own_source = source[:part]
        hidden = own_source + rms_scale(branch_attn, gain_two)
        normed_own = rms_scale(hidden, gain_three).astype(bf16)
        normed_ffw = grid.spread_all(normed_own)
        gu = dot(normed_ffw, full_gu)
        gate, upward = gu[:, :share], gu[:, share:]
        mixed = geglu(gate, upward).astype(bf16)
        branch_ffw = grid.reduce_all(
            lambda s: contract_cols(mixed[s * count : (s + 1) * count], full_dn).astype(bf16)
        )
        own_out = (hidden + rms_scale(branch_ffw, gain_four)).astype(bf16)

        d_out = lax.dynamic_slice_in_dim(cotangent, grid.rank * part, part, 0).astype(f32)
        d_branch_own, d_gain_four = rms_back(branch_ffw, gain_four, d_out)
        d_branch_ffw = grid.spread_all(d_branch_own.astype(bf16))
        d_mixed = dot(d_branch_ffw, full_dn)
        value_unused, pull = jax.vjp(geglu, gate, upward)
        d_gate, d_up = pull(d_mixed)
        d_gu = jnp.concatenate([d_gate.astype(bf16), d_up.astype(bf16)], axis=1)
        d_normed_ffw = grid.reduce_all(
            lambda s: contract_cols(d_gu[s * count : (s + 1) * count], full_gu).astype(bf16)
        )
        grad_dn = contract_rows(d_branch_ffw, mixed).astype(bf16)
        grad_gu = contract_rows(normed_ffw, d_gu).astype(bf16)
        blocks_dn = grid.return_blocks(grad_dn)
        blocks_gu = grid.return_blocks(grad_gu)
        grad_down = join_units(blocks_dn, cuts).T.astype(f32)
        grad_gate = join_units(blocks_gu[:, :, :share], cuts).astype(f32)
        grad_up = join_units(blocks_gu[:, :, share:], cuts).astype(f32)

        d_hidden_norm, d_gain_three = rms_back(hidden, gain_three, d_normed_ffw)
        d_hidden = d_out + d_hidden_norm
        d_branch_attn, d_gain_two = rms_back(branch_attn, gain_two, d_hidden)
        d_branch_attn = grid.spread_rank(d_branch_attn.astype(bf16))
        grad_output = contract_rows(d_branch_attn, attended).astype(bf16)
        grad_output = grid.scatter_rows(grad_output).T
        d_attended = dot(d_branch_attn, full_out).astype(bf16)
        d_att_five = d_attended.reshape(rows, ROW_LEN, local_kv, group, HD)
        d_values = jnp.einsum("rkgqs,rqkgd->rskd", probs, d_att_five, preferred_element_type=f32)
        d_probs = jnp.einsum("rqkgd,rskd->rkgqs", d_att_five, value_four, preferred_element_type=f32)
        d_soft = soft * (d_probs - jnp.sum(soft * d_probs, axis=-1, keepdims=True))
        d_capped = (d_soft * (1.0 - (capped / CAP) ** 2)).astype(bf16)
        d_queries = jnp.einsum(
            "rkgqs,rskd->rqkgd", d_capped, key_four, preferred_element_type=f32
        ).reshape(count, local_heads, HD)
        d_keys = jnp.einsum(
            "rkgqs,rqkgd->rskd", d_capped, query_five, preferred_element_type=f32
        ).reshape(count, local_kv, HD)
        d_query_proj = (rotate(d_queries, cosine, -sine) * scale).astype(bf16).reshape(count, q_cols)
        d_key_proj = rotate(d_keys, cosine, -sine).astype(bf16).reshape(count, k_cols)
        d_value_proj = d_values.reshape(count, k_cols).astype(bf16)
        d_qkv = jnp.concatenate([d_query_proj, d_key_proj, d_value_proj], axis=1)
        d_normed = grid.reduce_rank(contract_cols(d_qkv, full_qkv).astype(bf16)).astype(f32)
        grad_qkv = grid.scatter_rows(contract_rows(normed, d_qkv).astype(bf16))
        d_source, d_gain_one = rms_back(own_source, gain_one, d_normed)
        own_grad = (d_hidden + d_source).astype(bf16)

        d_gains = jnp.stack([d_gain_one, d_gain_two, d_gain_three, d_gain_four])
        for bit in grid.rank_bits():
            d_gains = d_gains + grid.swap_rank(d_gains, bit)
        d_gains = d_gains.reshape(4, grid.dp, shard).transpose(1, 0, 2).reshape(grid.dp * 4, shard)
        d_gains = grid.scatter_rows(d_gains)

        def place(block):
            whole = grid.spread_rank(block)
            out = jnp.zeros_like(whole)
            for at, k in zip(where, range(grid.tensor)):
                out = lax.dynamic_update_slice(out, whole[k * part : (k + 1) * part], (at, 0))
            return out

        return (
            place(own_out),
            place(own_grad),
            grad_qkv[:, :q_cols],
            grad_qkv[:, q_cols : q_cols + k_cols],
            grad_qkv[:, q_cols + k_cols :],
            grad_output,
            grad_gate,
            grad_up,
            grad_down,
            d_gains[0],
            d_gains[1],
            d_gains[2],
            d_gains[3],
        )

    return body


def solution(mesh):
    placed = (
        P("dp", None),
        P("dp", None),
        P("dp"),
        P("dp"),
        P("dp", "tensor"),
        P("dp", "tensor"),
        P("dp", "tensor"),
        P("tensor", "dp"),
        P("dp", "tensor"),
        P("dp", "tensor"),
        P("tensor", "dp"),
        P("dp"),
        P("dp"),
        P("dp"),
        P("dp"),
    )
    return jax.shard_map(
        make_body(Grid(mesh)),
        mesh=mesh,
        in_specs=placed,
        out_specs=(
            P("dp", None),
            P("dp", None),
            P("dp", "tensor"),
            P("dp", "tensor"),
            P("dp", "tensor"),
            P("tensor", "dp"),
            P("dp", "tensor"),
            P("dp", "tensor"),
            P("tensor", "dp"),
            P("dp"),
            P("dp"),
            P("dp"),
            P("dp"),
        ),
        check_vma=False,
    )
```

```python
import math

import jax
import jax.numpy as jnp
from jax import lax
from jax.experimental import pallas as pl
from jax.experimental.pallas import tpu as pltpu
from jax.sharding import PartitionSpec as P

HEADS = 8
KV = 4
HD = 256
ROW_LEN = 128
LANE = 128


EPS = 1e-06
CAP = 50.0
THETA = 10000.0

f32 = jnp.float32
bf16 = jnp.bfloat16


def rms_scale(field, gain):
    inverse = lax.rsqrt(jnp.mean(field * field, axis=-1, keepdims=True) + EPS)
    return field * inverse * gain


def rms_back(field, gain, grad):
    inverse = lax.rsqrt(jnp.mean(field * field, axis=-1, keepdims=True) + EPS)
    unit = field * inverse
    d_gain = jnp.sum(grad * unit, axis=0)
    scaled = grad * gain
    d_field = inverse * (scaled - unit * jnp.mean(scaled * unit, axis=-1, keepdims=True))
    return d_field, d_gain


def geglu(gate, upward):
    return jax.nn.gelu(gate, approximate=True) * upward


def rotate(field, cosine, sine):
    half = field.shape[-1] // 2
    first = field[..., :half]
    second = field[..., half:]
    return jnp.concatenate(
        [first * cosine - second * sine, second * cosine + first * sine], axis=-1
    )


def make_angles(positions, head_size):
    half = head_size // 2
    freqs = THETA ** (-(jnp.arange(half).astype(f32) * 2.0) / head_size)
    return positions.astype(f32)[:, None, None] * freqs[None, None, :]


def row_mask(segments, rows, length):
    seg_rows = segments.reshape(rows, length)
    same = seg_rows[:, :, None] == seg_rows[:, None, :]
    index = jnp.arange(length)
    causal = index[:, None] >= index[None, :]
    return jnp.logical_and(same, causal[None])


def dot(left, right):
    return jnp.dot(left, right, preferred_element_type=f32)


def contract_rows(left, right):
    return lax.dot_general(left, right, (((0,), (0,)), ((), ())), preferred_element_type=f32)


def contract_cols(left, right):
    return lax.dot_general(left, right, (((1,), (1,)), ((), ())), preferred_element_type=f32)


class Grid:
    def __init__(self, mesh):
        self.dp = mesh.shape["dp"]
        self.tensor = mesh.shape["tensor"]
        self.depth = 4 if self.dp % 4 == 0 else (2 if self.dp % 2 == 0 else 1)
        self.width = self.dp // self.depth

    def here(self):
        index = lax.axis_index("dp")
        self.deep = index // self.width
        self.wide = lax.rem(index, self.width)
        self.rank = lax.axis_index("tensor")

    def shift(self, value, step):
        pairs = [
            (z * self.width + y, ((z + step) % self.depth) * self.width + y)
            for z in range(self.depth)
            for y in range(self.width)
        ]
        return lax.ppermute(value, "dp", pairs)

    def swap_wide(self, value, bit):
        pairs = [
            (z * self.width + y, z * self.width + (y ^ bit))
            for z in range(self.depth)
            for y in range(self.width)
        ]
        return lax.ppermute(value, "dp", pairs)

    def swap_rank(self, value, bit):
        return lax.ppermute(value, "tensor", [(q, q ^ bit) for q in range(self.tensor)])

    def shift_wide(self, value, step):
        pairs = [
            (z * self.width + y, z * self.width + (y + step) % self.width)
            for z in range(self.depth)
            for y in range(self.width)
        ]
        return lax.ppermute(value, "dp", pairs)

    def wide_bits(self):
        return [1 << b for b in range(self.width.bit_length() - 1)]

    def rank_bits(self):
        return [1 << b for b in range(self.tensor.bit_length() - 1)]

    def assemble(self, pieces):
        rows, columns = pieces[0].shape
        out = jnp.zeros((self.dp, rows, columns), pieces[0].dtype)
        for step, piece in enumerate(pieces):
            group = {0: piece}
            for bit in self.wide_bits():
                for key in list(group):
                    group[key ^ bit] = self.swap_wide(group[key], bit)
            source = lax.rem(self.deep + self.depth - step, self.depth)
            for key, part in group.items():
                at = source * self.width + jnp.bitwise_xor(self.wide, key)
                out = lax.dynamic_update_slice(out, part[None], (at, 0, 0))
        return out.reshape(self.dp * rows, columns)

    def gather_rows(self, block):
        return self.assemble([block] + [self.shift(block, s) for s in range(1, self.depth)])

    def exchange_blocks(self, blocks):
        pieces = []
        for step in range(self.depth):
            to = lax.rem(self.deep + step, self.depth)
            part = lax.dynamic_index_in_dim(blocks, to, 0, keepdims=False)
            pieces.append(part if step == 0 else self.shift(part, step))
        return self.assemble(pieces)

    def reduce_width(self, full):
        rows, columns = full.shape[0] // self.dp, full.shape[1]
        held = full.reshape(self.depth, self.width, rows, columns)
        for bit in reversed(self.wide_bits()):
            held = held.reshape(self.depth, 2, bit, rows, columns)
            mine = lax.rem(self.wide // bit, 2)
            other = lax.dynamic_index_in_dim(held, 1 - mine, 1, keepdims=False)
            own = lax.dynamic_index_in_dim(held, mine, 1, keepdims=False)
            held = own + self.swap_wide(other, bit)
        return held.reshape(self.depth, rows, columns)

    def pick(self, held, step):
        to = lax.rem(self.deep + step, self.depth)
        return lax.dynamic_index_in_dim(held, to, 0, keepdims=False)

    def scatter_rows(self, full):
        held = self.reduce_width(full)
        total = self.pick(held, 0).astype(f32)
        for step in range(1, self.depth):
            total = total + self.shift(self.pick(held, step), step).astype(f32)
        return total

    def return_blocks(self, full):
        held = self.reduce_width(full)
        out = jnp.zeros_like(held)
        for step in range(self.depth):
            part = self.pick(held, step)
            part = part if step == 0 else self.shift(part, step)
            source = lax.rem(self.deep + self.depth - step, self.depth)
            out = lax.dynamic_update_slice(out, part[None], (source, 0, 0))
        return out

    def spread_rank(self, block):
        for bit in reversed(self.rank_bits()):
            block = jnp.concatenate([block, self.swap_rank(block, bit)], axis=0)
        return block

    def reduce_rank(self, full):
        for bit in self.rank_bits():
            half = full.shape[0] // 2
            full = full[:half] + self.swap_rank(full[half:], bit)
        return full

    def flips(self):
        order = [0]
        for bit in reversed(self.rank_bits()):
            order = order + [k ^ bit for k in order]
        return order

    def spread_all(self, block):
        parts = [self.spread_rank(block)]
        for step in range(1, self.depth):
            parts.append(self.spread_rank(self.shift(block, step)))
        return jnp.concatenate(parts, axis=0)

    def reduce_all(self, make_part):
        terms = []
        for step in list(range(1, self.depth)) + [0]:
            term = self.reduce_rank(make_part(step))
            terms.append(term if step == 0 else self.shift(term, -step))
        total = terms[-1].astype(f32)
        for term in terms[:-1]:
            total = total + term.astype(f32)
        return total


MESH = pl.DeviceIdType.MESH


def ffn_core(grid, backward, block, pieces, saved=None):
    deep_n, width = grid.depth, grid.width
    n, d = block.shape
    shard = pieces[0][0].shape[0]
    share = pieces[0][0].shape[1] // 3
    main = share // 256 * 256
    group = 4 * n
    n_pieces = len(pieces)
    tiles = [(a, a + 256) for a in range(0, main, 256)]

    def kernel(*refs):
        block_ref, refs = refs[0], refs[1:]
        piece_refs, refs = refs[:n_pieces], refs[n_pieces:]
        if backward:
            saved_ref, refs = refs[0], refs[1:]
            all_ref, mid_ref, out_ref = refs[:3]
            refs = refs[3:]
        else:
            all_ref, saved_ref, mid_ref, out_ref = refs[:4]
            refs = refs[4:]
        (buf, w_gu, w_dn, part, c_in, x_in, u_in, d_in, gu, mid, acc,
         w_sem, own_sem, out_sem, z_up, z_dn, z_got, x_put, x_got, c_put, c_got,
         rc_put, rc_got, rx_put, rx_got, rz_put, ru_got, rd_got) = refs

        dp = lax.axis_index("dp")
        q = lax.axis_index("tensor")
        z, y = dp // width, dp % width
        x, c = q // 2, q % 2
        at_x = (dp, (1 - x) * 2 + c)
        at_c = (dp, x * 2 + 1 - c)
        at_up = (dp + width, q)
        at_dn = (dp - width, q)
        low, high = z > 0, z < deep_n - 1

        def remote(src, dst, put, got, device):
            return pltpu.make_async_remote_copy(
                src_ref=src, dst_ref=dst, send_sem=put, recv_sem=got, device_id=device, device_id_type=MESH
            )

        def order(i):
            near = z + 1 - 2 * (z % 2)
            middle = 2 - z // 2
            far = 3 * (1 - z // 2)
            return jnp.where(i == 0, z, jnp.where(i == 1, near, jnp.where(i == 2, middle, far)))

        own = pltpu.make_async_copy(block_ref, buf.at[z, c, x], own_sem.at[0])
        own.start()
        loads = []
        for k, (source, key) in enumerate(keys):
            row = pl.multiple_of(((z + deep_n - source) % deep_n * width + (y + key) % width) * shard, math.gcd(shard, 16))
            loads.append(pltpu.make_async_copy(piece_refs[k].at[:, pl.ds(0, 2 * share)], w_gu.at[pl.ds(row, shard)], w_sem.at[k, 0]))
            loads.append(pltpu.make_async_copy(piece_refs[k].at[:, pl.ds(2 * share, share)], w_dn.at[pl.ds(row, shard)], w_sem.at[k, 1]))
        for load in loads:
            load.start()
        if backward:
            load = pltpu.make_async_copy(saved_ref, gu, own_sem.at[1])
            load.start()
            loads.append(load)

        barrier = pltpu.get_barrier_semaphore()
        pl.semaphore_signal(barrier, inc=1, device_id=at_x, device_id_type=MESH)
        pl.semaphore_signal(barrier, inc=1, device_id=at_c, device_id_type=MESH)

        @pl.when(low)
        def _():
            pl.semaphore_signal(barrier, inc=1, device_id=at_dn, device_id_type=MESH)

        @pl.when(high)
        def _():
            pl.semaphore_signal(barrier, inc=1, device_id=at_up, device_id_type=MESH)

        pl.semaphore_wait(barrier, 2 + (z + deep_n - 1) // deep_n + (2 * deep_n - 2 - z) // deep_n)

        own.wait()

        def hop_up(g):
            return remote(buf.at[g, c, x], buf.at[g, c, x], z_up.at[g], z_got.at[g], at_up)

        def hop_dn(g):
            return remote(buf.at[g, c, x], buf.at[g, c, x], z_dn.at[g], z_got.at[g], at_dn)

        def hop_x(g):
            return remote(buf.at[g, c, x], buf.at[g, c, x], x_put.at[g], x_got.at[g], at_x)

        def hop_c(g, far):
            xx = (1 - x) if far else x
            return remote(buf.at[g, c, xx], buf.at[g, c, xx], c_put.at[g, int(far)], c_got.at[g, int(far)], at_c)

        def got(sem, ref):
            remote(ref, ref, sem, sem, at_x).wait_recv()

        def back_c(g):
            return remote(part.at[g, 1 - c], c_in.at[g], rc_put.at[g], rc_got.at[g], at_c)

        def pass_on(g):
            @pl.when(jnp.logical_and(g <= z, high))
            def _():
                hop_up(g).start()

            @pl.when(jnp.logical_and(g >= z, low))
            def _():
                hop_dn(g).start()

            hop_x(g).start()
            hop_c(g, False).start()

        def put_part(g, right):
            @pl.loop(0, d // 256)
            def _(t):
                at = pl.multiple_of(t * 256, 256)
                value = lax.dot_general(
                    mid[g], right[pl.ds(at, 256), :], (((1,), (1,)), ((), ())), preferred_element_type=f32
                )
                part[g, :, :, :, pl.ds(at, 256)] = value.astype(bf16).reshape(2, 2, n, 256)

        def forward_group(g):
            tokens = lambda: buf[g].reshape(group, d)

            def save(lo, hi, gate, upward):
                inner = math.sqrt(2.0 / math.pi) * (gate + 0.044715 * gate * gate * gate)
                mid[g, :, lo:hi] = (0.5 * gate * (1.0 + jnp.tanh(inner)) * upward).astype(bf16)

            for lo, hi in tiles:
                gate = jnp.dot(tokens(), w_gu[:, lo:hi], preferred_element_type=f32)
                upward = jnp.dot(tokens(), w_gu[:, main + lo : main + hi], preferred_element_type=f32)
                gu[g, :, lo:hi] = gate.astype(bf16)
                gu[g, :, main + lo : main + hi] = upward.astype(bf16)
                save(lo, hi, gate, upward)
            if main < share:
                rest = share - main
                both = jnp.dot(tokens(), w_gu[:, 2 * main :], preferred_element_type=f32)
                gu[g, :, 2 * main :] = both.astype(bf16)
                save(main, share, both[:, :rest], both[:, rest:])
            put_part(g, w_dn)

        def backward_group(g):
            tokens = lambda: buf[g].reshape(group, d)

            def pull(lo, hi, gate_at, up_at):
                grad = jnp.dot(tokens(), w_dn[:, lo:hi], preferred_element_type=f32)
                gate = gu[g, :, gate_at : gate_at + hi - lo].astype(f32)
                upward = gu[g, :, up_at : up_at + hi - lo].astype(f32)
                factor = math.sqrt(2.0 / math.pi)
                square = gate * gate
                curve = jnp.tanh(factor * gate * (1.0 + 0.044715 * square))
                half = 0.5 * (1.0 + curve)
                slope = half + 0.5 * gate * (1.0 - curve * curve) * factor * (1.0 + 3.0 * 0.044715 * square)
                mid[g, :, gate_at : gate_at + hi - lo] = (grad * upward * slope).astype(bf16)
                mid[g, :, up_at : up_at + hi - lo] = (grad * gate * half).astype(bf16)

            for lo, hi in tiles:
                pull(lo, hi, lo, main + lo)
            if main < share:
                pull(main, share, 2 * main, main + share)
            put_part(g, w_gu)

        pass_on(z)

        @pl.loop(1, deep_n + 1)
        def _(i):
            @pl.when(i < deep_n)
            def _():
                g = order(i)
                got(z_got.at[g], buf.at[g, c, x])
                pass_on(g)

            g = order(i - 1)
            got(x_got.at[g], buf.at[g, c, 1 - x])
            hop_c(g, True).start()

            @pl.when(i == 1)
            def _():
                for load in loads:
                    load.wait()

            got(c_got.at[g, 0], buf.at[g, 1 - c, x])
            got(c_got.at[g, 1], buf.at[g, 1 - c, 1 - x])
            pltpu.make_async_copy(buf.at[g], all_ref.at[g], out_sem.at[g, 0]).start()
            if backward:
                backward_group(g)
            else:
                forward_group(g)
                pltpu.make_async_copy(gu.at[g], saved_ref.at[g], out_sem.at[g, 2]).start()
            back_c(g).start()
            pltpu.make_async_copy(mid.at[g], mid_ref.at[g], out_sem.at[g, 1]).start()

        def back_x(g):
            return remote(part.at[g, c, 1 - x], x_in.at[g], rx_put.at[g], rx_got.at[g], at_x)

        def back_up(g):
            return remote(part.at[g, c, x], u_in.at[g], rz_put.at[g], ru_got.at[g], at_up)

        def back_dn(g):
            return remote(part.at[g, c, x], d_in.at[g], rz_put.at[g], rd_got.at[g], at_dn)

        @pl.loop(0, deep_n)
        def _(i):
            g = order(deep_n - 1 - i)
            got(rc_got.at[g], c_in.at[g])
            part[g, c, 1 - x] = (part[g, c, 1 - x].astype(f32) + c_in[g, 1 - x].astype(f32)).astype(bf16)
            back_x(g).start()
            part[g, c, x] = (part[g, c, x].astype(f32) + c_in[g, x].astype(f32)).astype(bf16)

        @pl.loop(0, deep_n)
        def _(i):
            g = order(deep_n - 1 - i)
            got(rx_got.at[g], x_in.at[g])
            acc[...] = part[g, c, x].astype(f32) + x_in[g].astype(f32)

            @pl.when(jnp.logical_and(g >= z, low))
            def _():
                got(ru_got.at[g], u_in.at[g])
                acc[...] += u_in[g].astype(f32)

            @pl.when(jnp.logical_and(g <= z, high))
            def _():
                got(rd_got.at[g], d_in.at[g])
                acc[...] += d_in[g].astype(f32)

            @pl.when(g > z)
            def _():
                part[g, c, x] = acc[...].astype(bf16)
                back_up(g).start()

            @pl.when(g < z)
            def _():
                part[g, c, x] = acc[...].astype(bf16)
                back_dn(g).start()

        done = pltpu.make_async_copy(acc, out_ref, own_sem.at[0])
        done.start()

        @pl.loop(0, deep_n)
        def _(g):
            @pl.when(jnp.logical_and(g <= z, high))
            def _():
                hop_up(g).wait_send()

            @pl.when(jnp.logical_and(g >= z, low))
            def _():
                hop_dn(g).wait_send()

            hop_x(g).wait_send()
            hop_c(g, False).wait_send()
            hop_c(g, True).wait_send()
            back_c(g).wait_send()
            back_x(g).wait_send()

            @pl.when(g > z)
            def _():
                back_up(g).wait_send()

            @pl.when(g < z)
            def _():
                back_dn(g).wait_send()

            pltpu.make_async_copy(buf.at[g], all_ref.at[g], out_sem.at[g, 0]).wait()
            pltpu.make_async_copy(mid.at[g], mid_ref.at[g], out_sem.at[g, 1]).wait()
            if not backward:
                pltpu.make_async_copy(gu.at[g], saved_ref.at[g], out_sem.at[g, 2]).wait()

        done.wait()

    keys = [pair[1] for pair in pieces]
    arrays = [pair[0] for pair in pieces]
    shape = jax.ShapeDtypeStruct
    whole = shape((deep_n, 2, 2, n, d), bf16)
    wide_out = shape((deep_n, group, 2 * share), bf16)
    slim_out = shape((deep_n, group, share), bf16)
    last = shape((n, d), f32)
    outs = (whole, wide_out, last) if backward else (whole, wide_out, slim_out, last)
    operands = [block] + arrays + ([saved] if backward else [])
    anywhere = pl.BlockSpec(memory_space=pl.ANY)
    dma = pltpu.SemaphoreType.DMA
    flops = 2 * deep_n * group * d * share * 3
    return pl.pallas_call(
        kernel,
        out_shape=outs,
        in_specs=[anywhere] * len(operands),
        out_specs=tuple([anywhere] * len(outs)),
        scratch_shapes=[
            pltpu.VMEM((deep_n, 2, 2, n, d), bf16),
            pltpu.VMEM((d, 2 * share), bf16),
            pltpu.VMEM((d, share), bf16),
            pltpu.VMEM((deep_n, 2, 2, n, d), bf16),
            pltpu.VMEM((deep_n, 2, n, d), bf16),
            pltpu.VMEM((deep_n, n, d), bf16),
            pltpu.VMEM((deep_n, n, d), bf16),
            pltpu.VMEM((deep_n, n, d), bf16),
            pltpu.VMEM((deep_n, group, 2 * share), bf16),
            pltpu.VMEM((deep_n, group, 2 * share if backward else share), bf16),
            pltpu.VMEM((n, d), f32),
            dma((n_pieces, 2)),
            dma((2,)),
            dma((deep_n, 3)),
            dma((deep_n,)),
            dma((deep_n,)),
            dma((deep_n,)),
            dma((deep_n,)),
            dma((deep_n,)),
            dma((deep_n, 2)),
            dma((deep_n, 2)),
            dma((deep_n,)),
            dma((deep_n,)),
            dma((deep_n,)),
            dma((deep_n,)),
            dma((deep_n,)),
            dma((deep_n,)),
            dma((deep_n,)),
        ],
        compiler_params=pltpu.CompilerParams(
            collective_id=2 if backward else 1, has_side_effects=True, vmem_limit_bytes=64_000_000
        ),
        cost_estimate=pl.CostEstimate(flops=flops, bytes_accessed=60_000_000, transcendentals=0),
        name="ffn_backward" if backward else "ffn_forward",
    )(*operands)


def unit_cuts(units, parts):
    tiles = units // LANE
    edges = [(tiles * k + parts - 1) // parts for k in range(parts + 1)]
    starts = [e * LANE for e in edges[:-1]]
    sizes = [(b - a) * LANE for a, b in zip(edges[:-1], edges[1:])]
    return starts, sizes, max(sizes)


def cut_units(block, cuts):
    starts, sizes, share = cuts
    return jnp.stack(
        [
            jnp.pad(block[:, a : a + n], ((0, 0), (0, share - n))) if n < share else block[:, a : a + n]
            for a, n in zip(starts, sizes)
        ]
    )


def join_units(blocks, cuts):
    starts, sizes, share = cuts
    return jnp.concatenate([blocks[k, :, :n] for k, n in enumerate(sizes)], axis=1)


def make_body(grid):
    def body(
        inputs,
        cotangent,
        segments,
        positions,
        w_query,
        w_key,
        w_value,
        w_output,
        w_gate,
        w_up,
        w_down,
        gain_attn,
        gain_post_attn,
        gain_ffw,
        gain_post_ffw,
    ):
        grid.here()
        count, width = inputs.shape
        shard = w_query.shape[0]
        group = HEADS // KV
        local_kv = w_key.shape[1] // HD
        local_heads = local_kv * group
        q_cols, k_cols = w_query.shape[1], w_key.shape[1]
        scale = 1.0 / math.sqrt(HD)
        part = count // grid.tensor
        rows = count // ROW_LEN
        cuts = unit_cuts(w_gate.shape[1], grid.depth)
        share = cuts[2]
        main = share // 256 * 256

        gains = jnp.stack([gain_attn, gain_post_attn, gain_ffw, gain_post_ffw])
        gains = grid.gather_rows(gains).reshape(grid.dp, 4, shard)
        gains = gains.transpose(1, 0, 2).reshape(4, width).astype(f32)
        gain_one, gain_two, gain_three, gain_four = gains[0], gains[1], gains[2], gains[3]
        full_qkv = grid.gather_rows(jnp.concatenate([w_query, w_key, w_value], axis=1))
        full_out = grid.gather_rows(w_output.T)
        cut_gate, cut_up = cut_units(w_gate, cuts), cut_units(w_up, cuts)
        blocks = jnp.concatenate(
            [cut_gate[:, :, :main], cut_up[:, :, :main], cut_gate[:, :, main:], cut_up[:, :, main:], cut_units(w_down.T, cuts)],
            axis=2,
        )
        pieces = []
        for step in range(grid.depth):
            piece = grid.pick(blocks, step)
            piece = piece if step == 0 else grid.shift(piece, step)
            pieces.append((piece, (step, 0)))
            for over in range(1, grid.width):
                pieces.append((grid.shift_wide(piece, over), (step, grid.width - over)))

        where = [jnp.bitwise_xor(grid.rank, flip) * part for flip in grid.flips()]
        take = lambda a: jnp.concatenate(
            [lax.dynamic_slice_in_dim(a, at, part, 0) for at in where], axis=0
        )
        source = take(inputs).astype(f32)
        segs = take(segments)
        angles = make_angles(take(positions), HD)
        cosine, sine = jnp.cos(angles), jnp.sin(angles)

        normed = rms_scale(source, gain_one).astype(bf16)
        qkv = dot(normed, full_qkv)
        query_raw = qkv[:, :q_cols].reshape(count, local_heads, HD)
        key_raw = qkv[:, q_cols : q_cols + k_cols].reshape(count, local_kv, HD)
        queries = (rotate(query_raw, cosine, sine) * scale).astype(bf16)
        keys = rotate(key_raw, cosine, sine).astype(bf16)
        values = qkv[:, q_cols + k_cols :].astype(bf16)
        mask = row_mask(segs, rows, ROW_LEN)[:, None, None]
        query_five = queries.reshape(rows, ROW_LEN, local_kv, group, HD)
        key_four = keys.reshape(rows, ROW_LEN, local_kv, HD)
        value_four = values.reshape(rows, ROW_LEN, local_kv, HD)
        scores = jnp.einsum("rqkgd,rskd->rkgqs", query_five, key_four, preferred_element_type=f32)
        capped = CAP * jnp.tanh(scores / CAP)
        expo = jnp.where(mask, jnp.exp(capped), 0.0)
        total = jnp.sum(expo, axis=-1, keepdims=True)
        soft = expo / total
        probs = soft.astype(bf16)
        attended = jnp.einsum("rkgqs,rskd->rqkgd", probs, value_four, preferred_element_type=f32)
        attended = attended.reshape(count, local_heads * HD).astype(bf16)
        branch_attn = grid.reduce_rank(contract_cols(attended, full_out).astype(bf16)).astype(f32)

        own_source = source[:part]
        hidden = own_source + rms_scale(branch_attn, gain_two)
        normed_own = rms_scale(hidden, gain_three).astype(bf16)
        all_normed, saved, mixed, branch_ffw = ffn_core(grid, False, normed_own, pieces)
        own_out = (hidden + rms_scale(branch_ffw, gain_four)).astype(bf16)

        d_out = lax.dynamic_slice_in_dim(cotangent, grid.rank * part, part, 0).astype(f32)
        d_branch_own, d_gain_four = rms_back(branch_ffw, gain_four, d_out)
        all_back, d_gu, d_normed_ffw = ffn_core(grid, True, d_branch_own.astype(bf16), pieces, saved)
        tokens = all_normed.shape[0] * 4 * part
        d_gu = d_gu.reshape(tokens, 2 * share)
        grad_dn = contract_rows(all_back.reshape(tokens, width), mixed.reshape(tokens, share)).astype(bf16)
        grad_gu = contract_rows(all_normed.reshape(tokens, width), d_gu).astype(bf16)
        blocks_dn = grid.return_blocks(grad_dn)
        blocks_gu = grid.return_blocks(grad_gu)
        grad_down = join_units(blocks_dn, cuts).T.astype(f32)
        rest = 2 * main + share - main
        grad_gate = jnp.concatenate([blocks_gu[:, :, :main], blocks_gu[:, :, 2 * main : rest]], axis=2)
        grad_up = jnp.concatenate([blocks_gu[:, :, main : 2 * main], blocks_gu[:, :, rest:]], axis=2)
        grad_gate = join_units(grad_gate, cuts).astype(f32)
        grad_up = join_units(grad_up, cuts).astype(f32)

        d_hidden_norm, d_gain_three = rms_back(hidden, gain_three, d_normed_ffw)
        d_hidden = d_out + d_hidden_norm
        d_branch_attn, d_gain_two = rms_back(branch_attn, gain_two, d_hidden)
        d_branch_attn = grid.spread_rank(d_branch_attn.astype(bf16))
        grad_output = contract_rows(d_branch_attn, attended).astype(bf16)
        grad_output = grid.scatter_rows(grad_output).T
        d_attended = dot(d_branch_attn, full_out).astype(bf16)
        d_att_five = d_attended.reshape(rows, ROW_LEN, local_kv, group, HD)
        d_values = jnp.einsum("rkgqs,rqkgd->rskd", probs, d_att_five, preferred_element_type=f32)
        d_probs = jnp.einsum("rqkgd,rskd->rkgqs", d_att_five, value_four, preferred_element_type=f32)
        d_soft = soft * (d_probs - jnp.sum(soft * d_probs, axis=-1, keepdims=True))
        d_capped = (d_soft * (1.0 - (capped / CAP) ** 2)).astype(bf16)
        d_queries = jnp.einsum(
            "rkgqs,rskd->rqkgd", d_capped, key_four, preferred_element_type=f32
        ).reshape(count, local_heads, HD)
        d_keys = jnp.einsum(
            "rkgqs,rqkgd->rskd", d_capped, query_five, preferred_element_type=f32
        ).reshape(count, local_kv, HD)
        d_query_proj = (rotate(d_queries, cosine, -sine) * scale).astype(bf16).reshape(count, q_cols)
        d_key_proj = rotate(d_keys, cosine, -sine).astype(bf16).reshape(count, k_cols)
        d_value_proj = d_values.reshape(count, k_cols).astype(bf16)
        d_qkv = jnp.concatenate([d_query_proj, d_key_proj, d_value_proj], axis=1)
        d_normed = grid.reduce_rank(contract_cols(d_qkv, full_qkv).astype(bf16)).astype(f32)
        grad_qkv = grid.scatter_rows(contract_rows(normed, d_qkv).astype(bf16))
        d_source, d_gain_one = rms_back(own_source, gain_one, d_normed)
        own_grad = (d_hidden + d_source).astype(bf16)

        d_gains = jnp.stack([d_gain_one, d_gain_two, d_gain_three, d_gain_four])
        for bit in grid.rank_bits():
            d_gains = d_gains + grid.swap_rank(d_gains, bit)
        d_gains = d_gains.reshape(4, grid.dp, shard).transpose(1, 0, 2).reshape(grid.dp * 4, shard)
        d_gains = grid.scatter_rows(d_gains)

        def place(block):
            whole = grid.spread_rank(block)
            out = jnp.zeros_like(whole)
            for at, k in zip(where, range(grid.tensor)):
                out = lax.dynamic_update_slice(out, whole[k * part : (k + 1) * part], (at, 0))
            return out

        return (
            place(own_out),
            place(own_grad),
            grad_qkv[:, :q_cols],
            grad_qkv[:, q_cols : q_cols + k_cols],
            grad_qkv[:, q_cols + k_cols :],
            grad_output,
            grad_gate,
            grad_up,
            grad_down,
            d_gains[0],
            d_gains[1],
            d_gains[2],
            d_gains[3],
        )

    return body


def solution(mesh):
    placed = (
        P("dp", None),
        P("dp", None),
        P("dp"),
        P("dp"),
        P("dp", "tensor"),
        P("dp", "tensor"),
        P("dp", "tensor"),
        P("tensor", "dp"),
        P("dp", "tensor"),
        P("dp", "tensor"),
        P("tensor", "dp"),
        P("dp"),
        P("dp"),
        P("dp"),
        P("dp"),
    )
    return jax.shard_map(
        make_body(Grid(mesh)),
        mesh=mesh,
        in_specs=placed,
        out_specs=(
            P("dp", None),
            P("dp", None),
            P("dp", "tensor"),
            P("dp", "tensor"),
            P("dp", "tensor"),
            P("tensor", "dp"),
            P("dp", "tensor"),
            P("dp", "tensor"),
            P("tensor", "dp"),
            P("dp"),
            P("dp"),
            P("dp"),
            P("dp"),
        ),
        check_vma=False,
    )
```

```python
import math

import jax
import jax.numpy as jnp
from jax import lax
from jax.experimental import pallas as pl
from jax.experimental.pallas import tpu as pltpu
from jax.sharding import PartitionSpec as P

HEADS = 8
KV = 4
HD = 256
ROW_LEN = 128
LANE = 128


EPS = 1e-06
CAP = 50.0
THETA = 10000.0

f32 = jnp.float32
bf16 = jnp.bfloat16


def rms_scale(field, gain):
    inverse = lax.rsqrt(jnp.mean(field * field, axis=-1, keepdims=True) + EPS)
    return field * inverse * gain


def rms_back(field, gain, grad):
    inverse = lax.rsqrt(jnp.mean(field * field, axis=-1, keepdims=True) + EPS)
    unit = field * inverse
    d_gain = jnp.sum(grad * unit, axis=0)
    scaled = grad * gain
    d_field = inverse * (scaled - unit * jnp.mean(scaled * unit, axis=-1, keepdims=True))
    return d_field, d_gain


def geglu(gate, upward):
    return jax.nn.gelu(gate, approximate=True) * upward


def rotate(field, cosine, sine):
    half = field.shape[-1] // 2
    first = field[..., :half]
    second = field[..., half:]
    return jnp.concatenate(
        [first * cosine - second * sine, second * cosine + first * sine], axis=-1
    )


def make_angles(positions, head_size):
    half = head_size // 2
    freqs = THETA ** (-(jnp.arange(half).astype(f32) * 2.0) / head_size)
    return positions.astype(f32)[:, None, None] * freqs[None, None, :]


def row_mask(segments, rows, length):
    seg_rows = segments.reshape(rows, length)
    same = seg_rows[:, :, None] == seg_rows[:, None, :]
    index = jnp.arange(length)
    causal = index[:, None] >= index[None, :]
    return jnp.logical_and(same, causal[None])


def dot(left, right):
    return jnp.dot(left, right, preferred_element_type=f32)


def contract_rows(left, right):
    return lax.dot_general(left, right, (((0,), (0,)), ((), ())), preferred_element_type=f32)


def contract_cols(left, right):
    return lax.dot_general(left, right, (((1,), (1,)), ((), ())), preferred_element_type=f32)


class Grid:
    def __init__(self, mesh):
        self.dp = mesh.shape["dp"]
        self.tensor = mesh.shape["tensor"]
        self.depth = 4 if self.dp % 4 == 0 else (2 if self.dp % 2 == 0 else 1)
        self.width = self.dp // self.depth

    def here(self):
        index = lax.axis_index("dp")
        self.deep = index // self.width
        self.wide = lax.rem(index, self.width)
        self.rank = lax.axis_index("tensor")

    def shift(self, value, step):
        pairs = [
            (z * self.width + y, ((z + step) % self.depth) * self.width + y)
            for z in range(self.depth)
            for y in range(self.width)
        ]
        return lax.ppermute(value, "dp", pairs)

    def swap_wide(self, value, bit):
        pairs = [
            (z * self.width + y, z * self.width + (y ^ bit))
            for z in range(self.depth)
            for y in range(self.width)
        ]
        return lax.ppermute(value, "dp", pairs)

    def swap_rank(self, value, bit):
        return lax.ppermute(value, "tensor", [(q, q ^ bit) for q in range(self.tensor)])

    def wide_bits(self):
        return [1 << b for b in range(self.width.bit_length() - 1)]

    def rank_bits(self):
        return [1 << b for b in range(self.tensor.bit_length() - 1)]

    def reduce_width(self, full):
        rows, columns = full.shape[0] // self.dp, full.shape[1]
        held = full.reshape(self.depth, self.width, rows, columns)
        for bit in reversed(self.wide_bits()):
            held = held.reshape(self.depth, 2, bit, rows, columns)
            mine = lax.rem(self.wide // bit, 2)
            other = lax.dynamic_index_in_dim(held, 1 - mine, 1, keepdims=False)
            own = lax.dynamic_index_in_dim(held, mine, 1, keepdims=False)
            held = own + self.swap_wide(other, bit)
        return held.reshape(self.depth, rows, columns)

    def pick(self, held, step):
        to = lax.rem(self.deep + step, self.depth)
        return lax.dynamic_index_in_dim(held, to, 0, keepdims=False)

    def scatter_rows(self, full):
        held = self.reduce_width(full)
        total = self.pick(held, 0).astype(f32)
        for step in range(1, self.depth):
            total = total + self.shift(self.pick(held, step), step).astype(f32)
        return total

    def return_blocks(self, full):
        held = self.reduce_width(full)
        out = jnp.zeros_like(held)
        for step in range(self.depth):
            part = self.pick(held, step)
            part = part if step == 0 else self.shift(part, step)
            source = lax.rem(self.deep + self.depth - step, self.depth)
            out = lax.dynamic_update_slice(out, part[None], (source, 0, 0))
        return out

    def spread_rank(self, block):
        x, c = self.rank // 2, lax.rem(self.rank, 2)
        n, d = block.shape
        out = jnp.zeros((2, 2, n, d), block.dtype)
        for far_c in range(2):
            for far_x in range(2):
                part = block
                if far_x:
                    part = across
                if far_c:
                    part = self.swap_rank(part, 1)
                elif not far_x:
                    across = self.swap_rank(block, 2)
                out = lax.dynamic_update_slice(
                    out, part[None, None], (jnp.bitwise_xor(c, far_c), jnp.bitwise_xor(x, far_x), 0, 0)
                )
        return out.reshape(4 * n, d)

    def reduce_rank(self, full):
        x, c = self.rank // 2, lax.rem(self.rank, 2)
        held = full.reshape(2, 2, full.shape[0] // 4, full.shape[1])
        for at, bit in ((c, 1), (x, 2)):
            own = lax.dynamic_index_in_dim(held, at, 0, keepdims=False)
            other = lax.dynamic_index_in_dim(held, 1 - at, 0, keepdims=False)
            held = own + self.swap_rank(other, bit)
        return held


MESH = pl.DeviceIdType.MESH


class Spot:
    def __init__(self, grid):
        self.depth, self.width = grid.depth, grid.width
        self.dp = lax.axis_index("dp")
        self.q = lax.axis_index("tensor")
        self.z, self.y = self.dp // self.width, self.dp % self.width
        self.x, self.c = self.q // 2, self.q % 2
        self.at_x = (self.dp, (1 - self.x) * 2 + self.c)
        self.at_c = (self.dp, self.x * 2 + 1 - self.c)
        self.at_up = (self.dp + self.width, self.q)
        self.at_dn = (self.dp - self.width, self.q)
        self.low, self.high = self.z > 0, self.z < self.depth - 1

    def order(self, i):
        z = self.z
        near = z + 1 - 2 * (z % 2)
        middle = 2 - z // 2
        far = 3 * (1 - z // 2)
        return jnp.where(i == 0, z, jnp.where(i == 1, near, jnp.where(i == 2, middle, far)))

    def at_depth(self, z):
        return (z * self.width + self.y, self.q)

    def at_wide(self, over):
        return (self.z * self.width + (self.y + over) % self.width, self.q)


def remote(src, dst, put, got, device):
    return pltpu.make_async_remote_copy(
        src_ref=src, dst_ref=dst, send_sem=put, recv_sem=got, device_id=device, device_id_type=MESH
    )


def signal(semaphore, device):
    pl.semaphore_signal(semaphore, inc=1, device_id=device, device_id_type=MESH)


class Trade:
    def __init__(self, spot, buf, part, acc, c_in, x_in, u_in, d_in, sems):
        self.spot, self.buf, self.part, self.acc = spot, buf, part, acc
        self.c_in, self.x_in, self.u_in, self.d_in = c_in, x_in, u_in, d_in
        (self.z_up, self.z_dn, self.z_got, self.x_put, self.x_got, self.c_put, self.c_got,
         self.rc_put, self.rc_got, self.rx_put, self.rx_got, self.rz_put, self.ru_got, self.rd_got) = sems

    @staticmethod
    def semaphores(depth):
        dma = pltpu.SemaphoreType.DMA
        return [dma((depth,))] * 5 + [dma((depth, 2))] * 2 + [dma((depth,))] * 7

    @staticmethod
    def buffers(depth, n, d):
        return [
            pltpu.VMEM((depth, 2, 2, n, d), bf16),
            pltpu.VMEM((depth, 2, n, d), bf16),
            pltpu.VMEM((depth, n, d), bf16),
            pltpu.VMEM((depth, n, d), bf16),
            pltpu.VMEM((depth, n, d), bf16),
        ]

    def hop_up(self, g):
        s = self.spot
        return remote(self.buf.at[g, s.c, s.x], self.buf.at[g, s.c, s.x], self.z_up.at[g], self.z_got.at[g], s.at_up)

    def hop_dn(self, g):
        s = self.spot
        return remote(self.buf.at[g, s.c, s.x], self.buf.at[g, s.c, s.x], self.z_dn.at[g], self.z_got.at[g], s.at_dn)

    def hop_x(self, g):
        s = self.spot
        return remote(self.buf.at[g, s.c, s.x], self.buf.at[g, s.c, s.x], self.x_put.at[g], self.x_got.at[g], s.at_x)

    def hop_c(self, g, far):
        s = self.spot
        xx = (1 - s.x) if far else s.x
        return remote(
            self.buf.at[g, s.c, xx], self.buf.at[g, s.c, xx], self.c_put.at[g, int(far)], self.c_got.at[g, int(far)], s.at_c
        )

    def got(self, sem, ref):
        remote(ref, ref, sem, sem, self.spot.at_x).wait_recv()

    def pass_on(self, g):
        s = self.spot

        @pl.when(jnp.logical_and(g <= s.z, s.high))
        def _():
            self.hop_up(g).start()

        @pl.when(jnp.logical_and(g >= s.z, s.low))
        def _():
            self.hop_dn(g).start()

        self.hop_x(g).start()
        self.hop_c(g, False).start()

    def take_z(self, g):
        s = self.spot
        self.got(self.z_got.at[g], self.buf.at[g, s.c, s.x])
        self.pass_on(g)

    def take_rank(self, g):
        s = self.spot
        self.got(self.x_got.at[g], self.buf.at[g, s.c, 1 - s.x])
        self.hop_c(g, True).start()
        self.got(self.c_got.at[g, 0], self.buf.at[g, 1 - s.c, s.x])
        self.got(self.c_got.at[g, 1], self.buf.at[g, 1 - s.c, 1 - s.x])

    def back_c(self, g):
        s = self.spot
        return remote(self.part.at[g, 1 - s.c], self.c_in.at[g], self.rc_put.at[g], self.rc_got.at[g], s.at_c)

    def back_x(self, g):
        s = self.spot
        return remote(self.part.at[g, s.c, 1 - s.x], self.x_in.at[g], self.rx_put.at[g], self.rx_got.at[g], s.at_x)

    def back_up(self, g):
        s = self.spot
        return remote(self.part.at[g, s.c, s.x], self.u_in.at[g], self.rz_put.at[g], self.ru_got.at[g], s.at_up)

    def back_dn(self, g):
        s = self.spot
        return remote(self.part.at[g, s.c, s.x], self.d_in.at[g], self.rz_put.at[g], self.rd_got.at[g], s.at_dn)

    def add_c(self, g):
        s, part, c_in = self.spot, self.part, self.c_in
        self.got(self.rc_got.at[g], c_in.at[g])
        part[g, s.c, 1 - s.x] = (part[g, s.c, 1 - s.x].astype(f32) + c_in[g, 1 - s.x].astype(f32)).astype(bf16)
        self.back_x(g).start()
        part[g, s.c, s.x] = (part[g, s.c, s.x].astype(f32) + c_in[g, s.x].astype(f32)).astype(bf16)

    def add_xz(self, g):
        s, part, acc = self.spot, self.part, self.acc
        self.got(self.rx_got.at[g], self.x_in.at[g])
        acc[...] = part[g, s.c, s.x].astype(f32) + self.x_in[g].astype(f32)

        @pl.when(jnp.logical_and(g >= s.z, s.low))
        def _():
            self.got(self.ru_got.at[g], self.u_in.at[g])
            acc[...] += self.u_in[g].astype(f32)

        @pl.when(jnp.logical_and(g <= s.z, s.high))
        def _():
            self.got(self.rd_got.at[g], self.d_in.at[g])
            acc[...] += self.d_in[g].astype(f32)

        @pl.when(g > s.z)
        def _():
            part[g, s.c, s.x] = acc[...].astype(bf16)
            self.back_up(g).start()

        @pl.when(g < s.z)
        def _():
            part[g, s.c, s.x] = acc[...].astype(bf16)
            self.back_dn(g).start()

    def settle(self):
        s = self.spot

        @pl.loop(0, s.depth)
        def _(g):
            @pl.when(jnp.logical_and(g <= s.z, s.high))
            def _():
                self.hop_up(g).wait_send()

            @pl.when(jnp.logical_and(g >= s.z, s.low))
            def _():
                self.hop_dn(g).wait_send()

            self.hop_x(g).wait_send()
            self.hop_c(g, False).wait_send()
            self.hop_c(g, True).wait_send()
            self.back_c(g).wait_send()
            self.back_x(g).wait_send()

            @pl.when(g > s.z)
            def _():
                self.back_up(g).wait_send()

            @pl.when(g < s.z)
            def _():
                self.back_dn(g).wait_send()


def put_part(part, g, left, right, n, d):
    @pl.loop(0, d // 256)
    def _(t):
        at = pl.multiple_of(t * 256, 256)
        value = lax.dot_general(left[g], right[pl.ds(at, 256), :], (((1,), (1,)), ((), ())), preferred_element_type=f32)
        part[g, :, :, :, pl.ds(at, 256)] = value.astype(bf16).reshape(2, 2, n, 256)


def forward_group(g, buf, gu, mid, part, w_gu, w_dn, share):
    n, d = buf.shape[3:]
    main = share // 256 * 256
    tokens = lambda: buf[g].reshape(4 * n, d)

    def save(lo, hi, gate, upward):
        inner = math.sqrt(2.0 / math.pi) * (gate + 0.044715 * gate * gate * gate)
        mid[g, :, lo:hi] = (0.5 * gate * (1.0 + jnp.tanh(inner)) * upward).astype(bf16)

    for lo in range(0, main, 256):
        hi = lo + 256
        gate = jnp.dot(tokens(), w_gu[:, lo:hi], preferred_element_type=f32)
        upward = jnp.dot(tokens(), w_gu[:, main + lo : main + hi], preferred_element_type=f32)
        gu[g, :, lo:hi] = gate.astype(bf16)
        gu[g, :, main + lo : main + hi] = upward.astype(bf16)
        save(lo, hi, gate, upward)
    if main < share:
        rest = share - main
        both = jnp.dot(tokens(), w_gu[:, 2 * main :], preferred_element_type=f32)
        gu[g, :, 2 * main :] = both.astype(bf16)
        save(main, share, both[:, :rest], both[:, rest:])
    put_part(part, g, mid, w_dn, n, d)


def backward_group(g, buf, gu, mid, part, w_gu, w_dn, share):
    n, d = buf.shape[3:]
    main = share // 256 * 256
    tokens = lambda: buf[g].reshape(4 * n, d)

    def pull(lo, hi, gate_at, up_at):
        grad = jnp.dot(tokens(), w_dn[:, lo:hi], preferred_element_type=f32)
        gate = gu[g, :, gate_at : gate_at + hi - lo].astype(f32)
        upward = gu[g, :, up_at : up_at + hi - lo].astype(f32)
        factor = math.sqrt(2.0 / math.pi)
        square = gate * gate
        curve = jnp.tanh(factor * gate * (1.0 + 0.044715 * square))
        half = 0.5 * (1.0 + curve)
        slope = half + 0.5 * gate * (1.0 - curve * curve) * factor * (1.0 + 3.0 * 0.044715 * square)
        mid[g, :, gate_at : gate_at + hi - lo] = (grad * upward * slope).astype(bf16)
        mid[g, :, up_at : up_at + hi - lo] = (grad * gate * half).astype(bf16)

    for lo in range(0, main, 256):
        pull(lo, lo + 256, lo, main + lo)
    if main < share:
        pull(main, share, 2 * main, main + share)
    put_part(part, g, mid, w_gu, n, d)


def forward_kernel(grid, inputs, w_attn, blocks, gains, cosine, sine, mask, heads, kv_heads):
    depth, width, dp_n = grid.depth, grid.width, grid.dp
    count, d = inputs.shape
    n = count // 4
    shard, a_cols = w_attn.shape
    q_cols, k_cols = heads * HD, kv_heads * HD
    qkv_cols = q_cols + 2 * k_cols
    share = blocks.shape[2] // 3
    group = heads // kv_heads
    align = math.gcd(shard, 16)
    parts = ((0, qkv_cols), (qkv_cols, q_cols))
    scale = 1.0 / math.sqrt(HD)
    others = width - 1

    def kernel(
        x_ref, wa_ref, blk_ref, gain_ref, cos_ref, sin_ref, mask_ref,
        wa_all, wf_all, normed_out, qkv_out, att_out, branch_out, hidden_out, gains_out,
        all_out, gu_out, mid_out, ffw_out,
        buf, c_in, x_in, u_in, d_in, gain_in, ca_in, xa_in, acc, hid, full_gain, w_a, w_gu, w_dn,
        g_put, g_got, a_up, a_dn, a_got, ay_put, ay_got, f_put, f_got, fy_put, fy_got,
        la_sem, lf_sem, in_sem, o_sem, g_sem, ra_put, ra_got, *sems,
    ):
        s = Spot(grid)
        z, y, x, c = s.z, s.y, s.x, s.c

        def got(sem, ref):
            remote(ref, ref, sem, sem, s.at_x).wait_recv()

        def row(g, yy):
            return pl.multiple_of((g * width + yy) * shard, align)

        barrier = pltpu.get_barrier_semaphore()
        for k in range(1, dp_n):
            signal(barrier, ((s.dp + k) % dp_n, s.q))
        signal(barrier, s.at_x)
        signal(barrier, s.at_c)
        pl.semaphore_wait(barrier, dp_n + 1)

        def a_at(g, yy, k):
            return wa_all.at[g * width + yy, :, pl.ds(parts[k][0], parts[k][1])]

        def a_src(g, k, own):
            return wa_ref.at[:, pl.ds(parts[k][0], parts[k][1])] if own else a_at(g, y, k)

        def a_hop(g, k, own, up):
            return remote(
                a_src(g, k, own), a_at(g, y, k), (a_up if up else a_dn).at[g, k], a_got.at[g, k], s.at_up if up else s.at_dn
            )

        def a_wide(g, k, own, over):
            return remote(a_src(g, k, own), a_at(g, y, k), ay_put.at[g, k, over - 1], ay_got.at[g, k, over - 1], s.at_wide(over))

        def a_pass(g, k, own):
            @pl.when(jnp.logical_and(g <= z, s.high))
            def _():
                a_hop(g, k, own, True).start()

            @pl.when(jnp.logical_and(g >= z, s.low))
            def _():
                a_hop(g, k, own, False).start()

            for over in range(1, width):
                a_wide(g, k, own, over).start()

        def f_at(g, yy):
            return wf_all.at[g * width + yy]

        def f_hop(to):
            return remote(blk_ref.at[to], f_at(z, y), f_put.at[to], f_got.at[z], s.at_depth(to))

        def f_wide(g, own, over):
            return remote(
                blk_ref.at[z] if own else f_at(g, y), f_at(g, y), fy_put.at[g, over - 1], fy_got.at[g, over - 1], s.at_wide(over)
            )

        for k in range(1, dp_n):
            remote(gain_ref, gain_in.at[s.dp], g_put.at[k - 1], g_got.at[k - 1], ((s.dp + k) % dp_n, s.q)).start()
        for k in range(2):
            a_pass(z, k, True)
        ends = jnp.logical_or(z == 0, z == depth - 1)

        @pl.when(ends)
        def _():
            f_hop(s.order(1)).start()

        def attention(x_v, normed_v, qkv_v, att_v, part_a, cos_v, sin_v, mask_v):
            own_gain = pltpu.make_async_copy(gain_ref, gain_in.at[s.dp], in_sem.at[4])
            fills = [
                pltpu.make_async_copy(x_ref, x_v, in_sem.at[0]),
                pltpu.make_async_copy(cos_ref, cos_v, in_sem.at[1]),
                pltpu.make_async_copy(sin_ref, sin_v, in_sem.at[2]),
                pltpu.make_async_copy(mask_ref, mask_v, in_sem.at[3]),
                own_gain,
            ]
            for fill in fills:
                fill.start()

            def load(g, yy, k, own, slot):
                return pltpu.make_async_copy(
                    a_src(g, k, True) if own else a_at(g, yy, k),
                    w_a.at[pl.ds(row(g, yy), shard), pl.ds(parts[k][0], parts[k][1])],
                    la_sem.at[slot, k],
                )

            for k in range(2):
                load(z, y, k, True, 0).start()

            for k in range(1, dp_n):
                remote(
                    gain_in.at[0], gain_in.at[(s.dp + dp_n - k) % dp_n], g_put.at[k - 1], g_got.at[k - 1], s.at_x
                ).wait_recv()
            for fill in fills:
                fill.wait()
            whole = jnp.zeros((8, d), f32)
            for p in range(dp_n):
                one = gain_in[p].astype(f32)[:8]
                one = jnp.concatenate([one, jnp.zeros((8, d - one.shape[1]), f32)], axis=1)
                whole = whole + (pltpu.roll(one, p * shard, 1) if p else one)
            full_gain[...] = whole
            pltpu.make_async_copy(full_gain, gains_out, o_sem.at[0]).start()

            @pl.loop(0, count // 32)
            def _(i):
                at = pl.ds(pl.multiple_of(i * 32, 32), 32)
                value = x_v[at, :].astype(f32)
                inverse = lax.rsqrt(jnp.mean(value * value, axis=-1, keepdims=True) + EPS)
                normed_v[at, :] = (value * inverse * full_gain[0:1, :]).astype(bf16)

            pltpu.make_async_copy(normed_v, normed_out, o_sem.at[1]).start()

            for i in range(1, depth):
                g = s.order(i)
                for k in range(2):
                    got(a_got.at[g, k], a_at(g, y, k))
                    a_pass(g, k, False)
                    load(g, y, k, False, i * width).start()
                if i == 1:
                    f_hop(s.order(2)).start()
                    f_hop(s.order(3)).start()

            @pl.when(jnp.logical_not(ends))
            def _():
                f_hop(s.order(1)).start()

            for over in range(1, width):
                f_wide(z, True, over).start()
            for k in range(2):
                for i in range(depth):
                    g = s.order(i)
                    for over in range(1, width):
                        yy = (y + width - over) % width
                        got(ay_got.at[g, k, over - 1], a_at(g, yy, k))
                        load(g, yy, k, False, i * width + over).start()
                for i in range(depth):
                    g = s.order(i)
                    for over in range(width):
                        load(g, (y + width - over) % width, k, i + over == 0, i * width + over).wait()
                if k:
                    continue
                for h in range(heads + 2 * kv_heads):
                    value = jnp.dot(normed_v[...], w_a[:, h * HD : (h + 1) * HD], preferred_element_type=f32)
                    if h < heads + kv_heads:
                        half = HD // 2
                        first, second = value[:, :half], value[:, half:]
                        low = first * cos_v[...] - second * sin_v[...]
                        high = second * cos_v[...] + first * sin_v[...]
                        if h < heads:
                            low, high = low * scale, high * scale
                        qkv_v[:, h * HD : h * HD + half] = low.astype(bf16)
                        qkv_v[:, h * HD + half : (h + 1) * HD] = high.astype(bf16)
                    else:
                        qkv_v[:, h * HD : (h + 1) * HD] = value.astype(bf16)
                pltpu.make_async_copy(qkv_v, qkv_out, o_sem.at[2]).start()

                @pl.loop(0, count // ROW_LEN)
                def _(r):
                    at = pl.ds(pl.multiple_of(r * ROW_LEN, ROW_LEN), ROW_LEN)
                    allowed = mask_v[at, :] > 0.5
                    for h in range(heads):
                        kv = heads + h // group
                        scores = lax.dot_general(
                            qkv_v[at, h * HD : (h + 1) * HD],
                            qkv_v[at, kv * HD : (kv + 1) * HD],
                            (((1,), (1,)), ((), ())),
                            preferred_element_type=f32,
                        )
                        expo = jnp.where(allowed, jnp.exp(CAP * jnp.tanh(scores / CAP)), 0.0)
                        probs = (expo / jnp.sum(expo, axis=-1, keepdims=True)).astype(bf16)
                        kv = kv + kv_heads
                        value = jnp.dot(probs, qkv_v[at, kv * HD : (kv + 1) * HD], preferred_element_type=f32)
                        att_v[at, h * HD : (h + 1) * HD] = value.astype(bf16)

                pltpu.make_async_copy(att_v, att_out, o_sem.at[3]).start()

            @pl.loop(0, d // 256)
            def _(t):
                at = pl.multiple_of(t * 256, 256)
                value = lax.dot_general(
                    att_v[...], w_a[pl.ds(at, 256), qkv_cols:], (((1,), (1,)), ((), ())), preferred_element_type=f32
                )
                part_a[:, :, :, pl.ds(at, 256)] = value.astype(bf16).reshape(2, 2, n, 256)

            own_rows = pltpu.make_async_copy(
                w_a.at[pl.ds(row(z, y), shard)], wa_all.at[s.dp], o_sem.at[4]
            )
            own_rows.start()
            to_c = remote(part_a.at[1 - c], ca_in, ra_put.at[0], ra_got.at[0], s.at_c)
            to_c.start()
            to_c.wait_recv()
            part_a[c, 1 - x] = (part_a[c, 1 - x].astype(f32) + ca_in[1 - x].astype(f32)).astype(bf16)
            to_x = remote(part_a.at[c, 1 - x], xa_in, ra_put.at[1], ra_got.at[1], s.at_x)
            to_x.start()
            acc[...] = part_a[c, x].astype(f32) + ca_in[x].astype(f32)
            to_x.wait_recv()

            @pl.loop(0, n // 16)
            def _(i):
                at = pl.ds(pl.multiple_of(i * 16, 16), 16)
                branch = acc[at, :] + xa_in[at, :].astype(f32)
                acc[at, :] = branch
                inverse = lax.rsqrt(jnp.mean(branch * branch, axis=-1, keepdims=True) + EPS)
                mine = pl.ds(pl.multiple_of((c * 2 + x) * n + i * 16, 16), 16)
                hidden = x_v[mine, :].astype(f32) + branch * inverse * full_gain[1:2, :]
                hid[at, :] = hidden
                inverse = lax.rsqrt(jnp.mean(hidden * hidden, axis=-1, keepdims=True) + EPS)
                buf[z, c, x, at, :] = (hidden * inverse * full_gain[2:3, :]).astype(bf16)

            to_c.wait_send()
            to_x.wait_send()
            pltpu.make_async_copy(full_gain, gains_out, o_sem.at[0]).wait()
            pltpu.make_async_copy(normed_v, normed_out, o_sem.at[1]).wait()
            pltpu.make_async_copy(qkv_v, qkv_out, o_sem.at[2]).wait()
            pltpu.make_async_copy(att_v, att_out, o_sem.at[3]).wait()
            own_rows.wait()

        pl.run_scoped(
            attention,
            pltpu.VMEM((count, d), bf16),
            pltpu.VMEM((count, d), bf16),
            pltpu.VMEM((count, qkv_cols), bf16),
            pltpu.VMEM((count, q_cols), bf16),
            pltpu.VMEM((2, 2, n, d), bf16),
            pltpu.VMEM((count, HD // 2), f32),
            pltpu.VMEM((count, HD // 2), f32),
            pltpu.VMEM((count, ROW_LEN), f32),
        )

        def ffn(part, gu, mid, tot):
            trade = Trade(s, buf, part, tot, c_in, x_in, u_in, d_in, sems)
            trade.pass_on(z)
            saved = [
                pltpu.make_async_copy(acc, branch_out, o_sem.at[0]),
                pltpu.make_async_copy(hid, hidden_out, o_sem.at[1]),
            ]
            for save in saved:
                save.start()

            def load(g, yy, own, slot):
                at = pl.ds(row(g, yy), shard)
                source = blk_ref.at[z] if own else f_at(g, yy)
                return (
                    pltpu.make_async_copy(source.at[:, pl.ds(0, 2 * share)], w_gu.at[at], lf_sem.at[slot, 0]),
                    pltpu.make_async_copy(source.at[:, pl.ds(2 * share, share)], w_dn.at[at], lf_sem.at[slot, 1]),
                )

            for copy in load(z, y, True, 0):
                copy.start()

            def f_take(i):
                g = s.order(i)
                got(f_got.at[g], f_at(g, y))
                for over in range(1, width):
                    f_wide(g, False, over).start()
                for copy in load(g, y, False, i * width):
                    copy.start()

            def gather(i):
                trade.take_rank(s.order(i))
                pltpu.make_async_copy(buf.at[s.order(i)], all_out.at[s.order(i)], g_sem.at[i, 0]).start()

            for i in range(1, depth):
                f_take(i)
                trade.take_z(s.order(i))
                gather(i - 1)
            gather(depth - 1)

            for i in range(depth):
                g = s.order(i)
                for over in range(1, width):
                    yy = (y + width - over) % width
                    got(fy_got.at[g, over - 1], f_at(g, yy))
                    for copy in load(g, yy, False, i * width + over):
                        copy.start()
            for i in range(depth):
                g = s.order(i)
                for over in range(width):
                    for copy in load(g, (y + width - over) % width, i + over == 0, i * width + over):
                        copy.wait()
            at = pl.ds(row(z, y), shard)
            own_rows = [
                pltpu.make_async_copy(w_gu.at[at], wf_all.at[s.dp, :, pl.ds(0, 2 * share)], o_sem.at[2]),
                pltpu.make_async_copy(w_dn.at[at], wf_all.at[s.dp, :, pl.ds(2 * share, share)], o_sem.at[3]),
            ]
            for copy in own_rows:
                copy.start()

            def keep(g):
                return (
                    pltpu.make_async_copy(gu.at[g], gu_out.at[g], g_sem.at[g, 1]),
                    pltpu.make_async_copy(mid.at[g], mid_out.at[g], g_sem.at[g, 2]),
                )

            @pl.loop(0, depth)
            def _(i):
                g = s.order(depth - 1 - i)
                forward_group(g, buf, gu, mid, part, w_gu, w_dn, share)
                trade.back_c(g).start()
                for copy in keep(g):
                    copy.start()
                trade.add_c(g)

            @pl.loop(0, depth)
            def _(i):
                trade.add_xz(s.order(depth - 1 - i))

            last = pltpu.make_async_copy(tot, ffw_out, o_sem.at[4])
            last.start()
            trade.settle()
            for i in range(depth):
                g = s.order(i)
                pltpu.make_async_copy(buf.at[g], all_out.at[g], g_sem.at[i, 0]).wait()
                for copy in keep(g):
                    copy.wait()
            for copy in saved + own_rows:
                copy.wait()
            last.wait()

        pl.run_scoped(
            ffn,
            pltpu.VMEM((depth, 2, 2, n, d), bf16),
            pltpu.VMEM((depth, count, 2 * share), bf16),
            pltpu.VMEM((depth, count, share), bf16),
            pltpu.VMEM((n, d), f32),
        )

        for k in range(1, dp_n):
            remote(gain_ref, gain_in.at[s.dp], g_put.at[k - 1], g_got.at[k - 1], ((s.dp + k) % dp_n, s.q)).wait_send()
        for i in range(depth):
            g = s.order(i)
            for k in range(2):

                @pl.when(jnp.logical_and(g <= z, s.high))
                def _():
                    a_hop(g, k, i == 0, True).wait_send()

                @pl.when(jnp.logical_and(g >= z, s.low))
                def _():
                    a_hop(g, k, i == 0, False).wait_send()

                for over in range(1, width):
                    a_wide(g, k, i == 0, over).wait_send()
            for over in range(1, width):
                f_wide(g, i == 0, over).wait_send()
            if i:
                f_hop(g).wait_send()

    shape = jax.ShapeDtypeStruct
    outs = (
        shape((dp_n, shard, a_cols), bf16),
        shape((dp_n, shard, 3 * share), bf16),
        shape((count, d), bf16),
        shape((count, qkv_cols), bf16),
        shape((count, q_cols), bf16),
        shape((n, d), f32),
        shape((n, d), f32),
        shape((8, d), f32),
        shape((depth, 2, 2, n, d), bf16),
        shape((depth, count, 2 * share), bf16),
        shape((depth, count, share), bf16),
        shape((n, d), f32),
    )
    operands = (inputs, w_attn, blocks, gains, cosine, sine, mask)
    anywhere = pl.BlockSpec(memory_space=pl.ANY)
    dma = pltpu.SemaphoreType.DMA
    return pl.pallas_call(
        kernel,
        out_shape=outs,
        in_specs=[anywhere] * len(operands),
        out_specs=tuple([anywhere] * len(outs)),
        scratch_shapes=Trade.buffers(depth, n, d)
        + [
            pltpu.VMEM((dp_n,) + gains.shape, bf16),
            pltpu.VMEM((2, n, d), bf16),
            pltpu.VMEM((n, d), bf16),
            pltpu.VMEM((n, d), f32),
            pltpu.VMEM((n, d), f32),
            pltpu.VMEM((8, d), f32),
            pltpu.VMEM((d, a_cols), bf16),
            pltpu.VMEM((d, 2 * share), bf16),
            pltpu.VMEM((d, share), bf16),
            dma((dp_n - 1,)),
            dma((dp_n - 1,)),
            dma((depth, 2)),
            dma((depth, 2)),
            dma((depth, 2)),
            dma((depth, 2, others)),
            dma((depth, 2, others)),
            dma((depth,)),
            dma((depth,)),
            dma((depth, others)),
            dma((depth, others)),
            dma((dp_n, 2)),
            dma((dp_n, 2)),
            dma((5,)),
            dma((5,)),
            dma((depth, 3)),
            dma((2,)),
            dma((2,)),
        ]
        + Trade.semaphores(depth),
        compiler_params=pltpu.CompilerParams(collective_id=1, has_side_effects=True, vmem_limit_bytes=66_000_000),
        name="forward",
    )(*operands)


def backward_kernel(grid, block, weights, saved):
    depth = grid.depth
    n, d = block.shape
    count = 4 * n
    dp_n, shard = weights.shape[:2]
    share = weights.shape[2] // 3
    align = math.gcd(shard, 16)

    def kernel(block_ref, w_ref, gu_ref, all_out, mid_out, ffw_out, buf, c_in, x_in, u_in, d_in,
               w_gu, w_dn, part, gu, mid, acc, in_sem, w_sem, g_sem, *sems):
        s = Spot(grid)
        own = pltpu.make_async_copy(block_ref, buf.at[s.z, s.c, s.x], in_sem.at[0])
        loads = [pltpu.make_async_copy(gu_ref, gu, in_sem.at[1])]
        for p in range(dp_n):
            at = pl.ds(pl.multiple_of(p * shard, align), shard)
            loads.append(pltpu.make_async_copy(w_ref.at[p, :, pl.ds(0, 2 * share)], w_gu.at[at], w_sem.at[p, 0]))
            loads.append(pltpu.make_async_copy(w_ref.at[p, :, pl.ds(2 * share, share)], w_dn.at[at], w_sem.at[p, 1]))
        own.start()
        for load in loads:
            load.start()
        barrier = pltpu.get_barrier_semaphore()
        signal(barrier, s.at_x)
        signal(barrier, s.at_c)

        @pl.when(s.low)
        def _():
            signal(barrier, s.at_dn)

        @pl.when(s.high)
        def _():
            signal(barrier, s.at_up)

        pl.semaphore_wait(barrier, 2 + (s.z + depth - 1) // depth + (2 * depth - 2 - s.z) // depth)
        own.wait()
        trade = Trade(s, buf, part, acc, c_in, x_in, u_in, d_in, sems)
        trade.pass_on(s.z)

        def keep(g):
            return (
                pltpu.make_async_copy(buf.at[g], all_out.at[g], g_sem.at[g, 0]),
                pltpu.make_async_copy(mid.at[g], mid_out.at[g], g_sem.at[g, 1]),
            )

        @pl.loop(1, depth + 1)
        def _(i):
            @pl.when(i < depth)
            def _():
                trade.take_z(s.order(i))

            g = s.order(i - 1)
            trade.take_rank(g)

            @pl.when(i == 1)
            def _():
                for load in loads:
                    load.wait()

            backward_group(g, buf, gu, mid, part, w_gu, w_dn, share)
            trade.back_c(g).start()
            for copy in keep(g):
                copy.start()

        @pl.loop(0, depth)
        def _(i):
            trade.add_c(s.order(depth - 1 - i))

        @pl.loop(0, depth)
        def _(i):
            trade.add_xz(s.order(depth - 1 - i))

        last = pltpu.make_async_copy(acc, ffw_out, in_sem.at[0])
        last.start()
        trade.settle()

        @pl.loop(0, depth)
        def _(g):
            for copy in keep(g):
                copy.wait()

        last.wait()

    shape = jax.ShapeDtypeStruct
    outs = (
        shape((depth, 2, 2, n, d), bf16),
        shape((depth, count, 2 * share), bf16),
        shape((n, d), f32),
    )
    anywhere = pl.BlockSpec(memory_space=pl.ANY)
    dma = pltpu.SemaphoreType.DMA
    return pl.pallas_call(
        kernel,
        out_shape=outs,
        in_specs=[anywhere] * 3,
        out_specs=tuple([anywhere] * len(outs)),
        scratch_shapes=Trade.buffers(depth, n, d)
        + [
            pltpu.VMEM((d, 2 * share), bf16),
            pltpu.VMEM((d, share), bf16),
            pltpu.VMEM((depth, 2, 2, n, d), bf16),
            pltpu.VMEM((depth, count, 2 * share), bf16),
            pltpu.VMEM((depth, count, 2 * share), bf16),
            pltpu.VMEM((n, d), f32),
            dma((2,)),
            dma((dp_n, 2)),
            dma((depth, 2)),
        ]
        + Trade.semaphores(depth),
        compiler_params=pltpu.CompilerParams(collective_id=2, has_side_effects=True, vmem_limit_bytes=66_000_000),
        name="backward",
    )(block, weights, saved)


def unit_cuts(units, parts):
    tiles = units // LANE
    edges = [(tiles * k + parts - 1) // parts for k in range(parts + 1)]
    starts = [e * LANE for e in edges[:-1]]
    sizes = [(b - a) * LANE for a, b in zip(edges[:-1], edges[1:])]
    return starts, sizes, max(sizes)


def cut_units(block, cuts):
    starts, sizes, share = cuts
    return jnp.stack(
        [
            jnp.pad(block[:, a : a + n], ((0, 0), (0, share - n))) if n < share else block[:, a : a + n]
            for a, n in zip(starts, sizes)
        ]
    )


def join_units(blocks, cuts):
    starts, sizes, share = cuts
    return jnp.concatenate([blocks[k, :, :n] for k, n in enumerate(sizes)], axis=1)


def make_body(grid):
    def body(
        inputs,
        cotangent,
        segments,
        positions,
        w_query,
        w_key,
        w_value,
        w_output,
        w_gate,
        w_up,
        w_down,
        gain_attn,
        gain_post_attn,
        gain_ffw,
        gain_post_ffw,
    ):
        grid.here()
        count, width = inputs.shape
        shard = w_query.shape[0]
        group = HEADS // KV
        local_kv = w_key.shape[1] // HD
        local_heads = local_kv * group
        q_cols, k_cols = w_query.shape[1], w_key.shape[1]
        scale = 1.0 / math.sqrt(HD)
        part = count // grid.tensor
        rows = count // ROW_LEN
        cuts = unit_cuts(w_gate.shape[1], grid.depth)
        share = cuts[2]
        main = share // 256 * 256
        mine = (lax.rem(grid.rank, 2) * 2 + grid.rank // 2) * part

        gains = jnp.stack([gain_attn, gain_post_attn, gain_ffw, gain_post_ffw])
        gains = jnp.pad(gains, ((0, 12), (0, -shard % LANE)))
        angles = make_angles(positions, HD)[:, 0]
        cosine, sine = jnp.cos(angles), jnp.sin(angles)
        allowed = row_mask(segments, rows, ROW_LEN)
        cut_gate, cut_up = cut_units(w_gate, cuts), cut_units(w_up, cuts)
        blocks = jnp.concatenate(
            [cut_gate[:, :, :main], cut_up[:, :, :main], cut_gate[:, :, main:], cut_up[:, :, main:], cut_units(w_down.T, cuts)],
            axis=2,
        )
        w_attn = jnp.concatenate([w_query, w_key, w_value, w_output.T], axis=1)
        (full_attn, full_ffn, normed, qkv, attended, branch_attn, hidden, full_gains,
         all_normed, saved, mixed, branch_ffw) = forward_kernel(
            grid, inputs, w_attn, blocks, gains, cosine, sine,
            allowed.astype(f32).reshape(count, ROW_LEN), local_heads, local_kv,
        )
        gain_one, gain_two, gain_three, gain_four = (full_gains[k] for k in range(4))
        full_attn = full_attn.reshape(width, full_attn.shape[2])
        full_qkv, full_out = full_attn[:, : q_cols + 2 * k_cols], full_attn[:, q_cols + 2 * k_cols :]
        own_out = (hidden + rms_scale(branch_ffw, gain_four)).astype(bf16)

        d_out = lax.dynamic_slice_in_dim(cotangent, mine, part, 0).astype(f32)
        d_branch_own, d_gain_four = rms_back(branch_ffw, gain_four, d_out)
        all_back, d_gu, d_normed_ffw = backward_kernel(grid, d_branch_own.astype(bf16), full_ffn, saved)
        tokens = grid.depth * count
        d_gu = d_gu.reshape(tokens, 2 * share)
        grad_dn = contract_rows(all_back.reshape(tokens, width), mixed.reshape(tokens, share)).astype(bf16)
        grad_gu = contract_rows(all_normed.reshape(tokens, width), d_gu).astype(bf16)
        blocks_dn = grid.return_blocks(grad_dn)
        blocks_gu = grid.return_blocks(grad_gu)
        grad_down = join_units(blocks_dn, cuts).T.astype(f32)
        rest = 2 * main + share - main
        grad_gate = jnp.concatenate([blocks_gu[:, :, :main], blocks_gu[:, :, 2 * main : rest]], axis=2)
        grad_up = jnp.concatenate([blocks_gu[:, :, main : 2 * main], blocks_gu[:, :, rest:]], axis=2)
        grad_gate = join_units(grad_gate, cuts).astype(f32)
        grad_up = join_units(grad_up, cuts).astype(f32)

        d_hidden_norm, d_gain_three = rms_back(hidden, gain_three, d_normed_ffw)
        d_hidden = d_out + d_hidden_norm
        d_branch_attn, d_gain_two = rms_back(branch_attn, gain_two, d_hidden)
        d_branch_attn = grid.spread_rank(d_branch_attn.astype(bf16))
        grad_output = contract_rows(d_branch_attn, attended).astype(bf16)
        grad_output = grid.scatter_rows(grad_output).T
        d_attended = dot(d_branch_attn, full_out).astype(bf16)
        d_att_five = d_attended.reshape(rows, ROW_LEN, local_kv, group, HD)
        query_five = qkv[:, :q_cols].reshape(rows, ROW_LEN, local_kv, group, HD)
        key_four = qkv[:, q_cols : q_cols + k_cols].reshape(rows, ROW_LEN, local_kv, HD)
        value_four = qkv[:, q_cols + k_cols :].reshape(rows, ROW_LEN, local_kv, HD)
        scores = jnp.einsum("rqkgd,rskd->rkgqs", query_five, key_four, preferred_element_type=f32)
        capped = CAP * jnp.tanh(scores / CAP)
        expo = jnp.where(allowed[:, None, None], jnp.exp(capped), 0.0)
        soft = expo / jnp.sum(expo, axis=-1, keepdims=True)
        probs = soft.astype(bf16)
        turn_cos, turn_sin = cosine[:, None], sine[:, None]
        d_values = jnp.einsum("rkgqs,rqkgd->rskd", probs, d_att_five, preferred_element_type=f32)
        d_probs = jnp.einsum("rqkgd,rskd->rkgqs", d_att_five, value_four, preferred_element_type=f32)
        d_soft = soft * (d_probs - jnp.sum(soft * d_probs, axis=-1, keepdims=True))
        d_capped = (d_soft * (1.0 - (capped / CAP) ** 2)).astype(bf16)
        d_queries = jnp.einsum(
            "rkgqs,rskd->rqkgd", d_capped, key_four, preferred_element_type=f32
        ).reshape(count, local_heads, HD)
        d_keys = jnp.einsum(
            "rkgqs,rqkgd->rskd", d_capped, query_five, preferred_element_type=f32
        ).reshape(count, local_kv, HD)
        d_query_proj = (rotate(d_queries, turn_cos, -turn_sin) * scale).astype(bf16).reshape(count, q_cols)
        d_key_proj = rotate(d_keys, turn_cos, -turn_sin).astype(bf16).reshape(count, k_cols)
        d_value_proj = d_values.reshape(count, k_cols).astype(bf16)
        d_qkv = jnp.concatenate([d_query_proj, d_key_proj, d_value_proj], axis=1)
        d_normed = grid.reduce_rank(contract_cols(d_qkv, full_qkv).astype(bf16)).astype(f32)
        grad_qkv = grid.scatter_rows(contract_rows(normed, d_qkv).astype(bf16))
        own_source = lax.dynamic_slice_in_dim(inputs, mine, part, 0).astype(f32)
        d_source, d_gain_one = rms_back(own_source, gain_one, d_normed)
        own_grad = (d_hidden + d_source).astype(bf16)

        d_gains = jnp.stack([d_gain_one, d_gain_two, d_gain_three, d_gain_four])
        for bit in grid.rank_bits():
            d_gains = d_gains + grid.swap_rank(d_gains, bit)
        d_gains = d_gains.reshape(4, grid.dp, shard).transpose(1, 0, 2).reshape(grid.dp * 4, shard)
        d_gains = grid.scatter_rows(d_gains)

        return (
            grid.spread_rank(own_out),
            grid.spread_rank(own_grad),
            grad_qkv[:, :q_cols],
            grad_qkv[:, q_cols : q_cols + k_cols],
            grad_qkv[:, q_cols + k_cols :],
            grad_output,
            grad_gate,
            grad_up,
            grad_down,
            d_gains[0],
            d_gains[1],
            d_gains[2],
            d_gains[3],
        )

    return body


def solution(mesh):
    placed = (
        P("dp", None),
        P("dp", None),
        P("dp"),
        P("dp"),
        P("dp", "tensor"),
        P("dp", "tensor"),
        P("dp", "tensor"),
        P("tensor", "dp"),
        P("dp", "tensor"),
        P("dp", "tensor"),
        P("tensor", "dp"),
        P("dp"),
        P("dp"),
        P("dp"),
        P("dp"),
    )
    return jax.shard_map(
        make_body(Grid(mesh)),
        mesh=mesh,
        in_specs=placed,
        out_specs=(
            P("dp", None),
            P("dp", None),
            P("dp", "tensor"),
            P("dp", "tensor"),
            P("dp", "tensor"),
            P("tensor", "dp"),
            P("dp", "tensor"),
            P("dp", "tensor"),
            P("tensor", "dp"),
            P("dp"),
            P("dp"),
            P("dp"),
            P("dp"),
        ),
        check_vma=False,
    )
```

```python
import functools
import math

import jax
import jax.numpy as jnp
from jax import lax
from jax.experimental import pallas as pl
from jax.experimental.pallas import tpu as pltpu
from jax.sharding import PartitionSpec as P

HEADS = 8
KV = 4
HD = 256
ROW_LEN = 128
LANE = 128


EPS = 1e-06
CAP = 50.0
THETA = 10000.0

f32 = jnp.float32
bf16 = jnp.bfloat16


def rms_scale(field, gain):
    inverse = lax.rsqrt(jnp.mean(field * field, axis=-1, keepdims=True) + EPS)
    return field * inverse * gain


def rms_back(field, gain, grad):
    inverse = lax.rsqrt(jnp.mean(field * field, axis=-1, keepdims=True) + EPS)
    unit = field * inverse
    d_gain = jnp.sum(grad * unit, axis=0)
    scaled = grad * gain
    d_field = inverse * (scaled - unit * jnp.mean(scaled * unit, axis=-1, keepdims=True))
    return d_field, d_gain


def geglu(gate, upward):
    return jax.nn.gelu(gate, approximate=True) * upward


def rotate(field, cosine, sine):
    half = field.shape[-1] // 2
    first = field[..., :half]
    second = field[..., half:]
    return jnp.concatenate(
        [first * cosine - second * sine, second * cosine + first * sine], axis=-1
    )


def make_angles(positions, head_size):
    half = head_size // 2
    freqs = THETA ** (-(jnp.arange(half).astype(f32) * 2.0) / head_size)
    return positions.astype(f32)[:, None, None] * freqs[None, None, :]


def row_mask(segments, rows, length):
    seg_rows = segments.reshape(rows, length)
    same = seg_rows[:, :, None] == seg_rows[:, None, :]
    index = jnp.arange(length)
    causal = index[:, None] >= index[None, :]
    return jnp.logical_and(same, causal[None])


def dot(left, right):
    return jnp.dot(left, right, preferred_element_type=f32)


def contract_rows(left, right):
    return lax.dot_general(left, right, (((0,), (0,)), ((), ())), preferred_element_type=f32)


def contract_cols(left, right):
    return lax.dot_general(left, right, (((1,), (1,)), ((), ())), preferred_element_type=f32)


class Grid:
    def __init__(self, mesh):
        self.dp = mesh.shape["dp"]
        self.tensor = mesh.shape["tensor"]
        self.depth = 4 if self.dp % 4 == 0 else (2 if self.dp % 2 == 0 else 1)
        self.width = self.dp // self.depth

    def here(self):
        index = lax.axis_index("dp")
        self.deep = index // self.width
        self.wide = lax.rem(index, self.width)
        self.rank = lax.axis_index("tensor")

    def shift(self, value, step):
        pairs = [
            (z * self.width + y, ((z + step) % self.depth) * self.width + y)
            for z in range(self.depth)
            for y in range(self.width)
        ]
        return lax.ppermute(value, "dp", pairs)

    def swap_wide(self, value, bit):
        pairs = [
            (z * self.width + y, z * self.width + (y ^ bit))
            for z in range(self.depth)
            for y in range(self.width)
        ]
        return lax.ppermute(value, "dp", pairs)

    def swap_rank(self, value, bit):
        return lax.ppermute(value, "tensor", [(q, q ^ bit) for q in range(self.tensor)])

    def wide_bits(self):
        return [1 << b for b in range(self.width.bit_length() - 1)]

    def rank_bits(self):
        return [1 << b for b in range(self.tensor.bit_length() - 1)]

    def reduce_width(self, full):
        rows, columns = full.shape[0] // self.dp, full.shape[1]
        held = full.reshape(self.depth, self.width, rows, columns)
        for bit in reversed(self.wide_bits()):
            held = held.reshape(self.depth, 2, bit, rows, columns)
            mine = lax.rem(self.wide // bit, 2)
            other = lax.dynamic_index_in_dim(held, 1 - mine, 1, keepdims=False)
            own = lax.dynamic_index_in_dim(held, mine, 1, keepdims=False)
            held = own + self.swap_wide(other, bit)
        return held.reshape(self.depth, rows, columns)

    def pick(self, held, step):
        to = lax.rem(self.deep + step, self.depth)
        return lax.dynamic_index_in_dim(held, to, 0, keepdims=False)

    def scatter_rows(self, full):
        held = self.reduce_width(full)
        total = self.pick(held, 0).astype(f32)
        for step in range(1, self.depth):
            total = total + self.shift(self.pick(held, step), step).astype(f32)
        return total

    def return_blocks(self, full):
        held = self.reduce_width(full)
        out = jnp.zeros_like(held)
        for step in range(self.depth):
            part = self.pick(held, step)
            part = part if step == 0 else self.shift(part, step)
            source = lax.rem(self.deep + self.depth - step, self.depth)
            out = lax.dynamic_update_slice(out, part[None], (source, 0, 0))
        return out

    def spread_rank(self, block):
        x, c = self.rank // 2, lax.rem(self.rank, 2)
        n, d = block.shape
        out = jnp.zeros((2, 2, n, d), block.dtype)
        for far_c in range(2):
            for far_x in range(2):
                part = block
                if far_x:
                    part = across
                if far_c:
                    part = self.swap_rank(part, 1)
                elif not far_x:
                    across = self.swap_rank(block, 2)
                out = lax.dynamic_update_slice(
                    out, part[None, None], (jnp.bitwise_xor(c, far_c), jnp.bitwise_xor(x, far_x), 0, 0)
                )
        return out.reshape(4 * n, d)

    def reduce_rank(self, full):
        x, c = self.rank // 2, lax.rem(self.rank, 2)
        held = full.reshape(2, 2, full.shape[0] // 4, full.shape[1])
        for at, bit in ((c, 1), (x, 2)):
            own = lax.dynamic_index_in_dim(held, at, 0, keepdims=False)
            other = lax.dynamic_index_in_dim(held, 1 - at, 0, keepdims=False)
            held = own + self.swap_rank(other, bit)
        return held


MESH = pl.DeviceIdType.MESH


class Spot:
    def __init__(self, grid):
        self.depth, self.width = grid.depth, grid.width
        self.dp = lax.axis_index("dp")
        self.q = lax.axis_index("tensor")
        self.z, self.y = self.dp // self.width, self.dp % self.width
        self.x, self.c = self.q // 2, self.q % 2
        self.at_x = (self.dp, (1 - self.x) * 2 + self.c)
        self.at_c = (self.dp, self.x * 2 + 1 - self.c)
        self.at_up = (self.dp + self.width, self.q)
        self.at_dn = (self.dp - self.width, self.q)
        self.low, self.high = self.z > 0, self.z < self.depth - 1

    def order(self, i):
        z = self.z
        near = z + 1 - 2 * (z % 2)
        middle = 2 - z // 2
        far = 3 * (1 - z // 2)
        return jnp.where(i == 0, z, jnp.where(i == 1, near, jnp.where(i == 2, middle, far)))

    def at_depth(self, z):
        return (z * self.width + self.y, self.q)

    def at_wide(self, over):
        return (self.z * self.width + (self.y + over) % self.width, self.q)


def remote(src, dst, put, got, device):
    return pltpu.make_async_remote_copy(
        src_ref=src, dst_ref=dst, send_sem=put, recv_sem=got, device_id=device, device_id_type=MESH
    )


def signal(semaphore, device):
    pl.semaphore_signal(semaphore, inc=1, device_id=device, device_id_type=MESH)


class Trade:
    def __init__(self, spot, buf, part, acc, c_in, x_in, z_in, sems):
        self.spot, self.buf, self.part, self.acc = spot, buf, part, acc
        self.c_in, self.x_in, self.z_in = c_in, x_in, z_in
        (self.z_up, self.z_dn, self.z_got, self.x_put, self.x_got, self.c_put, self.c_got,
         self.rc_put, self.rc_got, self.rx_put, self.rx_got, self.rz_put, self.ru_got, self.rd_got) = sems

    @staticmethod
    def semaphores(depth):
        dma = pltpu.SemaphoreType.DMA
        return [dma((depth,))] * 5 + [dma((depth, 2))] * 2 + [dma((depth,))] * 7

    @staticmethod
    def buffers(depth, n, d):
        return [
            pltpu.VMEM((depth, 2, 2, n, d), bf16),
            pltpu.VMEM((depth, 2, n, d), bf16),
            pltpu.VMEM((depth, n, d), bf16),
            pltpu.VMEM((depth + 1, n, d), bf16),
        ]

    def hop_up(self, g):
        s = self.spot
        return remote(self.buf.at[g, s.c, s.x], self.buf.at[g, s.c, s.x], self.z_up.at[g], self.z_got.at[g], s.at_up)

    def hop_dn(self, g):
        s = self.spot
        return remote(self.buf.at[g, s.c, s.x], self.buf.at[g, s.c, s.x], self.z_dn.at[g], self.z_got.at[g], s.at_dn)

    def hop_x(self, g):
        s = self.spot
        return remote(self.buf.at[g, s.c, s.x], self.buf.at[g, s.c, s.x], self.x_put.at[g], self.x_got.at[g], s.at_x)

    def hop_c(self, g, far):
        s = self.spot
        xx = (1 - s.x) if far else s.x
        return remote(
            self.buf.at[g, s.c, xx], self.buf.at[g, s.c, xx], self.c_put.at[g, int(far)], self.c_got.at[g, int(far)], s.at_c
        )

    def got(self, sem, ref):
        remote(ref, ref, sem, sem, self.spot.at_x).wait_recv()

    def pass_on(self, g):
        s = self.spot

        @pl.when(jnp.logical_and(g <= s.z, s.high))
        def _():
            self.hop_up(g).start()

        @pl.when(jnp.logical_and(g >= s.z, s.low))
        def _():
            self.hop_dn(g).start()

        self.hop_x(g).start()
        self.hop_c(g, False).start()

    def take_z(self, g):
        s = self.spot
        self.got(self.z_got.at[g], self.buf.at[g, s.c, s.x])
        self.pass_on(g)

    def take_rank(self, g):
        s = self.spot
        self.got(self.x_got.at[g], self.buf.at[g, s.c, 1 - s.x])
        self.hop_c(g, True).start()
        self.got(self.c_got.at[g, 0], self.buf.at[g, 1 - s.c, s.x])
        self.got(self.c_got.at[g, 1], self.buf.at[g, 1 - s.c, 1 - s.x])

    def back_c(self, g):
        s = self.spot
        return remote(self.part.at[g, 1 - s.c], self.c_in.at[g], self.rc_put.at[g], self.rc_got.at[g], s.at_c)

    def back_x(self, g):
        s = self.spot
        return remote(self.part.at[g, s.c, 1 - s.x], self.x_in.at[g], self.rx_put.at[g], self.rx_got.at[g], s.at_x)

    def back_up(self, g):
        s = self.spot
        return remote(self.part.at[g, s.c, s.x], self.z_in.at[g], self.rz_put.at[g], self.ru_got.at[g], s.at_up)

    def back_dn(self, g):
        s = self.spot
        slot = jnp.where(g == s.z - 1, s.depth, g)
        return remote(self.part.at[g, s.c, s.x], self.z_in.at[slot], self.rz_put.at[g], self.rd_got.at[g], s.at_dn)

    def add_c(self, g):
        s, part, c_in = self.spot, self.part, self.c_in
        self.got(self.rc_got.at[g], c_in.at[g])
        part[g, s.c, 1 - s.x] = (part[g, s.c, 1 - s.x].astype(f32) + c_in[g, 1 - s.x].astype(f32)).astype(bf16)
        self.back_x(g).start()
        part[g, s.c, s.x] = (part[g, s.c, s.x].astype(f32) + c_in[g, s.x].astype(f32)).astype(bf16)

    def add_xz(self, g):
        s, part, acc = self.spot, self.part, self.acc
        self.got(self.rx_got.at[g], self.x_in.at[g])
        acc[...] = part[g, s.c, s.x].astype(f32) + self.x_in[g].astype(f32)

        @pl.when(jnp.logical_and(g >= s.z, s.low))
        def _():
            self.got(self.ru_got.at[g], self.z_in.at[g])
            acc[...] += self.z_in[g].astype(f32)

        @pl.when(jnp.logical_and(g <= s.z, s.high))
        def _():
            slot = jnp.where(g == s.z, s.depth, g)
            self.got(self.rd_got.at[g], self.z_in.at[slot])
            acc[...] += self.z_in[slot].astype(f32)

        @pl.when(g > s.z)
        def _():
            part[g, s.c, s.x] = acc[...].astype(bf16)
            self.back_up(g).start()

        @pl.when(g < s.z)
        def _():
            part[g, s.c, s.x] = acc[...].astype(bf16)
            self.back_dn(g).start()

    def settle(self):
        s = self.spot

        @pl.loop(0, s.depth)
        def _(g):
            @pl.when(jnp.logical_and(g <= s.z, s.high))
            def _():
                self.hop_up(g).wait_send()

            @pl.when(jnp.logical_and(g >= s.z, s.low))
            def _():
                self.hop_dn(g).wait_send()

            self.hop_x(g).wait_send()
            self.hop_c(g, False).wait_send()
            self.hop_c(g, True).wait_send()
            self.back_c(g).wait_send()
            self.back_x(g).wait_send()

            @pl.when(g > s.z)
            def _():
                self.back_up(g).wait_send()

            @pl.when(g < s.z)
            def _():
                self.back_dn(g).wait_send()


def put_part(part, g, left, right, n, d):
    @pl.loop(0, d // 256)
    def _(t):
        at = pl.multiple_of(t * 256, 256)
        value = lax.dot_general(left[g], right[pl.ds(at, 256), :], (((1,), (1,)), ((), ())), preferred_element_type=f32)
        part[g, :, :, :, pl.ds(at, 256)] = value.astype(bf16).reshape(2, 2, n, 256)


def forward_group(g, buf, gu, mid, part, w_gu, w_dn, share):
    n, d = buf.shape[3:]
    main = share // 256 * 256
    tokens = lambda: buf[g].reshape(4 * n, d)

    def save(lo, hi, gate, upward):
        inner = math.sqrt(2.0 / math.pi) * (gate + 0.044715 * gate * gate * gate)
        mid[g, :, lo:hi] = (0.5 * gate * (1.0 + jnp.tanh(inner)) * upward).astype(bf16)

    for lo in range(0, main, 256):
        hi = lo + 256
        gate = jnp.dot(tokens(), w_gu[:, lo:hi], preferred_element_type=f32)
        upward = jnp.dot(tokens(), w_gu[:, main + lo : main + hi], preferred_element_type=f32)
        gu[g, :, lo:hi] = gate.astype(bf16)
        gu[g, :, main + lo : main + hi] = upward.astype(bf16)
        save(lo, hi, gate, upward)
    if main < share:
        rest = share - main
        both = jnp.dot(tokens(), w_gu[:, 2 * main :], preferred_element_type=f32)
        gu[g, :, 2 * main :] = both.astype(bf16)
        save(main, share, both[:, :rest], both[:, rest:])
    put_part(part, g, mid, w_dn, n, d)


def backward_group(g, buf, gu, mid, part, w_gu, w_dn, share):
    n, d = buf.shape[3:]
    main = share // 256 * 256
    tokens = lambda: buf[g].reshape(4 * n, d)

    def pull(lo, hi, gate_at, up_at):
        grad = jnp.dot(tokens(), w_dn[:, lo:hi], preferred_element_type=f32)
        gate = gu[g, :, gate_at : gate_at + hi - lo].astype(f32)
        upward = gu[g, :, up_at : up_at + hi - lo].astype(f32)
        factor = math.sqrt(2.0 / math.pi)
        square = gate * gate
        curve = jnp.tanh(factor * gate * (1.0 + 0.044715 * square))
        half = 0.5 * (1.0 + curve)
        slope = half + 0.5 * gate * (1.0 - curve * curve) * factor * (1.0 + 3.0 * 0.044715 * square)
        mid[g, :, gate_at : gate_at + hi - lo] = (grad * upward * slope).astype(bf16)
        mid[g, :, up_at : up_at + hi - lo] = (grad * gate * half).astype(bf16)

    for lo in range(0, main, 256):
        pull(lo, lo + 256, lo, main + lo)
    if main < share:
        pull(main, share, 2 * main, main + share)
    put_part(part, g, mid, w_gu, n, d)


def forward_kernel(grid, inputs, w_attn, blocks, gains, cosine, sine, mask, heads, kv_heads):
    depth, width, dp_n = grid.depth, grid.width, grid.dp
    count, d = inputs.shape
    n = count // 4
    shard, a_cols = w_attn.shape
    q_cols, k_cols = heads * HD, kv_heads * HD
    qkv_cols = q_cols + 2 * k_cols
    share = blocks.shape[2] // 3
    group = heads // kv_heads
    align = math.gcd(shard, 16)
    parts = ((0, qkv_cols), (qkv_cols, q_cols))
    scale = 1.0 / math.sqrt(HD)
    others = width - 1

    def kernel(
        x_ref, wa_ref, blk_ref, gain_ref, cos_ref, sin_ref, mask_ref,
        wa_all, wf_all, normed_out, qkv_out, att_out, branch_out, hidden_out, gains_out,
        all_out, gu_out, mid_out, ffw_out,
        buf, c_in, x_in, z_in, gain_in, ca_in, xa_in, acc, hid, full_gain, w_a, w_gu, w_dn,
        g_put, g_got, a_up, a_dn, a_got, ay_put, ay_got, f_put, f_got, fy_put, fy_got,
        la_sem, lf_sem, in_sem, o_sem, g_sem, ra_put, ra_got, *sems,
    ):
        s = Spot(grid)
        z, y, x, c = s.z, s.y, s.x, s.c

        def got(sem, ref):
            remote(ref, ref, sem, sem, s.at_x).wait_recv()

        def row(g, yy):
            return pl.multiple_of((g * width + yy) * shard, align)

        barrier = pltpu.get_barrier_semaphore()
        for k in range(1, dp_n):
            signal(barrier, ((s.dp + k) % dp_n, s.q))
        signal(barrier, s.at_x)
        signal(barrier, s.at_c)
        pl.semaphore_wait(barrier, dp_n + 1)

        def a_at(g, yy, k):
            return wa_all.at[g * width + yy, :, pl.ds(parts[k][0], parts[k][1])]

        def a_src(g, k, own):
            return wa_ref.at[:, pl.ds(parts[k][0], parts[k][1])] if own else a_at(g, y, k)

        def a_hop(g, k, own, up):
            return remote(
                a_src(g, k, own), a_at(g, y, k), (a_up if up else a_dn).at[g, k], a_got.at[g, k], s.at_up if up else s.at_dn
            )

        def a_wide(g, k, own, over):
            return remote(a_src(g, k, own), a_at(g, y, k), ay_put.at[g, k, over - 1], ay_got.at[g, k, over - 1], s.at_wide(over))

        def a_pass(g, k, own):
            @pl.when(jnp.logical_and(g <= z, s.high))
            def _():
                a_hop(g, k, own, True).start()

            @pl.when(jnp.logical_and(g >= z, s.low))
            def _():
                a_hop(g, k, own, False).start()

            for over in range(1, width):
                a_wide(g, k, own, over).start()

        def f_at(g, yy):
            return wf_all.at[g * width + yy]

        def f_hop(to):
            return remote(blk_ref.at[to], f_at(z, y), f_put.at[to], f_got.at[z], s.at_depth(to))

        def f_wide(g, own, over):
            return remote(
                blk_ref.at[z] if own else f_at(g, y), f_at(g, y), fy_put.at[g, over - 1], fy_got.at[g, over - 1], s.at_wide(over)
            )

        for k in range(1, dp_n):
            remote(gain_ref, gain_in.at[s.dp], g_put.at[k - 1], g_got.at[k - 1], ((s.dp + k) % dp_n, s.q)).start()
        for k in range(2):
            a_pass(z, k, True)
        ends = jnp.logical_or(z == 0, z == depth - 1)

        @pl.when(ends)
        def _():
            f_hop(s.order(1)).start()

        def attention(x_v, normed_v, qkv_v, att_v, part_a, cos_v, sin_v, mask_v):
            own_gain = pltpu.make_async_copy(gain_ref, gain_in.at[s.dp], in_sem.at[4])
            fills = [
                pltpu.make_async_copy(x_ref, x_v, in_sem.at[0]),
                pltpu.make_async_copy(cos_ref, cos_v, in_sem.at[1]),
                pltpu.make_async_copy(sin_ref, sin_v, in_sem.at[2]),
                pltpu.make_async_copy(mask_ref, mask_v, in_sem.at[3]),
                own_gain,
            ]
            for fill in fills:
                fill.start()

            def load(g, yy, k, own, slot):
                return pltpu.make_async_copy(
                    a_src(g, k, True) if own else a_at(g, yy, k),
                    w_a.at[pl.ds(row(g, yy), shard), pl.ds(parts[k][0], parts[k][1])],
                    la_sem.at[slot, k],
                )

            for k in range(2):
                load(z, y, k, True, 0).start()

            for k in range(1, dp_n):
                remote(
                    gain_in.at[0], gain_in.at[(s.dp + dp_n - k) % dp_n], g_put.at[k - 1], g_got.at[k - 1], s.at_x
                ).wait_recv()
            for fill in fills:
                fill.wait()
            whole = jnp.zeros((8, d), f32)
            for p in range(dp_n):
                one = gain_in[p].astype(f32)[:8]
                one = jnp.concatenate([one, jnp.zeros((8, d - one.shape[1]), f32)], axis=1)
                whole = whole + (pltpu.roll(one, p * shard, 1) if p else one)
            full_gain[...] = whole
            pltpu.make_async_copy(full_gain, gains_out, o_sem.at[0]).start()

            @pl.loop(0, count // 32)
            def _(i):
                at = pl.ds(pl.multiple_of(i * 32, 32), 32)
                value = x_v[at, :].astype(f32)
                inverse = lax.rsqrt(jnp.mean(value * value, axis=-1, keepdims=True) + EPS)
                normed_v[at, :] = (value * inverse * full_gain[0:1, :]).astype(bf16)

            pltpu.make_async_copy(normed_v, normed_out, o_sem.at[1]).start()

            for i in range(1, depth):
                g = s.order(i)
                for k in range(2):
                    got(a_got.at[g, k], a_at(g, y, k))
                    a_pass(g, k, False)
                    load(g, y, k, False, i * width).start()
                if i == 1:
                    f_hop(s.order(2)).start()
                    f_hop(s.order(3)).start()

            @pl.when(jnp.logical_not(ends))
            def _():
                f_hop(s.order(1)).start()

            for over in range(1, width):
                f_wide(z, True, over).start()
            for k in range(2):
                for i in range(depth):
                    g = s.order(i)
                    for over in range(1, width):
                        yy = (y + width - over) % width
                        got(ay_got.at[g, k, over - 1], a_at(g, yy, k))
                        load(g, yy, k, False, i * width + over).start()
                for i in range(depth):
                    g = s.order(i)
                    for over in range(width):
                        load(g, (y + width - over) % width, k, i + over == 0, i * width + over).wait()
                if k:
                    continue
                for h in range(heads + 2 * kv_heads):
                    value = jnp.dot(normed_v[...], w_a[:, h * HD : (h + 1) * HD], preferred_element_type=f32)
                    if h < heads + kv_heads:
                        half = HD // 2
                        first, second = value[:, :half], value[:, half:]
                        low = first * cos_v[...] - second * sin_v[...]
                        high = second * cos_v[...] + first * sin_v[...]
                        if h < heads:
                            low, high = low * scale, high * scale
                        qkv_v[:, h * HD : h * HD + half] = low.astype(bf16)
                        qkv_v[:, h * HD + half : (h + 1) * HD] = high.astype(bf16)
                    else:
                        qkv_v[:, h * HD : (h + 1) * HD] = value.astype(bf16)
                pltpu.make_async_copy(qkv_v, qkv_out, o_sem.at[2]).start()

                @pl.loop(0, count // ROW_LEN)
                def _(r):
                    at = pl.ds(pl.multiple_of(r * ROW_LEN, ROW_LEN), ROW_LEN)
                    allowed = mask_v[at, :] > 0.5
                    for h in range(heads):
                        kv = heads + h // group
                        scores = lax.dot_general(
                            qkv_v[at, h * HD : (h + 1) * HD],
                            qkv_v[at, kv * HD : (kv + 1) * HD],
                            (((1,), (1,)), ((), ())),
                            preferred_element_type=f32,
                        )
                        expo = jnp.where(allowed, jnp.exp(CAP * jnp.tanh(scores / CAP)), 0.0)
                        probs = (expo / jnp.sum(expo, axis=-1, keepdims=True)).astype(bf16)
                        kv = kv + kv_heads
                        value = jnp.dot(probs, qkv_v[at, kv * HD : (kv + 1) * HD], preferred_element_type=f32)
                        att_v[at, h * HD : (h + 1) * HD] = value.astype(bf16)

                pltpu.make_async_copy(att_v, att_out, o_sem.at[3]).start()

            @pl.loop(0, d // 256)
            def _(t):
                at = pl.multiple_of(t * 256, 256)
                value = lax.dot_general(
                    att_v[...], w_a[pl.ds(at, 256), qkv_cols:], (((1,), (1,)), ((), ())), preferred_element_type=f32
                )
                part_a[:, :, :, pl.ds(at, 256)] = value.astype(bf16).reshape(2, 2, n, 256)

            own_rows = pltpu.make_async_copy(
                w_a.at[pl.ds(row(z, y), shard)], wa_all.at[s.dp], o_sem.at[4]
            )
            own_rows.start()
            to_c = remote(part_a.at[1 - c], ca_in, ra_put.at[0], ra_got.at[0], s.at_c)
            to_c.start()
            to_c.wait_recv()
            part_a[c, 1 - x] = (part_a[c, 1 - x].astype(f32) + ca_in[1 - x].astype(f32)).astype(bf16)
            to_x = remote(part_a.at[c, 1 - x], xa_in, ra_put.at[1], ra_got.at[1], s.at_x)
            to_x.start()
            acc[...] = part_a[c, x].astype(f32) + ca_in[x].astype(f32)
            to_x.wait_recv()

            @pl.loop(0, n // 16)
            def _(i):
                at = pl.ds(pl.multiple_of(i * 16, 16), 16)
                branch = acc[at, :] + xa_in[at, :].astype(f32)
                acc[at, :] = branch
                inverse = lax.rsqrt(jnp.mean(branch * branch, axis=-1, keepdims=True) + EPS)
                mine = pl.ds(pl.multiple_of((c * 2 + x) * n + i * 16, 16), 16)
                hidden = x_v[mine, :].astype(f32) + branch * inverse * full_gain[1:2, :]
                hid[at, :] = hidden
                inverse = lax.rsqrt(jnp.mean(hidden * hidden, axis=-1, keepdims=True) + EPS)
                buf[z, c, x, at, :] = (hidden * inverse * full_gain[2:3, :]).astype(bf16)

            to_c.wait_send()
            to_x.wait_send()
            pltpu.make_async_copy(full_gain, gains_out, o_sem.at[0]).wait()
            pltpu.make_async_copy(normed_v, normed_out, o_sem.at[1]).wait()
            pltpu.make_async_copy(qkv_v, qkv_out, o_sem.at[2]).wait()
            pltpu.make_async_copy(att_v, att_out, o_sem.at[3]).wait()
            own_rows.wait()

        pl.run_scoped(
            attention,
            pltpu.VMEM((count, d), bf16),
            pltpu.VMEM((count, d), bf16),
            pltpu.VMEM((count, qkv_cols), bf16),
            pltpu.VMEM((count, q_cols), bf16),
            pltpu.VMEM((2, 2, n, d), bf16),
            pltpu.VMEM((count, HD // 2), f32),
            pltpu.VMEM((count, HD // 2), f32),
            pltpu.VMEM((count, ROW_LEN), f32),
        )

        def ffn(part, gu, mid, tot):
            trade = Trade(s, buf, part, tot, c_in, x_in, z_in, sems)
            trade.pass_on(z)
            saved = [
                pltpu.make_async_copy(acc, branch_out, o_sem.at[0]),
                pltpu.make_async_copy(hid, hidden_out, o_sem.at[1]),
            ]
            for save in saved:
                save.start()

            def load(g, yy, own, slot):
                at = pl.ds(row(g, yy), shard)
                source = blk_ref.at[z] if own else f_at(g, yy)
                return (
                    pltpu.make_async_copy(source.at[:, pl.ds(0, 2 * share)], w_gu.at[at], lf_sem.at[slot, 0]),
                    pltpu.make_async_copy(source.at[:, pl.ds(2 * share, share)], w_dn.at[at], lf_sem.at[slot, 1]),
                )

            for copy in load(z, y, True, 0):
                copy.start()

            def f_take(i):
                g = s.order(i)
                got(f_got.at[g], f_at(g, y))
                for over in range(1, width):
                    f_wide(g, False, over).start()
                for copy in load(g, y, False, i * width):
                    copy.start()

            def gather(i):
                trade.take_rank(s.order(i))
                pltpu.make_async_copy(buf.at[s.order(i)], all_out.at[s.order(i)], g_sem.at[i, 0]).start()

            for i in range(1, depth):
                f_take(i)
                trade.take_z(s.order(i))
                gather(i - 1)
            gather(depth - 1)

            for i in range(depth):
                g = s.order(i)
                for over in range(1, width):
                    yy = (y + width - over) % width
                    got(fy_got.at[g, over - 1], f_at(g, yy))
                    for copy in load(g, yy, False, i * width + over):
                        copy.start()
            for i in range(depth):
                g = s.order(i)
                for over in range(width):
                    for copy in load(g, (y + width - over) % width, i + over == 0, i * width + over):
                        copy.wait()
            at = pl.ds(row(z, y), shard)
            own_rows = [
                pltpu.make_async_copy(w_gu.at[at], wf_all.at[s.dp, :, pl.ds(0, 2 * share)], o_sem.at[2]),
                pltpu.make_async_copy(w_dn.at[at], wf_all.at[s.dp, :, pl.ds(2 * share, share)], o_sem.at[3]),
            ]
            for copy in own_rows:
                copy.start()

            def keep(g):
                return (
                    pltpu.make_async_copy(gu.at[g], gu_out.at[g], g_sem.at[g, 1]),
                    pltpu.make_async_copy(mid.at[g], mid_out.at[g], g_sem.at[g, 2]),
                )

            @pl.loop(0, depth)
            def _(i):
                g = s.order(depth - 1 - i)
                forward_group(g, buf, gu, mid, part, w_gu, w_dn, share)
                trade.back_c(g).start()
                for copy in keep(g):
                    copy.start()
                trade.add_c(g)

            @pl.loop(0, depth)
            def _(i):
                trade.add_xz(s.order(depth - 1 - i))

            last = pltpu.make_async_copy(tot, ffw_out, o_sem.at[4])
            last.start()
            trade.settle()
            for i in range(depth):
                g = s.order(i)
                pltpu.make_async_copy(buf.at[g], all_out.at[g], g_sem.at[i, 0]).wait()
                for copy in keep(g):
                    copy.wait()
            for copy in saved + own_rows:
                copy.wait()
            last.wait()

        pl.run_scoped(
            ffn,
            pltpu.VMEM((depth, 2, 2, n, d), bf16),
            pltpu.VMEM((depth, count, 2 * share), bf16),
            pltpu.VMEM((depth, count, share), bf16),
            pltpu.VMEM((n, d), f32),
        )

        for k in range(1, dp_n):
            remote(gain_ref, gain_in.at[s.dp], g_put.at[k - 1], g_got.at[k - 1], ((s.dp + k) % dp_n, s.q)).wait_send()
        for i in range(depth):
            g = s.order(i)
            for k in range(2):

                @pl.when(jnp.logical_and(g <= z, s.high))
                def _():
                    a_hop(g, k, i == 0, True).wait_send()

                @pl.when(jnp.logical_and(g >= z, s.low))
                def _():
                    a_hop(g, k, i == 0, False).wait_send()

                for over in range(1, width):
                    a_wide(g, k, i == 0, over).wait_send()
            for over in range(1, width):
                f_wide(g, i == 0, over).wait_send()
            if i:
                f_hop(g).wait_send()

    shape = jax.ShapeDtypeStruct
    outs = (
        shape((dp_n, shard, a_cols), bf16),
        shape((dp_n, shard, 3 * share), bf16),
        shape((count, d), bf16),
        shape((count, qkv_cols), bf16),
        shape((count, q_cols), bf16),
        shape((n, d), f32),
        shape((n, d), f32),
        shape((8, d), f32),
        shape((depth, 2, 2, n, d), bf16),
        shape((depth, count, 2 * share), bf16),
        shape((depth, count, share), bf16),
        shape((n, d), f32),
    )
    operands = (inputs, w_attn, blocks, gains, cosine, sine, mask)
    anywhere = pl.BlockSpec(memory_space=pl.ANY)
    dma = pltpu.SemaphoreType.DMA
    return pl.pallas_call(
        kernel,
        out_shape=outs,
        in_specs=[anywhere] * len(operands),
        out_specs=tuple([anywhere] * len(outs)),
        scratch_shapes=Trade.buffers(depth, n, d)
        + [
            pltpu.VMEM((dp_n,) + gains.shape, bf16),
            pltpu.VMEM((2, n, d), bf16),
            pltpu.VMEM((n, d), bf16),
            pltpu.VMEM((n, d), f32),
            pltpu.VMEM((n, d), f32),
            pltpu.VMEM((8, d), f32),
            pltpu.VMEM((d, a_cols), bf16),
            pltpu.VMEM((d, 2 * share), bf16),
            pltpu.VMEM((d, share), bf16),
            dma((dp_n - 1,)),
            dma((dp_n - 1,)),
            dma((depth, 2)),
            dma((depth, 2)),
            dma((depth, 2)),
            dma((depth, 2, others)),
            dma((depth, 2, others)),
            dma((depth,)),
            dma((depth,)),
            dma((depth, others)),
            dma((depth, others)),
            dma((dp_n, 2)),
            dma((dp_n, 2)),
            dma((5,)),
            dma((5,)),
            dma((depth, 3)),
            dma((2,)),
            dma((2,)),
        ]
        + Trade.semaphores(depth),
        compiler_params=pltpu.CompilerParams(collective_id=1, has_side_effects=True, vmem_limit_bytes=66_000_000),
        name="forward",
    )(*operands)


def backward_kernel(grid, first, weights, saves, heads, kv_heads):
    depth, width, dp_n = grid.depth, grid.width, grid.dp
    n, d = first[0].shape
    count = 4 * n
    a_cols = weights[0].shape[1]
    shard = weights[1].shape[1]
    share = weights[1].shape[2] // 3
    q_cols, k_cols = heads * HD, kv_heads * HD
    qkv_cols = q_cols + 2 * k_cols
    group = heads // kv_heads
    align = math.gcd(shard, 16)
    others = width - 1
    scale = 1.0 / math.sqrt(HD)
    half = d // 2
    strip = 3 * LANE
    lanes = shard + -shard % LANE
    f_cols = ((0, 2 * share), (2 * share, share))

    def kernel(
        ffw_ref, hid_ref, att_branch_ref, cot_ref, x_ref, gain_ref,
        wa_ref, wf_ref, gu_ref, tok_ref, mix_ref, normed_ref, qkv_ref, att_ref, cos_ref, sin_ref, mask_ref,
        out_all, gin_all, f_out, a_out, yf, ya, gains_out,
        buf, c_in, x_in, z_in, w_gu, w_dn, g_attn, acc, dbr, own_out, gain_v, gain_acc,
        gain_put, gain_got, gain_x, gain_c,
        in_sem, w_sem, s_sem, o_sem, t_put, t_got, fy_put, fy_got, fz_put, fz_got, ay_put, ay_got, az_put, az_got,
        gg_put, gg_got, gt_put, gt_got, ra_put, ra_got, *sems,
    ):
        s = Spot(grid)
        z, y, x, c = s.z, s.y, s.x, s.c
        mine = pl.multiple_of((c * 2 + x) * n, n)

        def got(sem, ref):
            remote(ref, ref, sem, sem, s.at_x).wait_recv()

        def row(g, yy):
            return pl.ds(pl.multiple_of((g * width + yy) * shard, align), shard)

        def copy(src, dst, sem):
            return pltpu.make_async_copy(src, dst, sem)

        loads = []
        for p in range(dp_n):
            at = pl.ds(p * shard, shard)
            for k, where in enumerate((w_gu, w_dn)):
                loads.append(copy(wf_ref.at[p, :, pl.ds(f_cols[k][0], f_cols[k][1])], where.at[at], w_sem.at[p, k]))

        barrier = pltpu.get_barrier_semaphore()
        for k in range(1, dp_n):
            signal(barrier, ((s.dp + k) % dp_n, s.q))
        signal(barrier, s.at_x)
        signal(barrier, s.at_c)

        def norm_back(field, gain, grad, slot):
            inverse = lax.rsqrt(jnp.mean(field * field, axis=-1, keepdims=True) + EPS)
            unit = field * inverse
            terms = grad * unit
            gain_acc[slot] += terms[:8] + terms[8:]
            scaled = grad * gain
            return inverse * (scaled - unit * jnp.mean(scaled * unit, axis=-1, keepdims=True))

        def rows16(i):
            return pl.ds(pl.multiple_of(i * 16, 16), 16)

        gain_acc[...] = jnp.zeros_like(gain_acc)

        def open_up(field_v, hid_v, cot_v):
            fills = [
                copy(gain_ref, gain_v, in_sem.at[0]),
                copy(ffw_ref, field_v, in_sem.at[1]),
                copy(hid_ref, hid_v, in_sem.at[2]),
                copy(cot_ref.at[pl.ds(mine, n)], cot_v, in_sem.at[3]),
            ]
            for fill in fills:
                fill.start()
            for load in loads:
                load.start()
            for fill in fills:
                fill.wait()

            @pl.loop(0, n // 16)
            def _(i):
                at = rows16(i)
                field, grad = field_v[at, :], cot_v[at, :].astype(f32)
                inverse = lax.rsqrt(jnp.mean(field * field, axis=-1, keepdims=True) + EPS)
                own_out[at, :] = (hid_v[at, :] + field * inverse * gain_v[3:4, :]).astype(bf16)
                buf[z, c, x, at, :] = norm_back(field, gain_v[3:4, :], grad, 3).astype(bf16)

        pl.run_scoped(open_up, pltpu.VMEM((n, d), f32), pltpu.VMEM((n, d), f32), pltpu.VMEM((n, d), bf16))
        pl.semaphore_wait(barrier, dp_n + 1)

        def f_wide(g, over, k):
            yy = (y + over) % width
            return remote(
                (w_gu, w_dn)[k].at[row(g, yy)],
                yf.at[over - 1, g, :, pl.ds(f_cols[k][0], f_cols[k][1])],
                fy_put.at[g, over - 1, k], fy_got.at[g, over - 1, k], s.at_wide(over),
            )

        def f_deep(g, slot, stage):
            return remote(stage.at[slot], f_out.at[z], fz_put.at[g], fz_got.at[z], s.at_depth(g))

        def a_wide(g, over):
            yy = (y + over) % width
            return remote(
                g_attn.at[row(g, yy)], ya.at[over - 1, g], ay_put.at[g, over - 1], ay_got.at[g, over - 1], s.at_wide(over)
            )

        def a_deep(g, slot, stage):
            return remote(
                stage.at[slot, :, pl.ds(0, a_cols)], a_out.at[z], az_put.at[g], az_got.at[z], s.at_depth(g)
            )

        def f_sum(i, stage):
            g = s.order(i)
            slot = i % 2
            if i + 2 < depth:
                f_deep(s.order(i + 2), slot, stage).wait_send()
            own = [
                copy(where.at[row(g, y)], stage.at[slot, :, pl.ds(f_cols[k][0], f_cols[k][1])], s_sem.at[k])
                for k, where in enumerate((w_gu, w_dn))
            ]
            for part_copy in own:
                part_copy.start()
            for over in range(1, width):
                for k in range(2):
                    got(fy_got.at[g, over - 1, k], yf.at[over - 1, g, :, pl.ds(f_cols[k][0], f_cols[k][1])])
                bring = copy(yf.at[over - 1, g], stage.at[2], s_sem.at[2])
                bring.start()
                bring.wait()
                if over == 1:
                    for part_copy in own:
                        part_copy.wait()
                stage[slot] = (stage[slot].astype(f32) + stage[2].astype(f32)).astype(bf16)
            if width == 1:
                for part_copy in own:
                    part_copy.wait()
            if i:
                f_deep(g, slot, stage).start()
            else:
                copy(stage.at[slot], f_out.at[z], o_sem.at[0]).start()

        def a_sum(i, stage):
            g = s.order(i)
            slot = i % 2
            narrow = pl.ds(0, a_cols)
            if i + 2 < depth:
                a_deep(s.order(i + 2), slot, stage).wait_send()
            own = copy(g_attn.at[row(g, y)], stage.at[slot, :, narrow], s_sem.at[0])
            own.start()
            for over in range(1, width):
                got(ay_got.at[g, over - 1], ya.at[over - 1, g])
                bring = copy(ya.at[over - 1, g], stage.at[2, :, narrow], s_sem.at[2])
                bring.start()
                bring.wait()
                if over == 1:
                    own.wait()
                total = stage[slot, :, :a_cols].astype(f32) + stage[2, :, :a_cols].astype(f32)
                stage[slot, :, :a_cols] = total.astype(bf16)
            if width == 1:
                own.wait()
            if i:
                a_deep(g, slot, stage).start()
            else:
                copy(stage.at[slot, :, narrow], a_out.at[z], o_sem.at[1]).start()

        def ffn(part, mid, mix, strips):
            trade = Trade(s, buf, part, acc, c_in, x_in, z_in, sems)
            trade.pass_on(z)
            first_loads = loads + [copy(gu_ref, mid, in_sem.at[0])]
            first_loads[-1].start()
            mix_load = copy(mix_ref, mix, in_sem.at[1])
            mix_load.start()

            @pl.loop(1, depth + 1)
            def _(i):
                @pl.when(i < depth)
                def _():
                    trade.take_z(s.order(i))

                g = s.order(i - 1)
                trade.take_rank(g)

                @pl.when(i == 1)
                def _():
                    for load in first_loads:
                        load.wait()

                backward_group(g, buf, mid, mid, part, w_gu, w_dn, share)
                trade.back_c(g).start()

            n_strip = half // strip

            def bring(side, k):
                at = pl.multiple_of(side * half + k * strip, strip)
                return copy(tok_ref.at[:, :, pl.ds(at, strip)], strips.at[k % 2], in_sem.at[2 + k % 2])

            def weight_grads(side):
                @pl.loop(0, n_strip)
                def _(k):
                    bring(side, k).wait()
                    rows = pl.ds(pl.multiple_of(side * half + k * strip, strip), strip)

                    def product(left, right, where, cols):
                        where[rows, cols] = lax.dot_general(
                            left, right, (((0,), (0,)), ((), ())), preferred_element_type=f32
                        ).astype(bf16)

                    @pl.loop(0, 2 * share // 256)
                    def _(t):
                        cols = pl.ds(pl.multiple_of(t * 256, 256), 256)
                        left = strips[k % 2].reshape(depth * count, strip)
                        product(left, mid[:, :, cols].reshape(depth * count, 256), w_gu, cols)

                    @pl.when(k + 2 < n_strip)
                    def _():
                        bring(side, k + 2).start()

                    for lo in range(0, share, 256):
                        hi = min(lo + 256, share)
                        left = buf[:, :, :, :, rows].reshape(depth * count, strip)
                        right = mix[:, :, lo:hi].reshape(depth * count, hi - lo)
                        product(left, right, w_dn, slice(lo, hi))

            def send_wide(indices):
                for i in indices:
                    g = s.order(i)
                    for over in range(1, width):
                        for k in range(2):
                            f_wide(g, over, k).start()

            away = 1 - z // 2
            for k in range(2):
                bring(away, k).start()
            mix_load.wait()
            for i in reversed(range(depth)):
                trade.add_c(s.order(i))
            weight_grads(away)
            send_wide((3, 2))
            for k in range(2):
                bring(1 - away, k).start()
            trade.add_xz(s.order(3))
            weight_grads(1 - away)
            send_wide((1, 0))
            trade.add_xz(s.order(2))
            trade.add_xz(s.order(1))
            trade.add_xz(z)
            trade.settle()

        pl.run_scoped(
            ffn,
            pltpu.VMEM((depth, 2, 2, n, d), bf16),
            pltpu.VMEM((depth, count, 2 * share), bf16),
            pltpu.VMEM((depth, count, share), bf16),
            pltpu.VMEM((2, depth, count, strip), bf16),
        )

        def hop_x(where, src, kind):
            return remote(src, where.at[c, x], t_put.at[kind, 0], t_got.at[kind, 0], s.at_x)

        def hop_c(where, src, kind):
            return remote(src, where.at[c, x], t_put.at[kind, 1], t_got.at[kind, 1], s.at_c)

        def hop_far(where, kind):
            return remote(where.at[c, 1 - x], where.at[c, 1 - x], t_put.at[kind, 2], t_got.at[kind, 2], s.at_c)

        def spread(where, src, kind):
            hop_x(where, src, kind).start()
            hop_c(where, src, kind).start()

        def spread_on(where, kind):
            got(t_got.at[kind, 0], where.at[c, 1 - x])
            hop_far(where, kind).start()

        def spread_end(where, kind):
            got(t_got.at[kind, 1], where.at[1 - c, x])
            got(t_got.at[kind, 2], where.at[1 - c, 1 - x])

        def attention(stage, w_a, normed_v, qkv_v, att_v, d_att, d_qkv, part_a, cos_v, sin_v, mask_v, field_v, other_v, cot_v):
            own_x = copy(x_ref.at[pl.ds(mine, n)], cot_v.at[1], in_sem.at[4])
            fills = [
                copy(hid_ref, field_v, in_sem.at[0]),
                copy(att_branch_ref, other_v, in_sem.at[1]),
                copy(cot_ref.at[pl.ds(mine, n)], cot_v.at[0], in_sem.at[2]),
            ]
            later = [
                copy(wa_ref, w_a, w_sem.at[0, 0]),
                copy(att_ref, att_v, w_sem.at[0, 1]),
                copy(qkv_ref, qkv_v, w_sem.at[1, 0]),
                copy(normed_ref, normed_v, w_sem.at[1, 1]),
                copy(cos_ref, cos_v, in_sem.at[5]),
                copy(sin_ref, sin_v, in_sem.at[6]),
                copy(mask_ref, mask_v, in_sem.at[7]),
                own_x,
            ]
            for fill in fills + later:
                fill.start()
            for fill in fills:
                fill.wait()

            @pl.loop(0, n // 16)
            def _(i):
                at = rows16(i)
                d_hidden = cot_v[0, at, :].astype(f32) + norm_back(field_v[at, :], gain_v[2:3, :], acc[at, :], 2)
                acc[at, :] = d_hidden
                dbr[c, x, at, :] = norm_back(other_v[at, :], gain_v[1:2, :], d_hidden, 1).astype(bf16)

            spread(dbr, dbr.at[c, x], 0)
            spread(out_all, own_out, 1)
            copy(own_out, out_all.at[c, x], o_sem.at[2]).start()
            for fill in later:
                fill.wait()
            spread_on(dbr, 0)
            f_sum(2, stage)
            spread_end(dbr, 0)

            for lo in range(0, q_cols, HD):
                value = jnp.dot(
                    dbr[...].reshape(count, d), w_a[:, qkv_cols + lo : qkv_cols + lo + HD], preferred_element_type=f32
                )
                d_att[:, lo : lo + HD] = value.astype(bf16)

            def turn(value, factor, at):
                low, high = value[:, : HD // 2], value[:, HD // 2 :]
                cosine, sine = cos_v[at, :], sin_v[at, :]
                return (low * cosine + high * sine) * factor, (high * cosine - low * sine) * factor

            def contract(left, right, dims):
                return lax.dot_general(left, right, ((dims[0], dims[1]), ((), ())), preferred_element_type=f32)

            @pl.loop(0, count // ROW_LEN)
            def _(r):
                at = pl.ds(pl.multiple_of(r * ROW_LEN, ROW_LEN), ROW_LEN)
                allowed = mask_v[at, :] > 0.5
                for kv in range(kv_heads):
                    k_at, v_at = q_cols + kv * HD, q_cols + k_cols + kv * HD
                    key, val = qkv_v[at, k_at : k_at + HD], qkv_v[at, v_at : v_at + HD]
                    d_key = jnp.zeros((ROW_LEN, HD), f32)
                    d_val = jnp.zeros((ROW_LEN, HD), f32)
                    for h in range(kv * group, (kv + 1) * group):
                        query = qkv_v[at, h * HD : (h + 1) * HD]
                        grad = d_att[at, h * HD : (h + 1) * HD]
                        bent = jnp.tanh(contract(query, key, ((1,), (1,))) / CAP)
                        expo = jnp.where(allowed, jnp.exp(CAP * bent), 0.0)
                        soft = expo / jnp.sum(expo, axis=-1, keepdims=True)
                        d_val = d_val + contract(soft.astype(bf16), grad, ((0,), (0,)))
                        d_probs = contract(grad, val, ((1,), (1,)))
                        d_soft = soft * (d_probs - jnp.sum(soft * d_probs, axis=-1, keepdims=True))
                        d_cap = (d_soft * (1.0 - bent * bent)).astype(bf16)
                        d_key = d_key + contract(d_cap, query, ((0,), (0,)))
                        low, high = turn(contract(d_cap, key, ((1,), (0,))), scale, at)
                        d_qkv[at, h * HD : h * HD + HD // 2] = low.astype(bf16)
                        d_qkv[at, h * HD + HD // 2 : (h + 1) * HD] = high.astype(bf16)
                    low, high = turn(d_key, 1.0, at)
                    d_qkv[at, k_at : k_at + HD // 2] = low.astype(bf16)
                    d_qkv[at, k_at + HD // 2 : k_at + HD] = high.astype(bf16)
                    d_qkv[at, v_at : v_at + HD] = d_val.astype(bf16)

            def attn_grads(side):
                at = pl.multiple_of(side * half, LANE)
                rows = pl.ds(at, half)
                for lo in range(0, qkv_cols, 256):
                    value = contract(normed_v[:, rows], d_qkv[:, lo : lo + 256], ((0,), (0,)))
                    g_attn[rows, lo : lo + 256] = value.astype(bf16)
                for lo in range(0, q_cols, 256):
                    value = contract(dbr[:, :, :, rows].reshape(count, half), att_v[:, lo : lo + 256], ((0,), (0,)))
                    g_attn[rows, qkv_cols + lo : qkv_cols + lo + 256] = value.astype(bf16)

            away = 1 - z // 2
            attn_grads(away)
            for i in (3, 2):
                for over in range(1, width):
                    a_wide(s.order(i), over).start()
            attn_grads(1 - away)
            for i in (1, 0):
                for over in range(1, width):
                    a_wide(s.order(i), over).start()

            @pl.loop(0, d // 256)
            def _(t):
                at = pl.multiple_of(t * 256, 256)
                value = lax.dot_general(
                    d_qkv[...], w_a[pl.ds(at, 256), :qkv_cols], (((1,), (1,)), ((), ())), preferred_element_type=f32
                )
                part_a[:, :, :, pl.ds(at, 256)] = value.astype(bf16).reshape(2, 2, n, 256)

            to_c = remote(part_a.at[1 - c], c_in.at[0], ra_put.at[0], ra_got.at[0], s.at_c)
            to_c.start()
            to_c.wait_recv()
            part_a[c, 1 - x] = (part_a[c, 1 - x].astype(f32) + c_in[0, 1 - x].astype(f32)).astype(bf16)
            to_x = remote(part_a.at[c, 1 - x], x_in.at[0], ra_put.at[1], ra_got.at[1], s.at_x)
            to_x.start()
            field_v[...] = part_a[c, x].astype(f32) + c_in[0, x].astype(f32)
            spread_on(out_all, 1)
            to_x.wait_recv()
            hop_x(out_all, own_out, 1).wait_send()
            hop_c(out_all, own_out, 1).wait_send()
            copy(own_out, out_all.at[c, x], o_sem.at[2]).wait()

            @pl.loop(0, n // 16)
            def _(i):
                at = rows16(i)
                grad = field_v[at, :] + x_in[0, at, :].astype(f32)
                d_source = norm_back(cot_v[1, at, :].astype(f32), gain_v[0:1, :], grad, 0)
                own_out[at, :] = (acc[at, :] + d_source).astype(bf16)

            to_c.wait_send()
            to_x.wait_send()
            spread(gin_all, own_out, 2)
            copy(own_out, gin_all.at[c, x], o_sem.at[3]).start()

        def finish(stage):
            f_sum(3, stage)
            pl.run_scoped(
                functools.partial(attention, stage),
                pltpu.VMEM((d, a_cols), bf16),
                pltpu.VMEM((count, d), bf16),
                pltpu.VMEM((count, qkv_cols), bf16),
                pltpu.VMEM((count, q_cols), bf16),
                pltpu.VMEM((count, q_cols), bf16),
                pltpu.VMEM((count, qkv_cols), bf16),
                pltpu.VMEM((2, 2, n, d), bf16),
                pltpu.VMEM((count, HD // 2), f32),
                pltpu.VMEM((count, HD // 2), f32),
                pltpu.VMEM((count, ROW_LEN), f32),
                pltpu.VMEM((n, d), f32),
                pltpu.VMEM((n, d), f32),
                pltpu.VMEM((2, n, d), bf16),
            )

            for k in range(4):
                gain_v[k : k + 1, :] = jnp.sum(gain_acc[k], axis=0, keepdims=True)
            whole = gain_v[...]
            for p in range(dp_n):
                turned = pltpu.roll(whole, (d - p * shard) % d, 1) if p else whole
                gain_put[p] = turned[:, :lanes]

            def gain_hop(k):
                to = (s.dp + k) % dp_n
                return remote(gain_put.at[to], gain_got.at[s.dp], gg_put.at[k - 1], gg_got.at[k - 1], (to, s.q))

            f_sum(1, stage)
            for k in range(1, dp_n):
                gain_hop(k).start()
            spread_on(gin_all, 2)
            f_sum(0, stage)
            for k in range(1, dp_n):
                got(gg_got.at[k - 1], gain_got.at[(s.dp + dp_n - k) % dp_n])
            total = gain_put[s.dp]
            for k in range(1, dp_n):
                total = total + gain_got[(s.dp + dp_n - k) % dp_n]
            gain_x[0] = total
            across = remote(gain_x.at[0], gain_x.at[1], gt_put.at[0], gt_got.at[0], s.at_x)
            across.start()
            across.wait_recv()
            gain_c[0] = gain_x[0] + gain_x[1]
            beside = remote(gain_c.at[0], gain_c.at[1], gt_put.at[1], gt_got.at[1], s.at_c)
            beside.start()
            beside.wait_recv()
            gain_c[2] = gain_c[0] + gain_c[1]
            copy(gain_c.at[2], gains_out, o_sem.at[4]).start()

            f_deep(s.order(1), 1, stage).wait_send()
            copy(stage.at[0], f_out.at[z], o_sem.at[0]).wait()
            for i in reversed(range(depth)):
                a_sum(i, stage)

            spread_end(out_all, 1)
            spread_end(gin_all, 2)
            for i in range(1, depth):
                g = s.order(i)
                got(fz_got.at[g], f_out.at[g])
                got(az_got.at[g], a_out.at[g])
            for i in range(depth):
                g = s.order(i)
                for over in range(1, width):
                    for k in range(2):
                        f_wide(g, over, k).wait_send()
                    a_wide(g, over).wait_send()
            a_deep(s.order(1), 1, stage).wait_send()
            for kind, where, src in ((0, dbr, dbr.at[c, x]), (1, out_all, own_out), (2, gin_all, own_out)):
                if kind != 1:
                    hop_x(where, src, kind).wait_send()
                    hop_c(where, src, kind).wait_send()
                hop_far(where, kind).wait_send()
            for k in range(1, dp_n):
                gain_hop(k).wait_send()
            across.wait_send()
            beside.wait_send()
            copy(stage.at[0, :, pl.ds(0, a_cols)], a_out.at[z], o_sem.at[1]).wait()
            copy(own_out, gin_all.at[c, x], o_sem.at[3]).wait()
            copy(gain_c.at[2], gains_out, o_sem.at[4]).wait()

        pl.run_scoped(finish, pltpu.VMEM((3, shard, 3 * share), bf16))

    shape = jax.ShapeDtypeStruct
    outs = (
        shape((2, 2, n, d), bf16),
        shape((2, 2, n, d), bf16),
        shape((depth, shard, 3 * share), bf16),
        shape((depth, shard, a_cols), bf16),
        shape((max(others, 1), depth, shard, 3 * share), bf16),
        shape((max(others, 1), depth, shard, a_cols), bf16),
        shape((8, lanes), f32),
    )
    operands = tuple(first) + tuple(weights) + tuple(saves)
    anywhere = pl.BlockSpec(memory_space=pl.ANY)
    dma = pltpu.SemaphoreType.DMA
    return pl.pallas_call(
        kernel,
        out_shape=outs,
        in_specs=[anywhere] * len(operands),
        out_specs=tuple([anywhere] * len(outs)),
        scratch_shapes=Trade.buffers(depth, n, d)
        + [
            pltpu.VMEM((d, 2 * share), bf16),
            pltpu.VMEM((d, share), bf16),
            pltpu.VMEM((d, a_cols), bf16),
            pltpu.VMEM((n, d), f32),
            pltpu.VMEM((2, 2, n, d), bf16),
            pltpu.VMEM((n, d), bf16),
            pltpu.VMEM((8, d), f32),
            pltpu.VMEM((4, 8, d), f32),
            pltpu.VMEM((dp_n, 8, lanes), f32),
            pltpu.VMEM((dp_n, 8, lanes), f32),
            pltpu.VMEM((2, 8, lanes), f32),
            pltpu.VMEM((3, 8, lanes), f32),
            dma((8,)),
            dma((dp_n, 2)),
            dma((3,)),
            dma((5,)),
            dma((3, 3)),
            dma((3, 3)),
            dma((depth, max(others, 1), 2)),
            dma((depth, max(others, 1), 2)),
            dma((depth,)),
            dma((depth,)),
            dma((depth, max(others, 1))),
            dma((depth, max(others, 1))),
            dma((depth,)),
            dma((depth,)),
            dma((dp_n - 1,)),
            dma((dp_n - 1,)),
            dma((2,)),
            dma((2,)),
            dma((2,)),
            dma((2,)),
        ]
        + Trade.semaphores(depth),
        compiler_params=pltpu.CompilerParams(collective_id=2, has_side_effects=True, vmem_limit_bytes=67_043_328),
        name="backward",
    )(*operands)


def unit_cuts(units, parts):
    tiles = units // LANE
    edges = [(tiles * k + parts - 1) // parts for k in range(parts + 1)]
    starts = [e * LANE for e in edges[:-1]]
    sizes = [(b - a) * LANE for a, b in zip(edges[:-1], edges[1:])]
    return starts, sizes, max(sizes)


def cut_units(block, cuts):
    starts, sizes, share = cuts
    return jnp.stack(
        [
            jnp.pad(block[:, a : a + n], ((0, 0), (0, share - n))) if n < share else block[:, a : a + n]
            for a, n in zip(starts, sizes)
        ]
    )


def join_units(blocks, cuts):
    starts, sizes, share = cuts
    return jnp.concatenate([blocks[k, :, :n] for k, n in enumerate(sizes)], axis=1)


def make_body(grid):
    def body(
        inputs,
        cotangent,
        segments,
        positions,
        w_query,
        w_key,
        w_value,
        w_output,
        w_gate,
        w_up,
        w_down,
        gain_attn,
        gain_post_attn,
        gain_ffw,
        gain_post_ffw,
    ):
        grid.here()
        count, width = inputs.shape
        shard = w_query.shape[0]
        group = HEADS // KV
        local_kv = w_key.shape[1] // HD
        local_heads = local_kv * group
        q_cols, k_cols = w_query.shape[1], w_key.shape[1]
        scale = 1.0 / math.sqrt(HD)
        part = count // grid.tensor
        rows = count // ROW_LEN
        cuts = unit_cuts(w_gate.shape[1], grid.depth)
        share = cuts[2]
        main = share // 256 * 256

        gains = jnp.stack([gain_attn, gain_post_attn, gain_ffw, gain_post_ffw])
        gains = jnp.pad(gains, ((0, 12), (0, -shard % LANE)))
        angles = make_angles(positions, HD)[:, 0]
        cosine, sine = jnp.cos(angles), jnp.sin(angles)
        mask = row_mask(segments, rows, ROW_LEN).astype(f32).reshape(count, ROW_LEN)
        cut_gate, cut_up = cut_units(w_gate, cuts), cut_units(w_up, cuts)
        blocks = jnp.concatenate(
            [cut_gate[:, :, :main], cut_up[:, :, :main], cut_gate[:, :, main:], cut_up[:, :, main:], cut_units(w_down.T, cuts)],
            axis=2,
        )
        w_attn = jnp.concatenate([w_query, w_key, w_value, w_output.T], axis=1)
        (full_attn, full_ffn, normed, qkv, attended, branch_attn, hidden, full_gains,
         all_normed, saved, mixed, branch_ffw) = forward_kernel(
            grid, inputs, w_attn, blocks, gains, cosine, sine,
            mask, local_heads, local_kv,
        )
        full_attn = full_attn.reshape(width, full_attn.shape[2])
        out_all, gin_all, blocks_ffn, blocks_attn, _, _, d_gains = backward_kernel(
            grid,
            (branch_ffw, hidden, branch_attn, cotangent, inputs, full_gains),
            (full_attn, full_ffn),
            (saved, all_normed.reshape(grid.depth, count, width), mixed, normed, qkv, attended, cosine, sine, mask),
            local_heads, local_kv,
        )
        rest = 2 * main + share - main
        grad_gate = jnp.concatenate([blocks_ffn[:, :, :main], blocks_ffn[:, :, 2 * main : rest]], axis=2)
        grad_up = jnp.concatenate([blocks_ffn[:, :, main : 2 * main], blocks_ffn[:, :, rest : 2 * share]], axis=2)
        grad_gate = join_units(grad_gate, cuts).astype(f32)
        grad_up = join_units(grad_up, cuts).astype(f32)
        grad_down = join_units(blocks_ffn[:, :, 2 * share :], cuts).T.astype(f32)
        grad_attn = jnp.sum(blocks_attn.astype(f32), axis=0)
        qkv_cols = q_cols + 2 * k_cols

        return (
            out_all.reshape(count, width),
            gin_all.reshape(count, width),
            grad_attn[:, :q_cols],
            grad_attn[:, q_cols : q_cols + k_cols],
            grad_attn[:, q_cols + k_cols : qkv_cols],
            grad_attn[:, qkv_cols:].T,
            grad_gate,
            grad_up,
            grad_down,
            d_gains[0, :shard],
            d_gains[1, :shard],
            d_gains[2, :shard],
            d_gains[3, :shard],
        )

    return body


def solution(mesh):
    placed = (
        P("dp", None),
        P("dp", None),
        P("dp"),
        P("dp"),
        P("dp", "tensor"),
        P("dp", "tensor"),
        P("dp", "tensor"),
        P("tensor", "dp"),
        P("dp", "tensor"),
        P("dp", "tensor"),
        P("tensor", "dp"),
        P("dp"),
        P("dp"),
        P("dp"),
        P("dp"),
    )
    return jax.shard_map(
        make_body(Grid(mesh)),
        mesh=mesh,
        in_specs=placed,
        out_specs=(
            P("dp", None),
            P("dp", None),
            P("dp", "tensor"),
            P("dp", "tensor"),
            P("dp", "tensor"),
            P("tensor", "dp"),
            P("dp", "tensor"),
            P("dp", "tensor"),
            P("tensor", "dp"),
            P("dp"),
            P("dp"),
            P("dp"),
            P("dp"),
        ),
        check_vma=False,
    )
```

```python
import functools
import math

import jax
import jax.numpy as jnp
from jax import lax
from jax.experimental import pallas as pl
from jax.experimental.pallas import tpu as pltpu
from jax.sharding import PartitionSpec as P

HEADS = 8
KV = 4
HD = 256
ROW_LEN = 128
LANE = 128


EPS = 1e-06
CAP = 50.0
THETA = 10000.0

f32 = jnp.float32
bf16 = jnp.bfloat16


def rms_scale(field, gain):
    inverse = lax.rsqrt(jnp.mean(field * field, axis=-1, keepdims=True) + EPS)
    return field * inverse * gain


def rms_back(field, gain, grad):
    inverse = lax.rsqrt(jnp.mean(field * field, axis=-1, keepdims=True) + EPS)
    unit = field * inverse
    d_gain = jnp.sum(grad * unit, axis=0)
    scaled = grad * gain
    d_field = inverse * (scaled - unit * jnp.mean(scaled * unit, axis=-1, keepdims=True))
    return d_field, d_gain


def geglu(gate, upward):
    return jax.nn.gelu(gate, approximate=True) * upward


def rotate(field, cosine, sine):
    half = field.shape[-1] // 2
    first = field[..., :half]
    second = field[..., half:]
    return jnp.concatenate(
        [first * cosine - second * sine, second * cosine + first * sine], axis=-1
    )


def make_angles(positions, head_size):
    half = head_size // 2
    freqs = THETA ** (-(jnp.arange(half).astype(f32) * 2.0) / head_size)
    return positions.astype(f32)[:, None, None] * freqs[None, None, :]


def row_mask(segments, rows, length):
    seg_rows = segments.reshape(rows, length)
    same = seg_rows[:, :, None] == seg_rows[:, None, :]
    index = jnp.arange(length)
    causal = index[:, None] >= index[None, :]
    return jnp.logical_and(same, causal[None])


def dot(left, right):
    return jnp.dot(left, right, preferred_element_type=f32)


def contract_rows(left, right):
    return lax.dot_general(left, right, (((0,), (0,)), ((), ())), preferred_element_type=f32)


def contract_cols(left, right):
    return lax.dot_general(left, right, (((1,), (1,)), ((), ())), preferred_element_type=f32)


class Grid:
    def __init__(self, mesh):
        self.dp = mesh.shape["dp"]
        self.tensor = mesh.shape["tensor"]
        self.depth = 4 if self.dp % 4 == 0 else (2 if self.dp % 2 == 0 else 1)
        self.width = self.dp // self.depth

    def here(self):
        index = lax.axis_index("dp")
        self.deep = index // self.width
        self.wide = lax.rem(index, self.width)
        self.rank = lax.axis_index("tensor")

    def shift(self, value, step):
        pairs = [
            (z * self.width + y, ((z + step) % self.depth) * self.width + y)
            for z in range(self.depth)
            for y in range(self.width)
        ]
        return lax.ppermute(value, "dp", pairs)

    def swap_wide(self, value, bit):
        pairs = [
            (z * self.width + y, z * self.width + (y ^ bit))
            for z in range(self.depth)
            for y in range(self.width)
        ]
        return lax.ppermute(value, "dp", pairs)

    def swap_rank(self, value, bit):
        return lax.ppermute(value, "tensor", [(q, q ^ bit) for q in range(self.tensor)])

    def wide_bits(self):
        return [1 << b for b in range(self.width.bit_length() - 1)]

    def rank_bits(self):
        return [1 << b for b in range(self.tensor.bit_length() - 1)]

    def reduce_width(self, full):
        rows, columns = full.shape[0] // self.dp, full.shape[1]
        held = full.reshape(self.depth, self.width, rows, columns)
        for bit in reversed(self.wide_bits()):
            held = held.reshape(self.depth, 2, bit, rows, columns)
            mine = lax.rem(self.wide // bit, 2)
            other = lax.dynamic_index_in_dim(held, 1 - mine, 1, keepdims=False)
            own = lax.dynamic_index_in_dim(held, mine, 1, keepdims=False)
            held = own + self.swap_wide(other, bit)
        return held.reshape(self.depth, rows, columns)

    def pick(self, held, step):
        to = lax.rem(self.deep + step, self.depth)
        return lax.dynamic_index_in_dim(held, to, 0, keepdims=False)

    def scatter_rows(self, full):
        held = self.reduce_width(full)
        total = self.pick(held, 0).astype(f32)
        for step in range(1, self.depth):
            total = total + self.shift(self.pick(held, step), step).astype(f32)
        return total

    def return_blocks(self, full):
        held = self.reduce_width(full)
        out = jnp.zeros_like(held)
        for step in range(self.depth):
            part = self.pick(held, step)
            part = part if step == 0 else self.shift(part, step)
            source = lax.rem(self.deep + self.depth - step, self.depth)
            out = lax.dynamic_update_slice(out, part[None], (source, 0, 0))
        return out

    def spread_rank(self, block):
        x, c = self.rank // 2, lax.rem(self.rank, 2)
        n, d = block.shape
        out = jnp.zeros((2, 2, n, d), block.dtype)
        for far_c in range(2):
            for far_x in range(2):
                part = block
                if far_x:
                    part = across
                if far_c:
                    part = self.swap_rank(part, 1)
                elif not far_x:
                    across = self.swap_rank(block, 2)
                out = lax.dynamic_update_slice(
                    out, part[None, None], (jnp.bitwise_xor(c, far_c), jnp.bitwise_xor(x, far_x), 0, 0)
                )
        return out.reshape(4 * n, d)

    def reduce_rank(self, full):
        x, c = self.rank // 2, lax.rem(self.rank, 2)
        held = full.reshape(2, 2, full.shape[0] // 4, full.shape[1])
        for at, bit in ((c, 1), (x, 2)):
            own = lax.dynamic_index_in_dim(held, at, 0, keepdims=False)
            other = lax.dynamic_index_in_dim(held, 1 - at, 0, keepdims=False)
            held = own + self.swap_rank(other, bit)
        return held


MESH = pl.DeviceIdType.MESH


class Spot:
    def __init__(self, grid):
        self.depth, self.width = grid.depth, grid.width
        self.dp = lax.axis_index("dp")
        self.q = lax.axis_index("tensor")
        self.z, self.y = self.dp // self.width, self.dp % self.width
        self.x, self.c = self.q // 2, self.q % 2
        self.at_x = (self.dp, (1 - self.x) * 2 + self.c)
        self.at_c = (self.dp, self.x * 2 + 1 - self.c)
        self.at_up = (self.dp + self.width, self.q)
        self.at_dn = (self.dp - self.width, self.q)
        self.low, self.high = self.z > 0, self.z < self.depth - 1

    def order(self, i):
        z = self.z
        near = z + 1 - 2 * (z % 2)
        middle = 2 - z // 2
        far = 3 * (1 - z // 2)
        return jnp.where(i == 0, z, jnp.where(i == 1, near, jnp.where(i == 2, middle, far)))

    def at_depth(self, z):
        return (z * self.width + self.y, self.q)

    def at_wide(self, over):
        return (self.z * self.width + (self.y + over) % self.width, self.q)


def remote(src, dst, put, got, device):
    return pltpu.make_async_remote_copy(
        src_ref=src, dst_ref=dst, send_sem=put, recv_sem=got, device_id=device, device_id_type=MESH
    )


def signal(semaphore, device):
    pl.semaphore_signal(semaphore, inc=1, device_id=device, device_id_type=MESH)


class Trade:
    def __init__(self, spot, buf, part, acc, c_in, x_in, z_in, sems):
        self.spot, self.buf, self.part, self.acc = spot, buf, part, acc
        self.c_in, self.x_in, self.z_in = c_in, x_in, z_in
        (self.z_up, self.z_dn, self.z_got, self.x_put, self.x_got, self.c_put, self.c_got,
         self.rc_put, self.rc_got, self.rx_put, self.rx_got, self.rz_put, self.ru_got, self.rd_got) = sems

    @staticmethod
    def semaphores(depth):
        dma = pltpu.SemaphoreType.DMA
        return [dma((depth,))] * 5 + [dma((depth, 2))] * 2 + [dma((depth,))] * 7

    @staticmethod
    def buffers(depth, n, d):
        return [
            pltpu.VMEM((depth, 2, 2, n, d), bf16),
            pltpu.VMEM((depth, 2, n, d), bf16),
            pltpu.VMEM((depth, n, d), bf16),
            pltpu.VMEM((depth + 1, n, d), bf16),
        ]

    def hop_up(self, g):
        s = self.spot
        return remote(self.buf.at[g, s.c, s.x], self.buf.at[g, s.c, s.x], self.z_up.at[g], self.z_got.at[g], s.at_up)

    def hop_dn(self, g):
        s = self.spot
        return remote(self.buf.at[g, s.c, s.x], self.buf.at[g, s.c, s.x], self.z_dn.at[g], self.z_got.at[g], s.at_dn)

    def hop_x(self, g):
        s = self.spot
        return remote(self.buf.at[g, s.c, s.x], self.buf.at[g, s.c, s.x], self.x_put.at[g], self.x_got.at[g], s.at_x)

    def hop_c(self, g, far):
        s = self.spot
        xx = (1 - s.x) if far else s.x
        return remote(
            self.buf.at[g, s.c, xx], self.buf.at[g, s.c, xx], self.c_put.at[g, int(far)], self.c_got.at[g, int(far)], s.at_c
        )

    def got(self, sem, ref):
        remote(ref, ref, sem, sem, self.spot.at_x).wait_recv()

    def pass_on(self, g):
        s = self.spot

        @pl.when(jnp.logical_and(g <= s.z, s.high))
        def _():
            self.hop_up(g).start()

        @pl.when(jnp.logical_and(g >= s.z, s.low))
        def _():
            self.hop_dn(g).start()

        self.hop_x(g).start()
        self.hop_c(g, False).start()

    def take_z(self, g):
        s = self.spot
        self.got(self.z_got.at[g], self.buf.at[g, s.c, s.x])
        self.pass_on(g)

    def take_rank(self, g):
        s = self.spot
        self.got(self.x_got.at[g], self.buf.at[g, s.c, 1 - s.x])
        self.hop_c(g, True).start()
        self.got(self.c_got.at[g, 0], self.buf.at[g, 1 - s.c, s.x])
        self.got(self.c_got.at[g, 1], self.buf.at[g, 1 - s.c, 1 - s.x])

    def back_c(self, g):
        s = self.spot
        return remote(self.part.at[g, 1 - s.c], self.c_in.at[g], self.rc_put.at[g], self.rc_got.at[g], s.at_c)

    def back_x(self, g):
        s = self.spot
        return remote(self.part.at[g, s.c, 1 - s.x], self.x_in.at[g], self.rx_put.at[g], self.rx_got.at[g], s.at_x)

    def back_up(self, g):
        s = self.spot
        return remote(self.part.at[g, s.c, s.x], self.z_in.at[g], self.rz_put.at[g], self.ru_got.at[g], s.at_up)

    def back_dn(self, g):
        s = self.spot
        slot = jnp.where(g == s.z - 1, s.depth, g)
        return remote(self.part.at[g, s.c, s.x], self.z_in.at[slot], self.rz_put.at[g], self.rd_got.at[g], s.at_dn)

    def add_c(self, g):
        s, part, c_in = self.spot, self.part, self.c_in
        self.got(self.rc_got.at[g], c_in.at[g])
        part[g, s.c, 1 - s.x] = (part[g, s.c, 1 - s.x].astype(f32) + c_in[g, 1 - s.x].astype(f32)).astype(bf16)
        self.back_x(g).start()
        part[g, s.c, s.x] = (part[g, s.c, s.x].astype(f32) + c_in[g, s.x].astype(f32)).astype(bf16)

    def add_xz(self, g):
        s, part, acc = self.spot, self.part, self.acc
        self.got(self.rx_got.at[g], self.x_in.at[g])
        acc[...] = part[g, s.c, s.x].astype(f32) + self.x_in[g].astype(f32)

        @pl.when(jnp.logical_and(g >= s.z, s.low))
        def _():
            self.got(self.ru_got.at[g], self.z_in.at[g])
            acc[...] += self.z_in[g].astype(f32)

        @pl.when(jnp.logical_and(g <= s.z, s.high))
        def _():
            slot = jnp.where(g == s.z, s.depth, g)
            self.got(self.rd_got.at[g], self.z_in.at[slot])
            acc[...] += self.z_in[slot].astype(f32)

        @pl.when(g > s.z)
        def _():
            part[g, s.c, s.x] = acc[...].astype(bf16)
            self.back_up(g).start()

        @pl.when(g < s.z)
        def _():
            part[g, s.c, s.x] = acc[...].astype(bf16)
            self.back_dn(g).start()

    def settle(self):
        s = self.spot

        @pl.loop(0, s.depth)
        def _(g):
            @pl.when(jnp.logical_and(g <= s.z, s.high))
            def _():
                self.hop_up(g).wait_send()

            @pl.when(jnp.logical_and(g >= s.z, s.low))
            def _():
                self.hop_dn(g).wait_send()

            self.hop_x(g).wait_send()
            self.hop_c(g, False).wait_send()
            self.hop_c(g, True).wait_send()
            self.back_c(g).wait_send()
            self.back_x(g).wait_send()

            @pl.when(g > s.z)
            def _():
                self.back_up(g).wait_send()

            @pl.when(g < s.z)
            def _():
                self.back_dn(g).wait_send()


def put_part(part, g, left, right, n, d):
    @pl.loop(0, d // 256)
    def _(t):
        at = pl.multiple_of(t * 256, 256)
        value = lax.dot_general(left[g], right[pl.ds(at, 256), :], (((1,), (1,)), ((), ())), preferred_element_type=f32)
        part[g, :, :, :, pl.ds(at, 256)] = value.astype(bf16).reshape(2, 2, n, 256)


def forward_group(g, buf, gu, mid, part, w_gu, w_dn, share):
    n, d = buf.shape[3:]
    main = share // 256 * 256
    tokens = lambda: buf[g].reshape(4 * n, d)

    def save(lo, hi, gate, upward):
        inner = math.sqrt(2.0 / math.pi) * (gate + 0.044715 * gate * gate * gate)
        mid[g, :, lo:hi] = (0.5 * gate * (1.0 + jnp.tanh(inner)) * upward).astype(bf16)

    for lo in range(0, main, 256):
        hi = lo + 256
        gate = jnp.dot(tokens(), w_gu[:, lo:hi], preferred_element_type=f32)
        upward = jnp.dot(tokens(), w_gu[:, main + lo : main + hi], preferred_element_type=f32)
        gu[g, :, lo:hi] = gate.astype(bf16)
        gu[g, :, main + lo : main + hi] = upward.astype(bf16)
        save(lo, hi, gate, upward)
    if main < share:
        rest = share - main
        both = jnp.dot(tokens(), w_gu[:, 2 * main :], preferred_element_type=f32)
        gu[g, :, 2 * main :] = both.astype(bf16)
        save(main, share, both[:, :rest], both[:, rest:])
    put_part(part, g, mid, w_dn, n, d)


def backward_group(g, buf, gu, mid, part, w_gu, w_dn, share):
    n, d = buf.shape[3:]
    main = share // 256 * 256
    tokens = lambda: buf[g].reshape(4 * n, d)

    def pull(lo, hi, gate_at, up_at):
        grad = jnp.dot(tokens(), w_dn[:, lo:hi], preferred_element_type=f32)
        gate = gu[g, :, gate_at : gate_at + hi - lo].astype(f32)
        upward = gu[g, :, up_at : up_at + hi - lo].astype(f32)
        factor = math.sqrt(2.0 / math.pi)
        square = gate * gate
        curve = jnp.tanh(factor * gate * (1.0 + 0.044715 * square))
        half = 0.5 * (1.0 + curve)
        slope = half + 0.5 * gate * (1.0 - curve * curve) * factor * (1.0 + 3.0 * 0.044715 * square)
        mid[g, :, gate_at : gate_at + hi - lo] = (grad * upward * slope).astype(bf16)
        mid[g, :, up_at : up_at + hi - lo] = (grad * gate * half).astype(bf16)

    for lo in range(0, main, 256):
        pull(lo, lo + 256, lo, main + lo)
    if main < share:
        pull(main, share, 2 * main, main + share)
    put_part(part, g, mid, w_gu, n, d)


def forward_kernel(grid, inputs, w_attn, blocks, gains, cosine, sine, mask, heads, kv_heads):
    depth, width, dp_n = grid.depth, grid.width, grid.dp
    count, d = inputs.shape
    n = count // 4
    shard, a_cols = w_attn.shape
    q_cols, k_cols = heads * HD, kv_heads * HD
    qkv_cols = q_cols + 2 * k_cols
    share = blocks.shape[2] // 3
    group = heads // kv_heads
    align = math.gcd(shard, 16)
    parts = ((0, qkv_cols), (qkv_cols, q_cols))
    scale = 1.0 / math.sqrt(HD)
    others = width - 1

    def kernel(
        x_ref, wa_ref, blk_ref, gain_ref, cos_ref, sin_ref, mask_ref,
        wa_all, wf_all, normed_out, qkv_out, att_out, branch_out, hidden_out, gains_out,
        all_out, gu_out, mid_out, ffw_out,
        buf, c_in, x_in, z_in, gain_in, ca_in, xa_in, acc, hid, full_gain, w_a, w_gu, w_dn,
        g_put, g_got, a_up, a_dn, a_got, ay_put, ay_got, f_put, f_got, fy_put, fy_got,
        la_sem, lf_sem, in_sem, o_sem, g_sem, ra_put, ra_got, *sems,
    ):
        s = Spot(grid)
        z, y, x, c = s.z, s.y, s.x, s.c

        def got(sem, ref):
            remote(ref, ref, sem, sem, s.at_x).wait_recv()

        def row(g, yy):
            return pl.multiple_of((g * width + yy) * shard, align)

        barrier = pltpu.get_barrier_semaphore()
        for k in range(1, dp_n):
            signal(barrier, ((s.dp + k) % dp_n, s.q))
        signal(barrier, s.at_x)
        signal(barrier, s.at_c)
        pl.semaphore_wait(barrier, dp_n + 1)

        def a_at(g, yy, k):
            return wa_all.at[g * width + yy, :, pl.ds(parts[k][0], parts[k][1])]

        def a_src(g, k, own):
            return wa_ref.at[:, pl.ds(parts[k][0], parts[k][1])] if own else a_at(g, y, k)

        def a_hop(g, k, own, up):
            return remote(
                a_src(g, k, own), a_at(g, y, k), (a_up if up else a_dn).at[g, k], a_got.at[g, k], s.at_up if up else s.at_dn
            )

        def a_wide(g, k, own, over):
            return remote(a_src(g, k, own), a_at(g, y, k), ay_put.at[g, k, over - 1], ay_got.at[g, k, over - 1], s.at_wide(over))

        def a_pass(g, k, own):
            @pl.when(jnp.logical_and(g <= z, s.high))
            def _():
                a_hop(g, k, own, True).start()

            @pl.when(jnp.logical_and(g >= z, s.low))
            def _():
                a_hop(g, k, own, False).start()

            for over in range(1, width):
                a_wide(g, k, own, over).start()

        def f_at(g, yy):
            return wf_all.at[g * width + yy]

        def f_hop(to):
            return remote(blk_ref.at[to], f_at(z, y), f_put.at[to], f_got.at[z], s.at_depth(to))

        def f_wide(g, own, over):
            return remote(
                blk_ref.at[z] if own else f_at(g, y), f_at(g, y), fy_put.at[g, over - 1], fy_got.at[g, over - 1], s.at_wide(over)
            )

        for k in range(1, dp_n):
            remote(gain_ref, gain_in.at[s.dp], g_put.at[k - 1], g_got.at[k - 1], ((s.dp + k) % dp_n, s.q)).start()
        for k in range(2):
            a_pass(z, k, True)
        ends = jnp.logical_or(z == 0, z == depth - 1)

        @pl.when(ends)
        def _():
            f_hop(s.order(1)).start()

        def attention(x_v, normed_v, qkv_v, att_v, part_a, cos_v, sin_v, mask_v):
            own_gain = pltpu.make_async_copy(gain_ref, gain_in.at[s.dp], in_sem.at[4])
            fills = [
                pltpu.make_async_copy(x_ref, x_v, in_sem.at[0]),
                pltpu.make_async_copy(cos_ref, cos_v, in_sem.at[1]),
                pltpu.make_async_copy(sin_ref, sin_v, in_sem.at[2]),
                pltpu.make_async_copy(mask_ref, mask_v, in_sem.at[3]),
                own_gain,
            ]
            for fill in fills:
                fill.start()

            def load(g, yy, k, own, slot):
                return pltpu.make_async_copy(
                    a_src(g, k, True) if own else a_at(g, yy, k),
                    w_a.at[pl.ds(row(g, yy), shard), pl.ds(parts[k][0], parts[k][1])],
                    la_sem.at[slot, k],
                )

            for k in range(2):
                load(z, y, k, True, 0).start()

            for k in range(1, dp_n):
                remote(
                    gain_in.at[0], gain_in.at[(s.dp + dp_n - k) % dp_n], g_put.at[k - 1], g_got.at[k - 1], s.at_x
                ).wait_recv()
            for fill in fills:
                fill.wait()
            whole = jnp.zeros((8, d), f32)
            for p in range(dp_n):
                one = gain_in[p].astype(f32)[:8]
                one = jnp.concatenate([one, jnp.zeros((8, d - one.shape[1]), f32)], axis=1)
                whole = whole + (pltpu.roll(one, p * shard, 1) if p else one)
            full_gain[...] = whole
            pltpu.make_async_copy(full_gain, gains_out, o_sem.at[0]).start()

            @pl.loop(0, count // 32)
            def _(i):
                at = pl.ds(pl.multiple_of(i * 32, 32), 32)
                value = x_v[at, :].astype(f32)
                inverse = lax.rsqrt(jnp.mean(value * value, axis=-1, keepdims=True) + EPS)
                normed_v[at, :] = (value * inverse * full_gain[0:1, :]).astype(bf16)

            pltpu.make_async_copy(normed_v, normed_out, o_sem.at[1]).start()

            for i in range(1, depth):
                g = s.order(i)
                for k in range(2):
                    got(a_got.at[g, k], a_at(g, y, k))
                    a_pass(g, k, False)
                    load(g, y, k, False, i * width).start()
                if i == 1:
                    f_hop(s.order(2)).start()
                    f_hop(s.order(3)).start()

            @pl.when(jnp.logical_not(ends))
            def _():
                f_hop(s.order(1)).start()

            for over in range(1, width):
                f_wide(z, True, over).start()
            for k in range(2):
                for i in range(depth):
                    g = s.order(i)
                    for over in range(1, width):
                        yy = (y + width - over) % width
                        got(ay_got.at[g, k, over - 1], a_at(g, yy, k))
                        load(g, yy, k, False, i * width + over).start()
                for i in range(depth):
                    g = s.order(i)
                    for over in range(width):
                        load(g, (y + width - over) % width, k, i + over == 0, i * width + over).wait()
                if k:
                    continue
                for h in range(heads + 2 * kv_heads):
                    value = jnp.dot(normed_v[...], w_a[:, h * HD : (h + 1) * HD], preferred_element_type=f32)
                    if h < heads + kv_heads:
                        half = HD // 2
                        first, second = value[:, :half], value[:, half:]
                        low = first * cos_v[...] - second * sin_v[...]
                        high = second * cos_v[...] + first * sin_v[...]
                        if h < heads:
                            low, high = low * scale, high * scale
                        qkv_v[:, h * HD : h * HD + half] = low.astype(bf16)
                        qkv_v[:, h * HD + half : (h + 1) * HD] = high.astype(bf16)
                    else:
                        qkv_v[:, h * HD : (h + 1) * HD] = value.astype(bf16)
                pltpu.make_async_copy(qkv_v, qkv_out, o_sem.at[2]).start()

                @pl.loop(0, count // ROW_LEN)
                def _(r):
                    at = pl.ds(pl.multiple_of(r * ROW_LEN, ROW_LEN), ROW_LEN)
                    allowed = mask_v[at, :] > 0.5
                    for h in range(heads):
                        kv = heads + h // group
                        scores = lax.dot_general(
                            qkv_v[at, h * HD : (h + 1) * HD],
                            qkv_v[at, kv * HD : (kv + 1) * HD],
                            (((1,), (1,)), ((), ())),
                            preferred_element_type=f32,
                        )
                        expo = jnp.where(allowed, jnp.exp(CAP * jnp.tanh(scores / CAP)), 0.0)
                        probs = (expo / jnp.sum(expo, axis=-1, keepdims=True)).astype(bf16)
                        kv = kv + kv_heads
                        value = jnp.dot(probs, qkv_v[at, kv * HD : (kv + 1) * HD], preferred_element_type=f32)
                        att_v[at, h * HD : (h + 1) * HD] = value.astype(bf16)

                pltpu.make_async_copy(att_v, att_out, o_sem.at[3]).start()

            @pl.loop(0, d // 256)
            def _(t):
                at = pl.multiple_of(t * 256, 256)
                value = lax.dot_general(
                    att_v[...], w_a[pl.ds(at, 256), qkv_cols:], (((1,), (1,)), ((), ())), preferred_element_type=f32
                )
                part_a[:, :, :, pl.ds(at, 256)] = value.astype(bf16).reshape(2, 2, n, 256)

            own_rows = pltpu.make_async_copy(
                w_a.at[pl.ds(row(z, y), shard)], wa_all.at[s.dp], o_sem.at[4]
            )
            own_rows.start()
            to_c = remote(part_a.at[1 - c], ca_in, ra_put.at[0], ra_got.at[0], s.at_c)
            to_c.start()
            to_c.wait_recv()
            part_a[c, 1 - x] = (part_a[c, 1 - x].astype(f32) + ca_in[1 - x].astype(f32)).astype(bf16)
            to_x = remote(part_a.at[c, 1 - x], xa_in, ra_put.at[1], ra_got.at[1], s.at_x)
            to_x.start()
            acc[...] = part_a[c, x].astype(f32) + ca_in[x].astype(f32)
            to_x.wait_recv()

            @pl.loop(0, n // 16)
            def _(i):
                at = pl.ds(pl.multiple_of(i * 16, 16), 16)
                branch = acc[at, :] + xa_in[at, :].astype(f32)
                acc[at, :] = branch
                inverse = lax.rsqrt(jnp.mean(branch * branch, axis=-1, keepdims=True) + EPS)
                mine = pl.ds(pl.multiple_of((c * 2 + x) * n + i * 16, 16), 16)
                hidden = x_v[mine, :].astype(f32) + branch * inverse * full_gain[1:2, :]
                hid[at, :] = hidden
                inverse = lax.rsqrt(jnp.mean(hidden * hidden, axis=-1, keepdims=True) + EPS)
                buf[z, c, x, at, :] = (hidden * inverse * full_gain[2:3, :]).astype(bf16)

            to_c.wait_send()
            to_x.wait_send()
            pltpu.make_async_copy(full_gain, gains_out, o_sem.at[0]).wait()
            pltpu.make_async_copy(normed_v, normed_out, o_sem.at[1]).wait()
            pltpu.make_async_copy(qkv_v, qkv_out, o_sem.at[2]).wait()
            pltpu.make_async_copy(att_v, att_out, o_sem.at[3]).wait()
            own_rows.wait()

        pl.run_scoped(
            attention,
            pltpu.VMEM((count, d), bf16),
            pltpu.VMEM((count, d), bf16),
            pltpu.VMEM((count, qkv_cols), bf16),
            pltpu.VMEM((count, q_cols), bf16),
            pltpu.VMEM((2, 2, n, d), bf16),
            pltpu.VMEM((count, HD // 2), f32),
            pltpu.VMEM((count, HD // 2), f32),
            pltpu.VMEM((count, ROW_LEN), f32),
        )

        def ffn(part, gu, mid, tot):
            trade = Trade(s, buf, part, tot, c_in, x_in, z_in, sems)
            trade.pass_on(z)
            saved = [
                pltpu.make_async_copy(acc, branch_out, o_sem.at[0]),
                pltpu.make_async_copy(hid, hidden_out, o_sem.at[1]),
            ]
            for save in saved:
                save.start()

            def load(g, yy, own, slot):
                at = pl.ds(row(g, yy), shard)
                source = blk_ref.at[z] if own else f_at(g, yy)
                return (
                    pltpu.make_async_copy(source.at[:, pl.ds(0, 2 * share)], w_gu.at[at], lf_sem.at[slot, 0]),
                    pltpu.make_async_copy(source.at[:, pl.ds(2 * share, share)], w_dn.at[at], lf_sem.at[slot, 1]),
                )

            for copy in load(z, y, True, 0):
                copy.start()

            def f_take(i):
                g = s.order(i)
                got(f_got.at[g], f_at(g, y))
                for over in range(1, width):
                    f_wide(g, False, over).start()
                for copy in load(g, y, False, i * width):
                    copy.start()

            def gather(i):
                trade.take_rank(s.order(i))
                pltpu.make_async_copy(buf.at[s.order(i)], all_out.at[s.order(i)], g_sem.at[i, 0]).start()

            for i in range(1, depth):
                f_take(i)
                trade.take_z(s.order(i))
                gather(i - 1)
            gather(depth - 1)

            for i in range(depth):
                g = s.order(i)
                for over in range(1, width):
                    yy = (y + width - over) % width
                    got(fy_got.at[g, over - 1], f_at(g, yy))
                    for copy in load(g, yy, False, i * width + over):
                        copy.start()
            for i in range(depth):
                g = s.order(i)
                for over in range(width):
                    for copy in load(g, (y + width - over) % width, i + over == 0, i * width + over):
                        copy.wait()
            at = pl.ds(row(z, y), shard)
            own_rows = [
                pltpu.make_async_copy(w_gu.at[at], wf_all.at[s.dp, :, pl.ds(0, 2 * share)], o_sem.at[2]),
                pltpu.make_async_copy(w_dn.at[at], wf_all.at[s.dp, :, pl.ds(2 * share, share)], o_sem.at[3]),
            ]
            for copy in own_rows:
                copy.start()

            def keep(g):
                return (
                    pltpu.make_async_copy(gu.at[g], gu_out.at[g], g_sem.at[g, 1]),
                    pltpu.make_async_copy(mid.at[g], mid_out.at[g], g_sem.at[g, 2]),
                )

            @pl.loop(0, depth)
            def _(i):
                g = s.order(depth - 1 - i)
                forward_group(g, buf, gu, mid, part, w_gu, w_dn, share)
                trade.back_c(g).start()
                for copy in keep(g):
                    copy.start()
                trade.add_c(g)

            @pl.loop(0, depth)
            def _(i):
                trade.add_xz(s.order(depth - 1 - i))

            last = pltpu.make_async_copy(tot, ffw_out, o_sem.at[4])
            last.start()
            trade.settle()
            for i in range(depth):
                g = s.order(i)
                pltpu.make_async_copy(buf.at[g], all_out.at[g], g_sem.at[i, 0]).wait()
                for copy in keep(g):
                    copy.wait()
            for copy in saved + own_rows:
                copy.wait()
            last.wait()

        pl.run_scoped(
            ffn,
            pltpu.VMEM((depth, 2, 2, n, d), bf16),
            pltpu.VMEM((depth, count, 2 * share), bf16),
            pltpu.VMEM((depth, count, share), bf16),
            pltpu.VMEM((n, d), f32),
        )

        for k in range(1, dp_n):
            remote(gain_ref, gain_in.at[s.dp], g_put.at[k - 1], g_got.at[k - 1], ((s.dp + k) % dp_n, s.q)).wait_send()
        for i in range(depth):
            g = s.order(i)
            for k in range(2):

                @pl.when(jnp.logical_and(g <= z, s.high))
                def _():
                    a_hop(g, k, i == 0, True).wait_send()

                @pl.when(jnp.logical_and(g >= z, s.low))
                def _():
                    a_hop(g, k, i == 0, False).wait_send()

                for over in range(1, width):
                    a_wide(g, k, i == 0, over).wait_send()
            for over in range(1, width):
                f_wide(g, i == 0, over).wait_send()
            if i:
                f_hop(g).wait_send()

    shape = jax.ShapeDtypeStruct
    outs = (
        shape((dp_n, shard, a_cols), bf16),
        shape((dp_n, shard, 3 * share), bf16),
        shape((count, d), bf16),
        shape((count, qkv_cols), bf16),
        shape((count, q_cols), bf16),
        shape((n, d), f32),
        shape((n, d), f32),
        shape((8, d), f32),
        shape((depth, 2, 2, n, d), bf16),
        shape((depth, count, 2 * share), bf16),
        shape((depth, count, share), bf16),
        shape((n, d), f32),
    )
    operands = (inputs, w_attn, blocks, gains, cosine, sine, mask)
    anywhere = pl.BlockSpec(memory_space=pl.ANY)
    dma = pltpu.SemaphoreType.DMA
    return pl.pallas_call(
        kernel,
        out_shape=outs,
        in_specs=[anywhere] * len(operands),
        out_specs=tuple([anywhere] * len(outs)),
        scratch_shapes=Trade.buffers(depth, n, d)
        + [
            pltpu.VMEM((dp_n,) + gains.shape, bf16),
            pltpu.VMEM((2, n, d), bf16),
            pltpu.VMEM((n, d), bf16),
            pltpu.VMEM((n, d), f32),
            pltpu.VMEM((n, d), f32),
            pltpu.VMEM((8, d), f32),
            pltpu.VMEM((d, a_cols), bf16),
            pltpu.VMEM((d, 2 * share), bf16),
            pltpu.VMEM((d, share), bf16),
            dma((dp_n - 1,)),
            dma((dp_n - 1,)),
            dma((depth, 2)),
            dma((depth, 2)),
            dma((depth, 2)),
            dma((depth, 2, others)),
            dma((depth, 2, others)),
            dma((depth,)),
            dma((depth,)),
            dma((depth, others)),
            dma((depth, others)),
            dma((dp_n, 2)),
            dma((dp_n, 2)),
            dma((5,)),
            dma((5,)),
            dma((depth, 3)),
            dma((2,)),
            dma((2,)),
        ]
        + Trade.semaphores(depth),
        compiler_params=pltpu.CompilerParams(collective_id=1, has_side_effects=True, vmem_limit_bytes=66_000_000),
        name="forward",
    )(*operands)


def backward_kernel(grid, first, weights, saves, heads, kv_heads):
    depth, width, dp_n = grid.depth, grid.width, grid.dp
    n, d = first[0].shape
    count = 4 * n
    a_cols = weights[0].shape[1]
    shard = weights[1].shape[1]
    share = weights[1].shape[2] // 3
    q_cols, k_cols = heads * HD, kv_heads * HD
    qkv_cols = q_cols + 2 * k_cols
    group = heads // kv_heads
    align = math.gcd(shard, 16)
    others = width - 1
    scale = 1.0 / math.sqrt(HD)
    half = d // 2
    strip = 3 * LANE
    lanes = shard + -shard % LANE
    f_cols = ((0, 2 * share), (2 * share, share))

    def kernel(
        ffw_ref, hid_ref, att_branch_ref, cot_ref, x_ref, gain_ref,
        wa_ref, wf_ref, gu_ref, tok_ref, mix_ref, normed_ref, qkv_ref, att_ref, cos_ref, sin_ref, mask_ref,
        out_all, gin_all, f_out, a_out, yf, ya, az, gains_out,
        buf, c_in, x_in, z_in, w_gu, w_dn, g_attn, acc, dbr, own_out, gain_v, gain_acc,
        gain_put, gain_got, gain_x, gain_c,
        in_sem, w_sem, s_sem, o_sem, t_put, t_got, fy_put, fy_got, fz_put, fz_got, ay_put, ay_got, az_put, au_got, ad_got,
        gg_put, gg_got, gt_put, gt_got, ra_put, ra_got, *sems,
    ):
        s = Spot(grid)
        z, y, x, c = s.z, s.y, s.x, s.c
        mine = pl.multiple_of((c * 2 + x) * n, n)

        def got(sem, ref):
            remote(ref, ref, sem, sem, s.at_x).wait_recv()

        def row(g, yy):
            return pl.ds(pl.multiple_of((g * width + yy) * shard, align), shard)

        def copy(src, dst, sem):
            return pltpu.make_async_copy(src, dst, sem)

        loads = []
        for p in range(dp_n):
            at = pl.ds(p * shard, shard)
            for k, where in enumerate((w_gu, w_dn)):
                loads.append(copy(wf_ref.at[p, :, pl.ds(f_cols[k][0], f_cols[k][1])], where.at[at], w_sem.at[p, k]))

        barrier = pltpu.get_barrier_semaphore()
        for k in range(1, dp_n):
            signal(barrier, ((s.dp + k) % dp_n, s.q))
        signal(barrier, s.at_x)
        signal(barrier, s.at_c)

        def norm_back(field, gain, grad, slot):
            inverse = lax.rsqrt(jnp.mean(field * field, axis=-1, keepdims=True) + EPS)
            unit = field * inverse
            terms = grad * unit
            gain_acc[slot] += terms[:8] + terms[8:]
            scaled = grad * gain
            return inverse * (scaled - unit * jnp.mean(scaled * unit, axis=-1, keepdims=True))

        def rows16(i):
            return pl.ds(pl.multiple_of(i * 16, 16), 16)

        gain_acc[...] = jnp.zeros_like(gain_acc)

        def open_up(field_v, hid_v, cot_v):
            fills = [
                copy(gain_ref, gain_v, in_sem.at[0]),
                copy(ffw_ref, field_v, in_sem.at[1]),
                copy(hid_ref, hid_v, in_sem.at[2]),
                copy(cot_ref.at[pl.ds(mine, n)], cot_v, in_sem.at[3]),
            ]
            for fill in fills:
                fill.start()
            for load in loads:
                load.start()
            for fill in fills:
                fill.wait()

            @pl.loop(0, n // 16)
            def _(i):
                at = rows16(i)
                field, grad = field_v[at, :], cot_v[at, :].astype(f32)
                inverse = lax.rsqrt(jnp.mean(field * field, axis=-1, keepdims=True) + EPS)
                own_out[at, :] = (hid_v[at, :] + field * inverse * gain_v[3:4, :]).astype(bf16)
                buf[z, c, x, at, :] = norm_back(field, gain_v[3:4, :], grad, 3).astype(bf16)

        pl.run_scoped(open_up, pltpu.VMEM((n, d), f32), pltpu.VMEM((n, d), f32), pltpu.VMEM((n, d), bf16))
        pl.semaphore_wait(barrier, dp_n + 1)

        def f_wide(g, over, k):
            yy = (y + over) % width
            return remote(
                (w_gu, w_dn)[k].at[row(g, yy)],
                yf.at[over - 1, g, :, pl.ds(f_cols[k][0], f_cols[k][1])],
                fy_put.at[g, over - 1, k], fy_got.at[g, over - 1, k], s.at_wide(over),
            )

        def f_deep(g, slot, stage):
            return remote(stage.at[slot], f_out.at[z], fz_put.at[g], fz_got.at[z], s.at_depth(g))

        def a_wide(g, over):
            yy = (y + over) % width
            return remote(
                g_attn.at[row(g, yy)], ya.at[over - 1, g], ay_put.at[g, over - 1], ay_got.at[g, over - 1], s.at_wide(over)
            )

        def a_up(g, slot, stage):
            return remote(stage.at[slot, :, pl.ds(0, a_cols)], az.at[g], az_put.at[g], au_got.at[g], s.at_up)

        def a_dn(g, slot, stage):
            to = jnp.where(g == z - 1, depth, g)
            return remote(stage.at[slot, :, pl.ds(0, a_cols)], az.at[to], az_put.at[g], ad_got.at[g], s.at_dn)

        def a_left(g, slot, stage):
            @pl.when(g > z)
            def _():
                a_up(g, slot, stage).wait_send()

            @pl.when(g < z)
            def _():
                a_dn(g, slot, stage).wait_send()

        def f_sum(i, stage):
            g = s.order(i)
            slot = i % 2
            if i + 2 < depth:
                f_deep(s.order(i + 2), slot, stage).wait_send()
            own = [
                copy(where.at[row(g, y)], stage.at[slot, :, pl.ds(f_cols[k][0], f_cols[k][1])], s_sem.at[k])
                for k, where in enumerate((w_gu, w_dn))
            ]
            for part_copy in own:
                part_copy.start()
            for over in range(1, width):
                for k in range(2):
                    got(fy_got.at[g, over - 1, k], yf.at[over - 1, g, :, pl.ds(f_cols[k][0], f_cols[k][1])])
                bring = copy(yf.at[over - 1, g], stage.at[2], s_sem.at[2])
                bring.start()
                bring.wait()
                if over == 1:
                    for part_copy in own:
                        part_copy.wait()
                stage[slot] = (stage[slot].astype(f32) + stage[2].astype(f32)).astype(bf16)
            if width == 1:
                for part_copy in own:
                    part_copy.wait()
            if i:
                f_deep(g, slot, stage).start()
            else:
                copy(stage.at[slot], f_out.at[z], o_sem.at[0]).start()

        def a_sum(i, stage):
            g = s.order(i)
            slot = i % 2
            narrow = pl.ds(0, a_cols)
            if i + 2 < depth:
                a_left(s.order(i + 2), slot, stage)
            own = copy(g_attn.at[row(g, y)], stage.at[slot, :, narrow], s_sem.at[0])
            own.start()

            def add(source):
                bring = copy(source, stage.at[2, :, narrow], s_sem.at[2])
                bring.start()
                bring.wait()
                total = stage[slot, :, :a_cols].astype(f32) + stage[2, :, :a_cols].astype(f32)
                stage[slot, :, :a_cols] = total.astype(bf16)

            for over in range(1, width):
                got(ay_got.at[g, over - 1], ya.at[over - 1, g])
                if over == 1:
                    own.wait()
                add(ya.at[over - 1, g])
            if width == 1:
                own.wait()

            @pl.when(jnp.logical_and(g >= z, s.low))
            def _():
                got(au_got.at[g], az.at[g])
                add(az.at[g])

            @pl.when(jnp.logical_and(g <= z, s.high))
            def _():
                where = jnp.where(g == z, depth, g)
                got(ad_got.at[g], az.at[where])
                add(az.at[where])

            @pl.when(g > z)
            def _():
                a_up(g, slot, stage).start()

            @pl.when(g < z)
            def _():
                a_dn(g, slot, stage).start()

            if i == 0:
                copy(stage.at[slot, :, narrow], a_out, o_sem.at[1]).start()

        def ffn(part, mid, mix, strips):
            trade = Trade(s, buf, part, acc, c_in, x_in, z_in, sems)
            trade.pass_on(z)
            first_loads = loads + [copy(gu_ref, mid, in_sem.at[0])]
            first_loads[-1].start()
            mix_load = copy(mix_ref, mix, in_sem.at[1])
            mix_load.start()

            @pl.loop(1, depth + 1)
            def _(i):
                @pl.when(i < depth)
                def _():
                    trade.take_z(s.order(i))

                g = s.order(i - 1)
                trade.take_rank(g)

                @pl.when(i == 1)
                def _():
                    for load in first_loads:
                        load.wait()

                backward_group(g, buf, mid, mid, part, w_gu, w_dn, share)
                trade.back_c(g).start()

            n_strip = half // strip

            away = 1 - z // 2

            def strip_at(j):
                side = jnp.where(j < n_strip, away, 1 - away)
                return pl.multiple_of(side * half + j % n_strip * strip, strip)

            def bring(j):
                return copy(tok_ref.at[:, :, pl.ds(strip_at(j), strip)], strips.at[j % 2], in_sem.at[2 + j % 2])

            def weight_grads(j):
                bring(j).wait()
                rows = pl.ds(strip_at(j), strip)

                def product(left, right, where, cols):
                    where[rows, cols] = lax.dot_general(
                        left, right, (((0,), (0,)), ((), ())), preferred_element_type=f32
                    ).astype(bf16)

                @pl.loop(0, 2 * share // 256)
                def _(t):
                    cols = pl.ds(pl.multiple_of(t * 256, 256), 256)
                    left = strips[j % 2].reshape(depth * count, strip)
                    product(left, mid[:, :, cols].reshape(depth * count, 256), w_gu, cols)

                @pl.when(j + 2 < 2 * n_strip)
                def _():
                    bring(j + 2).start()

                for lo in range(0, share, 256):
                    hi = min(lo + 256, share)
                    left = buf[:, :, :, :, rows].reshape(depth * count, strip)
                    right = mix[:, :, lo:hi].reshape(depth * count, hi - lo)
                    product(left, right, w_dn, slice(lo, hi))

            def send_wide(indices):
                for i in indices:
                    g = s.order(i)
                    for over in range(1, width):
                        for k in range(2):
                            f_wide(g, over, k).start()

            ends = jnp.logical_or(z == 0, z == depth - 1)
            inner = jnp.logical_not(ends)
            for j in range(2):
                bring(j).start()
            mix_load.wait()
            for i in reversed(range(depth)):
                trade.add_c(s.order(i))

            @pl.loop(0, 2 * n_strip)
            def _(j):
                weight_grads(j)

                @pl.when(jnp.logical_and(j == n_strip - 2, ends))
                def _():
                    trade.add_xz(s.order(3))

                @pl.when(j == n_strip - 1)
                def _():
                    send_wide((3, 2))

                @pl.when(jnp.logical_and(j == n_strip, ends))
                def _():
                    trade.add_xz(s.order(2))

                @pl.when(jnp.logical_and(j == n_strip + 1, inner))
                def _():
                    trade.add_xz(s.order(3))

            send_wide((1, 0))

            @pl.when(inner)
            def _():
                trade.add_xz(s.order(2))

            trade.add_xz(s.order(1))
            trade.add_xz(z)
            trade.settle()

        pl.run_scoped(
            ffn,
            pltpu.VMEM((depth, 2, 2, n, d), bf16),
            pltpu.VMEM((depth, count, 2 * share), bf16),
            pltpu.VMEM((depth, count, share), bf16),
            pltpu.VMEM((2, depth, count, strip), bf16),
        )

        def hop_x(where, src, kind):
            return remote(src, where.at[c, x], t_put.at[kind, 0], t_got.at[kind, 0], s.at_x)

        def hop_c(where, src, kind):
            return remote(src, where.at[c, x], t_put.at[kind, 1], t_got.at[kind, 1], s.at_c)

        def hop_far(where, kind):
            return remote(where.at[c, 1 - x], where.at[c, 1 - x], t_put.at[kind, 2], t_got.at[kind, 2], s.at_c)

        def spread(where, src, kind):
            hop_x(where, src, kind).start()
            hop_c(where, src, kind).start()

        def spread_on(where, kind):
            got(t_got.at[kind, 0], where.at[c, 1 - x])
            hop_far(where, kind).start()

        def spread_end(where, kind):
            got(t_got.at[kind, 1], where.at[1 - c, x])
            got(t_got.at[kind, 2], where.at[1 - c, 1 - x])

        def attention(stage, w_a, normed_v, qkv_v, att_v, d_att, d_qkv, part_a, cos_v, sin_v, mask_v, field_v, other_v, cot_v):
            own_x = copy(x_ref.at[pl.ds(mine, n)], cot_v.at[1], in_sem.at[4])
            fills = [
                copy(hid_ref, field_v, in_sem.at[0]),
                copy(att_branch_ref, other_v, in_sem.at[1]),
                copy(cot_ref.at[pl.ds(mine, n)], cot_v.at[0], in_sem.at[2]),
            ]
            later = [
                copy(wa_ref, w_a, w_sem.at[0, 0]),
                copy(att_ref, att_v, w_sem.at[0, 1]),
                copy(qkv_ref, qkv_v, w_sem.at[1, 0]),
                copy(normed_ref, normed_v, w_sem.at[1, 1]),
                copy(cos_ref, cos_v, in_sem.at[5]),
                copy(sin_ref, sin_v, in_sem.at[6]),
                copy(mask_ref, mask_v, in_sem.at[7]),
                own_x,
            ]
            for fill in fills + later:
                fill.start()
            for fill in fills:
                fill.wait()

            @pl.loop(0, n // 16)
            def _(i):
                at = rows16(i)
                d_hidden = cot_v[0, at, :].astype(f32) + norm_back(field_v[at, :], gain_v[2:3, :], acc[at, :], 2)
                acc[at, :] = d_hidden
                dbr[c, x, at, :] = norm_back(other_v[at, :], gain_v[1:2, :], d_hidden, 1).astype(bf16)

            spread(dbr, dbr.at[c, x], 0)
            spread(out_all, own_out, 1)
            copy(own_out, out_all.at[c, x], o_sem.at[2]).start()
            for fill in later:
                fill.wait()
            spread_on(dbr, 0)
            f_sum(2, stage)
            spread_end(dbr, 0)

            for lo in range(0, q_cols, HD):
                value = jnp.dot(
                    dbr[...].reshape(count, d), w_a[:, qkv_cols + lo : qkv_cols + lo + HD], preferred_element_type=f32
                )
                d_att[:, lo : lo + HD] = value.astype(bf16)

            def turn(value, factor, at):
                low, high = value[:, : HD // 2], value[:, HD // 2 :]
                cosine, sine = cos_v[at, :], sin_v[at, :]
                return (low * cosine + high * sine) * factor, (high * cosine - low * sine) * factor

            def contract(left, right, dims):
                return lax.dot_general(left, right, ((dims[0], dims[1]), ((), ())), preferred_element_type=f32)

            @pl.loop(0, count // ROW_LEN)
            def _(r):
                at = pl.ds(pl.multiple_of(r * ROW_LEN, ROW_LEN), ROW_LEN)
                allowed = mask_v[at, :] > 0.5
                for kv in range(kv_heads):
                    k_at, v_at = q_cols + kv * HD, q_cols + k_cols + kv * HD
                    key, val = qkv_v[at, k_at : k_at + HD], qkv_v[at, v_at : v_at + HD]
                    d_key = jnp.zeros((ROW_LEN, HD), f32)
                    d_val = jnp.zeros((ROW_LEN, HD), f32)
                    for h in range(kv * group, (kv + 1) * group):
                        query = qkv_v[at, h * HD : (h + 1) * HD]
                        grad = d_att[at, h * HD : (h + 1) * HD]
                        bent = jnp.tanh(contract(query, key, ((1,), (1,))) / CAP)
                        expo = jnp.where(allowed, jnp.exp(CAP * bent), 0.0)
                        soft = expo / jnp.sum(expo, axis=-1, keepdims=True)
                        d_val = d_val + contract(soft.astype(bf16), grad, ((0,), (0,)))
                        d_probs = contract(grad, val, ((1,), (1,)))
                        d_soft = soft * (d_probs - jnp.sum(soft * d_probs, axis=-1, keepdims=True))
                        d_cap = (d_soft * (1.0 - bent * bent)).astype(bf16)
                        d_key = d_key + contract(d_cap, query, ((0,), (0,)))
                        low, high = turn(contract(d_cap, key, ((1,), (0,))), scale, at)
                        d_qkv[at, h * HD : h * HD + HD // 2] = low.astype(bf16)
                        d_qkv[at, h * HD + HD // 2 : (h + 1) * HD] = high.astype(bf16)
                    low, high = turn(d_key, 1.0, at)
                    d_qkv[at, k_at : k_at + HD // 2] = low.astype(bf16)
                    d_qkv[at, k_at + HD // 2 : k_at + HD] = high.astype(bf16)
                    d_qkv[at, v_at : v_at + HD] = d_val.astype(bf16)

            def attn_grads(side):
                at = pl.multiple_of(side * half, LANE)
                rows = pl.ds(at, half)
                for lo in range(0, qkv_cols, 256):
                    value = contract(normed_v[:, rows], d_qkv[:, lo : lo + 256], ((0,), (0,)))
                    g_attn[rows, lo : lo + 256] = value.astype(bf16)
                for lo in range(0, q_cols, 256):
                    value = contract(dbr[:, :, :, rows].reshape(count, half), att_v[:, lo : lo + 256], ((0,), (0,)))
                    g_attn[rows, qkv_cols + lo : qkv_cols + lo + 256] = value.astype(bf16)

            away = 1 - z // 2
            attn_grads(away)
            for i in (3, 2):
                for over in range(1, width):
                    a_wide(s.order(i), over).start()
            attn_grads(1 - away)
            for i in (1, 0):
                for over in range(1, width):
                    a_wide(s.order(i), over).start()

            @pl.loop(0, d // 256)
            def _(t):
                at = pl.multiple_of(t * 256, 256)
                value = lax.dot_general(
                    d_qkv[...], w_a[pl.ds(at, 256), :qkv_cols], (((1,), (1,)), ((), ())), preferred_element_type=f32
                )
                part_a[:, :, :, pl.ds(at, 256)] = value.astype(bf16).reshape(2, 2, n, 256)

            to_c = remote(part_a.at[1 - c], c_in.at[0], ra_put.at[0], ra_got.at[0], s.at_c)
            to_c.start()
            to_c.wait_recv()
            part_a[c, 1 - x] = (part_a[c, 1 - x].astype(f32) + c_in[0, 1 - x].astype(f32)).astype(bf16)
            to_x = remote(part_a.at[c, 1 - x], x_in.at[0], ra_put.at[1], ra_got.at[1], s.at_x)
            to_x.start()
            field_v[...] = part_a[c, x].astype(f32) + c_in[0, x].astype(f32)
            f_sum(1, stage)
            spread_on(out_all, 1)
            to_x.wait_recv()
            hop_x(out_all, own_out, 1).wait_send()
            hop_c(out_all, own_out, 1).wait_send()
            copy(own_out, out_all.at[c, x], o_sem.at[2]).wait()

            @pl.loop(0, n // 16)
            def _(i):
                at = rows16(i)
                grad = field_v[at, :] + x_in[0, at, :].astype(f32)
                d_source = norm_back(cot_v[1, at, :].astype(f32), gain_v[0:1, :], grad, 0)
                own_out[at, :] = (acc[at, :] + d_source).astype(bf16)

            to_c.wait_send()
            to_x.wait_send()
            spread(gin_all, own_out, 2)
            copy(own_out, gin_all.at[c, x], o_sem.at[3]).start()

        def finish(stage):
            f_sum(3, stage)
            pl.run_scoped(
                functools.partial(attention, stage),
                pltpu.VMEM((d, a_cols), bf16),
                pltpu.VMEM((count, d), bf16),
                pltpu.VMEM((count, qkv_cols), bf16),
                pltpu.VMEM((count, q_cols), bf16),
                pltpu.VMEM((count, q_cols), bf16),
                pltpu.VMEM((count, qkv_cols), bf16),
                pltpu.VMEM((2, 2, n, d), bf16),
                pltpu.VMEM((count, HD // 2), f32),
                pltpu.VMEM((count, HD // 2), f32),
                pltpu.VMEM((count, ROW_LEN), f32),
                pltpu.VMEM((n, d), f32),
                pltpu.VMEM((n, d), f32),
                pltpu.VMEM((2, n, d), bf16),
            )

            for k in range(4):
                gain_v[k : k + 1, :] = jnp.sum(gain_acc[k], axis=0, keepdims=True)
            whole = gain_v[...]
            for p in range(dp_n):
                turned = pltpu.roll(whole, (d - p * shard) % d, 1) if p else whole
                gain_put[p] = turned[:, :lanes]

            def gain_hop(k):
                to = (s.dp + k) % dp_n
                return remote(gain_put.at[to], gain_got.at[s.dp], gg_put.at[k - 1], gg_got.at[k - 1], (to, s.q))

            for k in range(1, dp_n):
                gain_hop(k).start()
            spread_on(gin_all, 2)
            f_sum(0, stage)

            f_deep(s.order(1), 1, stage).wait_send()
            copy(stage.at[0], f_out.at[z], o_sem.at[0]).wait()
            for i in reversed(range(depth)):
                a_sum(i, stage)

            for k in range(1, dp_n):
                got(gg_got.at[k - 1], gain_got.at[(s.dp + dp_n - k) % dp_n])
            total = gain_put[s.dp]
            for k in range(1, dp_n):
                total = total + gain_got[(s.dp + dp_n - k) % dp_n]
            gain_x[0] = total
            across = remote(gain_x.at[0], gain_x.at[1], gt_put.at[0], gt_got.at[0], s.at_x)
            across.start()
            across.wait_recv()
            gain_c[0] = gain_x[0] + gain_x[1]
            beside = remote(gain_c.at[0], gain_c.at[1], gt_put.at[1], gt_got.at[1], s.at_c)
            beside.start()
            beside.wait_recv()
            gain_c[2] = gain_c[0] + gain_c[1]
            copy(gain_c.at[2], gains_out, o_sem.at[4]).start()

            spread_end(out_all, 1)
            spread_end(gin_all, 2)
            for i in range(1, depth):
                g = s.order(i)
                got(fz_got.at[g], f_out.at[g])
            for i in range(depth):
                g = s.order(i)
                for over in range(1, width):
                    for k in range(2):
                        f_wide(g, over, k).wait_send()
                    a_wide(g, over).wait_send()
            a_left(s.order(1), 1, stage)
            for kind, where, src in ((0, dbr, dbr.at[c, x]), (1, out_all, own_out), (2, gin_all, own_out)):
                if kind != 1:
                    hop_x(where, src, kind).wait_send()
                    hop_c(where, src, kind).wait_send()
                hop_far(where, kind).wait_send()
            for k in range(1, dp_n):
                gain_hop(k).wait_send()
            across.wait_send()
            beside.wait_send()
            copy(stage.at[0, :, pl.ds(0, a_cols)], a_out, o_sem.at[1]).wait()
            copy(own_out, gin_all.at[c, x], o_sem.at[3]).wait()
            copy(gain_c.at[2], gains_out, o_sem.at[4]).wait()

        pl.run_scoped(finish, pltpu.VMEM((3, shard, 3 * share), bf16))

    shape = jax.ShapeDtypeStruct
    outs = (
        shape((2, 2, n, d), bf16),
        shape((2, 2, n, d), bf16),
        shape((depth, shard, 3 * share), bf16),
        shape((shard, a_cols), bf16),
        shape((max(others, 1), depth, shard, 3 * share), bf16),
        shape((max(others, 1), depth, shard, a_cols), bf16),
        shape((depth + 1, shard, a_cols), bf16),
        shape((8, lanes), f32),
    )
    operands = tuple(first) + tuple(weights) + tuple(saves)
    anywhere = pl.BlockSpec(memory_space=pl.ANY)
    dma = pltpu.SemaphoreType.DMA
    return pl.pallas_call(
        kernel,
        out_shape=outs,
        in_specs=[anywhere] * len(operands),
        out_specs=tuple([anywhere] * len(outs)),
        scratch_shapes=Trade.buffers(depth, n, d)
        + [
            pltpu.VMEM((d, 2 * share), bf16),
            pltpu.VMEM((d, share), bf16),
            pltpu.VMEM((d, a_cols), bf16),
            pltpu.VMEM((n, d), f32),
            pltpu.VMEM((2, 2, n, d), bf16),
            pltpu.VMEM((n, d), bf16),
            pltpu.VMEM((8, d), f32),
            pltpu.VMEM((4, 8, d), f32),
            pltpu.VMEM((dp_n, 8, lanes), f32),
            pltpu.VMEM((dp_n, 8, lanes), f32),
            pltpu.VMEM((2, 8, lanes), f32),
            pltpu.VMEM((3, 8, lanes), f32),
            dma((8,)),
            dma((dp_n, 2)),
            dma((3,)),
            dma((5,)),
            dma((3, 3)),
            dma((3, 3)),
            dma((depth, max(others, 1), 2)),
            dma((depth, max(others, 1), 2)),
            dma((depth,)),
            dma((depth,)),
            dma((depth, max(others, 1))),
            dma((depth, max(others, 1))),
            dma((depth,)),
            dma((depth,)),
            dma((depth,)),
            dma((dp_n - 1,)),
            dma((dp_n - 1,)),
            dma((2,)),
            dma((2,)),
            dma((2,)),
            dma((2,)),
        ]
        + Trade.semaphores(depth),
        compiler_params=pltpu.CompilerParams(collective_id=2, has_side_effects=True, vmem_limit_bytes=67_043_328),
        name="backward",
    )(*operands)


def unit_cuts(units, parts):
    tiles = units // LANE
    edges = [(tiles * k + parts - 1) // parts for k in range(parts + 1)]
    starts = [e * LANE for e in edges[:-1]]
    sizes = [(b - a) * LANE for a, b in zip(edges[:-1], edges[1:])]
    return starts, sizes, max(sizes)


def cut_units(block, cuts):
    starts, sizes, share = cuts
    return jnp.stack(
        [
            jnp.pad(block[:, a : a + n], ((0, 0), (0, share - n))) if n < share else block[:, a : a + n]
            for a, n in zip(starts, sizes)
        ]
    )


def join_units(blocks, cuts):
    starts, sizes, share = cuts
    return jnp.concatenate([blocks[k, :, :n] for k, n in enumerate(sizes)], axis=1)


def make_body(grid):
    def body(
        inputs,
        cotangent,
        segments,
        positions,
        w_query,
        w_key,
        w_value,
        w_output,
        w_gate,
        w_up,
        w_down,
        gain_attn,
        gain_post_attn,
        gain_ffw,
        gain_post_ffw,
    ):
        grid.here()
        count, width = inputs.shape
        shard = w_query.shape[0]
        group = HEADS // KV
        local_kv = w_key.shape[1] // HD
        local_heads = local_kv * group
        q_cols, k_cols = w_query.shape[1], w_key.shape[1]
        scale = 1.0 / math.sqrt(HD)
        part = count // grid.tensor
        rows = count // ROW_LEN
        cuts = unit_cuts(w_gate.shape[1], grid.depth)
        share = cuts[2]
        main = share // 256 * 256

        gains = jnp.stack([gain_attn, gain_post_attn, gain_ffw, gain_post_ffw])
        gains = jnp.pad(gains, ((0, 12), (0, -shard % LANE)))
        angles = make_angles(positions, HD)[:, 0]
        cosine, sine = jnp.cos(angles), jnp.sin(angles)
        mask = row_mask(segments, rows, ROW_LEN).astype(f32).reshape(count, ROW_LEN)
        cut_gate, cut_up = cut_units(w_gate, cuts), cut_units(w_up, cuts)
        blocks = jnp.concatenate(
            [cut_gate[:, :, :main], cut_up[:, :, :main], cut_gate[:, :, main:], cut_up[:, :, main:], cut_units(w_down.T, cuts)],
            axis=2,
        )
        w_attn = jnp.concatenate([w_query, w_key, w_value, w_output.T], axis=1)
        (full_attn, full_ffn, normed, qkv, attended, branch_attn, hidden, full_gains,
         all_normed, saved, mixed, branch_ffw) = forward_kernel(
            grid, inputs, w_attn, blocks, gains, cosine, sine,
            mask, local_heads, local_kv,
        )
        full_attn = full_attn.reshape(width, full_attn.shape[2])
        out_all, gin_all, blocks_ffn, grad_attn, _, _, _, d_gains = backward_kernel(
            grid,
            (branch_ffw, hidden, branch_attn, cotangent, inputs, full_gains),
            (full_attn, full_ffn),
            (saved, all_normed.reshape(grid.depth, count, width), mixed, normed, qkv, attended, cosine, sine, mask),
            local_heads, local_kv,
        )
        rest = 2 * main + share - main
        grad_gate = jnp.concatenate([blocks_ffn[:, :, :main], blocks_ffn[:, :, 2 * main : rest]], axis=2)
        grad_up = jnp.concatenate([blocks_ffn[:, :, main : 2 * main], blocks_ffn[:, :, rest : 2 * share]], axis=2)
        grad_gate = join_units(grad_gate, cuts).astype(f32)
        grad_up = join_units(grad_up, cuts).astype(f32)
        grad_down = join_units(blocks_ffn[:, :, 2 * share :], cuts).T.astype(f32)
        grad_attn = grad_attn.astype(f32)
        qkv_cols = q_cols + 2 * k_cols

        return (
            out_all.reshape(count, width),
            gin_all.reshape(count, width),
            grad_attn[:, :q_cols],
            grad_attn[:, q_cols : q_cols + k_cols],
            grad_attn[:, q_cols + k_cols : qkv_cols],
            grad_attn[:, qkv_cols:].T,
            grad_gate,
            grad_up,
            grad_down,
            d_gains[0, :shard],
            d_gains[1, :shard],
            d_gains[2, :shard],
            d_gains[3, :shard],
        )

    return body


def solution(mesh):
    placed = (
        P("dp", None),
        P("dp", None),
        P("dp"),
        P("dp"),
        P("dp", "tensor"),
        P("dp", "tensor"),
        P("dp", "tensor"),
        P("tensor", "dp"),
        P("dp", "tensor"),
        P("dp", "tensor"),
        P("tensor", "dp"),
        P("dp"),
        P("dp"),
        P("dp"),
        P("dp"),
    )
    return jax.shard_map(
        make_body(Grid(mesh)),
        mesh=mesh,
        in_specs=placed,
        out_specs=(
            P("dp", None),
            P("dp", None),
            P("dp", "tensor"),
            P("dp", "tensor"),
            P("dp", "tensor"),
            P("tensor", "dp"),
            P("dp", "tensor"),
            P("dp", "tensor"),
            P("tensor", "dp"),
            P("dp"),
            P("dp"),
            P("dp"),
            P("dp"),
        ),
        check_vma=False,
    )
```

```python
import functools
import math

import jax
import jax.numpy as jnp
from jax import lax
from jax.experimental import pallas as pl
from jax.experimental.pallas import tpu as pltpu
from jax.sharding import PartitionSpec as P

HEADS = 8
KV = 4
HD = 256
ROW_LEN = 128
LANE = 128


EPS = 1e-06
CAP = 50.0
THETA = 10000.0

f32 = jnp.float32
bf16 = jnp.bfloat16


def rms_scale(field, gain):
    inverse = lax.rsqrt(jnp.mean(field * field, axis=-1, keepdims=True) + EPS)
    return field * inverse * gain


def rms_back(field, gain, grad):
    inverse = lax.rsqrt(jnp.mean(field * field, axis=-1, keepdims=True) + EPS)
    unit = field * inverse
    d_gain = jnp.sum(grad * unit, axis=0)
    scaled = grad * gain
    d_field = inverse * (scaled - unit * jnp.mean(scaled * unit, axis=-1, keepdims=True))
    return d_field, d_gain


def geglu(gate, upward):
    return jax.nn.gelu(gate, approximate=True) * upward


def rotate(field, cosine, sine):
    half = field.shape[-1] // 2
    first = field[..., :half]
    second = field[..., half:]
    return jnp.concatenate(
        [first * cosine - second * sine, second * cosine + first * sine], axis=-1
    )


def make_angles(positions, head_size):
    half = head_size // 2
    freqs = THETA ** (-(jnp.arange(half).astype(f32) * 2.0) / head_size)
    return positions.astype(f32)[:, None, None] * freqs[None, None, :]


def row_mask(segments, rows, length):
    seg_rows = segments.reshape(rows, length)
    same = seg_rows[:, :, None] == seg_rows[:, None, :]
    index = jnp.arange(length)
    causal = index[:, None] >= index[None, :]
    return jnp.logical_and(same, causal[None])


def dot(left, right):
    return jnp.dot(left, right, preferred_element_type=f32)


def contract_rows(left, right):
    return lax.dot_general(left, right, (((0,), (0,)), ((), ())), preferred_element_type=f32)


def contract_cols(left, right):
    return lax.dot_general(left, right, (((1,), (1,)), ((), ())), preferred_element_type=f32)


class Grid:
    def __init__(self, mesh):
        self.dp = mesh.shape["dp"]
        self.tensor = mesh.shape["tensor"]
        self.depth = 4 if self.dp % 4 == 0 else (2 if self.dp % 2 == 0 else 1)
        self.width = self.dp // self.depth

    def here(self):
        index = lax.axis_index("dp")
        self.deep = index // self.width
        self.wide = lax.rem(index, self.width)
        self.rank = lax.axis_index("tensor")

    def shift(self, value, step):
        pairs = [
            (z * self.width + y, ((z + step) % self.depth) * self.width + y)
            for z in range(self.depth)
            for y in range(self.width)
        ]
        return lax.ppermute(value, "dp", pairs)

    def swap_wide(self, value, bit):
        pairs = [
            (z * self.width + y, z * self.width + (y ^ bit))
            for z in range(self.depth)
            for y in range(self.width)
        ]
        return lax.ppermute(value, "dp", pairs)

    def swap_rank(self, value, bit):
        return lax.ppermute(value, "tensor", [(q, q ^ bit) for q in range(self.tensor)])

    def wide_bits(self):
        return [1 << b for b in range(self.width.bit_length() - 1)]

    def rank_bits(self):
        return [1 << b for b in range(self.tensor.bit_length() - 1)]

    def reduce_width(self, full):
        rows, columns = full.shape[0] // self.dp, full.shape[1]
        held = full.reshape(self.depth, self.width, rows, columns)
        for bit in reversed(self.wide_bits()):
            held = held.reshape(self.depth, 2, bit, rows, columns)
            mine = lax.rem(self.wide // bit, 2)
            other = lax.dynamic_index_in_dim(held, 1 - mine, 1, keepdims=False)
            own = lax.dynamic_index_in_dim(held, mine, 1, keepdims=False)
            held = own + self.swap_wide(other, bit)
        return held.reshape(self.depth, rows, columns)

    def pick(self, held, step):
        to = lax.rem(self.deep + step, self.depth)
        return lax.dynamic_index_in_dim(held, to, 0, keepdims=False)

    def scatter_rows(self, full):
        held = self.reduce_width(full)
        total = self.pick(held, 0).astype(f32)
        for step in range(1, self.depth):
            total = total + self.shift(self.pick(held, step), step).astype(f32)
        return total

    def return_blocks(self, full):
        held = self.reduce_width(full)
        out = jnp.zeros_like(held)
        for step in range(self.depth):
            part = self.pick(held, step)
            part = part if step == 0 else self.shift(part, step)
            source = lax.rem(self.deep + self.depth - step, self.depth)
            out = lax.dynamic_update_slice(out, part[None], (source, 0, 0))
        return out

    def spread_rank(self, block):
        x, c = self.rank // 2, lax.rem(self.rank, 2)
        n, d = block.shape
        out = jnp.zeros((2, 2, n, d), block.dtype)
        for far_c in range(2):
            for far_x in range(2):
                part = block
                if far_x:
                    part = across
                if far_c:
                    part = self.swap_rank(part, 1)
                elif not far_x:
                    across = self.swap_rank(block, 2)
                out = lax.dynamic_update_slice(
                    out, part[None, None], (jnp.bitwise_xor(c, far_c), jnp.bitwise_xor(x, far_x), 0, 0)
                )
        return out.reshape(4 * n, d)

    def reduce_rank(self, full):
        x, c = self.rank // 2, lax.rem(self.rank, 2)
        held = full.reshape(2, 2, full.shape[0] // 4, full.shape[1])
        for at, bit in ((c, 1), (x, 2)):
            own = lax.dynamic_index_in_dim(held, at, 0, keepdims=False)
            other = lax.dynamic_index_in_dim(held, 1 - at, 0, keepdims=False)
            held = own + self.swap_rank(other, bit)
        return held


MESH = pl.DeviceIdType.MESH


class Spot:
    def __init__(self, grid):
        self.depth, self.width = grid.depth, grid.width
        self.dp = lax.axis_index("dp")
        self.q = lax.axis_index("tensor")
        self.z, self.y = self.dp // self.width, self.dp % self.width
        self.x, self.c = self.q // 2, self.q % 2
        self.at_x = (self.dp, (1 - self.x) * 2 + self.c)
        self.at_c = (self.dp, self.x * 2 + 1 - self.c)
        self.at_up = (self.dp + self.width, self.q)
        self.at_dn = (self.dp - self.width, self.q)
        self.low, self.high = self.z > 0, self.z < self.depth - 1

    def order(self, i):
        z = self.z
        near = z + 1 - 2 * (z % 2)
        middle = 2 - z // 2
        far = 3 * (1 - z // 2)
        return jnp.where(i == 0, z, jnp.where(i == 1, near, jnp.where(i == 2, middle, far)))

    def at_depth(self, z):
        return (z * self.width + self.y, self.q)

    def at_wide(self, over):
        return (self.z * self.width + (self.y + over) % self.width, self.q)


def remote(src, dst, put, got, device):
    return pltpu.make_async_remote_copy(
        src_ref=src, dst_ref=dst, send_sem=put, recv_sem=got, device_id=device, device_id_type=MESH
    )


def signal(semaphore, device):
    pl.semaphore_signal(semaphore, inc=1, device_id=device, device_id_type=MESH)


class Trade:
    def __init__(self, spot, buf, part, acc, c_in, x_in, z_in, sems):
        self.spot, self.buf, self.part, self.acc = spot, buf, part, acc
        self.c_in, self.x_in, self.z_in = c_in, x_in, z_in
        (self.z_up, self.z_dn, self.z_got, self.x_put, self.x_got, self.c_put, self.c_got,
         self.rc_put, self.rc_got, self.rx_put, self.rx_got, self.rz_put, self.ru_got, self.rd_got) = sems

    @staticmethod
    def semaphores(depth):
        dma = pltpu.SemaphoreType.DMA
        return [dma((depth,))] * 5 + [dma((depth, 2))] * 2 + [dma((depth,))] * 7

    @staticmethod
    def buffers(depth, n, d):
        return [
            pltpu.VMEM((depth, 2, 2, n, d), bf16),
            pltpu.VMEM((depth, 2, n, d), bf16),
            pltpu.VMEM((depth, n, d), bf16),
            pltpu.VMEM((depth + 1, n, d), bf16),
        ]

    def hop_up(self, g):
        s = self.spot
        return remote(self.buf.at[g, s.c, s.x], self.buf.at[g, s.c, s.x], self.z_up.at[g], self.z_got.at[g], s.at_up)

    def hop_dn(self, g):
        s = self.spot
        return remote(self.buf.at[g, s.c, s.x], self.buf.at[g, s.c, s.x], self.z_dn.at[g], self.z_got.at[g], s.at_dn)

    def hop_x(self, g):
        s = self.spot
        return remote(self.buf.at[g, s.c, s.x], self.buf.at[g, s.c, s.x], self.x_put.at[g], self.x_got.at[g], s.at_x)

    def hop_c(self, g, far):
        s = self.spot
        xx = (1 - s.x) if far else s.x
        return remote(
            self.buf.at[g, s.c, xx], self.buf.at[g, s.c, xx], self.c_put.at[g, int(far)], self.c_got.at[g, int(far)], s.at_c
        )

    def got(self, sem, ref):
        remote(ref, ref, sem, sem, self.spot.at_x).wait_recv()

    def pass_on(self, g):
        s = self.spot

        @pl.when(jnp.logical_and(g <= s.z, s.high))
        def _():
            self.hop_up(g).start()

        @pl.when(jnp.logical_and(g >= s.z, s.low))
        def _():
            self.hop_dn(g).start()

        self.hop_x(g).start()
        self.hop_c(g, False).start()

    def take_z(self, g):
        s = self.spot
        self.got(self.z_got.at[g], self.buf.at[g, s.c, s.x])
        self.pass_on(g)

    def take_rank(self, g):
        s = self.spot
        self.got(self.x_got.at[g], self.buf.at[g, s.c, 1 - s.x])
        self.hop_c(g, True).start()
        self.got(self.c_got.at[g, 0], self.buf.at[g, 1 - s.c, s.x])
        self.got(self.c_got.at[g, 1], self.buf.at[g, 1 - s.c, 1 - s.x])

    def back_c(self, g):
        s = self.spot
        return remote(self.part.at[g, 1 - s.c], self.c_in.at[g], self.rc_put.at[g], self.rc_got.at[g], s.at_c)

    def back_x(self, g):
        s = self.spot
        return remote(self.part.at[g, s.c, 1 - s.x], self.x_in.at[g], self.rx_put.at[g], self.rx_got.at[g], s.at_x)

    def back_up(self, g):
        s = self.spot
        return remote(self.part.at[g, s.c, s.x], self.z_in.at[g], self.rz_put.at[g], self.ru_got.at[g], s.at_up)

    def back_dn(self, g):
        s = self.spot
        slot = jnp.where(g == s.z - 1, s.depth, g)
        return remote(self.part.at[g, s.c, s.x], self.z_in.at[slot], self.rz_put.at[g], self.rd_got.at[g], s.at_dn)

    def add_c(self, g):
        s, part, c_in = self.spot, self.part, self.c_in
        self.got(self.rc_got.at[g], c_in.at[g])
        part[g, s.c, 1 - s.x] = (part[g, s.c, 1 - s.x].astype(f32) + c_in[g, 1 - s.x].astype(f32)).astype(bf16)
        self.back_x(g).start()
        part[g, s.c, s.x] = (part[g, s.c, s.x].astype(f32) + c_in[g, s.x].astype(f32)).astype(bf16)

    def add_xz(self, g):
        s, part, acc = self.spot, self.part, self.acc
        self.got(self.rx_got.at[g], self.x_in.at[g])
        acc[...] = part[g, s.c, s.x].astype(f32) + self.x_in[g].astype(f32)

        @pl.when(jnp.logical_and(g >= s.z, s.low))
        def _():
            self.got(self.ru_got.at[g], self.z_in.at[g])
            acc[...] += self.z_in[g].astype(f32)

        @pl.when(jnp.logical_and(g <= s.z, s.high))
        def _():
            slot = jnp.where(g == s.z, s.depth, g)
            self.got(self.rd_got.at[g], self.z_in.at[slot])
            acc[...] += self.z_in[slot].astype(f32)

        @pl.when(g > s.z)
        def _():
            part[g, s.c, s.x] = acc[...].astype(bf16)
            self.back_up(g).start()

        @pl.when(g < s.z)
        def _():
            part[g, s.c, s.x] = acc[...].astype(bf16)
            self.back_dn(g).start()

    def settle(self):
        s = self.spot

        @pl.loop(0, s.depth)
        def _(g):
            @pl.when(jnp.logical_and(g <= s.z, s.high))
            def _():
                self.hop_up(g).wait_send()

            @pl.when(jnp.logical_and(g >= s.z, s.low))
            def _():
                self.hop_dn(g).wait_send()

            self.hop_x(g).wait_send()
            self.hop_c(g, False).wait_send()
            self.hop_c(g, True).wait_send()
            self.back_c(g).wait_send()
            self.back_x(g).wait_send()

            @pl.when(g > s.z)
            def _():
                self.back_up(g).wait_send()

            @pl.when(g < s.z)
            def _():
                self.back_dn(g).wait_send()


def put_part(part, g, left, right, n, d):
    @pl.loop(0, d // 256)
    def _(t):
        at = pl.multiple_of(t * 256, 256)
        value = lax.dot_general(left[g], right[pl.ds(at, 256), :], (((1,), (1,)), ((), ())), preferred_element_type=f32)
        part[g, :, :, :, pl.ds(at, 256)] = value.astype(bf16).reshape(2, 2, n, 256)


def forward_group(g, buf, gu, mid, w_gu, share):
    n, d = buf.shape[3:]
    main = share // 256 * 256
    tokens = lambda: buf[g].reshape(4 * n, d)

    def save(lo, hi, gate, upward):
        inner = math.sqrt(2.0 / math.pi) * (gate + 0.044715 * gate * gate * gate)
        mid[g, :, lo:hi] = (0.5 * gate * (1.0 + jnp.tanh(inner)) * upward).astype(bf16)

    for lo in range(0, main, 256):
        hi = lo + 256
        gate = jnp.dot(tokens(), w_gu[:, lo:hi], preferred_element_type=f32)
        upward = jnp.dot(tokens(), w_gu[:, main + lo : main + hi], preferred_element_type=f32)
        gu[g, :, lo:hi] = gate.astype(bf16)
        gu[g, :, main + lo : main + hi] = upward.astype(bf16)
        save(lo, hi, gate, upward)
    if main < share:
        rest = share - main
        both = jnp.dot(tokens(), w_gu[:, 2 * main :], preferred_element_type=f32)
        gu[g, :, 2 * main :] = both.astype(bf16)
        save(main, share, both[:, :rest], both[:, rest:])


def backward_group(g, buf, gu, mid, part, w_gu, w_dn, share):
    n, d = buf.shape[3:]
    main = share // 256 * 256
    tokens = lambda: buf[g].reshape(4 * n, d)

    def pull(lo, hi, gate_at, up_at):
        grad = jnp.dot(tokens(), w_dn[:, lo:hi], preferred_element_type=f32)
        gate = gu[g, :, gate_at : gate_at + hi - lo].astype(f32)
        upward = gu[g, :, up_at : up_at + hi - lo].astype(f32)
        factor = math.sqrt(2.0 / math.pi)
        square = gate * gate
        curve = jnp.tanh(factor * gate * (1.0 + 0.044715 * square))
        half = 0.5 * (1.0 + curve)
        slope = half + 0.5 * gate * (1.0 - curve * curve) * factor * (1.0 + 3.0 * 0.044715 * square)
        mid[g, :, gate_at : gate_at + hi - lo] = (grad * upward * slope).astype(bf16)
        mid[g, :, up_at : up_at + hi - lo] = (grad * gate * half).astype(bf16)

    for lo in range(0, main, 256):
        pull(lo, lo + 256, lo, main + lo)
    if main < share:
        pull(main, share, 2 * main, main + share)
    put_part(part, g, mid, w_gu, n, d)


def forward_kernel(grid, inputs, w_attn, wide_blocks, slim_blocks, gains, cosine, sine, mask, heads, kv_heads):
    depth, width, dp_n = grid.depth, grid.width, grid.dp
    count, d = inputs.shape
    n = count // 4
    shard, a_cols = w_attn.shape
    q_cols, k_cols = heads * HD, kv_heads * HD
    qkv_cols = q_cols + 2 * k_cols
    share = slim_blocks.shape[2]
    group = heads // kv_heads
    align = math.gcd(shard, 16)
    parts = ((0, qkv_cols), (qkv_cols, q_cols))
    scale = 1.0 / math.sqrt(HD)
    others = width - 1

    def kernel(
        x_ref, wa_ref, blk_wide, blk_slim, gain_ref, cos_ref, sin_ref, mask_ref,
        wa_all, wide_all, slim_all, normed_out, qkv_out, att_out, branch_out, hidden_out, gains_out,
        all_out, gu_out, mid_out, ffw_out,
        buf, c_in, x_in, z_in, gain_in, ca_in, xa_in, acc, hid, full_gain, w_a, w_gu, w_dn,
        g_put, g_got, a_up, a_dn, a_got, ay_put, ay_got, f_put, f_got, fy_put, fy_got,
        la_sem, lf_sem, in_sem, o_sem, g_sem, ra_put, ra_got, *sems,
    ):
        s = Spot(grid)
        z, y, x, c = s.z, s.y, s.x, s.c

        def got(sem, ref):
            remote(ref, ref, sem, sem, s.at_x).wait_recv()

        def row(g, yy):
            return pl.multiple_of((g * width + yy) * shard, align)

        barrier = pltpu.get_barrier_semaphore()
        for k in range(1, dp_n):
            signal(barrier, ((s.dp + k) % dp_n, s.q))
        signal(barrier, s.at_x)
        signal(barrier, s.at_c)
        pl.semaphore_wait(barrier, dp_n + 1)

        def a_at(g, yy, k):
            return wa_all.at[g * width + yy, :, pl.ds(parts[k][0], parts[k][1])]

        def a_src(g, k, own):
            return wa_ref.at[:, pl.ds(parts[k][0], parts[k][1])] if own else a_at(g, y, k)

        def a_hop(g, k, own, up):
            return remote(
                a_src(g, k, own), a_at(g, y, k), (a_up if up else a_dn).at[g, k], a_got.at[g, k], s.at_up if up else s.at_dn
            )

        def a_wide(g, k, own, over):
            return remote(a_src(g, k, own), a_at(g, y, k), ay_put.at[g, k, over - 1], ay_got.at[g, k, over - 1], s.at_wide(over))

        def a_pass(g, k, own):
            @pl.when(jnp.logical_and(g <= z, s.high))
            def _():
                a_hop(g, k, own, True).start()

            @pl.when(jnp.logical_and(g >= z, s.low))
            def _():
                a_hop(g, k, own, False).start()

            for over in range(1, width):
                a_wide(g, k, own, over).start()

        def f_at(g, yy, k):
            return (wide_all, slim_all)[k].at[g * width + yy]

        def f_own(g, k):
            return (blk_wide, blk_slim)[k].at[g]

        def f_hop(to, k):
            return remote(f_own(to, k), f_at(z, y, k), f_put.at[to, k], f_got.at[z, k], s.at_depth(to))

        def f_wide(g, own, over, k):
            source = f_own(z, k) if own else f_at(g, y, k)
            return remote(source, f_at(g, y, k), fy_put.at[g, over - 1, k], fy_got.at[g, over - 1, k], s.at_wide(over))

        ends = jnp.logical_or(z == 0, z == depth - 1)
        inner = jnp.logical_not(ends)

        def f_hops(i, k):
            @pl.when(ends)
            def _():
                for j in {1: (1,), 3: (2, 3)}.get(i, ()):
                    f_hop(s.order(j), k).start()

            @pl.when(inner)
            def _():
                for j in {3: (2, 3, 1)}.get(i, ()):
                    f_hop(s.order(j), k).start()

        for k in range(1, dp_n):
            remote(gain_ref, gain_in.at[s.dp], g_put.at[k - 1], g_got.at[k - 1], ((s.dp + k) % dp_n, s.q)).start()
        for k in range(2):
            a_pass(z, k, True)

        def attention(x_v, normed_v, qkv_v, att_v, part_a, cos_v, sin_v, mask_v):
            own_gain = pltpu.make_async_copy(gain_ref, gain_in.at[s.dp], in_sem.at[4])
            fills = [
                pltpu.make_async_copy(x_ref, x_v, in_sem.at[0]),
                pltpu.make_async_copy(cos_ref, cos_v, in_sem.at[1]),
                pltpu.make_async_copy(sin_ref, sin_v, in_sem.at[2]),
                pltpu.make_async_copy(mask_ref, mask_v, in_sem.at[3]),
                own_gain,
            ]
            for fill in fills:
                fill.start()

            def load(g, yy, k, own, slot):
                return pltpu.make_async_copy(
                    a_src(g, k, True) if own else a_at(g, yy, k),
                    w_a.at[pl.ds(row(g, yy), shard), pl.ds(parts[k][0], parts[k][1])],
                    la_sem.at[slot, k],
                )

            for k in range(2):
                load(z, y, k, True, 0).start()

            for k in range(1, dp_n):
                remote(
                    gain_in.at[0], gain_in.at[(s.dp + dp_n - k) % dp_n], g_put.at[k - 1], g_got.at[k - 1], s.at_x
                ).wait_recv()
            for fill in fills:
                fill.wait()
            whole = jnp.zeros((8, d), f32)
            for p in range(dp_n):
                one = gain_in[p].astype(f32)[:8]
                one = jnp.concatenate([one, jnp.zeros((8, d - one.shape[1]), f32)], axis=1)
                whole = whole + (pltpu.roll(one, p * shard, 1) if p else one)
            full_gain[...] = whole
            pltpu.make_async_copy(full_gain, gains_out, o_sem.at[0]).start()

            @pl.loop(0, count // 32)
            def _(i):
                at = pl.ds(pl.multiple_of(i * 32, 32), 32)
                value = x_v[at, :].astype(f32)
                inverse = lax.rsqrt(jnp.mean(value * value, axis=-1, keepdims=True) + EPS)
                normed_v[at, :] = (value * inverse * full_gain[0:1, :]).astype(bf16)

            pltpu.make_async_copy(normed_v, normed_out, o_sem.at[1]).start()

            for i in range(1, depth):
                g = s.order(i)
                for k in range(2):
                    got(a_got.at[g, k], a_at(g, y, k))
                    a_pass(g, k, False)
                    load(g, y, k, False, i * width).start()
                f_hops(i, 0)
            for over in range(1, width):
                f_wide(z, True, over, 0).start()
            for k in range(2):
                for i in range(depth):
                    g = s.order(i)
                    for over in range(1, width):
                        yy = (y + width - over) % width
                        got(ay_got.at[g, k, over - 1], a_at(g, yy, k))
                        load(g, yy, k, False, i * width + over).start()
                for i in range(depth):
                    g = s.order(i)
                    for over in range(width):
                        load(g, (y + width - over) % width, k, i + over == 0, i * width + over).wait()
                if k:
                    continue
                for h in range(heads + 2 * kv_heads):
                    value = jnp.dot(normed_v[...], w_a[:, h * HD : (h + 1) * HD], preferred_element_type=f32)
                    if h < heads + kv_heads:
                        half = HD // 2
                        first, second = value[:, :half], value[:, half:]
                        low = first * cos_v[...] - second * sin_v[...]
                        high = second * cos_v[...] + first * sin_v[...]
                        if h < heads:
                            low, high = low * scale, high * scale
                        qkv_v[:, h * HD : h * HD + half] = low.astype(bf16)
                        qkv_v[:, h * HD + half : (h + 1) * HD] = high.astype(bf16)
                    else:
                        qkv_v[:, h * HD : (h + 1) * HD] = value.astype(bf16)
                pltpu.make_async_copy(qkv_v, qkv_out, o_sem.at[2]).start()

                @pl.loop(0, count // ROW_LEN)
                def _(r):
                    at = pl.ds(pl.multiple_of(r * ROW_LEN, ROW_LEN), ROW_LEN)
                    allowed = mask_v[at, :] > 0.5
                    for h in range(heads):
                        kv = heads + h // group
                        scores = lax.dot_general(
                            qkv_v[at, h * HD : (h + 1) * HD],
                            qkv_v[at, kv * HD : (kv + 1) * HD],
                            (((1,), (1,)), ((), ())),
                            preferred_element_type=f32,
                        )
                        expo = jnp.where(allowed, jnp.exp(CAP * jnp.tanh(scores / CAP)), 0.0)
                        probs = (expo / jnp.sum(expo, axis=-1, keepdims=True)).astype(bf16)
                        kv = kv + kv_heads
                        value = jnp.dot(probs, qkv_v[at, kv * HD : (kv + 1) * HD], preferred_element_type=f32)
                        att_v[at, h * HD : (h + 1) * HD] = value.astype(bf16)

                pltpu.make_async_copy(att_v, att_out, o_sem.at[3]).start()

            @pl.loop(0, d // 256)
            def _(t):
                at = pl.multiple_of(t * 256, 256)
                value = lax.dot_general(
                    att_v[...], w_a[pl.ds(at, 256), qkv_cols:], (((1,), (1,)), ((), ())), preferred_element_type=f32
                )
                part_a[:, :, :, pl.ds(at, 256)] = value.astype(bf16).reshape(2, 2, n, 256)

            own_rows = pltpu.make_async_copy(
                w_a.at[pl.ds(row(z, y), shard)], wa_all.at[s.dp], o_sem.at[4]
            )
            own_rows.start()
            to_c = remote(part_a.at[1 - c], ca_in, ra_put.at[0], ra_got.at[0], s.at_c)
            to_c.start()
            to_c.wait_recv()
            part_a[c, 1 - x] = (part_a[c, 1 - x].astype(f32) + ca_in[1 - x].astype(f32)).astype(bf16)
            to_x = remote(part_a.at[c, 1 - x], xa_in, ra_put.at[1], ra_got.at[1], s.at_x)
            to_x.start()
            acc[...] = part_a[c, x].astype(f32) + ca_in[x].astype(f32)
            to_x.wait_recv()

            @pl.loop(0, n // 16)
            def _(i):
                at = pl.ds(pl.multiple_of(i * 16, 16), 16)
                branch = acc[at, :] + xa_in[at, :].astype(f32)
                acc[at, :] = branch
                inverse = lax.rsqrt(jnp.mean(branch * branch, axis=-1, keepdims=True) + EPS)
                mine = pl.ds(pl.multiple_of((c * 2 + x) * n + i * 16, 16), 16)
                hidden = x_v[mine, :].astype(f32) + branch * inverse * full_gain[1:2, :]
                hid[at, :] = hidden
                inverse = lax.rsqrt(jnp.mean(hidden * hidden, axis=-1, keepdims=True) + EPS)
                buf[z, c, x, at, :] = (hidden * inverse * full_gain[2:3, :]).astype(bf16)

            to_c.wait_send()
            to_x.wait_send()
            pltpu.make_async_copy(full_gain, gains_out, o_sem.at[0]).wait()
            pltpu.make_async_copy(normed_v, normed_out, o_sem.at[1]).wait()
            pltpu.make_async_copy(qkv_v, qkv_out, o_sem.at[2]).wait()
            pltpu.make_async_copy(att_v, att_out, o_sem.at[3]).wait()
            own_rows.wait()

        pl.run_scoped(
            attention,
            pltpu.VMEM((count, d), bf16),
            pltpu.VMEM((count, d), bf16),
            pltpu.VMEM((count, qkv_cols), bf16),
            pltpu.VMEM((count, q_cols), bf16),
            pltpu.VMEM((2, 2, n, d), bf16),
            pltpu.VMEM((count, HD // 2), f32),
            pltpu.VMEM((count, HD // 2), f32),
            pltpu.VMEM((count, ROW_LEN), f32),
        )

        def ffn(part, gu, mid, tot):
            trade = Trade(s, buf, part, tot, c_in, x_in, z_in, sems)
            trade.pass_on(z)
            saved = [
                pltpu.make_async_copy(acc, branch_out, o_sem.at[0]),
                pltpu.make_async_copy(hid, hidden_out, o_sem.at[1]),
            ]
            for save in saved:
                save.start()

            def load(g, yy, own, slot, k):
                source = f_own(z, k) if own else f_at(g, yy, k)
                return pltpu.make_async_copy(source, (w_gu, w_dn)[k].at[pl.ds(row(g, yy), shard)], lf_sem.at[slot, k])

            for k in range(2):
                load(z, y, True, 0, k).start()

            def f_take(i, k):
                g = s.order(i)
                got(f_got.at[g, k], f_at(g, y, k))
                for over in range(1, width):
                    f_wide(g, False, over, k).start()
                load(g, y, False, i * width, k).start()

            def f_rest(k):
                for i in range(depth):
                    g = s.order(i)
                    for over in range(1, width):
                        yy = (y + width - over) % width
                        got(fy_got.at[g, over - 1, k], f_at(g, yy, k))
                        load(g, yy, False, i * width + over, k).start()
                for i in range(depth):
                    for over in range(width):
                        load(s.order(i), (y + width - over) % width, i + over == 0, i * width + over, k).wait()

            def gather(i):
                trade.take_rank(s.order(i))
                pltpu.make_async_copy(buf.at[s.order(i)], all_out.at[s.order(i)], g_sem.at[i, 0]).start()

            for i in range(1, depth):
                f_take(i, 0)
            for over in range(1, width):
                f_wide(z, True, over, 1).start()
            for i in range(1, depth):
                trade.take_z(s.order(i))
                f_hops(i, 1)
                gather(i - 1)
            gather(depth - 1)
            f_rest(0)

            def keep(g):
                return (
                    pltpu.make_async_copy(gu.at[g], gu_out.at[g], g_sem.at[g, 1]),
                    pltpu.make_async_copy(mid.at[g], mid_out.at[g], g_sem.at[g, 2]),
                )

            @pl.loop(0, depth)
            def _(i):
                @pl.when(i > 0)
                def _():
                    f_take(i, 1)

                g = s.order(depth - 1 - i)
                forward_group(g, buf, gu, mid, w_gu, share)
                for copy in keep(g):
                    copy.start()

            f_rest(1)
            at = pl.ds(row(z, y), shard)
            own_rows = [
                pltpu.make_async_copy((w_gu, w_dn)[k].at[at], f_at(z, y, k), o_sem.at[2 + k]) for k in range(2)
            ]
            for copy in own_rows:
                copy.start()

            @pl.loop(0, depth)
            def _(i):
                g = s.order(depth - 1 - i)
                put_part(part, g, mid, w_dn, n, d)
                trade.back_c(g).start()
                trade.add_c(g)

                @pl.when(jnp.logical_and(i == 1, ends))
                def _():
                    trade.add_xz(s.order(depth - 1))

            @pl.when(inner)
            def _():
                trade.add_xz(s.order(depth - 1))

            for i in reversed(range(depth - 1)):
                trade.add_xz(s.order(i))

            last = pltpu.make_async_copy(tot, ffw_out, o_sem.at[4])
            last.start()
            trade.settle()
            for i in range(depth):
                g = s.order(i)
                pltpu.make_async_copy(buf.at[g], all_out.at[g], g_sem.at[i, 0]).wait()
                for copy in keep(g):
                    copy.wait()
            for copy in saved + own_rows:
                copy.wait()
            last.wait()

        pl.run_scoped(
            ffn,
            pltpu.VMEM((depth, 2, 2, n, d), bf16),
            pltpu.VMEM((depth, count, 2 * share), bf16),
            pltpu.VMEM((depth, count, share), bf16),
            pltpu.VMEM((n, d), f32),
        )

        for k in range(1, dp_n):
            remote(gain_ref, gain_in.at[s.dp], g_put.at[k - 1], g_got.at[k - 1], ((s.dp + k) % dp_n, s.q)).wait_send()
        for i in range(depth):
            g = s.order(i)
            for k in range(2):

                @pl.when(jnp.logical_and(g <= z, s.high))
                def _():
                    a_hop(g, k, i == 0, True).wait_send()

                @pl.when(jnp.logical_and(g >= z, s.low))
                def _():
                    a_hop(g, k, i == 0, False).wait_send()

                for over in range(1, width):
                    a_wide(g, k, i == 0, over).wait_send()
            for k in range(2):
                for over in range(1, width):
                    f_wide(g, i == 0, over, k).wait_send()
                if i:
                    f_hop(g, k).wait_send()

    shape = jax.ShapeDtypeStruct
    outs = (
        shape((dp_n, shard, a_cols), bf16),
        shape((dp_n, shard, 2 * share), bf16),
        shape((dp_n, shard, share), bf16),
        shape((count, d), bf16),
        shape((count, qkv_cols), bf16),
        shape((count, q_cols), bf16),
        shape((n, d), f32),
        shape((n, d), f32),
        shape((8, d), f32),
        shape((depth, 2, 2, n, d), bf16),
        shape((depth, count, 2 * share), bf16),
        shape((depth, count, share), bf16),
        shape((n, d), f32),
    )
    operands = (inputs, w_attn, wide_blocks, slim_blocks, gains, cosine, sine, mask)
    anywhere = pl.BlockSpec(memory_space=pl.ANY)
    dma = pltpu.SemaphoreType.DMA
    return pl.pallas_call(
        kernel,
        out_shape=outs,
        in_specs=[anywhere] * len(operands),
        out_specs=tuple([anywhere] * len(outs)),
        scratch_shapes=Trade.buffers(depth, n, d)
        + [
            pltpu.VMEM((dp_n,) + gains.shape, bf16),
            pltpu.VMEM((2, n, d), bf16),
            pltpu.VMEM((n, d), bf16),
            pltpu.VMEM((n, d), f32),
            pltpu.VMEM((n, d), f32),
            pltpu.VMEM((8, d), f32),
            pltpu.VMEM((d, a_cols), bf16),
            pltpu.VMEM((d, 2 * share), bf16),
            pltpu.VMEM((d, share), bf16),
            dma((dp_n - 1,)),
            dma((dp_n - 1,)),
            dma((depth, 2)),
            dma((depth, 2)),
            dma((depth, 2)),
            dma((depth, 2, others)),
            dma((depth, 2, others)),
            dma((depth, 2)),
            dma((depth, 2)),
            dma((depth, others, 2)),
            dma((depth, others, 2)),
            dma((dp_n, 2)),
            dma((dp_n, 2)),
            dma((5,)),
            dma((5,)),
            dma((depth, 3)),
            dma((2,)),
            dma((2,)),
        ]
        + Trade.semaphores(depth),
        compiler_params=pltpu.CompilerParams(collective_id=1, has_side_effects=True, vmem_limit_bytes=66_000_000),
        name="forward",
    )(*operands)


def backward_kernel(grid, first, weights, saves, heads, kv_heads):
    depth, width, dp_n = grid.depth, grid.width, grid.dp
    n, d = first[0].shape
    count = 4 * n
    a_cols = weights[0].shape[1]
    shard = weights[1].shape[1]
    share = weights[2].shape[2]
    q_cols, k_cols = heads * HD, kv_heads * HD
    qkv_cols = q_cols + 2 * k_cols
    group = heads // kv_heads
    align = math.gcd(shard, 16)
    others = width - 1
    scale = 1.0 / math.sqrt(HD)
    half = d // 2
    strip = 3 * LANE
    lanes = shard + -shard % LANE
    f_cols = ((0, 2 * share), (2 * share, share))

    def kernel(
        ffw_ref, hid_ref, att_branch_ref, cot_ref, x_ref, gain_ref,
        wa_ref, wide_ref, slim_ref, gu_ref, tok_ref, mix_ref, normed_ref, qkv_ref, att_ref, cos_ref, sin_ref, mask_ref,
        out_all, gin_all, f_out, a_out, yf, ya, az, gains_out,
        buf, c_in, x_in, z_in, w_gu, w_dn, g_attn, acc, dbr, own_out, gain_v, gain_acc,
        gain_put, gain_got, gain_x, gain_c,
        in_sem, w_sem, s_sem, o_sem, t_put, t_got, fy_put, fy_got, fz_put, fz_got, ay_put, ay_got, az_put, au_got, ad_got,
        gg_put, gg_got, gt_put, gt_got, ra_put, ra_got, *sems,
    ):
        s = Spot(grid)
        z, y, x, c = s.z, s.y, s.x, s.c
        mine = pl.multiple_of((c * 2 + x) * n, n)

        def got(sem, ref):
            remote(ref, ref, sem, sem, s.at_x).wait_recv()

        def row(g, yy):
            return pl.ds(pl.multiple_of((g * width + yy) * shard, align), shard)

        def copy(src, dst, sem):
            return pltpu.make_async_copy(src, dst, sem)

        loads = []
        for p in range(dp_n):
            at = pl.ds(p * shard, shard)
            for k, (source, where) in enumerate(((wide_ref, w_gu), (slim_ref, w_dn))):
                loads.append(copy(source.at[p], where.at[at], w_sem.at[p, k]))

        barrier = pltpu.get_barrier_semaphore()
        for k in range(1, dp_n):
            signal(barrier, ((s.dp + k) % dp_n, s.q))
        signal(barrier, s.at_x)
        signal(barrier, s.at_c)

        def norm_back(field, gain, grad, slot):
            inverse = lax.rsqrt(jnp.mean(field * field, axis=-1, keepdims=True) + EPS)
            unit = field * inverse
            terms = grad * unit
            gain_acc[slot] += terms[:8] + terms[8:]
            scaled = grad * gain
            return inverse * (scaled - unit * jnp.mean(scaled * unit, axis=-1, keepdims=True))

        def rows16(i):
            return pl.ds(pl.multiple_of(i * 16, 16), 16)

        gain_acc[...] = jnp.zeros_like(gain_acc)

        def open_up(field_v, hid_v, cot_v):
            fills = [
                copy(gain_ref, gain_v, in_sem.at[0]),
                copy(ffw_ref, field_v, in_sem.at[1]),
                copy(hid_ref, hid_v, in_sem.at[2]),
                copy(cot_ref.at[pl.ds(mine, n)], cot_v, in_sem.at[3]),
            ]
            for fill in fills:
                fill.start()
            for load in loads:
                load.start()
            for fill in fills:
                fill.wait()

            @pl.loop(0, n // 16)
            def _(i):
                at = rows16(i)
                field, grad = field_v[at, :], cot_v[at, :].astype(f32)
                inverse = lax.rsqrt(jnp.mean(field * field, axis=-1, keepdims=True) + EPS)
                own_out[at, :] = (hid_v[at, :] + field * inverse * gain_v[3:4, :]).astype(bf16)
                buf[z, c, x, at, :] = norm_back(field, gain_v[3:4, :], grad, 3).astype(bf16)

        pl.run_scoped(open_up, pltpu.VMEM((n, d), f32), pltpu.VMEM((n, d), f32), pltpu.VMEM((n, d), bf16))
        pl.semaphore_wait(barrier, dp_n + 1)

        def f_wide(g, over, k):
            yy = (y + over) % width
            return remote(
                (w_gu, w_dn)[k].at[row(g, yy)],
                yf.at[over - 1, g, :, pl.ds(f_cols[k][0], f_cols[k][1])],
                fy_put.at[g, over - 1, k], fy_got.at[g, over - 1, k], s.at_wide(over),
            )

        def f_deep(g, slot, stage):
            return remote(stage.at[slot], f_out.at[z], fz_put.at[g], fz_got.at[z], s.at_depth(g))

        def a_wide(g, over):
            yy = (y + over) % width
            return remote(
                g_attn.at[row(g, yy)], ya.at[over - 1, g], ay_put.at[g, over - 1], ay_got.at[g, over - 1], s.at_wide(over)
            )

        def a_up(g, slot, stage):
            return remote(stage.at[slot, :, pl.ds(0, a_cols)], az.at[g], az_put.at[g], au_got.at[g], s.at_up)

        def a_dn(g, slot, stage):
            to = jnp.where(g == z - 1, depth, g)
            return remote(stage.at[slot, :, pl.ds(0, a_cols)], az.at[to], az_put.at[g], ad_got.at[g], s.at_dn)

        def a_left(g, slot, stage):
            @pl.when(g > z)
            def _():
                a_up(g, slot, stage).wait_send()

            @pl.when(g < z)
            def _():
                a_dn(g, slot, stage).wait_send()

        def f_sum(i, stage):
            g = s.order(i)
            slot = i % 2
            if i + 2 < depth:
                f_deep(s.order(i + 2), slot, stage).wait_send()
            own = [
                copy(where.at[row(g, y)], stage.at[slot, :, pl.ds(f_cols[k][0], f_cols[k][1])], s_sem.at[k])
                for k, where in enumerate((w_gu, w_dn))
            ]
            for part_copy in own:
                part_copy.start()
            for over in range(1, width):
                for k in range(2):
                    got(fy_got.at[g, over - 1, k], yf.at[over - 1, g, :, pl.ds(f_cols[k][0], f_cols[k][1])])
                bring = copy(yf.at[over - 1, g], stage.at[2], s_sem.at[2])
                bring.start()
                bring.wait()
                if over == 1:
                    for part_copy in own:
                        part_copy.wait()
                stage[slot] = (stage[slot].astype(f32) + stage[2].astype(f32)).astype(bf16)
            if width == 1:
                for part_copy in own:
                    part_copy.wait()
            if i:
                f_deep(g, slot, stage).start()
            else:
                copy(stage.at[slot], f_out.at[z], o_sem.at[0]).start()

        def a_sum(i, stage):
            g = s.order(i)
            slot = i % 2
            narrow = pl.ds(0, a_cols)
            if i + 2 < depth:
                a_left(s.order(i + 2), slot, stage)
            own = copy(g_attn.at[row(g, y)], stage.at[slot, :, narrow], s_sem.at[0])
            own.start()

            def add(source):
                bring = copy(source, stage.at[2, :, narrow], s_sem.at[2])
                bring.start()
                bring.wait()
                total = stage[slot, :, :a_cols].astype(f32) + stage[2, :, :a_cols].astype(f32)
                stage[slot, :, :a_cols] = total.astype(bf16)

            for over in range(1, width):
                got(ay_got.at[g, over - 1], ya.at[over - 1, g])
                if over == 1:
                    own.wait()
                add(ya.at[over - 1, g])
            if width == 1:
                own.wait()

            @pl.when(jnp.logical_and(g >= z, s.low))
            def _():
                got(au_got.at[g], az.at[g])
                add(az.at[g])

            @pl.when(jnp.logical_and(g <= z, s.high))
            def _():
                where = jnp.where(g == z, depth, g)
                got(ad_got.at[g], az.at[where])
                add(az.at[where])

            @pl.when(g > z)
            def _():
                a_up(g, slot, stage).start()

            @pl.when(g < z)
            def _():
                a_dn(g, slot, stage).start()

            if i == 0:
                copy(stage.at[slot, :, narrow], a_out, o_sem.at[1]).start()

        def ffn(part, mid, mix, strips):
            trade = Trade(s, buf, part, acc, c_in, x_in, z_in, sems)
            trade.pass_on(z)
            first_loads = loads + [copy(gu_ref, mid, in_sem.at[0])]
            first_loads[-1].start()
            mix_load = copy(mix_ref, mix, in_sem.at[1])
            mix_load.start()

            @pl.loop(1, depth + 1)
            def _(i):
                @pl.when(i < depth)
                def _():
                    trade.take_z(s.order(i))

                g = s.order(i - 1)
                trade.take_rank(g)

                @pl.when(i == 1)
                def _():
                    for load in first_loads:
                        load.wait()

                backward_group(g, buf, mid, mid, part, w_gu, w_dn, share)
                trade.back_c(g).start()

            n_strip = half // strip

            away = 1 - z // 2

            def strip_at(j):
                side = jnp.where(j < n_strip, away, 1 - away)
                return pl.multiple_of(side * half + j % n_strip * strip, strip)

            def bring(j):
                return copy(tok_ref.at[:, :, pl.ds(strip_at(j), strip)], strips.at[j % 2], in_sem.at[2 + j % 2])

            def weight_grads(j):
                bring(j).wait()
                rows = pl.ds(strip_at(j), strip)

                def product(left, right, where, cols):
                    where[rows, cols] = lax.dot_general(
                        left, right, (((0,), (0,)), ((), ())), preferred_element_type=f32
                    ).astype(bf16)

                @pl.loop(0, 2 * share // 256)
                def _(t):
                    cols = pl.ds(pl.multiple_of(t * 256, 256), 256)
                    left = strips[j % 2].reshape(depth * count, strip)
                    product(left, mid[:, :, cols].reshape(depth * count, 256), w_gu, cols)

                @pl.when(j + 2 < 2 * n_strip)
                def _():
                    bring(j + 2).start()

                for lo in range(0, share, 256):
                    hi = min(lo + 256, share)
                    left = buf[:, :, :, :, rows].reshape(depth * count, strip)
                    right = mix[:, :, lo:hi].reshape(depth * count, hi - lo)
                    product(left, right, w_dn, slice(lo, hi))

            def send_wide(indices):
                for i in indices:
                    g = s.order(i)
                    for over in range(1, width):
                        for k in range(2):
                            f_wide(g, over, k).start()

            ends = jnp.logical_or(z == 0, z == depth - 1)
            inner = jnp.logical_not(ends)
            for j in range(2):
                bring(j).start()
            mix_load.wait()
            for i in reversed(range(depth)):
                trade.add_c(s.order(i))

            @pl.loop(0, 2 * n_strip)
            def _(j):
                weight_grads(j)

                @pl.when(jnp.logical_and(j == n_strip - 2, ends))
                def _():
                    trade.add_xz(s.order(3))

                @pl.when(j == n_strip - 1)
                def _():
                    send_wide((3, 2))

                @pl.when(jnp.logical_and(j == n_strip, ends))
                def _():
                    trade.add_xz(s.order(2))

                @pl.when(jnp.logical_and(j == n_strip + 1, inner))
                def _():
                    trade.add_xz(s.order(3))

            send_wide((1, 0))

            @pl.when(inner)
            def _():
                trade.add_xz(s.order(2))

            trade.add_xz(s.order(1))
            trade.add_xz(z)
            trade.settle()

        pl.run_scoped(
            ffn,
            pltpu.VMEM((depth, 2, 2, n, d), bf16),
            pltpu.VMEM((depth, count, 2 * share), bf16),
            pltpu.VMEM((depth, count, share), bf16),
            pltpu.VMEM((2, depth, count, strip), bf16),
        )

        def hop_x(where, src, kind):
            return remote(src, where.at[c, x], t_put.at[kind, 0], t_got.at[kind, 0], s.at_x)

        def hop_c(where, src, kind):
            return remote(src, where.at[c, x], t_put.at[kind, 1], t_got.at[kind, 1], s.at_c)

        def hop_far(where, kind):
            return remote(where.at[c, 1 - x], where.at[c, 1 - x], t_put.at[kind, 2], t_got.at[kind, 2], s.at_c)

        def spread(where, src, kind):
            hop_x(where, src, kind).start()
            hop_c(where, src, kind).start()

        def spread_on(where, kind):
            got(t_got.at[kind, 0], where.at[c, 1 - x])
            hop_far(where, kind).start()

        def spread_end(where, kind):
            got(t_got.at[kind, 1], where.at[1 - c, x])
            got(t_got.at[kind, 2], where.at[1 - c, 1 - x])

        def attention(stage, w_a, normed_v, qkv_v, att_v, d_att, d_qkv, part_a, cos_v, sin_v, mask_v, field_v, other_v, cot_v):
            own_x = copy(x_ref.at[pl.ds(mine, n)], cot_v.at[1], in_sem.at[4])
            fills = [
                copy(hid_ref, field_v, in_sem.at[0]),
                copy(att_branch_ref, other_v, in_sem.at[1]),
                copy(cot_ref.at[pl.ds(mine, n)], cot_v.at[0], in_sem.at[2]),
            ]
            later = [
                copy(wa_ref, w_a, w_sem.at[0, 0]),
                copy(att_ref, att_v, w_sem.at[0, 1]),
                copy(qkv_ref, qkv_v, w_sem.at[1, 0]),
                copy(normed_ref, normed_v, w_sem.at[1, 1]),
                copy(cos_ref, cos_v, in_sem.at[5]),
                copy(sin_ref, sin_v, in_sem.at[6]),
                copy(mask_ref, mask_v, in_sem.at[7]),
                own_x,
            ]
            for fill in fills + later:
                fill.start()
            for fill in fills:
                fill.wait()

            @pl.loop(0, n // 16)
            def _(i):
                at = rows16(i)
                d_hidden = cot_v[0, at, :].astype(f32) + norm_back(field_v[at, :], gain_v[2:3, :], acc[at, :], 2)
                acc[at, :] = d_hidden
                dbr[c, x, at, :] = norm_back(other_v[at, :], gain_v[1:2, :], d_hidden, 1).astype(bf16)

            spread(dbr, dbr.at[c, x], 0)
            spread(out_all, own_out, 1)
            copy(own_out, out_all.at[c, x], o_sem.at[2]).start()
            for fill in later:
                fill.wait()
            spread_on(dbr, 0)
            f_sum(2, stage)
            spread_end(dbr, 0)

            for lo in range(0, q_cols, HD):
                value = jnp.dot(
                    dbr[...].reshape(count, d), w_a[:, qkv_cols + lo : qkv_cols + lo + HD], preferred_element_type=f32
                )
                d_att[:, lo : lo + HD] = value.astype(bf16)

            def turn(value, factor, at):
                low, high = value[:, : HD // 2], value[:, HD // 2 :]
                cosine, sine = cos_v[at, :], sin_v[at, :]
                return (low * cosine + high * sine) * factor, (high * cosine - low * sine) * factor

            def contract(left, right, dims):
                return lax.dot_general(left, right, ((dims[0], dims[1]), ((), ())), preferred_element_type=f32)

            @pl.loop(0, count // ROW_LEN)
            def _(r):
                at = pl.ds(pl.multiple_of(r * ROW_LEN, ROW_LEN), ROW_LEN)
                allowed = mask_v[at, :] > 0.5
                for kv in range(kv_heads):
                    k_at, v_at = q_cols + kv * HD, q_cols + k_cols + kv * HD
                    key, val = qkv_v[at, k_at : k_at + HD], qkv_v[at, v_at : v_at + HD]
                    d_key = jnp.zeros((ROW_LEN, HD), f32)
                    d_val = jnp.zeros((ROW_LEN, HD), f32)
                    for h in range(kv * group, (kv + 1) * group):
                        query = qkv_v[at, h * HD : (h + 1) * HD]
                        grad = d_att[at, h * HD : (h + 1) * HD]
                        bent = jnp.tanh(contract(query, key, ((1,), (1,))) / CAP)
                        expo = jnp.where(allowed, jnp.exp(CAP * bent), 0.0)
                        soft = expo / jnp.sum(expo, axis=-1, keepdims=True)
                        d_val = d_val + contract(soft.astype(bf16), grad, ((0,), (0,)))
                        d_probs = contract(grad, val, ((1,), (1,)))
                        d_soft = soft * (d_probs - jnp.sum(soft * d_probs, axis=-1, keepdims=True))
                        d_cap = (d_soft * (1.0 - bent * bent)).astype(bf16)
                        d_key = d_key + contract(d_cap, query, ((0,), (0,)))
                        low, high = turn(contract(d_cap, key, ((1,), (0,))), scale, at)
                        d_qkv[at, h * HD : h * HD + HD // 2] = low.astype(bf16)
                        d_qkv[at, h * HD + HD // 2 : (h + 1) * HD] = high.astype(bf16)
                    low, high = turn(d_key, 1.0, at)
                    d_qkv[at, k_at : k_at + HD // 2] = low.astype(bf16)
                    d_qkv[at, k_at + HD // 2 : k_at + HD] = high.astype(bf16)
                    d_qkv[at, v_at : v_at + HD] = d_val.astype(bf16)

            def attn_grads(side):
                at = pl.multiple_of(side * half, LANE)
                rows = pl.ds(at, half)
                for lo in range(0, qkv_cols, 256):
                    value = contract(normed_v[:, rows], d_qkv[:, lo : lo + 256], ((0,), (0,)))
                    g_attn[rows, lo : lo + 256] = value.astype(bf16)
                for lo in range(0, q_cols, 256):
                    value = contract(dbr[:, :, :, rows].reshape(count, half), att_v[:, lo : lo + 256], ((0,), (0,)))
                    g_attn[rows, qkv_cols + lo : qkv_cols + lo + 256] = value.astype(bf16)

            away = 1 - z // 2
            attn_grads(away)
            for i in (3, 2):
                for over in range(1, width):
                    a_wide(s.order(i), over).start()
            attn_grads(1 - away)
            for i in (1, 0):
                for over in range(1, width):
                    a_wide(s.order(i), over).start()

            @pl.loop(0, d // 256)
            def _(t):
                at = pl.multiple_of(t * 256, 256)
                value = lax.dot_general(
                    d_qkv[...], w_a[pl.ds(at, 256), :qkv_cols], (((1,), (1,)), ((), ())), preferred_element_type=f32
                )
                part_a[:, :, :, pl.ds(at, 256)] = value.astype(bf16).reshape(2, 2, n, 256)

            to_c = remote(part_a.at[1 - c], c_in.at[0], ra_put.at[0], ra_got.at[0], s.at_c)
            to_c.start()
            to_c.wait_recv()
            part_a[c, 1 - x] = (part_a[c, 1 - x].astype(f32) + c_in[0, 1 - x].astype(f32)).astype(bf16)
            to_x = remote(part_a.at[c, 1 - x], x_in.at[0], ra_put.at[1], ra_got.at[1], s.at_x)
            to_x.start()
            field_v[...] = part_a[c, x].astype(f32) + c_in[0, x].astype(f32)
            f_sum(1, stage)
            spread_on(out_all, 1)
            to_x.wait_recv()
            hop_x(out_all, own_out, 1).wait_send()
            hop_c(out_all, own_out, 1).wait_send()
            copy(own_out, out_all.at[c, x], o_sem.at[2]).wait()

            @pl.loop(0, n // 16)
            def _(i):
                at = rows16(i)
                grad = field_v[at, :] + x_in[0, at, :].astype(f32)
                d_source = norm_back(cot_v[1, at, :].astype(f32), gain_v[0:1, :], grad, 0)
                own_out[at, :] = (acc[at, :] + d_source).astype(bf16)

            to_c.wait_send()
            to_x.wait_send()
            spread(gin_all, own_out, 2)
            copy(own_out, gin_all.at[c, x], o_sem.at[3]).start()

        def finish(stage):
            f_sum(3, stage)
            pl.run_scoped(
                functools.partial(attention, stage),
                pltpu.VMEM((d, a_cols), bf16),
                pltpu.VMEM((count, d), bf16),
                pltpu.VMEM((count, qkv_cols), bf16),
                pltpu.VMEM((count, q_cols), bf16),
                pltpu.VMEM((count, q_cols), bf16),
                pltpu.VMEM((count, qkv_cols), bf16),
                pltpu.VMEM((2, 2, n, d), bf16),
                pltpu.VMEM((count, HD // 2), f32),
                pltpu.VMEM((count, HD // 2), f32),
                pltpu.VMEM((count, ROW_LEN), f32),
                pltpu.VMEM((n, d), f32),
                pltpu.VMEM((n, d), f32),
                pltpu.VMEM((2, n, d), bf16),
            )

            for k in range(4):
                gain_v[k : k + 1, :] = jnp.sum(gain_acc[k], axis=0, keepdims=True)
            whole = gain_v[...]
            for p in range(dp_n):
                turned = pltpu.roll(whole, (d - p * shard) % d, 1) if p else whole
                gain_put[p] = turned[:, :lanes]

            def gain_hop(k):
                to = (s.dp + k) % dp_n
                return remote(gain_put.at[to], gain_got.at[s.dp], gg_put.at[k - 1], gg_got.at[k - 1], (to, s.q))

            for k in range(1, dp_n):
                gain_hop(k).start()
            spread_on(gin_all, 2)
            f_sum(0, stage)

            f_deep(s.order(1), 1, stage).wait_send()
            copy(stage.at[0], f_out.at[z], o_sem.at[0]).wait()
            for i in reversed(range(depth)):
                a_sum(i, stage)

            for k in range(1, dp_n):
                got(gg_got.at[k - 1], gain_got.at[(s.dp + dp_n - k) % dp_n])
            total = gain_put[s.dp]
            for k in range(1, dp_n):
                total = total + gain_got[(s.dp + dp_n - k) % dp_n]
            gain_x[0] = total
            across = remote(gain_x.at[0], gain_x.at[1], gt_put.at[0], gt_got.at[0], s.at_x)
            across.start()
            across.wait_recv()
            gain_c[0] = gain_x[0] + gain_x[1]
            beside = remote(gain_c.at[0], gain_c.at[1], gt_put.at[1], gt_got.at[1], s.at_c)
            beside.start()
            beside.wait_recv()
            gain_c[2] = gain_c[0] + gain_c[1]
            copy(gain_c.at[2], gains_out, o_sem.at[4]).start()

            spread_end(out_all, 1)
            spread_end(gin_all, 2)
            for i in range(1, depth):
                g = s.order(i)
                got(fz_got.at[g], f_out.at[g])
            for i in range(depth):
                g = s.order(i)
                for over in range(1, width):
                    for k in range(2):
                        f_wide(g, over, k).wait_send()
                    a_wide(g, over).wait_send()
            a_left(s.order(1), 1, stage)
            for kind, where, src in ((0, dbr, dbr.at[c, x]), (1, out_all, own_out), (2, gin_all, own_out)):
                if kind != 1:
                    hop_x(where, src, kind).wait_send()
                    hop_c(where, src, kind).wait_send()
                hop_far(where, kind).wait_send()
            for k in range(1, dp_n):
                gain_hop(k).wait_send()
            across.wait_send()
            beside.wait_send()
            copy(stage.at[0, :, pl.ds(0, a_cols)], a_out, o_sem.at[1]).wait()
            copy(own_out, gin_all.at[c, x], o_sem.at[3]).wait()
            copy(gain_c.at[2], gains_out, o_sem.at[4]).wait()

        pl.run_scoped(finish, pltpu.VMEM((3, shard, 3 * share), bf16))

    shape = jax.ShapeDtypeStruct
    outs = (
        shape((2, 2, n, d), bf16),
        shape((2, 2, n, d), bf16),
        shape((depth, shard, 3 * share), bf16),
        shape((shard, a_cols), bf16),
        shape((max(others, 1), depth, shard, 3 * share), bf16),
        shape((max(others, 1), depth, shard, a_cols), bf16),
        shape((depth + 1, shard, a_cols), bf16),
        shape((8, lanes), f32),
    )
    operands = tuple(first) + tuple(weights) + tuple(saves)
    anywhere = pl.BlockSpec(memory_space=pl.ANY)
    dma = pltpu.SemaphoreType.DMA
    return pl.pallas_call(
        kernel,
        out_shape=outs,
        in_specs=[anywhere] * len(operands),
        out_specs=tuple([anywhere] * len(outs)),
        scratch_shapes=Trade.buffers(depth, n, d)
        + [
            pltpu.VMEM((d, 2 * share), bf16),
            pltpu.VMEM((d, share), bf16),
            pltpu.VMEM((d, a_cols), bf16),
            pltpu.VMEM((n, d), f32),
            pltpu.VMEM((2, 2, n, d), bf16),
            pltpu.VMEM((n, d), bf16),
            pltpu.VMEM((8, d), f32),
            pltpu.VMEM((4, 8, d), f32),
            pltpu.VMEM((dp_n, 8, lanes), f32),
            pltpu.VMEM((dp_n, 8, lanes), f32),
            pltpu.VMEM((2, 8, lanes), f32),
            pltpu.VMEM((3, 8, lanes), f32),
            dma((8,)),
            dma((dp_n, 2)),
            dma((3,)),
            dma((5,)),
            dma((3, 3)),
            dma((3, 3)),
            dma((depth, max(others, 1), 2)),
            dma((depth, max(others, 1), 2)),
            dma((depth,)),
            dma((depth,)),
            dma((depth, max(others, 1))),
            dma((depth, max(others, 1))),
            dma((depth,)),
            dma((depth,)),
            dma((depth,)),
            dma((dp_n - 1,)),
            dma((dp_n - 1,)),
            dma((2,)),
            dma((2,)),
            dma((2,)),
            dma((2,)),
        ]
        + Trade.semaphores(depth),
        compiler_params=pltpu.CompilerParams(collective_id=2, has_side_effects=True, vmem_limit_bytes=67_043_328),
        name="backward",
    )(*operands)


def unit_cuts(units, parts):
    tiles = units // LANE
    edges = [(tiles * k + parts - 1) // parts for k in range(parts + 1)]
    starts = [e * LANE for e in edges[:-1]]
    sizes = [(b - a) * LANE for a, b in zip(edges[:-1], edges[1:])]
    return starts, sizes, max(sizes)


def cut_units(block, cuts):
    starts, sizes, share = cuts
    return jnp.stack(
        [
            jnp.pad(block[:, a : a + n], ((0, 0), (0, share - n))) if n < share else block[:, a : a + n]
            for a, n in zip(starts, sizes)
        ]
    )


def join_units(blocks, cuts):
    starts, sizes, share = cuts
    return jnp.concatenate([blocks[k, :, :n] for k, n in enumerate(sizes)], axis=1)


def make_body(grid):
    def body(
        inputs,
        cotangent,
        segments,
        positions,
        w_query,
        w_key,
        w_value,
        w_output,
        w_gate,
        w_up,
        w_down,
        gain_attn,
        gain_post_attn,
        gain_ffw,
        gain_post_ffw,
    ):
        grid.here()
        count, width = inputs.shape
        shard = w_query.shape[0]
        group = HEADS // KV
        local_kv = w_key.shape[1] // HD
        local_heads = local_kv * group
        q_cols, k_cols = w_query.shape[1], w_key.shape[1]
        scale = 1.0 / math.sqrt(HD)
        part = count // grid.tensor
        rows = count // ROW_LEN
        cuts = unit_cuts(w_gate.shape[1], grid.depth)
        share = cuts[2]
        main = share // 256 * 256

        gains = jnp.stack([gain_attn, gain_post_attn, gain_ffw, gain_post_ffw])
        gains = jnp.pad(gains, ((0, 12), (0, -shard % LANE)))
        angles = make_angles(positions, HD)[:, 0]
        cosine, sine = jnp.cos(angles), jnp.sin(angles)
        mask = row_mask(segments, rows, ROW_LEN).astype(f32).reshape(count, ROW_LEN)
        cut_gate, cut_up = cut_units(w_gate, cuts), cut_units(w_up, cuts)
        wide_blocks = jnp.concatenate(
            [cut_gate[:, :, :main], cut_up[:, :, :main], cut_gate[:, :, main:], cut_up[:, :, main:]], axis=2
        )
        slim_blocks = cut_units(w_down.T, cuts)
        w_attn = jnp.concatenate([w_query, w_key, w_value, w_output.T], axis=1)
        (full_attn, full_wide, full_slim, normed, qkv, attended, branch_attn, hidden, full_gains,
         all_normed, saved, mixed, branch_ffw) = forward_kernel(
            grid, inputs, w_attn, wide_blocks, slim_blocks, gains, cosine, sine,
            mask, local_heads, local_kv,
        )
        full_attn = full_attn.reshape(width, full_attn.shape[2])
        out_all, gin_all, blocks_ffn, grad_attn, _, _, _, d_gains = backward_kernel(
            grid,
            (branch_ffw, hidden, branch_attn, cotangent, inputs, full_gains),
            (full_attn, full_wide, full_slim),
            (saved, all_normed.reshape(grid.depth, count, width), mixed, normed, qkv, attended, cosine, sine, mask),
            local_heads, local_kv,
        )
        rest = 2 * main + share - main
        grad_gate = jnp.concatenate([blocks_ffn[:, :, :main], blocks_ffn[:, :, 2 * main : rest]], axis=2)
        grad_up = jnp.concatenate([blocks_ffn[:, :, main : 2 * main], blocks_ffn[:, :, rest : 2 * share]], axis=2)
        grad_gate = join_units(grad_gate, cuts).astype(f32)
        grad_up = join_units(grad_up, cuts).astype(f32)
        grad_down = join_units(blocks_ffn[:, :, 2 * share :], cuts).T.astype(f32)
        grad_attn = grad_attn.astype(f32)
        qkv_cols = q_cols + 2 * k_cols

        return (
            out_all.reshape(count, width),
            gin_all.reshape(count, width),
            grad_attn[:, :q_cols],
            grad_attn[:, q_cols : q_cols + k_cols],
            grad_attn[:, q_cols + k_cols : qkv_cols],
            grad_attn[:, qkv_cols:].T,
            grad_gate,
            grad_up,
            grad_down,
            d_gains[0, :shard],
            d_gains[1, :shard],
            d_gains[2, :shard],
            d_gains[3, :shard],
        )

    return body


def solution(mesh):
    placed = (
        P("dp", None),
        P("dp", None),
        P("dp"),
        P("dp"),
        P("dp", "tensor"),
        P("dp", "tensor"),
        P("dp", "tensor"),
        P("tensor", "dp"),
        P("dp", "tensor"),
        P("dp", "tensor"),
        P("tensor", "dp"),
        P("dp"),
        P("dp"),
        P("dp"),
        P("dp"),
    )
    return jax.shard_map(
        make_body(Grid(mesh)),
        mesh=mesh,
        in_specs=placed,
        out_specs=(
            P("dp", None),
            P("dp", None),
            P("dp", "tensor"),
            P("dp", "tensor"),
            P("dp", "tensor"),
            P("tensor", "dp"),
            P("dp", "tensor"),
            P("dp", "tensor"),
            P("tensor", "dp"),
            P("dp"),
            P("dp"),
            P("dp"),
            P("dp"),
        ),
        check_vma=False,
    )
```

```python
import functools
import math

import jax
import jax.numpy as jnp
from jax import lax
from jax.experimental import pallas as pl
from jax.experimental.pallas import tpu as pltpu
from jax.sharding import PartitionSpec as P

HEADS = 8
KV = 4
HD = 256
ROW_LEN = 128
LANE = 128


EPS = 1e-06
CAP = 50.0
THETA = 10000.0

f32 = jnp.float32
bf16 = jnp.bfloat16


def rms_scale(field, gain):
    inverse = lax.rsqrt(jnp.mean(field * field, axis=-1, keepdims=True) + EPS)
    return field * inverse * gain


def rms_back(field, gain, grad):
    inverse = lax.rsqrt(jnp.mean(field * field, axis=-1, keepdims=True) + EPS)
    unit = field * inverse
    d_gain = jnp.sum(grad * unit, axis=0)
    scaled = grad * gain
    d_field = inverse * (scaled - unit * jnp.mean(scaled * unit, axis=-1, keepdims=True))
    return d_field, d_gain


def geglu(gate, upward):
    return jax.nn.gelu(gate, approximate=True) * upward


def rotate(field, cosine, sine):
    half = field.shape[-1] // 2
    first = field[..., :half]
    second = field[..., half:]
    return jnp.concatenate(
        [first * cosine - second * sine, second * cosine + first * sine], axis=-1
    )


def make_angles(positions, head_size):
    half = head_size // 2
    freqs = THETA ** (-(jnp.arange(half).astype(f32) * 2.0) / head_size)
    return positions.astype(f32)[:, None, None] * freqs[None, None, :]


def row_mask(segments, rows, length):
    seg_rows = segments.reshape(rows, length)
    same = seg_rows[:, :, None] == seg_rows[:, None, :]
    index = jnp.arange(length)
    causal = index[:, None] >= index[None, :]
    return jnp.logical_and(same, causal[None])


def dot(left, right):
    return jnp.dot(left, right, preferred_element_type=f32)


def contract_rows(left, right):
    return lax.dot_general(left, right, (((0,), (0,)), ((), ())), preferred_element_type=f32)


def contract_cols(left, right):
    return lax.dot_general(left, right, (((1,), (1,)), ((), ())), preferred_element_type=f32)


class Grid:
    def __init__(self, mesh):
        self.dp = mesh.shape["dp"]
        self.tensor = mesh.shape["tensor"]
        self.depth = 4 if self.dp % 4 == 0 else (2 if self.dp % 2 == 0 else 1)
        self.width = self.dp // self.depth

    def here(self):
        index = lax.axis_index("dp")
        self.deep = index // self.width
        self.wide = lax.rem(index, self.width)
        self.rank = lax.axis_index("tensor")

    def shift(self, value, step):
        pairs = [
            (z * self.width + y, ((z + step) % self.depth) * self.width + y)
            for z in range(self.depth)
            for y in range(self.width)
        ]
        return lax.ppermute(value, "dp", pairs)

    def swap_wide(self, value, bit):
        pairs = [
            (z * self.width + y, z * self.width + (y ^ bit))
            for z in range(self.depth)
            for y in range(self.width)
        ]
        return lax.ppermute(value, "dp", pairs)

    def swap_rank(self, value, bit):
        return lax.ppermute(value, "tensor", [(q, q ^ bit) for q in range(self.tensor)])

    def wide_bits(self):
        return [1 << b for b in range(self.width.bit_length() - 1)]

    def rank_bits(self):
        return [1 << b for b in range(self.tensor.bit_length() - 1)]

    def reduce_width(self, full):
        rows, columns = full.shape[0] // self.dp, full.shape[1]
        held = full.reshape(self.depth, self.width, rows, columns)
        for bit in reversed(self.wide_bits()):
            held = held.reshape(self.depth, 2, bit, rows, columns)
            mine = lax.rem(self.wide // bit, 2)
            other = lax.dynamic_index_in_dim(held, 1 - mine, 1, keepdims=False)
            own = lax.dynamic_index_in_dim(held, mine, 1, keepdims=False)
            held = own + self.swap_wide(other, bit)
        return held.reshape(self.depth, rows, columns)

    def pick(self, held, step):
        to = lax.rem(self.deep + step, self.depth)
        return lax.dynamic_index_in_dim(held, to, 0, keepdims=False)

    def scatter_rows(self, full):
        held = self.reduce_width(full)
        total = self.pick(held, 0).astype(f32)
        for step in range(1, self.depth):
            total = total + self.shift(self.pick(held, step), step).astype(f32)
        return total

    def return_blocks(self, full):
        held = self.reduce_width(full)
        out = jnp.zeros_like(held)
        for step in range(self.depth):
            part = self.pick(held, step)
            part = part if step == 0 else self.shift(part, step)
            source = lax.rem(self.deep + self.depth - step, self.depth)
            out = lax.dynamic_update_slice(out, part[None], (source, 0, 0))
        return out

    def spread_rank(self, block):
        x, c = self.rank // 2, lax.rem(self.rank, 2)
        n, d = block.shape
        out = jnp.zeros((2, 2, n, d), block.dtype)
        for far_c in range(2):
            for far_x in range(2):
                part = block
                if far_x:
                    part = across
                if far_c:
                    part = self.swap_rank(part, 1)
                elif not far_x:
                    across = self.swap_rank(block, 2)
                out = lax.dynamic_update_slice(
                    out, part[None, None], (jnp.bitwise_xor(c, far_c), jnp.bitwise_xor(x, far_x), 0, 0)
                )
        return out.reshape(4 * n, d)

    def reduce_rank(self, full):
        x, c = self.rank // 2, lax.rem(self.rank, 2)
        held = full.reshape(2, 2, full.shape[0] // 4, full.shape[1])
        for at, bit in ((c, 1), (x, 2)):
            own = lax.dynamic_index_in_dim(held, at, 0, keepdims=False)
            other = lax.dynamic_index_in_dim(held, 1 - at, 0, keepdims=False)
            held = own + self.swap_rank(other, bit)
        return held


MESH = pl.DeviceIdType.MESH


class Spot:
    def __init__(self, grid):
        self.depth, self.width = grid.depth, grid.width
        self.dp = lax.axis_index("dp")
        self.q = lax.axis_index("tensor")
        self.z, self.y = self.dp // self.width, self.dp % self.width
        self.x, self.c = self.q // 2, self.q % 2
        self.at_x = (self.dp, (1 - self.x) * 2 + self.c)
        self.at_c = (self.dp, self.x * 2 + 1 - self.c)
        self.at_up = (self.dp + self.width, self.q)
        self.at_dn = (self.dp - self.width, self.q)
        self.low, self.high = self.z > 0, self.z < self.depth - 1

    def order(self, i):
        z = self.z
        near = z + 1 - 2 * (z % 2)
        middle = 2 - z // 2
        far = 3 * (1 - z // 2)
        return jnp.where(i == 0, z, jnp.where(i == 1, near, jnp.where(i == 2, middle, far)))

    def at_depth(self, z):
        return (z * self.width + self.y, self.q)

    def at_wide(self, over):
        return (self.z * self.width + (self.y + over) % self.width, self.q)


def remote(src, dst, put, got, device):
    return pltpu.make_async_remote_copy(
        src_ref=src, dst_ref=dst, send_sem=put, recv_sem=got, device_id=device, device_id_type=MESH
    )


def signal(semaphore, device):
    pl.semaphore_signal(semaphore, inc=1, device_id=device, device_id_type=MESH)


class Trade:
    def __init__(self, spot, buf, part, acc, c_in, x_in, z_in, sems):
        self.spot, self.buf, self.part, self.acc = spot, buf, part, acc
        self.c_in, self.x_in, self.z_in = c_in, x_in, z_in
        (self.z_up, self.z_dn, self.z_got, self.x_put, self.x_got, self.c_put, self.c_got,
         self.rc_put, self.rc_got, self.rx_put, self.rx_got, self.rz_put, self.ru_got, self.rd_got) = sems

    @staticmethod
    def semaphores(depth):
        dma = pltpu.SemaphoreType.DMA
        return [dma((depth,))] * 5 + [dma((depth, 2))] * 2 + [dma((depth,))] * 7

    @staticmethod
    def buffers(depth, n, d):
        return [
            pltpu.VMEM((depth, 2, 2, n, d), bf16),
            pltpu.VMEM((depth, 2, n, d), bf16),
            pltpu.VMEM((depth, n, d), bf16),
            pltpu.VMEM((depth + 1, n, d), bf16),
        ]

    def hop_up(self, g):
        s = self.spot
        return remote(self.buf.at[g, s.c, s.x], self.buf.at[g, s.c, s.x], self.z_up.at[g], self.z_got.at[g], s.at_up)

    def hop_dn(self, g):
        s = self.spot
        return remote(self.buf.at[g, s.c, s.x], self.buf.at[g, s.c, s.x], self.z_dn.at[g], self.z_got.at[g], s.at_dn)

    def hop_x(self, g):
        s = self.spot
        return remote(self.buf.at[g, s.c, s.x], self.buf.at[g, s.c, s.x], self.x_put.at[g], self.x_got.at[g], s.at_x)

    def hop_c(self, g, far):
        s = self.spot
        xx = (1 - s.x) if far else s.x
        return remote(
            self.buf.at[g, s.c, xx], self.buf.at[g, s.c, xx], self.c_put.at[g, int(far)], self.c_got.at[g, int(far)], s.at_c
        )

    def got(self, sem, ref):
        remote(ref, ref, sem, sem, self.spot.at_x).wait_recv()

    def pass_on(self, g):
        s = self.spot

        @pl.when(jnp.logical_and(g <= s.z, s.high))
        def _():
            self.hop_up(g).start()

        @pl.when(jnp.logical_and(g >= s.z, s.low))
        def _():
            self.hop_dn(g).start()

        self.hop_x(g).start()
        self.hop_c(g, False).start()

    def take_z(self, g):
        s = self.spot
        self.got(self.z_got.at[g], self.buf.at[g, s.c, s.x])
        self.pass_on(g)

    def take_rank(self, g):
        s = self.spot
        self.got(self.x_got.at[g], self.buf.at[g, s.c, 1 - s.x])
        self.hop_c(g, True).start()
        self.got(self.c_got.at[g, 0], self.buf.at[g, 1 - s.c, s.x])
        self.got(self.c_got.at[g, 1], self.buf.at[g, 1 - s.c, 1 - s.x])

    def back_c(self, g):
        s = self.spot
        return remote(self.part.at[g, 1 - s.c], self.c_in.at[g], self.rc_put.at[g], self.rc_got.at[g], s.at_c)

    def back_x(self, g):
        s = self.spot
        return remote(self.part.at[g, s.c, 1 - s.x], self.x_in.at[g], self.rx_put.at[g], self.rx_got.at[g], s.at_x)

    def back_up(self, g):
        s = self.spot
        return remote(self.part.at[g, s.c, s.x], self.z_in.at[g], self.rz_put.at[g], self.ru_got.at[g], s.at_up)

    def back_dn(self, g):
        s = self.spot
        slot = jnp.where(g == s.z - 1, s.depth, g)
        return remote(self.part.at[g, s.c, s.x], self.z_in.at[slot], self.rz_put.at[g], self.rd_got.at[g], s.at_dn)

    def add_c(self, g):
        s, part, c_in = self.spot, self.part, self.c_in
        self.got(self.rc_got.at[g], c_in.at[g])
        part[g, s.c, 1 - s.x] = (part[g, s.c, 1 - s.x].astype(f32) + c_in[g, 1 - s.x].astype(f32)).astype(bf16)
        self.back_x(g).start()
        part[g, s.c, s.x] = (part[g, s.c, s.x].astype(f32) + c_in[g, s.x].astype(f32)).astype(bf16)

    def add_xz(self, g):
        s, part, acc = self.spot, self.part, self.acc
        self.got(self.rx_got.at[g], self.x_in.at[g])
        acc[...] = part[g, s.c, s.x].astype(f32) + self.x_in[g].astype(f32)

        @pl.when(jnp.logical_and(g >= s.z, s.low))
        def _():
            self.got(self.ru_got.at[g], self.z_in.at[g])
            acc[...] += self.z_in[g].astype(f32)

        @pl.when(jnp.logical_and(g <= s.z, s.high))
        def _():
            slot = jnp.where(g == s.z, s.depth, g)
            self.got(self.rd_got.at[g], self.z_in.at[slot])
            acc[...] += self.z_in[slot].astype(f32)

        @pl.when(g > s.z)
        def _():
            part[g, s.c, s.x] = acc[...].astype(bf16)
            self.back_up(g).start()

        @pl.when(g < s.z)
        def _():
            part[g, s.c, s.x] = acc[...].astype(bf16)
            self.back_dn(g).start()

    def settle(self):
        s = self.spot

        @pl.loop(0, s.depth)
        def _(g):
            @pl.when(jnp.logical_and(g <= s.z, s.high))
            def _():
                self.hop_up(g).wait_send()

            @pl.when(jnp.logical_and(g >= s.z, s.low))
            def _():
                self.hop_dn(g).wait_send()

            self.hop_x(g).wait_send()
            self.hop_c(g, False).wait_send()
            self.hop_c(g, True).wait_send()
            self.back_c(g).wait_send()
            self.back_x(g).wait_send()

            @pl.when(g > s.z)
            def _():
                self.back_up(g).wait_send()

            @pl.when(g < s.z)
            def _():
                self.back_dn(g).wait_send()


def put_part(part, g, left, right, n, d):
    @pl.loop(0, d // 256)
    def _(t):
        at = pl.multiple_of(t * 256, 256)
        value = lax.dot_general(left[g], right[pl.ds(at, 256), :], (((1,), (1,)), ((), ())), preferred_element_type=f32)
        part[g, :, :, :, pl.ds(at, 256)] = value.astype(bf16).reshape(2, 2, n, 256)


def forward_group(g, buf, gu, mid, w_gu, share):
    n, d = buf.shape[3:]
    main = share // 256 * 256
    tokens = lambda: buf[g].reshape(4 * n, d)

    def save(lo, hi, gate, upward):
        inner = math.sqrt(2.0 / math.pi) * (gate + 0.044715 * gate * gate * gate)
        mid[g, :, lo:hi] = (0.5 * gate * (1.0 + jnp.tanh(inner)) * upward).astype(bf16)

    for lo in range(0, main, 256):
        hi = lo + 256
        gate = jnp.dot(tokens(), w_gu[:, lo:hi], preferred_element_type=f32)
        upward = jnp.dot(tokens(), w_gu[:, main + lo : main + hi], preferred_element_type=f32)
        gu[g, :, lo:hi] = gate.astype(bf16)
        gu[g, :, main + lo : main + hi] = upward.astype(bf16)
        save(lo, hi, gate, upward)
    if main < share:
        rest = share - main
        both = jnp.dot(tokens(), w_gu[:, 2 * main :], preferred_element_type=f32)
        gu[g, :, 2 * main :] = both.astype(bf16)
        save(main, share, both[:, :rest], both[:, rest:])


def backward_group(g, buf, gu, mid, part, w_gu, w_dn, share):
    n, d = buf.shape[3:]
    main = share // 256 * 256
    tokens = lambda: buf[g].reshape(4 * n, d)

    def pull(lo, hi, gate_at, up_at):
        grad = jnp.dot(tokens(), w_dn[:, lo:hi], preferred_element_type=f32)
        gate = gu[g, :, gate_at : gate_at + hi - lo].astype(f32)
        upward = gu[g, :, up_at : up_at + hi - lo].astype(f32)
        factor = math.sqrt(2.0 / math.pi)
        square = gate * gate
        curve = jnp.tanh(factor * gate * (1.0 + 0.044715 * square))
        half = 0.5 * (1.0 + curve)
        slope = half + 0.5 * gate * (1.0 - curve * curve) * factor * (1.0 + 3.0 * 0.044715 * square)
        mid[g, :, gate_at : gate_at + hi - lo] = (grad * upward * slope).astype(bf16)
        mid[g, :, up_at : up_at + hi - lo] = (grad * gate * half).astype(bf16)

    for lo in range(0, main, 256):
        pull(lo, lo + 256, lo, main + lo)
    if main < share:
        pull(main, share, 2 * main, main + share)
    put_part(part, g, mid, w_gu, n, d)


def forward_kernel(grid, inputs, w_attn, wide_blocks, slim_blocks, gains, cosine, sine, mask, heads, kv_heads):
    depth, width, dp_n = grid.depth, grid.width, grid.dp
    count, d = inputs.shape
    n = count // 4
    shard, a_cols = w_attn.shape
    q_cols, k_cols = heads * HD, kv_heads * HD
    qkv_cols = q_cols + 2 * k_cols
    share = slim_blocks.shape[2]
    group = heads // kv_heads
    align = math.gcd(shard, 16)
    parts = ((0, qkv_cols), (qkv_cols, q_cols))
    scale = 1.0 / math.sqrt(HD)
    others = width - 1

    def kernel(
        x_ref, wa_ref, blk_wide, blk_slim, gain_ref, cos_ref, sin_ref, mask_ref,
        wa_all, wide_all, slim_all, normed_out, qkv_out, att_out, branch_out, hidden_out, gains_out,
        all_out, gu_out, mid_out, ffw_out,
        buf, c_in, x_in, z_in, gain_in, ca_in, xa_in, acc, hid, full_gain, w_a, w_gu, w_dn,
        g_put, g_got, a_up, a_dn, a_got, ay_put, ay_got, f_put, f_got, fy_put, fy_got,
        la_sem, lf_sem, in_sem, o_sem, g_sem, ra_put, ra_got, *sems,
    ):
        s = Spot(grid)
        z, y, x, c = s.z, s.y, s.x, s.c

        def got(sem, ref):
            remote(ref, ref, sem, sem, s.at_x).wait_recv()

        def row(g, yy):
            return pl.multiple_of((g * width + yy) * shard, align)

        barrier = pltpu.get_barrier_semaphore()
        for k in range(1, dp_n):
            signal(barrier, ((s.dp + k) % dp_n, s.q))
        signal(barrier, s.at_x)
        signal(barrier, s.at_c)
        pl.semaphore_wait(barrier, dp_n + 1)

        def a_at(g, yy, k):
            return wa_all.at[g * width + yy, :, pl.ds(parts[k][0], parts[k][1])]

        def a_src(g, k, own):
            return wa_ref.at[:, pl.ds(parts[k][0], parts[k][1])] if own else a_at(g, y, k)

        def a_hop(g, k, own, up):
            return remote(
                a_src(g, k, own), a_at(g, y, k), (a_up if up else a_dn).at[g, k], a_got.at[g, k], s.at_up if up else s.at_dn
            )

        def a_wide(g, k, own, over):
            return remote(a_src(g, k, own), a_at(g, y, k), ay_put.at[g, k, over - 1], ay_got.at[g, k, over - 1], s.at_wide(over))

        def a_pass(g, k, own):
            @pl.when(jnp.logical_and(g <= z, s.high))
            def _():
                a_hop(g, k, own, True).start()

            @pl.when(jnp.logical_and(g >= z, s.low))
            def _():
                a_hop(g, k, own, False).start()

            for over in range(1, width):
                a_wide(g, k, own, over).start()

        def f_at(g, yy, k):
            return (wide_all, slim_all)[k].at[g * width + yy]

        def f_own(g, k):
            return (blk_wide, blk_slim)[k].at[g]

        def f_hop(to, k):
            return remote(f_own(to, k), f_at(z, y, k), f_put.at[to, k], f_got.at[z, k], s.at_depth(to))

        def f_wide(g, own, over, k):
            source = f_own(z, k) if own else f_at(g, y, k)
            return remote(source, f_at(g, y, k), fy_put.at[g, over - 1, k], fy_got.at[g, over - 1, k], s.at_wide(over))

        ends = jnp.logical_or(z == 0, z == depth - 1)
        inner = jnp.logical_not(ends)

        def f_hops(i, k):
            @pl.when(ends)
            def _():
                for j in {1: (1,), 2: (2,), 3: (3,)}.get(i, ()):
                    f_hop(s.order(j), k).start()

            @pl.when(inner)
            def _():
                for j in {3: (2, 3, 1)}.get(i, ()):
                    f_hop(s.order(j), k).start()

        for k in range(1, dp_n):
            remote(gain_ref, gain_in.at[s.dp], g_put.at[k - 1], g_got.at[k - 1], ((s.dp + k) % dp_n, s.q)).start()
        for k in range(2):
            a_pass(z, k, True)

        def attention(x_v, normed_v, qkv_v, att_v, part_a, cos_v, sin_v, mask_v):
            own_gain = pltpu.make_async_copy(gain_ref, gain_in.at[s.dp], in_sem.at[4])
            fills = [
                pltpu.make_async_copy(x_ref, x_v, in_sem.at[0]),
                pltpu.make_async_copy(cos_ref, cos_v, in_sem.at[1]),
                pltpu.make_async_copy(sin_ref, sin_v, in_sem.at[2]),
                pltpu.make_async_copy(mask_ref, mask_v, in_sem.at[3]),
                own_gain,
            ]
            for fill in fills:
                fill.start()

            def load(g, yy, k, own, slot):
                return pltpu.make_async_copy(
                    a_src(g, k, True) if own else a_at(g, yy, k),
                    w_a.at[pl.ds(row(g, yy), shard), pl.ds(parts[k][0], parts[k][1])],
                    la_sem.at[slot, k],
                )

            for k in range(2):
                load(z, y, k, True, 0).start()

            for k in range(1, dp_n):
                remote(
                    gain_in.at[0], gain_in.at[(s.dp + dp_n - k) % dp_n], g_put.at[k - 1], g_got.at[k - 1], s.at_x
                ).wait_recv()
            for fill in fills:
                fill.wait()
            whole = jnp.zeros((8, d), f32)
            for p in range(dp_n):
                one = gain_in[p].astype(f32)[:8]
                one = jnp.concatenate([one, jnp.zeros((8, d - one.shape[1]), f32)], axis=1)
                whole = whole + (pltpu.roll(one, p * shard, 1) if p else one)
            full_gain[...] = whole
            pltpu.make_async_copy(full_gain, gains_out, o_sem.at[0]).start()

            @pl.loop(0, count // 32)
            def _(i):
                at = pl.ds(pl.multiple_of(i * 32, 32), 32)
                value = x_v[at, :].astype(f32)
                inverse = lax.rsqrt(jnp.mean(value * value, axis=-1, keepdims=True) + EPS)
                normed_v[at, :] = (value * inverse * full_gain[0:1, :]).astype(bf16)

            pltpu.make_async_copy(normed_v, normed_out, o_sem.at[1]).start()

            for i in range(1, depth):
                g = s.order(i)
                for k in range(2):
                    got(a_got.at[g, k], a_at(g, y, k))
                    a_pass(g, k, False)
                    load(g, y, k, False, i * width).start()
                f_hops(i, 0)
            for over in range(1, width):
                f_wide(z, True, over, 0).start()
            for k in range(2):
                for i in range(depth):
                    g = s.order(i)
                    for over in range(1, width):
                        yy = (y + width - over) % width
                        got(ay_got.at[g, k, over - 1], a_at(g, yy, k))
                        load(g, yy, k, False, i * width + over).start()
                for i in range(depth):
                    g = s.order(i)
                    for over in range(width):
                        load(g, (y + width - over) % width, k, i + over == 0, i * width + over).wait()
                if k:
                    continue
                for h in range(heads + 2 * kv_heads):
                    value = jnp.dot(normed_v[...], w_a[:, h * HD : (h + 1) * HD], preferred_element_type=f32)
                    if h < heads + kv_heads:
                        half = HD // 2
                        first, second = value[:, :half], value[:, half:]
                        low = first * cos_v[...] - second * sin_v[...]
                        high = second * cos_v[...] + first * sin_v[...]
                        if h < heads:
                            low, high = low * scale, high * scale
                        qkv_v[:, h * HD : h * HD + half] = low.astype(bf16)
                        qkv_v[:, h * HD + half : (h + 1) * HD] = high.astype(bf16)
                    else:
                        qkv_v[:, h * HD : (h + 1) * HD] = value.astype(bf16)
                pltpu.make_async_copy(qkv_v, qkv_out, o_sem.at[2]).start()

                @pl.loop(0, count // ROW_LEN)
                def _(r):
                    at = pl.ds(pl.multiple_of(r * ROW_LEN, ROW_LEN), ROW_LEN)
                    allowed = mask_v[at, :] > 0.5
                    for h in range(heads):
                        kv = heads + h // group
                        scores = lax.dot_general(
                            qkv_v[at, h * HD : (h + 1) * HD],
                            qkv_v[at, kv * HD : (kv + 1) * HD],
                            (((1,), (1,)), ((), ())),
                            preferred_element_type=f32,
                        )
                        expo = jnp.where(allowed, jnp.exp(CAP * jnp.tanh(scores / CAP)), 0.0)
                        probs = (expo / jnp.sum(expo, axis=-1, keepdims=True)).astype(bf16)
                        kv = kv + kv_heads
                        value = jnp.dot(probs, qkv_v[at, kv * HD : (kv + 1) * HD], preferred_element_type=f32)
                        att_v[at, h * HD : (h + 1) * HD] = value.astype(bf16)

                pltpu.make_async_copy(att_v, att_out, o_sem.at[3]).start()

            @pl.loop(0, d // 256)
            def _(t):
                at = pl.multiple_of(t * 256, 256)
                value = lax.dot_general(
                    att_v[...], w_a[pl.ds(at, 256), qkv_cols:], (((1,), (1,)), ((), ())), preferred_element_type=f32
                )
                part_a[:, :, :, pl.ds(at, 256)] = value.astype(bf16).reshape(2, 2, n, 256)

            own_rows = pltpu.make_async_copy(
                w_a.at[pl.ds(row(z, y), shard)], wa_all.at[s.dp], o_sem.at[4]
            )
            own_rows.start()
            to_c = remote(part_a.at[1 - c], ca_in, ra_put.at[0], ra_got.at[0], s.at_c)
            to_c.start()
            to_c.wait_recv()
            part_a[c, 1 - x] = (part_a[c, 1 - x].astype(f32) + ca_in[1 - x].astype(f32)).astype(bf16)
            to_x = remote(part_a.at[c, 1 - x], xa_in, ra_put.at[1], ra_got.at[1], s.at_x)
            to_x.start()
            acc[...] = part_a[c, x].astype(f32) + ca_in[x].astype(f32)
            to_x.wait_recv()

            @pl.loop(0, n // 16)
            def _(i):
                at = pl.ds(pl.multiple_of(i * 16, 16), 16)
                branch = acc[at, :] + xa_in[at, :].astype(f32)
                acc[at, :] = branch
                inverse = lax.rsqrt(jnp.mean(branch * branch, axis=-1, keepdims=True) + EPS)
                mine = pl.ds(pl.multiple_of((c * 2 + x) * n + i * 16, 16), 16)
                hidden = x_v[mine, :].astype(f32) + branch * inverse * full_gain[1:2, :]
                hid[at, :] = hidden
                inverse = lax.rsqrt(jnp.mean(hidden * hidden, axis=-1, keepdims=True) + EPS)
                buf[z, c, x, at, :] = (hidden * inverse * full_gain[2:3, :]).astype(bf16)

            to_c.wait_send()
            to_x.wait_send()
            pltpu.make_async_copy(full_gain, gains_out, o_sem.at[0]).wait()
            pltpu.make_async_copy(normed_v, normed_out, o_sem.at[1]).wait()
            pltpu.make_async_copy(qkv_v, qkv_out, o_sem.at[2]).wait()
            pltpu.make_async_copy(att_v, att_out, o_sem.at[3]).wait()
            own_rows.wait()

        pl.run_scoped(
            attention,
            pltpu.VMEM((count, d), bf16),
            pltpu.VMEM((count, d), bf16),
            pltpu.VMEM((count, qkv_cols), bf16),
            pltpu.VMEM((count, q_cols), bf16),
            pltpu.VMEM((2, 2, n, d), bf16),
            pltpu.VMEM((count, HD // 2), f32),
            pltpu.VMEM((count, HD // 2), f32),
            pltpu.VMEM((count, ROW_LEN), f32),
        )

        def ffn(part, gu, mid, tot):
            trade = Trade(s, buf, part, tot, c_in, x_in, z_in, sems)
            trade.pass_on(z)
            saved = [
                pltpu.make_async_copy(acc, branch_out, o_sem.at[0]),
                pltpu.make_async_copy(hid, hidden_out, o_sem.at[1]),
            ]
            for save in saved:
                save.start()

            def load(g, yy, own, slot, k):
                source = f_own(z, k) if own else f_at(g, yy, k)
                return pltpu.make_async_copy(source, (w_gu, w_dn)[k].at[pl.ds(row(g, yy), shard)], lf_sem.at[slot, k])

            for k in range(2):
                load(z, y, True, 0, k).start()

            def f_take(i, k):
                g = s.order(i)
                got(f_got.at[g, k], f_at(g, y, k))
                for over in range(1, width):
                    f_wide(g, False, over, k).start()
                load(g, y, False, i * width, k).start()

            def f_rest(k):
                for i in range(depth):
                    g = s.order(i)
                    for over in range(1, width):
                        yy = (y + width - over) % width
                        got(fy_got.at[g, over - 1, k], f_at(g, yy, k))
                        load(g, yy, False, i * width + over, k).start()
                for i in range(depth):
                    for over in range(width):
                        load(s.order(i), (y + width - over) % width, i + over == 0, i * width + over, k).wait()

            def gather(i):
                trade.take_rank(s.order(i))
                pltpu.make_async_copy(buf.at[s.order(i)], all_out.at[s.order(i)], g_sem.at[i, 0]).start()

            for i in range(1, depth):
                f_take(i, 0)
            for over in range(1, width):
                f_wide(z, True, over, 1).start()
            for i in range(1, depth):
                trade.take_z(s.order(i))
                f_hops(i, 1)
                gather(i - 1)
            gather(depth - 1)
            f_rest(0)

            def keep(g):
                return (
                    pltpu.make_async_copy(gu.at[g], gu_out.at[g], g_sem.at[g, 1]),
                    pltpu.make_async_copy(mid.at[g], mid_out.at[g], g_sem.at[g, 2]),
                )

            @pl.loop(0, depth)
            def _(i):
                @pl.when(i > 0)
                def _():
                    f_take(i, 1)

                g = s.order(depth - 1 - i)
                forward_group(g, buf, gu, mid, w_gu, share)
                for copy in keep(g):
                    copy.start()

            f_rest(1)
            at = pl.ds(row(z, y), shard)
            own_rows = [
                pltpu.make_async_copy((w_gu, w_dn)[k].at[at], f_at(z, y, k), o_sem.at[2 + k]) for k in range(2)
            ]
            for copy in own_rows:
                copy.start()

            @pl.loop(0, depth)
            def _(i):
                g = s.order(depth - 1 - i)
                put_part(part, g, mid, w_dn, n, d)
                trade.back_c(g).start()
                trade.add_c(g)

                @pl.when(jnp.logical_and(i == 1, ends))
                def _():
                    trade.add_xz(s.order(depth - 1))

            @pl.when(inner)
            def _():
                trade.add_xz(s.order(depth - 1))

            for i in reversed(range(depth - 1)):
                trade.add_xz(s.order(i))

            last = pltpu.make_async_copy(tot, ffw_out, o_sem.at[4])
            last.start()
            trade.settle()
            for i in range(depth):
                g = s.order(i)
                pltpu.make_async_copy(buf.at[g], all_out.at[g], g_sem.at[i, 0]).wait()
                for copy in keep(g):
                    copy.wait()
            for copy in saved + own_rows:
                copy.wait()
            last.wait()

        pl.run_scoped(
            ffn,
            pltpu.VMEM((depth, 2, 2, n, d), bf16),
            pltpu.VMEM((depth, count, 2 * share), bf16),
            pltpu.VMEM((depth, count, share), bf16),
            pltpu.VMEM((n, d), f32),
        )

        for k in range(1, dp_n):
            remote(gain_ref, gain_in.at[s.dp], g_put.at[k - 1], g_got.at[k - 1], ((s.dp + k) % dp_n, s.q)).wait_send()
        for i in range(depth):
            g = s.order(i)
            for k in range(2):

                @pl.when(jnp.logical_and(g <= z, s.high))
                def _():
                    a_hop(g, k, i == 0, True).wait_send()

                @pl.when(jnp.logical_and(g >= z, s.low))
                def _():
                    a_hop(g, k, i == 0, False).wait_send()

                for over in range(1, width):
                    a_wide(g, k, i == 0, over).wait_send()
            for k in range(2):
                for over in range(1, width):
                    f_wide(g, i == 0, over, k).wait_send()
                if i:
                    f_hop(g, k).wait_send()

    shape = jax.ShapeDtypeStruct
    outs = (
        shape((dp_n, shard, a_cols), bf16),
        shape((dp_n, shard, 2 * share), bf16),
        shape((dp_n, shard, share), bf16),
        shape((count, d), bf16),
        shape((count, qkv_cols), bf16),
        shape((count, q_cols), bf16),
        shape((n, d), f32),
        shape((n, d), f32),
        shape((8, d), f32),
        shape((depth, 2, 2, n, d), bf16),
        shape((depth, count, 2 * share), bf16),
        shape((depth, count, share), bf16),
        shape((n, d), f32),
    )
    operands = (inputs, w_attn, wide_blocks, slim_blocks, gains, cosine, sine, mask)
    anywhere = pl.BlockSpec(memory_space=pl.ANY)
    dma = pltpu.SemaphoreType.DMA
    return pl.pallas_call(
        kernel,
        out_shape=outs,
        in_specs=[anywhere] * len(operands),
        out_specs=tuple([anywhere] * len(outs)),
        scratch_shapes=Trade.buffers(depth, n, d)
        + [
            pltpu.VMEM((dp_n,) + gains.shape, bf16),
            pltpu.VMEM((2, n, d), bf16),
            pltpu.VMEM((n, d), bf16),
            pltpu.VMEM((n, d), f32),
            pltpu.VMEM((n, d), f32),
            pltpu.VMEM((8, d), f32),
            pltpu.VMEM((d, a_cols), bf16),
            pltpu.VMEM((d, 2 * share), bf16),
            pltpu.VMEM((d, share), bf16),
            dma((dp_n - 1,)),
            dma((dp_n - 1,)),
            dma((depth, 2)),
            dma((depth, 2)),
            dma((depth, 2)),
            dma((depth, 2, others)),
            dma((depth, 2, others)),
            dma((depth, 2)),
            dma((depth, 2)),
            dma((depth, others, 2)),
            dma((depth, others, 2)),
            dma((dp_n, 2)),
            dma((dp_n, 2)),
            dma((5,)),
            dma((5,)),
            dma((depth, 3)),
            dma((2,)),
            dma((2,)),
        ]
        + Trade.semaphores(depth),
        compiler_params=pltpu.CompilerParams(collective_id=1, has_side_effects=True, vmem_limit_bytes=66_000_000),
        name="forward",
    )(*operands)


def backward_kernel(grid, first, weights, saves, heads, kv_heads):
    depth, width, dp_n = grid.depth, grid.width, grid.dp
    n, d = first[0].shape
    count = 4 * n
    a_cols = weights[0].shape[1]
    shard = weights[1].shape[1]
    share = weights[2].shape[2]
    q_cols, k_cols = heads * HD, kv_heads * HD
    qkv_cols = q_cols + 2 * k_cols
    group = heads // kv_heads
    align = math.gcd(shard, 16)
    others = width - 1
    scale = 1.0 / math.sqrt(HD)
    half = d // 2
    strip = 3 * LANE
    lanes = shard + -shard % LANE
    f_cols = ((0, 2 * share), (2 * share, share))

    def kernel(
        ffw_ref, hid_ref, att_branch_ref, cot_ref, x_ref, gain_ref,
        wa_ref, wide_ref, slim_ref, gu_ref, tok_ref, mix_ref, normed_ref, qkv_ref, att_ref, cos_ref, sin_ref, mask_ref,
        out_all, gin_all, f_out, a_out, yf, ya, az, gains_out,
        buf, c_in, x_in, z_in, w_gu, w_dn, g_attn, acc, dbr, own_out, gain_v, gain_acc,
        gain_put, gain_got, gain_x, gain_c,
        in_sem, w_sem, s_sem, o_sem, t_put, t_got, fy_put, fy_got, fz_put, fz_got, ay_put, ay_got, az_put, au_got, ad_got,
        gg_put, gg_got, gt_put, gt_got, ra_put, ra_got, *sems,
    ):
        s = Spot(grid)
        z, y, x, c = s.z, s.y, s.x, s.c
        mine = pl.multiple_of((c * 2 + x) * n, n)

        def got(sem, ref):
            remote(ref, ref, sem, sem, s.at_x).wait_recv()

        def row(g, yy):
            return pl.ds(pl.multiple_of((g * width + yy) * shard, align), shard)

        def copy(src, dst, sem):
            return pltpu.make_async_copy(src, dst, sem)

        loads = []
        for p in range(dp_n):
            at = pl.ds(p * shard, shard)
            for k, (source, where) in enumerate(((wide_ref, w_gu), (slim_ref, w_dn))):
                loads.append(copy(source.at[p], where.at[at], w_sem.at[p, k]))

        barrier = pltpu.get_barrier_semaphore()
        for k in range(1, dp_n):
            signal(barrier, ((s.dp + k) % dp_n, s.q))
        signal(barrier, s.at_x)
        signal(barrier, s.at_c)

        def norm_back(field, gain, grad, slot):
            inverse = lax.rsqrt(jnp.mean(field * field, axis=-1, keepdims=True) + EPS)
            unit = field * inverse
            terms = grad * unit
            gain_acc[slot] += terms[:8] + terms[8:]
            scaled = grad * gain
            return inverse * (scaled - unit * jnp.mean(scaled * unit, axis=-1, keepdims=True))

        def rows16(i):
            return pl.ds(pl.multiple_of(i * 16, 16), 16)

        gain_acc[...] = jnp.zeros_like(gain_acc)

        def open_up(field_v, hid_v, cot_v):
            fills = [
                copy(gain_ref, gain_v, in_sem.at[0]),
                copy(ffw_ref, field_v, in_sem.at[1]),
                copy(hid_ref, hid_v, in_sem.at[2]),
                copy(cot_ref.at[pl.ds(mine, n)], cot_v, in_sem.at[3]),
            ]
            for fill in fills:
                fill.start()
            for load in loads:
                load.start()
            for fill in fills:
                fill.wait()

            @pl.loop(0, n // 16)
            def _(i):
                at = rows16(i)
                field, grad = field_v[at, :], cot_v[at, :].astype(f32)
                inverse = lax.rsqrt(jnp.mean(field * field, axis=-1, keepdims=True) + EPS)
                own_out[at, :] = (hid_v[at, :] + field * inverse * gain_v[3:4, :]).astype(bf16)
                buf[z, c, x, at, :] = norm_back(field, gain_v[3:4, :], grad, 3).astype(bf16)

        pl.run_scoped(open_up, pltpu.VMEM((n, d), f32), pltpu.VMEM((n, d), f32), pltpu.VMEM((n, d), bf16))
        pl.semaphore_wait(barrier, dp_n + 1)

        def f_wide(g, over, k):
            yy = (y + over) % width
            return remote(
                (w_gu, w_dn)[k].at[row(g, yy)],
                yf.at[over - 1, g, :, pl.ds(f_cols[k][0], f_cols[k][1])],
                fy_put.at[g, over - 1, k], fy_got.at[g, over - 1, k], s.at_wide(over),
            )

        def f_deep(g, slot, stage):
            return remote(stage.at[slot], f_out.at[z], fz_put.at[g], fz_got.at[z], s.at_depth(g))

        def a_wide(g, over):
            yy = (y + over) % width
            return remote(
                g_attn.at[row(g, yy)], ya.at[over - 1, g], ay_put.at[g, over - 1], ay_got.at[g, over - 1], s.at_wide(over)
            )

        def a_up(g, slot, stage):
            return remote(stage.at[slot, :, pl.ds(0, a_cols)], az.at[g], az_put.at[g], au_got.at[g], s.at_up)

        def a_dn(g, slot, stage):
            to = jnp.where(g == z - 1, depth, g)
            return remote(stage.at[slot, :, pl.ds(0, a_cols)], az.at[to], az_put.at[g], ad_got.at[g], s.at_dn)

        def a_left(g, slot, stage):
            @pl.when(g > z)
            def _():
                a_up(g, slot, stage).wait_send()

            @pl.when(g < z)
            def _():
                a_dn(g, slot, stage).wait_send()

        def f_sum(i, stage):
            g = s.order(i)
            slot = i % 2
            if i + 2 < depth:
                f_deep(s.order(i + 2), slot, stage).wait_send()
            own = [
                copy(where.at[row(g, y)], stage.at[slot, :, pl.ds(f_cols[k][0], f_cols[k][1])], s_sem.at[k])
                for k, where in enumerate((w_gu, w_dn))
            ]
            for part_copy in own:
                part_copy.start()
            for over in range(1, width):
                for k in range(2):
                    got(fy_got.at[g, over - 1, k], yf.at[over - 1, g, :, pl.ds(f_cols[k][0], f_cols[k][1])])
                bring = copy(yf.at[over - 1, g], stage.at[2], s_sem.at[2])
                bring.start()
                bring.wait()
                if over == 1:
                    for part_copy in own:
                        part_copy.wait()
                stage[slot] = (stage[slot].astype(f32) + stage[2].astype(f32)).astype(bf16)
            if width == 1:
                for part_copy in own:
                    part_copy.wait()
            if i:
                f_deep(g, slot, stage).start()
            else:
                copy(stage.at[slot], f_out.at[z], o_sem.at[0]).start()

        def a_sum(i, stage):
            g = s.order(i)
            slot = i % 2
            narrow = pl.ds(0, a_cols)
            if i + 2 < depth:
                a_left(s.order(i + 2), slot, stage)
            own = copy(g_attn.at[row(g, y)], stage.at[slot, :, narrow], s_sem.at[0])
            own.start()

            def add(source):
                bring = copy(source, stage.at[2, :, narrow], s_sem.at[2])
                bring.start()
                bring.wait()
                total = stage[slot, :, :a_cols].astype(f32) + stage[2, :, :a_cols].astype(f32)
                stage[slot, :, :a_cols] = total.astype(bf16)

            for over in range(1, width):
                got(ay_got.at[g, over - 1], ya.at[over - 1, g])
                if over == 1:
                    own.wait()
                add(ya.at[over - 1, g])
            if width == 1:
                own.wait()

            @pl.when(jnp.logical_and(g >= z, s.low))
            def _():
                got(au_got.at[g], az.at[g])
                add(az.at[g])

            @pl.when(jnp.logical_and(g <= z, s.high))
            def _():
                where = jnp.where(g == z, depth, g)
                got(ad_got.at[g], az.at[where])
                add(az.at[where])

            @pl.when(g > z)
            def _():
                a_up(g, slot, stage).start()

            @pl.when(g < z)
            def _():
                a_dn(g, slot, stage).start()

            if i == 0:
                copy(stage.at[slot, :, narrow], a_out, o_sem.at[1]).start()

        def ffn(part, mid, mix, strips):
            trade = Trade(s, buf, part, acc, c_in, x_in, z_in, sems)
            trade.pass_on(z)
            first_loads = loads + [copy(gu_ref, mid, in_sem.at[0])]
            first_loads[-1].start()
            mix_load = copy(mix_ref, mix, in_sem.at[1])
            mix_load.start()

            @pl.loop(1, depth + 1)
            def _(i):
                @pl.when(i < depth)
                def _():
                    trade.take_z(s.order(i))

                g = s.order(i - 1)
                trade.take_rank(g)

                @pl.when(i == 1)
                def _():
                    for load in first_loads:
                        load.wait()

                backward_group(g, buf, mid, mid, part, w_gu, w_dn, share)
                trade.back_c(g).start()

            n_strip = half // strip
            assert 2 * strip >= d // depth and n_strip > 2

            away = 1 - z // 2

            def strip_at(j):
                side = jnp.where(j < n_strip, away, 1 - away)
                return pl.multiple_of(side * half + j % n_strip * strip, strip)

            def bring(j):
                return copy(tok_ref.at[:, :, pl.ds(strip_at(j), strip)], strips.at[j % 2], in_sem.at[2 + j % 2])

            def weight_grads(j):
                bring(j).wait()
                rows = pl.ds(strip_at(j), strip)

                def product(left, right, where, cols):
                    where[rows, cols] = lax.dot_general(
                        left, right, (((0,), (0,)), ((), ())), preferred_element_type=f32
                    ).astype(bf16)

                @pl.loop(0, 2 * share // 256)
                def _(t):
                    cols = pl.ds(pl.multiple_of(t * 256, 256), 256)
                    left = strips[j % 2].reshape(depth * count, strip)
                    product(left, mid[:, :, cols].reshape(depth * count, 256), w_gu, cols)

                @pl.when(j + 2 < 2 * n_strip)
                def _():
                    bring(j + 2).start()

                for lo in range(0, share, 256):
                    hi = min(lo + 256, share)
                    left = buf[:, :, :, :, rows].reshape(depth * count, strip)
                    right = mix[:, :, lo:hi].reshape(depth * count, hi - lo)
                    product(left, right, w_dn, slice(lo, hi))

            def send_wide(g):
                for over in range(1, width):
                    for k in range(2):
                        f_wide(g, over, k).start()

            ends = jnp.logical_or(z == 0, z == depth - 1)
            inner = jnp.logical_not(ends)
            for j in range(2):
                bring(j).start()
            mix_load.wait()
            for i in reversed(range(depth)):
                trade.add_c(s.order(i))

            @pl.loop(0, 2 * n_strip)
            def _(j):
                weight_grads(j)

                @pl.when(jnp.logical_and(j == n_strip - 2, ends))
                def _():
                    trade.add_xz(s.order(3))

                @pl.when(jnp.logical_or(j == 1, j == n_strip - 1))
                def _():
                    send_wide(2 * away + jnp.where(j == 1, 0, 1))

                @pl.when(jnp.logical_and(j == n_strip, ends))
                def _():
                    trade.add_xz(s.order(2))

                @pl.when(jnp.logical_and(j == n_strip + 1, inner))
                def _():
                    trade.add_xz(s.order(3))

            send_wide(s.order(1))
            send_wide(z)

            @pl.when(inner)
            def _():
                trade.add_xz(s.order(2))

            trade.add_xz(s.order(1))
            trade.add_xz(z)
            trade.settle()

        pl.run_scoped(
            ffn,
            pltpu.VMEM((depth, 2, 2, n, d), bf16),
            pltpu.VMEM((depth, count, 2 * share), bf16),
            pltpu.VMEM((depth, count, share), bf16),
            pltpu.VMEM((2, depth, count, strip), bf16),
        )

        def hop_x(where, src, kind):
            return remote(src, where.at[c, x], t_put.at[kind, 0], t_got.at[kind, 0], s.at_x)

        def hop_c(where, src, kind):
            return remote(src, where.at[c, x], t_put.at[kind, 1], t_got.at[kind, 1], s.at_c)

        def hop_far(where, kind):
            return remote(where.at[c, 1 - x], where.at[c, 1 - x], t_put.at[kind, 2], t_got.at[kind, 2], s.at_c)

        def spread(where, src, kind):
            hop_x(where, src, kind).start()
            hop_c(where, src, kind).start()

        def spread_on(where, kind):
            got(t_got.at[kind, 0], where.at[c, 1 - x])
            hop_far(where, kind).start()

        def spread_end(where, kind):
            got(t_got.at[kind, 1], where.at[1 - c, x])
            got(t_got.at[kind, 2], where.at[1 - c, 1 - x])

        def attention(stage, w_a, normed_v, qkv_v, att_v, d_att, d_qkv, part_a, cos_v, sin_v, mask_v, field_v, other_v, cot_v):
            own_x = copy(x_ref.at[pl.ds(mine, n)], cot_v.at[1], in_sem.at[4])
            fills = [
                copy(hid_ref, field_v, in_sem.at[0]),
                copy(att_branch_ref, other_v, in_sem.at[1]),
                copy(cot_ref.at[pl.ds(mine, n)], cot_v.at[0], in_sem.at[2]),
            ]
            later = [
                copy(wa_ref, w_a, w_sem.at[0, 0]),
                copy(att_ref, att_v, w_sem.at[0, 1]),
                copy(qkv_ref, qkv_v, w_sem.at[1, 0]),
                copy(normed_ref, normed_v, w_sem.at[1, 1]),
                copy(cos_ref, cos_v, in_sem.at[5]),
                copy(sin_ref, sin_v, in_sem.at[6]),
                copy(mask_ref, mask_v, in_sem.at[7]),
                own_x,
            ]
            for fill in fills + later:
                fill.start()
            for fill in fills:
                fill.wait()

            @pl.loop(0, n // 16)
            def _(i):
                at = rows16(i)
                d_hidden = cot_v[0, at, :].astype(f32) + norm_back(field_v[at, :], gain_v[2:3, :], acc[at, :], 2)
                acc[at, :] = d_hidden
                dbr[c, x, at, :] = norm_back(other_v[at, :], gain_v[1:2, :], d_hidden, 1).astype(bf16)

            spread(dbr, dbr.at[c, x], 0)
            spread(out_all, own_out, 1)
            copy(own_out, out_all.at[c, x], o_sem.at[2]).start()
            for fill in later:
                fill.wait()
            spread_on(dbr, 0)
            f_sum(2, stage)
            spread_end(dbr, 0)

            for lo in range(0, q_cols, HD):
                value = jnp.dot(
                    dbr[...].reshape(count, d), w_a[:, qkv_cols + lo : qkv_cols + lo + HD], preferred_element_type=f32
                )
                d_att[:, lo : lo + HD] = value.astype(bf16)

            def turn(value, factor, at):
                low, high = value[:, : HD // 2], value[:, HD // 2 :]
                cosine, sine = cos_v[at, :], sin_v[at, :]
                return (low * cosine + high * sine) * factor, (high * cosine - low * sine) * factor

            def contract(left, right, dims):
                return lax.dot_general(left, right, ((dims[0], dims[1]), ((), ())), preferred_element_type=f32)

            @pl.loop(0, count // ROW_LEN)
            def _(r):
                at = pl.ds(pl.multiple_of(r * ROW_LEN, ROW_LEN), ROW_LEN)
                allowed = mask_v[at, :] > 0.5
                for kv in range(kv_heads):
                    k_at, v_at = q_cols + kv * HD, q_cols + k_cols + kv * HD
                    key, val = qkv_v[at, k_at : k_at + HD], qkv_v[at, v_at : v_at + HD]
                    d_key = jnp.zeros((ROW_LEN, HD), f32)
                    d_val = jnp.zeros((ROW_LEN, HD), f32)
                    for h in range(kv * group, (kv + 1) * group):
                        query = qkv_v[at, h * HD : (h + 1) * HD]
                        grad = d_att[at, h * HD : (h + 1) * HD]
                        bent = jnp.tanh(contract(query, key, ((1,), (1,))) / CAP)
                        expo = jnp.where(allowed, jnp.exp(CAP * bent), 0.0)
                        soft = expo / jnp.sum(expo, axis=-1, keepdims=True)
                        d_val = d_val + contract(soft.astype(bf16), grad, ((0,), (0,)))
                        d_probs = contract(grad, val, ((1,), (1,)))
                        d_soft = soft * (d_probs - jnp.sum(soft * d_probs, axis=-1, keepdims=True))
                        d_cap = (d_soft * (1.0 - bent * bent)).astype(bf16)
                        d_key = d_key + contract(d_cap, query, ((0,), (0,)))
                        low, high = turn(contract(d_cap, key, ((1,), (0,))), scale, at)
                        d_qkv[at, h * HD : h * HD + HD // 2] = low.astype(bf16)
                        d_qkv[at, h * HD + HD // 2 : (h + 1) * HD] = high.astype(bf16)
                    low, high = turn(d_key, 1.0, at)
                    d_qkv[at, k_at : k_at + HD // 2] = low.astype(bf16)
                    d_qkv[at, k_at + HD // 2 : k_at + HD] = high.astype(bf16)
                    d_qkv[at, v_at : v_at + HD] = d_val.astype(bf16)

            def attn_grads(side):
                at = pl.multiple_of(side * half, LANE)
                rows = pl.ds(at, half)
                for lo in range(0, qkv_cols, 256):
                    value = contract(normed_v[:, rows], d_qkv[:, lo : lo + 256], ((0,), (0,)))
                    g_attn[rows, lo : lo + 256] = value.astype(bf16)
                for lo in range(0, q_cols, 256):
                    value = contract(dbr[:, :, :, rows].reshape(count, half), att_v[:, lo : lo + 256], ((0,), (0,)))
                    g_attn[rows, qkv_cols + lo : qkv_cols + lo + 256] = value.astype(bf16)

            away = 1 - z // 2
            attn_grads(away)
            for i in (3, 2):
                for over in range(1, width):
                    a_wide(s.order(i), over).start()
            attn_grads(1 - away)
            for i in (1, 0):
                for over in range(1, width):
                    a_wide(s.order(i), over).start()

            @pl.loop(0, d // 256)
            def _(t):
                at = pl.multiple_of(t * 256, 256)
                value = lax.dot_general(
                    d_qkv[...], w_a[pl.ds(at, 256), :qkv_cols], (((1,), (1,)), ((), ())), preferred_element_type=f32
                )
                part_a[:, :, :, pl.ds(at, 256)] = value.astype(bf16).reshape(2, 2, n, 256)

            to_c = remote(part_a.at[1 - c], c_in.at[0], ra_put.at[0], ra_got.at[0], s.at_c)
            to_c.start()
            to_c.wait_recv()
            part_a[c, 1 - x] = (part_a[c, 1 - x].astype(f32) + c_in[0, 1 - x].astype(f32)).astype(bf16)
            to_x = remote(part_a.at[c, 1 - x], x_in.at[0], ra_put.at[1], ra_got.at[1], s.at_x)
            to_x.start()
            field_v[...] = part_a[c, x].astype(f32) + c_in[0, x].astype(f32)
            f_sum(1, stage)
            spread_on(out_all, 1)
            to_x.wait_recv()
            hop_x(out_all, own_out, 1).wait_send()
            hop_c(out_all, own_out, 1).wait_send()
            copy(own_out, out_all.at[c, x], o_sem.at[2]).wait()

            @pl.loop(0, n // 16)
            def _(i):
                at = rows16(i)
                grad = field_v[at, :] + x_in[0, at, :].astype(f32)
                d_source = norm_back(cot_v[1, at, :].astype(f32), gain_v[0:1, :], grad, 0)
                own_out[at, :] = (acc[at, :] + d_source).astype(bf16)

            to_c.wait_send()
            to_x.wait_send()
            spread(gin_all, own_out, 2)
            copy(own_out, gin_all.at[c, x], o_sem.at[3]).start()

        def finish(stage):
            f_sum(3, stage)
            pl.run_scoped(
                functools.partial(attention, stage),
                pltpu.VMEM((d, a_cols), bf16),
                pltpu.VMEM((count, d), bf16),
                pltpu.VMEM((count, qkv_cols), bf16),
                pltpu.VMEM((count, q_cols), bf16),
                pltpu.VMEM((count, q_cols), bf16),
                pltpu.VMEM((count, qkv_cols), bf16),
                pltpu.VMEM((2, 2, n, d), bf16),
                pltpu.VMEM((count, HD // 2), f32),
                pltpu.VMEM((count, HD // 2), f32),
                pltpu.VMEM((count, ROW_LEN), f32),
                pltpu.VMEM((n, d), f32),
                pltpu.VMEM((n, d), f32),
                pltpu.VMEM((2, n, d), bf16),
            )

            for k in range(4):
                gain_v[k : k + 1, :] = jnp.sum(gain_acc[k], axis=0, keepdims=True)
            whole = gain_v[...]
            for p in range(dp_n):
                turned = pltpu.roll(whole, (d - p * shard) % d, 1) if p else whole
                gain_put[p] = turned[:, :lanes]

            def gain_hop(k):
                to = (s.dp + k) % dp_n
                return remote(gain_put.at[to], gain_got.at[s.dp], gg_put.at[k - 1], gg_got.at[k - 1], (to, s.q))

            for k in range(1, dp_n):
                gain_hop(k).start()
            spread_on(gin_all, 2)
            f_sum(0, stage)

            f_deep(s.order(1), 1, stage).wait_send()
            copy(stage.at[0], f_out.at[z], o_sem.at[0]).wait()
            for i in reversed(range(depth)):
                a_sum(i, stage)

            for k in range(1, dp_n):
                got(gg_got.at[k - 1], gain_got.at[(s.dp + dp_n - k) % dp_n])
            total = gain_put[s.dp]
            for k in range(1, dp_n):
                total = total + gain_got[(s.dp + dp_n - k) % dp_n]
            gain_x[0] = total
            across = remote(gain_x.at[0], gain_x.at[1], gt_put.at[0], gt_got.at[0], s.at_x)
            across.start()
            across.wait_recv()
            gain_c[0] = gain_x[0] + gain_x[1]
            beside = remote(gain_c.at[0], gain_c.at[1], gt_put.at[1], gt_got.at[1], s.at_c)
            beside.start()
            beside.wait_recv()
            gain_c[2] = gain_c[0] + gain_c[1]
            copy(gain_c.at[2], gains_out, o_sem.at[4]).start()

            spread_end(out_all, 1)
            spread_end(gin_all, 2)
            for i in range(1, depth):
                g = s.order(i)
                got(fz_got.at[g], f_out.at[g])
            for i in range(depth):
                g = s.order(i)
                for over in range(1, width):
                    for k in range(2):
                        f_wide(g, over, k).wait_send()
                    a_wide(g, over).wait_send()
            a_left(s.order(1), 1, stage)
            for kind, where, src in ((0, dbr, dbr.at[c, x]), (1, out_all, own_out), (2, gin_all, own_out)):
                if kind != 1:
                    hop_x(where, src, kind).wait_send()
                    hop_c(where, src, kind).wait_send()
                hop_far(where, kind).wait_send()
            for k in range(1, dp_n):
                gain_hop(k).wait_send()
            across.wait_send()
            beside.wait_send()
            copy(stage.at[0, :, pl.ds(0, a_cols)], a_out, o_sem.at[1]).wait()
            copy(own_out, gin_all.at[c, x], o_sem.at[3]).wait()
            copy(gain_c.at[2], gains_out, o_sem.at[4]).wait()

        pl.run_scoped(finish, pltpu.VMEM((3, shard, 3 * share), bf16))

    shape = jax.ShapeDtypeStruct
    outs = (
        shape((2, 2, n, d), bf16),
        shape((2, 2, n, d), bf16),
        shape((depth, shard, 3 * share), bf16),
        shape((shard, a_cols), bf16),
        shape((max(others, 1), depth, shard, 3 * share), bf16),
        shape((max(others, 1), depth, shard, a_cols), bf16),
        shape((depth + 1, shard, a_cols), bf16),
        shape((8, lanes), f32),
    )
    operands = tuple(first) + tuple(weights) + tuple(saves)
    anywhere = pl.BlockSpec(memory_space=pl.ANY)
    dma = pltpu.SemaphoreType.DMA
    return pl.pallas_call(
        kernel,
        out_shape=outs,
        in_specs=[anywhere] * len(operands),
        out_specs=tuple([anywhere] * len(outs)),
        scratch_shapes=Trade.buffers(depth, n, d)
        + [
            pltpu.VMEM((d, 2 * share), bf16),
            pltpu.VMEM((d, share), bf16),
            pltpu.VMEM((d, a_cols), bf16),
            pltpu.VMEM((n, d), f32),
            pltpu.VMEM((2, 2, n, d), bf16),
            pltpu.VMEM((n, d), bf16),
            pltpu.VMEM((8, d), f32),
            pltpu.VMEM((4, 8, d), f32),
            pltpu.VMEM((dp_n, 8, lanes), f32),
            pltpu.VMEM((dp_n, 8, lanes), f32),
            pltpu.VMEM((2, 8, lanes), f32),
            pltpu.VMEM((3, 8, lanes), f32),
            dma((8,)),
            dma((dp_n, 2)),
            dma((3,)),
            dma((5,)),
            dma((3, 3)),
            dma((3, 3)),
            dma((depth, max(others, 1), 2)),
            dma((depth, max(others, 1), 2)),
            dma((depth,)),
            dma((depth,)),
            dma((depth, max(others, 1))),
            dma((depth, max(others, 1))),
            dma((depth,)),
            dma((depth,)),
            dma((depth,)),
            dma((dp_n - 1,)),
            dma((dp_n - 1,)),
            dma((2,)),
            dma((2,)),
            dma((2,)),
            dma((2,)),
        ]
        + Trade.semaphores(depth),
        compiler_params=pltpu.CompilerParams(collective_id=2, has_side_effects=True, vmem_limit_bytes=67_043_328),
        name="backward",
    )(*operands)


def unit_cuts(units, parts):
    tiles = units // LANE
    edges = [(tiles * k + parts - 1) // parts for k in range(parts + 1)]
    starts = [e * LANE for e in edges[:-1]]
    sizes = [(b - a) * LANE for a, b in zip(edges[:-1], edges[1:])]
    return starts, sizes, max(sizes)


def cut_units(block, cuts):
    starts, sizes, share = cuts
    return jnp.stack(
        [
            jnp.pad(block[:, a : a + n], ((0, 0), (0, share - n))) if n < share else block[:, a : a + n]
            for a, n in zip(starts, sizes)
        ]
    )


def join_units(blocks, cuts):
    starts, sizes, share = cuts
    return jnp.concatenate([blocks[k, :, :n] for k, n in enumerate(sizes)], axis=1)


def make_body(grid):
    def body(
        inputs,
        cotangent,
        segments,
        positions,
        w_query,
        w_key,
        w_value,
        w_output,
        w_gate,
        w_up,
        w_down,
        gain_attn,
        gain_post_attn,
        gain_ffw,
        gain_post_ffw,
    ):
        grid.here()
        count, width = inputs.shape
        shard = w_query.shape[0]
        group = HEADS // KV
        local_kv = w_key.shape[1] // HD
        local_heads = local_kv * group
        q_cols, k_cols = w_query.shape[1], w_key.shape[1]
        scale = 1.0 / math.sqrt(HD)
        part = count // grid.tensor
        rows = count // ROW_LEN
        cuts = unit_cuts(w_gate.shape[1], grid.depth)
        share = cuts[2]
        main = share // 256 * 256

        gains = 0.0
        line = lax.broadcasted_iota(jnp.int32, (16, shard + -shard % LANE), 0)
        for k, gain in enumerate((gain_attn, gain_post_attn, gain_ffw, gain_post_ffw)):
            gains = gains + jnp.where(line == k, jnp.pad(gain, (0, -shard % LANE)).astype(f32), 0.0)
        gains = gains.astype(bf16)
        angles = make_angles(positions, HD)[:, 0]
        cosine, sine = jnp.cos(angles), jnp.sin(angles)
        mask = row_mask(segments, rows, ROW_LEN).astype(f32).reshape(count, ROW_LEN)
        cut_gate, cut_up = cut_units(w_gate, cuts), cut_units(w_up, cuts)
        wide_blocks = jnp.concatenate(
            [cut_gate[:, :, :main], cut_up[:, :, :main], cut_gate[:, :, main:], cut_up[:, :, main:]], axis=2
        )
        slim_blocks = cut_units(w_down.T, cuts)
        w_attn = jnp.concatenate([w_query, w_key, w_value, w_output.T], axis=1)
        (full_attn, full_wide, full_slim, normed, qkv, attended, branch_attn, hidden, full_gains,
         all_normed, saved, mixed, branch_ffw) = forward_kernel(
            grid, inputs, w_attn, wide_blocks, slim_blocks, gains, cosine, sine,
            mask, local_heads, local_kv,
        )
        full_attn = full_attn.reshape(width, full_attn.shape[2])
        out_all, gin_all, blocks_ffn, grad_attn, _, _, _, d_gains = backward_kernel(
            grid,
            (branch_ffw, hidden, branch_attn, cotangent, inputs, full_gains),
            (full_attn, full_wide, full_slim),
            (saved, all_normed.reshape(grid.depth, count, width), mixed, normed, qkv, attended, cosine, sine, mask),
            local_heads, local_kv,
        )
        gate, upward = [], []
        for k, size in enumerate(cuts[1]):
            low, rest = min(size, main), max(size - main, 0)
            gate.append(blocks_ffn[k, :, :low])
            upward.append(blocks_ffn[k, :, main : main + low])
            if rest:
                gate.append(blocks_ffn[k, :, 2 * main : 2 * main + rest])
                upward.append(blocks_ffn[k, :, main + share : main + share + rest])
        grad_gate = jnp.concatenate(gate, axis=1).astype(f32)
        grad_up = jnp.concatenate(upward, axis=1).astype(f32)
        grad_down = join_units(blocks_ffn[:, :, 2 * share :], cuts).T.astype(f32)
        qkv_cols = q_cols + 2 * k_cols

        return (
            out_all.reshape(count, width),
            gin_all.reshape(count, width),
            grad_attn[:, :q_cols].astype(f32),
            grad_attn[:, q_cols : q_cols + k_cols].astype(f32),
            grad_attn[:, q_cols + k_cols : qkv_cols].astype(f32),
            grad_attn[:, qkv_cols:].T.astype(f32),
            grad_gate,
            grad_up,
            grad_down,
            d_gains[0, :shard],
            d_gains[1, :shard],
            d_gains[2, :shard],
            d_gains[3, :shard],
        )

    return body


def solution(mesh):
    placed = (
        P("dp", None),
        P("dp", None),
        P("dp"),
        P("dp"),
        P("dp", "tensor"),
        P("dp", "tensor"),
        P("dp", "tensor"),
        P("tensor", "dp"),
        P("dp", "tensor"),
        P("dp", "tensor"),
        P("tensor", "dp"),
        P("dp"),
        P("dp"),
        P("dp"),
        P("dp"),
    )
    return jax.shard_map(
        make_body(Grid(mesh)),
        mesh=mesh,
        in_specs=placed,
        out_specs=(
            P("dp", None),
            P("dp", None),
            P("dp", "tensor"),
            P("dp", "tensor"),
            P("dp", "tensor"),
            P("tensor", "dp"),
            P("dp", "tensor"),
            P("dp", "tensor"),
            P("tensor", "dp"),
            P("dp"),
            P("dp"),
            P("dp"),
            P("dp"),
        ),
        check_vma=False,
    )
```

```python
import functools
import math

import jax
import jax.numpy as jnp
from jax import lax
from jax.experimental import pallas as pl
from jax.experimental.pallas import tpu as pltpu
from jax.sharding import PartitionSpec as P

HEADS = 8
KV = 4
HD = 256
ROW_LEN = 128
LANE = 128


EPS = 1e-06
CAP = 50.0
THETA = 10000.0

f32 = jnp.float32
bf16 = jnp.bfloat16


def rms_scale(field, gain):
    inverse = lax.rsqrt(jnp.mean(field * field, axis=-1, keepdims=True) + EPS)
    return field * inverse * gain


def rms_back(field, gain, grad):
    inverse = lax.rsqrt(jnp.mean(field * field, axis=-1, keepdims=True) + EPS)
    unit = field * inverse
    d_gain = jnp.sum(grad * unit, axis=0)
    scaled = grad * gain
    d_field = inverse * (scaled - unit * jnp.mean(scaled * unit, axis=-1, keepdims=True))
    return d_field, d_gain


def geglu(gate, upward):
    return jax.nn.gelu(gate, approximate=True) * upward


def rotate(field, cosine, sine):
    half = field.shape[-1] // 2
    first = field[..., :half]
    second = field[..., half:]
    return jnp.concatenate(
        [first * cosine - second * sine, second * cosine + first * sine], axis=-1
    )


def make_angles(positions, head_size):
    half = head_size // 2
    freqs = THETA ** (-(jnp.arange(half).astype(f32) * 2.0) / head_size)
    return positions.astype(f32)[:, None, None] * freqs[None, None, :]


def row_mask(segments, rows, length):
    seg_rows = segments.reshape(rows, length)
    same = seg_rows[:, :, None] == seg_rows[:, None, :]
    index = jnp.arange(length)
    causal = index[:, None] >= index[None, :]
    return jnp.logical_and(same, causal[None])


def dot(left, right):
    return jnp.dot(left, right, preferred_element_type=f32)


def contract_rows(left, right):
    return lax.dot_general(left, right, (((0,), (0,)), ((), ())), preferred_element_type=f32)


def contract_cols(left, right):
    return lax.dot_general(left, right, (((1,), (1,)), ((), ())), preferred_element_type=f32)


class Grid:
    def __init__(self, mesh):
        self.dp = mesh.shape["dp"]
        self.tensor = mesh.shape["tensor"]
        self.depth = 4 if self.dp % 4 == 0 else (2 if self.dp % 2 == 0 else 1)
        self.width = self.dp // self.depth

    def here(self):
        index = lax.axis_index("dp")
        self.deep = index // self.width
        self.wide = lax.rem(index, self.width)
        self.rank = lax.axis_index("tensor")

    def shift(self, value, step):
        pairs = [
            (z * self.width + y, ((z + step) % self.depth) * self.width + y)
            for z in range(self.depth)
            for y in range(self.width)
        ]
        return lax.ppermute(value, "dp", pairs)

    def swap_wide(self, value, bit):
        pairs = [
            (z * self.width + y, z * self.width + (y ^ bit))
            for z in range(self.depth)
            for y in range(self.width)
        ]
        return lax.ppermute(value, "dp", pairs)

    def swap_rank(self, value, bit):
        return lax.ppermute(value, "tensor", [(q, q ^ bit) for q in range(self.tensor)])

    def wide_bits(self):
        return [1 << b for b in range(self.width.bit_length() - 1)]

    def rank_bits(self):
        return [1 << b for b in range(self.tensor.bit_length() - 1)]

    def reduce_width(self, full):
        rows, columns = full.shape[0] // self.dp, full.shape[1]
        held = full.reshape(self.depth, self.width, rows, columns)
        for bit in reversed(self.wide_bits()):
            held = held.reshape(self.depth, 2, bit, rows, columns)
            mine = lax.rem(self.wide // bit, 2)
            other = lax.dynamic_index_in_dim(held, 1 - mine, 1, keepdims=False)
            own = lax.dynamic_index_in_dim(held, mine, 1, keepdims=False)
            held = own + self.swap_wide(other, bit)
        return held.reshape(self.depth, rows, columns)

    def pick(self, held, step):
        to = lax.rem(self.deep + step, self.depth)
        return lax.dynamic_index_in_dim(held, to, 0, keepdims=False)

    def scatter_rows(self, full):
        held = self.reduce_width(full)
        total = self.pick(held, 0).astype(f32)
        for step in range(1, self.depth):
            total = total + self.shift(self.pick(held, step), step).astype(f32)
        return total

    def return_blocks(self, full):
        held = self.reduce_width(full)
        out = jnp.zeros_like(held)
        for step in range(self.depth):
            part = self.pick(held, step)
            part = part if step == 0 else self.shift(part, step)
            source = lax.rem(self.deep + self.depth - step, self.depth)
            out = lax.dynamic_update_slice(out, part[None], (source, 0, 0))
        return out

    def spread_rank(self, block):
        x, c = self.rank // 2, lax.rem(self.rank, 2)
        n, d = block.shape
        out = jnp.zeros((2, 2, n, d), block.dtype)
        for far_c in range(2):
            for far_x in range(2):
                part = block
                if far_x:
                    part = across
                if far_c:
                    part = self.swap_rank(part, 1)
                elif not far_x:
                    across = self.swap_rank(block, 2)
                out = lax.dynamic_update_slice(
                    out, part[None, None], (jnp.bitwise_xor(c, far_c), jnp.bitwise_xor(x, far_x), 0, 0)
                )
        return out.reshape(4 * n, d)

    def reduce_rank(self, full):
        x, c = self.rank // 2, lax.rem(self.rank, 2)
        held = full.reshape(2, 2, full.shape[0] // 4, full.shape[1])
        for at, bit in ((c, 1), (x, 2)):
            own = lax.dynamic_index_in_dim(held, at, 0, keepdims=False)
            other = lax.dynamic_index_in_dim(held, 1 - at, 0, keepdims=False)
            held = own + self.swap_rank(other, bit)
        return held


MESH = pl.DeviceIdType.MESH


class Spot:
    def __init__(self, grid):
        self.depth, self.width = grid.depth, grid.width
        self.dp = lax.axis_index("dp")
        self.q = lax.axis_index("tensor")
        self.z, self.y = self.dp // self.width, self.dp % self.width
        self.x, self.c = self.q // 2, self.q % 2
        self.at_x = (self.dp, (1 - self.x) * 2 + self.c)
        self.at_c = (self.dp, self.x * 2 + 1 - self.c)
        self.at_up = (self.dp + self.width, self.q)
        self.at_dn = (self.dp - self.width, self.q)
        self.low, self.high = self.z > 0, self.z < self.depth - 1

    def order(self, i):
        z = self.z
        near = z + 1 - 2 * (z % 2)
        middle = 2 - z // 2
        far = 3 * (1 - z // 2)
        return jnp.where(i == 0, z, jnp.where(i == 1, near, jnp.where(i == 2, middle, far)))

    def at_depth(self, z):
        return (z * self.width + self.y, self.q)

    def at_wide(self, over):
        return (self.z * self.width + (self.y + over) % self.width, self.q)


def remote(src, dst, put, got, device):
    return pltpu.make_async_remote_copy(
        src_ref=src, dst_ref=dst, send_sem=put, recv_sem=got, device_id=device, device_id_type=MESH
    )


def signal(semaphore, device):
    pl.semaphore_signal(semaphore, inc=1, device_id=device, device_id_type=MESH)


class Trade:
    def __init__(self, spot, buf, part, acc, c_in, x_in, z_in, sems):
        self.spot, self.buf, self.part, self.acc = spot, buf, part, acc
        self.c_in, self.x_in, self.z_in = c_in, x_in, z_in
        (self.z_up, self.z_dn, self.z_got, self.x_put, self.x_got, self.c_put, self.c_got,
         self.rc_put, self.rc_got, self.rx_put, self.rx_got, self.rz_put, self.ru_got, self.rd_got) = sems

    @staticmethod
    def semaphores(depth):
        dma = pltpu.SemaphoreType.DMA
        return [dma((depth,))] * 5 + [dma((depth, 2))] * 2 + [dma((depth,))] * 7

    @staticmethod
    def buffers(depth, n, d):
        return [
            pltpu.VMEM((depth, 2, 2, n, d), bf16),
            pltpu.VMEM((depth, 2, n, d), bf16),
            pltpu.VMEM((depth, n, d), bf16),
            pltpu.VMEM((depth + 1, n, d), bf16),
        ]

    def hop_up(self, g):
        s = self.spot
        return remote(self.buf.at[g, s.c, s.x], self.buf.at[g, s.c, s.x], self.z_up.at[g], self.z_got.at[g], s.at_up)

    def hop_dn(self, g):
        s = self.spot
        return remote(self.buf.at[g, s.c, s.x], self.buf.at[g, s.c, s.x], self.z_dn.at[g], self.z_got.at[g], s.at_dn)

    def hop_x(self, g):
        s = self.spot
        return remote(self.buf.at[g, s.c, s.x], self.buf.at[g, s.c, s.x], self.x_put.at[g], self.x_got.at[g], s.at_x)

    def hop_c(self, g, far):
        s = self.spot
        xx = (1 - s.x) if far else s.x
        return remote(
            self.buf.at[g, s.c, xx], self.buf.at[g, s.c, xx], self.c_put.at[g, int(far)], self.c_got.at[g, int(far)], s.at_c
        )

    def got(self, sem, ref):
        remote(ref, ref, sem, sem, self.spot.at_x).wait_recv()

    def pass_on(self, g):
        s = self.spot

        @pl.when(jnp.logical_and(g <= s.z, s.high))
        def _():
            self.hop_up(g).start()

        @pl.when(jnp.logical_and(g >= s.z, s.low))
        def _():
            self.hop_dn(g).start()

        self.hop_x(g).start()
        self.hop_c(g, False).start()

    def take_z(self, g):
        s = self.spot
        self.got(self.z_got.at[g], self.buf.at[g, s.c, s.x])
        self.pass_on(g)

    def take_rank(self, g):
        s = self.spot
        self.got(self.x_got.at[g], self.buf.at[g, s.c, 1 - s.x])
        self.hop_c(g, True).start()
        self.got(self.c_got.at[g, 0], self.buf.at[g, 1 - s.c, s.x])
        self.got(self.c_got.at[g, 1], self.buf.at[g, 1 - s.c, 1 - s.x])

    def back_c(self, g):
        s = self.spot
        return remote(self.part.at[g, 1 - s.c], self.c_in.at[g], self.rc_put.at[g], self.rc_got.at[g], s.at_c)

    def back_x(self, g):
        s = self.spot
        return remote(self.part.at[g, s.c, 1 - s.x], self.x_in.at[g], self.rx_put.at[g], self.rx_got.at[g], s.at_x)

    def back_up(self, g):
        s = self.spot
        return remote(self.part.at[g, s.c, s.x], self.z_in.at[g], self.rz_put.at[g], self.ru_got.at[g], s.at_up)

    def back_dn(self, g):
        s = self.spot
        slot = jnp.where(g == s.z - 1, s.depth, g)
        return remote(self.part.at[g, s.c, s.x], self.z_in.at[slot], self.rz_put.at[g], self.rd_got.at[g], s.at_dn)

    def add_c(self, g):
        s, part, c_in = self.spot, self.part, self.c_in
        self.got(self.rc_got.at[g], c_in.at[g])
        part[g, s.c, 1 - s.x] = (part[g, s.c, 1 - s.x].astype(f32) + c_in[g, 1 - s.x].astype(f32)).astype(bf16)
        self.back_x(g).start()
        part[g, s.c, s.x] = (part[g, s.c, s.x].astype(f32) + c_in[g, s.x].astype(f32)).astype(bf16)

    def add_xz(self, g):
        s, part, acc = self.spot, self.part, self.acc
        self.got(self.rx_got.at[g], self.x_in.at[g])
        acc[...] = part[g, s.c, s.x].astype(f32) + self.x_in[g].astype(f32)

        @pl.when(jnp.logical_and(g >= s.z, s.low))
        def _():
            self.got(self.ru_got.at[g], self.z_in.at[g])
            acc[...] += self.z_in[g].astype(f32)

        @pl.when(jnp.logical_and(g <= s.z, s.high))
        def _():
            slot = jnp.where(g == s.z, s.depth, g)
            self.got(self.rd_got.at[g], self.z_in.at[slot])
            acc[...] += self.z_in[slot].astype(f32)

        @pl.when(g > s.z)
        def _():
            part[g, s.c, s.x] = acc[...].astype(bf16)
            self.back_up(g).start()

        @pl.when(g < s.z)
        def _():
            part[g, s.c, s.x] = acc[...].astype(bf16)
            self.back_dn(g).start()

    def settle(self):
        s = self.spot

        @pl.loop(0, s.depth)
        def _(g):
            @pl.when(jnp.logical_and(g <= s.z, s.high))
            def _():
                self.hop_up(g).wait_send()

            @pl.when(jnp.logical_and(g >= s.z, s.low))
            def _():
                self.hop_dn(g).wait_send()

            self.hop_x(g).wait_send()
            self.hop_c(g, False).wait_send()
            self.hop_c(g, True).wait_send()
            self.back_c(g).wait_send()
            self.back_x(g).wait_send()

            @pl.when(g > s.z)
            def _():
                self.back_up(g).wait_send()

            @pl.when(g < s.z)
            def _():
                self.back_dn(g).wait_send()


def put_part(part, g, left, right, n, d):
    @pl.loop(0, d // 256)
    def _(t):
        at = pl.multiple_of(t * 256, 256)
        value = lax.dot_general(left[g], right[pl.ds(at, 256), :], (((1,), (1,)), ((), ())), preferred_element_type=f32)
        part[g, :, :, :, pl.ds(at, 256)] = value.astype(bf16).reshape(2, 2, n, 256)


def forward_group(g, buf, gu, mid, w_gu, share):
    n, d = buf.shape[3:]
    main = share // 256 * 256
    tokens = lambda: buf[g].reshape(4 * n, d)

    def save(lo, hi, gate, upward):
        inner = math.sqrt(2.0 / math.pi) * (gate + 0.044715 * gate * gate * gate)
        mid[g, :, lo:hi] = (0.5 * gate * (1.0 + jnp.tanh(inner)) * upward).astype(bf16)

    for lo in range(0, main, 256):
        hi = lo + 256
        gate = jnp.dot(tokens(), w_gu[:, lo:hi], preferred_element_type=f32)
        upward = jnp.dot(tokens(), w_gu[:, main + lo : main + hi], preferred_element_type=f32)
        gu[g, :, lo:hi] = gate.astype(bf16)
        gu[g, :, main + lo : main + hi] = upward.astype(bf16)
        save(lo, hi, gate, upward)
    if main < share:
        rest = share - main
        both = jnp.dot(tokens(), w_gu[:, 2 * main :], preferred_element_type=f32)
        gu[g, :, 2 * main :] = both.astype(bf16)
        save(main, share, both[:, :rest], both[:, rest:])


def backward_group(g, buf, gu, mid, part, w_gu, w_dn, share):
    n, d = buf.shape[3:]
    main = share // 256 * 256
    tokens = lambda: buf[g].reshape(4 * n, d)

    def pull(lo, hi, gate_at, up_at):
        grad = jnp.dot(tokens(), w_dn[:, lo:hi], preferred_element_type=f32)
        gate = gu[g, :, gate_at : gate_at + hi - lo].astype(f32)
        upward = gu[g, :, up_at : up_at + hi - lo].astype(f32)
        factor = math.sqrt(2.0 / math.pi)
        square = gate * gate
        curve = jnp.tanh(factor * gate * (1.0 + 0.044715 * square))
        half = 0.5 * (1.0 + curve)
        slope = half + 0.5 * gate * (1.0 - curve * curve) * factor * (1.0 + 3.0 * 0.044715 * square)
        mid[g, :, gate_at : gate_at + hi - lo] = (grad * upward * slope).astype(bf16)
        mid[g, :, up_at : up_at + hi - lo] = (grad * gate * half).astype(bf16)

    for lo in range(0, main, 256):
        pull(lo, lo + 256, lo, main + lo)
    if main < share:
        pull(main, share, 2 * main, main + share)
    put_part(part, g, mid, w_gu, n, d)


def forward_kernel(grid, inputs, w_attn, wide_blocks, slim_blocks, gains, cosine, sine, mask, heads, kv_heads):
    depth, width, dp_n = grid.depth, grid.width, grid.dp
    count, d = inputs.shape
    n = count // 4
    shard, a_cols = w_attn.shape
    q_cols, k_cols = heads * HD, kv_heads * HD
    qkv_cols = q_cols + 2 * k_cols
    share = slim_blocks.shape[2]
    group = heads // kv_heads
    align = math.gcd(shard, 16)
    parts = ((0, qkv_cols), (qkv_cols, q_cols))
    scale = 1.0 / math.sqrt(HD)
    others = width - 1

    def kernel(
        x_ref, wa_ref, blk_wide, blk_slim, gain_ref, cos_ref, sin_ref, mask_ref,
        wa_all, wide_all, slim_all, normed_out, qkv_out, att_out, branch_out, hidden_out, gains_out,
        all_out, gu_out, mid_out, ffw_out,
        buf, c_in, x_in, z_in, gain_in, ca_in, xa_in, acc, hid, full_gain, w_a, w_gu, w_dn,
        g_put, g_got, a_up, a_dn, a_got, ay_put, ay_got, f_put, f_got, fy_put, fy_got,
        la_sem, lf_sem, in_sem, o_sem, g_sem, ra_put, ra_got, *sems,
    ):
        s = Spot(grid)
        z, y, x, c = s.z, s.y, s.x, s.c

        def got(sem, ref):
            remote(ref, ref, sem, sem, s.at_x).wait_recv()

        def row(g, yy):
            return pl.multiple_of((g * width + yy) * shard, align)

        barrier = pltpu.get_barrier_semaphore()
        for k in range(1, dp_n):
            signal(barrier, ((s.dp + k) % dp_n, s.q))
        signal(barrier, s.at_x)
        signal(barrier, s.at_c)
        pl.semaphore_wait(barrier, dp_n + 1)

        def a_at(g, yy, k):
            return wa_all.at[g * width + yy, :, pl.ds(parts[k][0], parts[k][1])]

        def a_src(g, k, own):
            return wa_ref.at[:, pl.ds(parts[k][0], parts[k][1])] if own else a_at(g, y, k)

        def a_hop(g, k, own, up):
            return remote(
                a_src(g, k, own), a_at(g, y, k), (a_up if up else a_dn).at[g, k], a_got.at[g, k], s.at_up if up else s.at_dn
            )

        def a_wide(g, k, own, over):
            return remote(a_src(g, k, own), a_at(g, y, k), ay_put.at[g, k, over - 1], ay_got.at[g, k, over - 1], s.at_wide(over))

        def a_pass(g, k, own):
            @pl.when(jnp.logical_and(g <= z, s.high))
            def _():
                a_hop(g, k, own, True).start()

            @pl.when(jnp.logical_and(g >= z, s.low))
            def _():
                a_hop(g, k, own, False).start()

            for over in range(1, width):
                a_wide(g, k, own, over).start()

        def f_at(g, yy, k):
            return (wide_all, slim_all)[k].at[g * width + yy]

        def f_own(g, k):
            return (blk_wide, blk_slim)[k].at[g]

        def f_hop(to, k):
            return remote(f_own(to, k), f_at(z, y, k), f_put.at[to, k], f_got.at[z, k], s.at_depth(to))

        def f_wide(g, own, over, k):
            source = f_own(z, k) if own else f_at(g, y, k)
            return remote(source, f_at(g, y, k), fy_put.at[g, over - 1, k], fy_got.at[g, over - 1, k], s.at_wide(over))

        ends = jnp.logical_or(z == 0, z == depth - 1)
        inner = jnp.logical_not(ends)

        def f_hops(i, k):
            @pl.when(ends)
            def _():
                for j in {1: (1,), 2: (2,), 3: (3,)}.get(i, ()):
                    f_hop(s.order(j), k).start()

            @pl.when(inner)
            def _():
                for j in {3: (2, 3, 1)}.get(i, ()):
                    f_hop(s.order(j), k).start()

        for k in range(1, dp_n):
            remote(gain_ref, gain_in.at[s.dp], g_put.at[k - 1], g_got.at[k - 1], ((s.dp + k) % dp_n, s.q)).start()
        for k in range(2):
            a_pass(z, k, True)

        def attention(x_v, normed_v, qkv_v, att_v, part_a, cos_v, sin_v, mask_v):
            own_gain = pltpu.make_async_copy(gain_ref, gain_in.at[s.dp], in_sem.at[4])
            fills = [
                pltpu.make_async_copy(x_ref, x_v, in_sem.at[0]),
                pltpu.make_async_copy(cos_ref, cos_v, in_sem.at[1]),
                pltpu.make_async_copy(sin_ref, sin_v, in_sem.at[2]),
                pltpu.make_async_copy(mask_ref, mask_v, in_sem.at[3]),
                own_gain,
            ]
            for fill in fills:
                fill.start()

            def load(g, yy, k, own, slot):
                return pltpu.make_async_copy(
                    a_src(g, k, True) if own else a_at(g, yy, k),
                    w_a.at[pl.ds(row(g, yy), shard), pl.ds(parts[k][0], parts[k][1])],
                    la_sem.at[slot, k],
                )

            for k in range(2):
                load(z, y, k, True, 0).start()

            for k in range(1, dp_n):
                remote(
                    gain_in.at[0], gain_in.at[(s.dp + dp_n - k) % dp_n], g_put.at[k - 1], g_got.at[k - 1], s.at_x
                ).wait_recv()
            for fill in fills:
                fill.wait()
            whole = jnp.zeros((8, d), f32)
            for p in range(dp_n):
                one = gain_in[p].astype(f32)[:8]
                one = jnp.concatenate([one, jnp.zeros((8, d - one.shape[1]), f32)], axis=1)
                whole = whole + (pltpu.roll(one, p * shard, 1) if p else one)
            full_gain[...] = whole
            pltpu.make_async_copy(full_gain, gains_out, o_sem.at[0]).start()

            @pl.loop(0, count // 32)
            def _(i):
                at = pl.ds(pl.multiple_of(i * 32, 32), 32)
                value = x_v[at, :].astype(f32)
                inverse = lax.rsqrt(jnp.mean(value * value, axis=-1, keepdims=True) + EPS)
                normed_v[at, :] = (value * inverse * full_gain[0:1, :]).astype(bf16)

            pltpu.make_async_copy(normed_v, normed_out, o_sem.at[1]).start()

            for i in range(1, depth):
                g = s.order(i)
                for k in range(2):
                    got(a_got.at[g, k], a_at(g, y, k))
                    a_pass(g, k, False)
                    load(g, y, k, False, i * width).start()
                f_hops(i, 0)
            for over in range(1, width):
                f_wide(z, True, over, 0).start()
            for k in range(2):
                for i in range(depth):
                    g = s.order(i)
                    for over in range(1, width):
                        yy = (y + width - over) % width
                        got(ay_got.at[g, k, over - 1], a_at(g, yy, k))
                        load(g, yy, k, False, i * width + over).start()
                for i in range(depth):
                    g = s.order(i)
                    for over in range(width):
                        load(g, (y + width - over) % width, k, i + over == 0, i * width + over).wait()
                if k:
                    continue
                for h in range(heads + 2 * kv_heads):
                    value = jnp.dot(normed_v[...], w_a[:, h * HD : (h + 1) * HD], preferred_element_type=f32)
                    if h < heads + kv_heads:
                        half = HD // 2
                        first, second = value[:, :half], value[:, half:]
                        low = first * cos_v[...] - second * sin_v[...]
                        high = second * cos_v[...] + first * sin_v[...]
                        if h < heads:
                            low, high = low * scale, high * scale
                        qkv_v[:, h * HD : h * HD + half] = low.astype(bf16)
                        qkv_v[:, h * HD + half : (h + 1) * HD] = high.astype(bf16)
                    else:
                        qkv_v[:, h * HD : (h + 1) * HD] = value.astype(bf16)
                pltpu.make_async_copy(qkv_v, qkv_out, o_sem.at[2]).start()

                @pl.loop(0, count // ROW_LEN)
                def _(r):
                    at = pl.ds(pl.multiple_of(r * ROW_LEN, ROW_LEN), ROW_LEN)
                    allowed = mask_v[at, :] > 0.5
                    for h in range(heads):
                        kv = heads + h // group
                        scores = lax.dot_general(
                            qkv_v[at, h * HD : (h + 1) * HD],
                            qkv_v[at, kv * HD : (kv + 1) * HD],
                            (((1,), (1,)), ((), ())),
                            preferred_element_type=f32,
                        )
                        expo = jnp.where(allowed, jnp.exp(CAP * jnp.tanh(scores / CAP)), 0.0)
                        probs = (expo / jnp.sum(expo, axis=-1, keepdims=True)).astype(bf16)
                        kv = kv + kv_heads
                        value = jnp.dot(probs, qkv_v[at, kv * HD : (kv + 1) * HD], preferred_element_type=f32)
                        att_v[at, h * HD : (h + 1) * HD] = value.astype(bf16)

                pltpu.make_async_copy(att_v, att_out, o_sem.at[3]).start()

            @pl.loop(0, d // 256)
            def _(t):
                at = pl.multiple_of(t * 256, 256)
                value = lax.dot_general(
                    att_v[...], w_a[pl.ds(at, 256), qkv_cols:], (((1,), (1,)), ((), ())), preferred_element_type=f32
                )
                part_a[:, :, :, pl.ds(at, 256)] = value.astype(bf16).reshape(2, 2, n, 256)

            own_rows = pltpu.make_async_copy(
                w_a.at[pl.ds(row(z, y), shard)], wa_all.at[s.dp], o_sem.at[4]
            )
            own_rows.start()
            to_c = remote(part_a.at[1 - c], ca_in, ra_put.at[0], ra_got.at[0], s.at_c)
            to_c.start()
            to_c.wait_recv()
            part_a[c, 1 - x] = (part_a[c, 1 - x].astype(f32) + ca_in[1 - x].astype(f32)).astype(bf16)
            to_x = remote(part_a.at[c, 1 - x], xa_in, ra_put.at[1], ra_got.at[1], s.at_x)
            to_x.start()
            acc[...] = part_a[c, x].astype(f32) + ca_in[x].astype(f32)
            to_x.wait_recv()

            @pl.loop(0, n // 16)
            def _(i):
                at = pl.ds(pl.multiple_of(i * 16, 16), 16)
                branch = acc[at, :] + xa_in[at, :].astype(f32)
                acc[at, :] = branch
                inverse = lax.rsqrt(jnp.mean(branch * branch, axis=-1, keepdims=True) + EPS)
                mine = pl.ds(pl.multiple_of((c * 2 + x) * n + i * 16, 16), 16)
                hidden = x_v[mine, :].astype(f32) + branch * inverse * full_gain[1:2, :]
                hid[at, :] = hidden
                inverse = lax.rsqrt(jnp.mean(hidden * hidden, axis=-1, keepdims=True) + EPS)
                buf[z, c, x, at, :] = (hidden * inverse * full_gain[2:3, :]).astype(bf16)

            to_c.wait_send()
            to_x.wait_send()
            pltpu.make_async_copy(full_gain, gains_out, o_sem.at[0]).wait()
            pltpu.make_async_copy(normed_v, normed_out, o_sem.at[1]).wait()
            pltpu.make_async_copy(qkv_v, qkv_out, o_sem.at[2]).wait()
            pltpu.make_async_copy(att_v, att_out, o_sem.at[3]).wait()
            own_rows.wait()

        pl.run_scoped(
            attention,
            pltpu.VMEM((count, d), bf16),
            pltpu.VMEM((count, d), bf16),
            pltpu.VMEM((count, qkv_cols), bf16),
            pltpu.VMEM((count, q_cols), bf16),
            pltpu.VMEM((2, 2, n, d), bf16),
            pltpu.VMEM((count, HD // 2), f32),
            pltpu.VMEM((count, HD // 2), f32),
            pltpu.VMEM((count, ROW_LEN), f32),
        )

        def ffn(part, gu, mid, tot):
            trade = Trade(s, buf, part, tot, c_in, x_in, z_in, sems)
            trade.pass_on(z)
            saved = [
                pltpu.make_async_copy(acc, branch_out, o_sem.at[0]),
                pltpu.make_async_copy(hid, hidden_out, o_sem.at[1]),
            ]
            for save in saved:
                save.start()

            def load(g, yy, own, slot, k):
                source = f_own(z, k) if own else f_at(g, yy, k)
                return pltpu.make_async_copy(source, (w_gu, w_dn)[k].at[pl.ds(row(g, yy), shard)], lf_sem.at[slot, k])

            for k in range(2):
                load(z, y, True, 0, k).start()

            def f_take(i, k):
                g = s.order(i)
                got(f_got.at[g, k], f_at(g, y, k))
                for over in range(1, width):
                    f_wide(g, False, over, k).start()
                load(g, y, False, i * width, k).start()

            def f_rest(k):
                for i in range(depth):
                    g = s.order(i)
                    for over in range(1, width):
                        yy = (y + width - over) % width
                        got(fy_got.at[g, over - 1, k], f_at(g, yy, k))
                        load(g, yy, False, i * width + over, k).start()
                for i in range(depth):
                    for over in range(width):
                        load(s.order(i), (y + width - over) % width, i + over == 0, i * width + over, k).wait()

            def gather(i):
                trade.take_rank(s.order(i))
                pltpu.make_async_copy(buf.at[s.order(i)], all_out.at[s.order(i)], g_sem.at[i, 0]).start()

            for i in range(1, depth):
                f_take(i, 0)
            for over in range(1, width):
                f_wide(z, True, over, 1).start()
            for i in range(1, depth):
                trade.take_z(s.order(i))
                f_hops(i, 1)
                gather(i - 1)
            gather(depth - 1)
            f_rest(0)

            def keep(g):
                return (
                    pltpu.make_async_copy(gu.at[g], gu_out.at[g], g_sem.at[g, 1]),
                    pltpu.make_async_copy(mid.at[g], mid_out.at[g], g_sem.at[g, 2]),
                )

            @pl.loop(0, depth)
            def _(i):
                @pl.when(i > 0)
                def _():
                    f_take(i, 1)

                g = s.order(depth - 1 - i)
                forward_group(g, buf, gu, mid, w_gu, share)
                for copy in keep(g):
                    copy.start()

            f_rest(1)
            at = pl.ds(row(z, y), shard)
            own_rows = [
                pltpu.make_async_copy((w_gu, w_dn)[k].at[at], f_at(z, y, k), o_sem.at[2 + k]) for k in range(2)
            ]
            for copy in own_rows:
                copy.start()

            @pl.loop(0, depth)
            def _(i):
                g = s.order(depth - 1 - i)
                put_part(part, g, mid, w_dn, n, d)
                trade.back_c(g).start()
                trade.add_c(g)

                @pl.when(jnp.logical_and(i == 1, ends))
                def _():
                    trade.add_xz(s.order(depth - 1))

            @pl.when(inner)
            def _():
                trade.add_xz(s.order(depth - 1))

            for i in reversed(range(depth - 1)):
                trade.add_xz(s.order(i))

            last = pltpu.make_async_copy(tot, ffw_out, o_sem.at[4])
            last.start()
            trade.settle()
            for i in range(depth):
                g = s.order(i)
                pltpu.make_async_copy(buf.at[g], all_out.at[g], g_sem.at[i, 0]).wait()
                for copy in keep(g):
                    copy.wait()
            for copy in saved + own_rows:
                copy.wait()
            last.wait()

        pl.run_scoped(
            ffn,
            pltpu.VMEM((depth, 2, 2, n, d), bf16),
            pltpu.VMEM((depth, count, 2 * share), bf16),
            pltpu.VMEM((depth, count, share), bf16),
            pltpu.VMEM((n, d), f32),
        )

        for k in range(1, dp_n):
            remote(gain_ref, gain_in.at[s.dp], g_put.at[k - 1], g_got.at[k - 1], ((s.dp + k) % dp_n, s.q)).wait_send()
        for i in range(depth):
            g = s.order(i)
            for k in range(2):

                @pl.when(jnp.logical_and(g <= z, s.high))
                def _():
                    a_hop(g, k, i == 0, True).wait_send()

                @pl.when(jnp.logical_and(g >= z, s.low))
                def _():
                    a_hop(g, k, i == 0, False).wait_send()

                for over in range(1, width):
                    a_wide(g, k, i == 0, over).wait_send()
            for k in range(2):
                for over in range(1, width):
                    f_wide(g, i == 0, over, k).wait_send()
                if i:
                    f_hop(g, k).wait_send()

    shape = jax.ShapeDtypeStruct
    outs = (
        shape((dp_n, shard, a_cols), bf16),
        shape((dp_n, shard, 2 * share), bf16),
        shape((dp_n, shard, share), bf16),
        shape((count, d), bf16),
        shape((count, qkv_cols), bf16),
        shape((count, q_cols), bf16),
        shape((n, d), f32),
        shape((n, d), f32),
        shape((8, d), f32),
        shape((depth, 2, 2, n, d), bf16),
        shape((depth, count, 2 * share), bf16),
        shape((depth, count, share), bf16),
        shape((n, d), f32),
    )
    operands = (inputs, w_attn, wide_blocks, slim_blocks, gains, cosine, sine, mask)
    anywhere = pl.BlockSpec(memory_space=pl.ANY)
    dma = pltpu.SemaphoreType.DMA
    return pl.pallas_call(
        kernel,
        out_shape=outs,
        in_specs=[anywhere] * len(operands),
        out_specs=tuple([anywhere] * len(outs)),
        scratch_shapes=Trade.buffers(depth, n, d)
        + [
            pltpu.VMEM((dp_n,) + gains.shape, bf16),
            pltpu.VMEM((2, n, d), bf16),
            pltpu.VMEM((n, d), bf16),
            pltpu.VMEM((n, d), f32),
            pltpu.VMEM((n, d), f32),
            pltpu.VMEM((8, d), f32),
            pltpu.VMEM((d, a_cols), bf16),
            pltpu.VMEM((d, 2 * share), bf16),
            pltpu.VMEM((d, share), bf16),
            dma((dp_n - 1,)),
            dma((dp_n - 1,)),
            dma((depth, 2)),
            dma((depth, 2)),
            dma((depth, 2)),
            dma((depth, 2, others)),
            dma((depth, 2, others)),
            dma((depth, 2)),
            dma((depth, 2)),
            dma((depth, others, 2)),
            dma((depth, others, 2)),
            dma((dp_n, 2)),
            dma((dp_n, 2)),
            dma((5,)),
            dma((5,)),
            dma((depth, 3)),
            dma((2,)),
            dma((2,)),
        ]
        + Trade.semaphores(depth),
        compiler_params=pltpu.CompilerParams(collective_id=1, has_side_effects=True, vmem_limit_bytes=66_000_000),
        name="forward",
    )(*operands)


def backward_kernel(grid, first, weights, saves, heads, kv_heads, sizes):
    depth, width, dp_n = grid.depth, grid.width, grid.dp
    n, d = first[0].shape
    count = 4 * n
    a_cols = weights[0].shape[1]
    shard = weights[1].shape[1]
    share = weights[2].shape[2]
    q_cols, k_cols = heads * HD, kv_heads * HD
    qkv_cols = q_cols + 2 * k_cols
    group = heads // kv_heads
    align = math.gcd(shard, 16)
    others = width - 1
    scale = 1.0 / math.sqrt(HD)
    half = d // 2
    strip = 3 * LANE
    lanes = shard + -shard % LANE
    f_cols = ((0, 2 * share), (2 * share, share))
    main = share // 256 * 256
    f_parts = ((0, 2 * main), (2 * share, main))
    if main < share:
        f_parts = f_parts + ((2 * main, 2 * (share - main)), (2 * share + main, share - main))
    assert min(sizes) >= main

    def kernel(
        ffw_ref, hid_ref, att_branch_ref, cot_ref, x_ref, gain_ref,
        wa_ref, wide_ref, slim_ref, gu_ref, tok_ref, mix_ref, normed_ref, qkv_ref, att_ref, cos_ref, sin_ref, mask_ref,
        out_all, gin_all, f_out, a_out, yf, ya, az, gains_out,
        buf, c_in, x_in, z_in, w_gu, w_dn, g_attn, acc, dbr, own_out, gain_v, gain_acc,
        gain_put, gain_got, gain_x, gain_c,
        in_sem, w_sem, s_sem, o_sem, t_put, t_got, fy_put, fy_got, fz_put, fz_got, ay_put, ay_got, az_put, au_got, ad_got,
        gg_put, gg_got, gt_put, gt_got, ra_put, ra_got, *sems,
    ):
        s = Spot(grid)
        z, y, x, c = s.z, s.y, s.x, s.c
        mine = pl.multiple_of((c * 2 + x) * n, n)

        def got(sem, ref):
            remote(ref, ref, sem, sem, s.at_x).wait_recv()

        def row(g, yy):
            return pl.ds(pl.multiple_of((g * width + yy) * shard, align), shard)

        def copy(src, dst, sem):
            return pltpu.make_async_copy(src, dst, sem)

        loads = []
        for p in range(dp_n):
            at = pl.ds(p * shard, shard)
            for k, (source, where) in enumerate(((wide_ref, w_gu), (slim_ref, w_dn))):
                loads.append(copy(source.at[p], where.at[at], w_sem.at[p, k]))

        barrier = pltpu.get_barrier_semaphore()
        for k in range(1, dp_n):
            signal(barrier, ((s.dp + k) % dp_n, s.q))
        signal(barrier, s.at_x)
        signal(barrier, s.at_c)

        def norm_back(field, gain, grad, slot):
            inverse = lax.rsqrt(jnp.mean(field * field, axis=-1, keepdims=True) + EPS)
            unit = field * inverse
            terms = grad * unit
            gain_acc[slot] += terms[:8] + terms[8:]
            scaled = grad * gain
            return inverse * (scaled - unit * jnp.mean(scaled * unit, axis=-1, keepdims=True))

        def rows16(i):
            return pl.ds(pl.multiple_of(i * 16, 16), 16)

        gain_acc[...] = jnp.zeros_like(gain_acc)

        def open_up(field_v, hid_v, cot_v):
            fills = [
                copy(gain_ref, gain_v, in_sem.at[0]),
                copy(ffw_ref, field_v, in_sem.at[1]),
                copy(hid_ref, hid_v, in_sem.at[2]),
                copy(cot_ref.at[pl.ds(mine, n)], cot_v, in_sem.at[3]),
            ]
            for fill in fills:
                fill.start()
            for load in loads:
                load.start()
            for fill in fills:
                fill.wait()

            @pl.loop(0, n // 16)
            def _(i):
                at = rows16(i)
                field, grad = field_v[at, :], cot_v[at, :].astype(f32)
                inverse = lax.rsqrt(jnp.mean(field * field, axis=-1, keepdims=True) + EPS)
                own_out[at, :] = (hid_v[at, :] + field * inverse * gain_v[3:4, :]).astype(bf16)
                buf[z, c, x, at, :] = norm_back(field, gain_v[3:4, :], grad, 3).astype(bf16)

        pl.run_scoped(open_up, pltpu.VMEM((n, d), f32), pltpu.VMEM((n, d), f32), pltpu.VMEM((n, d), bf16))
        pl.semaphore_wait(barrier, dp_n + 1)

        def f_wide(g, over, k):
            yy = (y + over) % width
            return remote(
                (w_gu, w_dn)[k].at[row(g, yy)],
                yf.at[over - 1, g, :, pl.ds(f_cols[k][0], f_cols[k][1])],
                fy_put.at[g, over - 1, k], fy_got.at[g, over - 1, k], s.at_wide(over),
            )

        def full(g):
            return functools.reduce(jnp.logical_or, [g == k for k in range(depth) if sizes[k] > main] or [g < 0])

        def f_deep(g, slot, stage, p):
            cols = pl.ds(f_parts[p][0], f_parts[p][1])
            return remote(stage.at[slot, :, cols], f_out.at[z, :, cols], fz_put.at[g, p], fz_got.at[z, p], s.at_depth(g))

        def f_deeps(do):
            for p in (0, 1):
                do(p)
            if len(f_parts) > 2:

                @pl.when(full(z))
                def _():
                    for p in (2, 3):
                        do(p)

        def a_wide(g, over):
            yy = (y + over) % width
            return remote(
                g_attn.at[row(g, yy)], ya.at[over - 1, g], ay_put.at[g, over - 1], ay_got.at[g, over - 1], s.at_wide(over)
            )

        def a_up(g, slot, stage):
            return remote(stage.at[slot, :, pl.ds(0, a_cols)], az.at[g], az_put.at[g], au_got.at[g], s.at_up)

        def a_dn(g, slot, stage):
            to = jnp.where(g == z - 1, depth, g)
            return remote(stage.at[slot, :, pl.ds(0, a_cols)], az.at[to], az_put.at[g], ad_got.at[g], s.at_dn)

        def a_left(g, slot, stage):
            @pl.when(g > z)
            def _():
                a_up(g, slot, stage).wait_send()

            @pl.when(g < z)
            def _():
                a_dn(g, slot, stage).wait_send()

        def f_sum(i, stage):
            g = s.order(i)
            slot = i % 2
            if i + 2 < depth:
                f_deeps(lambda p: f_deep(s.order(i + 2), slot, stage, p).wait_send())
            own = [
                copy(where.at[row(g, y)], stage.at[slot, :, pl.ds(f_cols[k][0], f_cols[k][1])], s_sem.at[k])
                for k, where in enumerate((w_gu, w_dn))
            ]
            for part_copy in own:
                part_copy.start()
            for over in range(1, width):
                for k in range(2):
                    got(fy_got.at[g, over - 1, k], yf.at[over - 1, g, :, pl.ds(f_cols[k][0], f_cols[k][1])])
                bring = copy(yf.at[over - 1, g], stage.at[2], s_sem.at[2])
                bring.start()
                bring.wait()
                if over == 1:
                    for part_copy in own:
                        part_copy.wait()
                stage[slot] = (stage[slot].astype(f32) + stage[2].astype(f32)).astype(bf16)
            if width == 1:
                for part_copy in own:
                    part_copy.wait()
            if i:
                f_deeps(lambda p: f_deep(g, slot, stage, p).start())
            else:
                copy(stage.at[slot], f_out.at[z], o_sem.at[0]).start()

        def a_sum(i, stage):
            g = s.order(i)
            slot = i % 2
            narrow = pl.ds(0, a_cols)
            if i + 2 < depth:
                a_left(s.order(i + 2), slot, stage)
            own = copy(g_attn.at[row(g, y)], stage.at[slot, :, narrow], s_sem.at[0])
            own.start()

            def add(source):
                bring = copy(source, stage.at[2, :, narrow], s_sem.at[2])
                bring.start()
                bring.wait()
                total = stage[slot, :, :a_cols].astype(f32) + stage[2, :, :a_cols].astype(f32)
                stage[slot, :, :a_cols] = total.astype(bf16)

            for over in range(1, width):
                got(ay_got.at[g, over - 1], ya.at[over - 1, g])
                if over == 1:
                    own.wait()
                add(ya.at[over - 1, g])
            if width == 1:
                own.wait()

            @pl.when(jnp.logical_and(g >= z, s.low))
            def _():
                got(au_got.at[g], az.at[g])
                add(az.at[g])

            @pl.when(jnp.logical_and(g <= z, s.high))
            def _():
                where = jnp.where(g == z, depth, g)
                got(ad_got.at[g], az.at[where])
                add(az.at[where])

            @pl.when(g > z)
            def _():
                a_up(g, slot, stage).start()

            @pl.when(g < z)
            def _():
                a_dn(g, slot, stage).start()

            if i == 0:
                copy(stage.at[slot, :, narrow], a_out, o_sem.at[1]).start()

        def ffn(part, mid, mix, strips):
            trade = Trade(s, buf, part, acc, c_in, x_in, z_in, sems)
            trade.pass_on(z)
            first_loads = loads + [copy(gu_ref, mid, in_sem.at[0])]
            first_loads[-1].start()
            mix_load = copy(mix_ref, mix, in_sem.at[1])
            mix_load.start()

            @pl.loop(1, depth + 1)
            def _(i):
                @pl.when(i < depth)
                def _():
                    trade.take_z(s.order(i))

                g = s.order(i - 1)
                trade.take_rank(g)

                @pl.when(i == 1)
                def _():
                    for load in first_loads:
                        load.wait()

                backward_group(g, buf, mid, mid, part, w_gu, w_dn, share)
                trade.back_c(g).start()

            n_strip = half // strip
            assert 2 * strip >= d // depth and n_strip > 2

            away = 1 - z // 2

            def strip_at(j):
                side = jnp.where(j < n_strip, away, 1 - away)
                return pl.multiple_of(side * half + j % n_strip * strip, strip)

            def bring(j):
                return copy(tok_ref.at[:, :, pl.ds(strip_at(j), strip)], strips.at[j % 2], in_sem.at[2 + j % 2])

            def weight_grads(j):
                bring(j).wait()
                rows = pl.ds(strip_at(j), strip)

                def product(left, right, where, cols):
                    where[rows, cols] = lax.dot_general(
                        left, right, (((0,), (0,)), ((), ())), preferred_element_type=f32
                    ).astype(bf16)

                @pl.loop(0, 2 * share // 256)
                def _(t):
                    cols = pl.ds(pl.multiple_of(t * 256, 256), 256)
                    left = strips[j % 2].reshape(depth * count, strip)
                    product(left, mid[:, :, cols].reshape(depth * count, 256), w_gu, cols)

                @pl.when(j + 2 < 2 * n_strip)
                def _():
                    bring(j + 2).start()

                for lo in range(0, share, 256):
                    hi = min(lo + 256, share)
                    left = buf[:, :, :, :, rows].reshape(depth * count, strip)
                    right = mix[:, :, lo:hi].reshape(depth * count, hi - lo)
                    product(left, right, w_dn, slice(lo, hi))

            def send_wide(g):
                for over in range(1, width):
                    for k in range(2):
                        f_wide(g, over, k).start()

            ends = jnp.logical_or(z == 0, z == depth - 1)
            inner = jnp.logical_not(ends)
            for j in range(2):
                bring(j).start()
            mix_load.wait()
            for i in reversed(range(depth)):
                trade.add_c(s.order(i))

            @pl.loop(0, 2 * n_strip)
            def _(j):
                weight_grads(j)

                @pl.when(jnp.logical_and(j == n_strip - 2, ends))
                def _():
                    trade.add_xz(s.order(3))

                @pl.when(jnp.logical_or(j == 1, j == n_strip - 1))
                def _():
                    send_wide(2 * away + jnp.where(j == 1, 0, 1))

                @pl.when(jnp.logical_and(j == n_strip, ends))
                def _():
                    trade.add_xz(s.order(2))

                @pl.when(jnp.logical_and(j == n_strip + 1, inner))
                def _():
                    trade.add_xz(s.order(3))

            send_wide(s.order(1))
            send_wide(z)

            @pl.when(inner)
            def _():
                trade.add_xz(s.order(2))

            trade.add_xz(s.order(1))
            trade.add_xz(z)
            trade.settle()

        pl.run_scoped(
            ffn,
            pltpu.VMEM((depth, 2, 2, n, d), bf16),
            pltpu.VMEM((depth, count, 2 * share), bf16),
            pltpu.VMEM((depth, count, share), bf16),
            pltpu.VMEM((2, depth, count, strip), bf16),
        )

        def hop_x(where, src, kind):
            return remote(src, where.at[c, x], t_put.at[kind, 0], t_got.at[kind, 0], s.at_x)

        def hop_c(where, src, kind):
            return remote(src, where.at[c, x], t_put.at[kind, 1], t_got.at[kind, 1], s.at_c)

        def hop_far(where, kind):
            return remote(where.at[c, 1 - x], where.at[c, 1 - x], t_put.at[kind, 2], t_got.at[kind, 2], s.at_c)

        def spread(where, src, kind):
            hop_x(where, src, kind).start()
            hop_c(where, src, kind).start()

        def spread_on(where, kind):
            got(t_got.at[kind, 0], where.at[c, 1 - x])
            hop_far(where, kind).start()

        def spread_end(where, kind):
            got(t_got.at[kind, 1], where.at[1 - c, x])
            got(t_got.at[kind, 2], where.at[1 - c, 1 - x])

        def attention(stage, w_a, normed_v, qkv_v, att_v, d_att, d_qkv, part_a, cos_v, sin_v, mask_v, field_v, other_v, cot_v):
            own_x = copy(x_ref.at[pl.ds(mine, n)], cot_v.at[1], in_sem.at[4])
            fills = [
                copy(hid_ref, field_v, in_sem.at[0]),
                copy(att_branch_ref, other_v, in_sem.at[1]),
                copy(cot_ref.at[pl.ds(mine, n)], cot_v.at[0], in_sem.at[2]),
            ]
            later = [
                copy(wa_ref, w_a, w_sem.at[0, 0]),
                copy(att_ref, att_v, w_sem.at[0, 1]),
                copy(qkv_ref, qkv_v, w_sem.at[1, 0]),
                copy(normed_ref, normed_v, w_sem.at[1, 1]),
                copy(cos_ref, cos_v, in_sem.at[5]),
                copy(sin_ref, sin_v, in_sem.at[6]),
                copy(mask_ref, mask_v, in_sem.at[7]),
                own_x,
            ]
            for fill in fills + later:
                fill.start()
            for fill in fills:
                fill.wait()

            @pl.loop(0, n // 16)
            def _(i):
                at = rows16(i)
                d_hidden = cot_v[0, at, :].astype(f32) + norm_back(field_v[at, :], gain_v[2:3, :], acc[at, :], 2)
                acc[at, :] = d_hidden
                dbr[c, x, at, :] = norm_back(other_v[at, :], gain_v[1:2, :], d_hidden, 1).astype(bf16)

            spread(dbr, dbr.at[c, x], 0)
            spread(out_all, own_out, 1)
            copy(own_out, out_all.at[c, x], o_sem.at[2]).start()
            for fill in later:
                fill.wait()
            spread_on(dbr, 0)
            f_sum(2, stage)
            spread_end(dbr, 0)

            for lo in range(0, q_cols, HD):
                value = jnp.dot(
                    dbr[...].reshape(count, d), w_a[:, qkv_cols + lo : qkv_cols + lo + HD], preferred_element_type=f32
                )
                d_att[:, lo : lo + HD] = value.astype(bf16)

            def turn(value, factor, at):
                low, high = value[:, : HD // 2], value[:, HD // 2 :]
                cosine, sine = cos_v[at, :], sin_v[at, :]
                return (low * cosine + high * sine) * factor, (high * cosine - low * sine) * factor

            def contract(left, right, dims):
                return lax.dot_general(left, right, ((dims[0], dims[1]), ((), ())), preferred_element_type=f32)

            @pl.loop(0, count // ROW_LEN)
            def _(r):
                at = pl.ds(pl.multiple_of(r * ROW_LEN, ROW_LEN), ROW_LEN)
                allowed = mask_v[at, :] > 0.5
                for kv in range(kv_heads):
                    k_at, v_at = q_cols + kv * HD, q_cols + k_cols + kv * HD
                    key, val = qkv_v[at, k_at : k_at + HD], qkv_v[at, v_at : v_at + HD]
                    d_key = jnp.zeros((ROW_LEN, HD), f32)
                    d_val = jnp.zeros((ROW_LEN, HD), f32)
                    for h in range(kv * group, (kv + 1) * group):
                        query = qkv_v[at, h * HD : (h + 1) * HD]
                        grad = d_att[at, h * HD : (h + 1) * HD]
                        bent = jnp.tanh(contract(query, key, ((1,), (1,))) / CAP)
                        expo = jnp.where(allowed, jnp.exp(CAP * bent), 0.0)
                        soft = expo / jnp.sum(expo, axis=-1, keepdims=True)
                        d_val = d_val + contract(soft.astype(bf16), grad, ((0,), (0,)))
                        d_probs = contract(grad, val, ((1,), (1,)))
                        d_soft = soft * (d_probs - jnp.sum(soft * d_probs, axis=-1, keepdims=True))
                        d_cap = (d_soft * (1.0 - bent * bent)).astype(bf16)
                        d_key = d_key + contract(d_cap, query, ((0,), (0,)))
                        low, high = turn(contract(d_cap, key, ((1,), (0,))), scale, at)
                        d_qkv[at, h * HD : h * HD + HD // 2] = low.astype(bf16)
                        d_qkv[at, h * HD + HD // 2 : (h + 1) * HD] = high.astype(bf16)
                    low, high = turn(d_key, 1.0, at)
                    d_qkv[at, k_at : k_at + HD // 2] = low.astype(bf16)
                    d_qkv[at, k_at + HD // 2 : k_at + HD] = high.astype(bf16)
                    d_qkv[at, v_at : v_at + HD] = d_val.astype(bf16)

            def attn_grads(side):
                at = pl.multiple_of(side * half, LANE)
                rows = pl.ds(at, half)
                for lo in range(0, qkv_cols, 256):
                    value = contract(normed_v[:, rows], d_qkv[:, lo : lo + 256], ((0,), (0,)))
                    g_attn[rows, lo : lo + 256] = value.astype(bf16)
                for lo in range(0, q_cols, 256):
                    value = contract(dbr[:, :, :, rows].reshape(count, half), att_v[:, lo : lo + 256], ((0,), (0,)))
                    g_attn[rows, qkv_cols + lo : qkv_cols + lo + 256] = value.astype(bf16)

            away = 1 - z // 2
            attn_grads(away)
            for i in (3, 2):
                for over in range(1, width):
                    a_wide(s.order(i), over).start()
            attn_grads(1 - away)
            for i in (1, 0):
                for over in range(1, width):
                    a_wide(s.order(i), over).start()

            @pl.loop(0, d // 256)
            def _(t):
                at = pl.multiple_of(t * 256, 256)
                value = lax.dot_general(
                    d_qkv[...], w_a[pl.ds(at, 256), :qkv_cols], (((1,), (1,)), ((), ())), preferred_element_type=f32
                )
                part_a[:, :, :, pl.ds(at, 256)] = value.astype(bf16).reshape(2, 2, n, 256)

            to_c = remote(part_a.at[1 - c], c_in.at[0], ra_put.at[0], ra_got.at[0], s.at_c)
            to_c.start()
            to_c.wait_recv()
            part_a[c, 1 - x] = (part_a[c, 1 - x].astype(f32) + c_in[0, 1 - x].astype(f32)).astype(bf16)
            to_x = remote(part_a.at[c, 1 - x], x_in.at[0], ra_put.at[1], ra_got.at[1], s.at_x)
            to_x.start()
            field_v[...] = part_a[c, x].astype(f32) + c_in[0, x].astype(f32)
            f_sum(1, stage)
            spread_on(out_all, 1)
            to_x.wait_recv()
            hop_x(out_all, own_out, 1).wait_send()
            hop_c(out_all, own_out, 1).wait_send()
            copy(own_out, out_all.at[c, x], o_sem.at[2]).wait()

            @pl.loop(0, n // 16)
            def _(i):
                at = rows16(i)
                grad = field_v[at, :] + x_in[0, at, :].astype(f32)
                d_source = norm_back(cot_v[1, at, :].astype(f32), gain_v[0:1, :], grad, 0)
                own_out[at, :] = (acc[at, :] + d_source).astype(bf16)

            to_c.wait_send()
            to_x.wait_send()
            spread(gin_all, own_out, 2)
            copy(own_out, gin_all.at[c, x], o_sem.at[3]).start()

        def finish(stage):
            f_sum(3, stage)
            pl.run_scoped(
                functools.partial(attention, stage),
                pltpu.VMEM((d, a_cols), bf16),
                pltpu.VMEM((count, d), bf16),
                pltpu.VMEM((count, qkv_cols), bf16),
                pltpu.VMEM((count, q_cols), bf16),
                pltpu.VMEM((count, q_cols), bf16),
                pltpu.VMEM((count, qkv_cols), bf16),
                pltpu.VMEM((2, 2, n, d), bf16),
                pltpu.VMEM((count, HD // 2), f32),
                pltpu.VMEM((count, HD // 2), f32),
                pltpu.VMEM((count, ROW_LEN), f32),
                pltpu.VMEM((n, d), f32),
                pltpu.VMEM((n, d), f32),
                pltpu.VMEM((2, n, d), bf16),
            )

            for k in range(4):
                gain_v[k : k + 1, :] = jnp.sum(gain_acc[k], axis=0, keepdims=True)
            whole = gain_v[...]
            for p in range(dp_n):
                turned = pltpu.roll(whole, (d - p * shard) % d, 1) if p else whole
                gain_put[p] = turned[:, :lanes]

            def gain_hop(k):
                to = (s.dp + k) % dp_n
                return remote(gain_put.at[to], gain_got.at[s.dp], gg_put.at[k - 1], gg_got.at[k - 1], (to, s.q))

            for k in range(1, dp_n):
                gain_hop(k).start()
            spread_on(gin_all, 2)
            f_sum(0, stage)

            f_deeps(lambda p: f_deep(s.order(1), 1, stage, p).wait_send())
            copy(stage.at[0], f_out.at[z], o_sem.at[0]).wait()
            for i in reversed(range(1, depth)):
                a_sum(i, stage)
            for k in range(1, dp_n):
                got(gg_got.at[k - 1], gain_got.at[(s.dp + dp_n - k) % dp_n])
            total = gain_put[s.dp]
            for k in range(1, dp_n):
                total = total + gain_got[(s.dp + dp_n - k) % dp_n]
            gain_x[0] = total
            across = remote(gain_x.at[0], gain_x.at[1], gt_put.at[0], gt_got.at[0], s.at_x)
            across.start()
            a_sum(0, stage)
            across.wait_recv()
            gain_c[0] = gain_x[0] + gain_x[1]
            beside = remote(gain_c.at[0], gain_c.at[1], gt_put.at[1], gt_got.at[1], s.at_c)
            beside.start()
            beside.wait_recv()
            gain_c[2] = gain_c[0] + gain_c[1]
            copy(gain_c.at[2], gains_out, o_sem.at[4]).start()

            spread_end(out_all, 1)
            spread_end(gin_all, 2)
            for i in range(1, depth):
                g = s.order(i)
                for p in (0, 1):
                    got(fz_got.at[g, p], f_out.at[g, :, pl.ds(f_parts[p][0], f_parts[p][1])])
                if len(f_parts) > 2:

                    @pl.when(full(g))
                    def _():
                        for p in (2, 3):
                            got(fz_got.at[g, p], f_out.at[g, :, pl.ds(f_parts[p][0], f_parts[p][1])])

            for i in range(depth):
                g = s.order(i)
                for over in range(1, width):
                    for k in range(2):
                        f_wide(g, over, k).wait_send()
                    a_wide(g, over).wait_send()
            a_left(s.order(1), 1, stage)
            for kind, where, src in ((0, dbr, dbr.at[c, x]), (1, out_all, own_out), (2, gin_all, own_out)):
                if kind != 1:
                    hop_x(where, src, kind).wait_send()
                    hop_c(where, src, kind).wait_send()
                hop_far(where, kind).wait_send()
            for k in range(1, dp_n):
                gain_hop(k).wait_send()
            across.wait_send()
            beside.wait_send()
            copy(stage.at[0, :, pl.ds(0, a_cols)], a_out, o_sem.at[1]).wait()
            copy(own_out, gin_all.at[c, x], o_sem.at[3]).wait()
            copy(gain_c.at[2], gains_out, o_sem.at[4]).wait()

        pl.run_scoped(finish, pltpu.VMEM((3, shard, 3 * share), bf16))

    shape = jax.ShapeDtypeStruct
    outs = (
        shape((2, 2, n, d), bf16),
        shape((2, 2, n, d), bf16),
        shape((depth, shard, 3 * share), bf16),
        shape((shard, a_cols), bf16),
        shape((max(others, 1), depth, shard, 3 * share), bf16),
        shape((max(others, 1), depth, shard, a_cols), bf16),
        shape((depth + 1, shard, a_cols), bf16),
        shape((8, lanes), f32),
    )
    operands = tuple(first) + tuple(weights) + tuple(saves)
    anywhere = pl.BlockSpec(memory_space=pl.ANY)
    dma = pltpu.SemaphoreType.DMA
    return pl.pallas_call(
        kernel,
        out_shape=outs,
        in_specs=[anywhere] * len(operands),
        out_specs=tuple([anywhere] * len(outs)),
        scratch_shapes=Trade.buffers(depth, n, d)
        + [
            pltpu.VMEM((d, 2 * share), bf16),
            pltpu.VMEM((d, share), bf16),
            pltpu.VMEM((d, a_cols), bf16),
            pltpu.VMEM((n, d), f32),
            pltpu.VMEM((2, 2, n, d), bf16),
            pltpu.VMEM((n, d), bf16),
            pltpu.VMEM((8, d), f32),
            pltpu.VMEM((4, 8, d), f32),
            pltpu.VMEM((dp_n, 8, lanes), f32),
            pltpu.VMEM((dp_n, 8, lanes), f32),
            pltpu.VMEM((2, 8, lanes), f32),
            pltpu.VMEM((3, 8, lanes), f32),
            dma((8,)),
            dma((dp_n, 2)),
            dma((3,)),
            dma((5,)),
            dma((3, 3)),
            dma((3, 3)),
            dma((depth, max(others, 1), 2)),
            dma((depth, max(others, 1), 2)),
            dma((depth, 4)),
            dma((depth, 4)),
            dma((depth, max(others, 1))),
            dma((depth, max(others, 1))),
            dma((depth,)),
            dma((depth,)),
            dma((depth,)),
            dma((dp_n - 1,)),
            dma((dp_n - 1,)),
            dma((2,)),
            dma((2,)),
            dma((2,)),
            dma((2,)),
        ]
        + Trade.semaphores(depth),
        compiler_params=pltpu.CompilerParams(collective_id=2, has_side_effects=True, vmem_limit_bytes=67_043_328),
        name="backward",
    )(*operands)


def unit_cuts(units, parts):
    tiles = units // LANE
    edges = [(tiles * k + parts - 1) // parts for k in range(parts + 1)]
    starts = [e * LANE for e in edges[:-1]]
    sizes = [(b - a) * LANE for a, b in zip(edges[:-1], edges[1:])]
    return starts, sizes, max(sizes)


def cut_units(block, cuts):
    starts, sizes, share = cuts
    return jnp.stack(
        [
            jnp.pad(block[:, a : a + n], ((0, 0), (0, share - n))) if n < share else block[:, a : a + n]
            for a, n in zip(starts, sizes)
        ]
    )


def join_units(blocks, cuts):
    starts, sizes, share = cuts
    return jnp.concatenate([blocks[k, :, :n] for k, n in enumerate(sizes)], axis=1)


def make_body(grid):
    def body(
        inputs,
        cotangent,
        segments,
        positions,
        w_query,
        w_key,
        w_value,
        w_output,
        w_gate,
        w_up,
        w_down,
        gain_attn,
        gain_post_attn,
        gain_ffw,
        gain_post_ffw,
    ):
        grid.here()
        count, width = inputs.shape
        shard = w_query.shape[0]
        group = HEADS // KV
        local_kv = w_key.shape[1] // HD
        local_heads = local_kv * group
        q_cols, k_cols = w_query.shape[1], w_key.shape[1]
        scale = 1.0 / math.sqrt(HD)
        part = count // grid.tensor
        rows = count // ROW_LEN
        cuts = unit_cuts(w_gate.shape[1], grid.depth)
        share = cuts[2]
        main = share // 256 * 256

        gains = 0.0
        line = lax.broadcasted_iota(jnp.int32, (16, shard + -shard % LANE), 0)
        for k, gain in enumerate((gain_attn, gain_post_attn, gain_ffw, gain_post_ffw)):
            gains = gains + jnp.where(line == k, jnp.pad(gain, (0, -shard % LANE)).astype(f32), 0.0)
        gains = gains.astype(bf16)
        angles = make_angles(positions, HD)[:, 0]
        cosine, sine = jnp.cos(angles), jnp.sin(angles)
        mask = row_mask(segments, rows, ROW_LEN).astype(f32).reshape(count, ROW_LEN)
        cut_gate, cut_up = cut_units(w_gate, cuts), cut_units(w_up, cuts)
        wide_blocks = jnp.concatenate(
            [cut_gate[:, :, :main], cut_up[:, :, :main], cut_gate[:, :, main:], cut_up[:, :, main:]], axis=2
        )
        slim_blocks = cut_units(w_down.T, cuts)
        w_attn = jnp.concatenate([w_query, w_key, w_value, w_output.T], axis=1)
        (full_attn, full_wide, full_slim, normed, qkv, attended, branch_attn, hidden, full_gains,
         all_normed, saved, mixed, branch_ffw) = forward_kernel(
            grid, inputs, w_attn, wide_blocks, slim_blocks, gains, cosine, sine,
            mask, local_heads, local_kv,
        )
        full_attn = full_attn.reshape(width, full_attn.shape[2])
        out_all, gin_all, blocks_ffn, grad_attn, _, _, _, d_gains = backward_kernel(
            grid,
            (branch_ffw, hidden, branch_attn, cotangent, inputs, full_gains),
            (full_attn, full_wide, full_slim),
            (saved, all_normed.reshape(grid.depth, count, width), mixed, normed, qkv, attended, cosine, sine, mask),
            local_heads, local_kv, cuts[1],
        )
        gate, upward = [], []
        for k, size in enumerate(cuts[1]):
            low, rest = min(size, main), max(size - main, 0)
            gate.append(blocks_ffn[k, :, :low])
            upward.append(blocks_ffn[k, :, main : main + low])
            if rest:
                gate.append(blocks_ffn[k, :, 2 * main : 2 * main + rest])
                upward.append(blocks_ffn[k, :, main + share : main + share + rest])
        grad_gate = jnp.concatenate(gate, axis=1).astype(f32)
        grad_up = jnp.concatenate(upward, axis=1).astype(f32)
        grad_down = join_units(blocks_ffn[:, :, 2 * share :], cuts).T.astype(f32)
        qkv_cols = q_cols + 2 * k_cols

        return (
            out_all.reshape(count, width),
            gin_all.reshape(count, width),
            grad_attn[:, :q_cols].astype(f32),
            grad_attn[:, q_cols : q_cols + k_cols].astype(f32),
            grad_attn[:, q_cols + k_cols : qkv_cols].astype(f32),
            grad_attn[:, qkv_cols:].T.astype(f32),
            grad_gate,
            grad_up,
            grad_down,
            d_gains[0, :shard],
            d_gains[1, :shard],
            d_gains[2, :shard],
            d_gains[3, :shard],
        )

    return body


def solution(mesh):
    placed = (
        P("dp", None),
        P("dp", None),
        P("dp"),
        P("dp"),
        P("dp", "tensor"),
        P("dp", "tensor"),
        P("dp", "tensor"),
        P("tensor", "dp"),
        P("dp", "tensor"),
        P("dp", "tensor"),
        P("tensor", "dp"),
        P("dp"),
        P("dp"),
        P("dp"),
        P("dp"),
    )
    return jax.shard_map(
        make_body(Grid(mesh)),
        mesh=mesh,
        in_specs=placed,
        out_specs=(
            P("dp", None),
            P("dp", None),
            P("dp", "tensor"),
            P("dp", "tensor"),
            P("dp", "tensor"),
            P("tensor", "dp"),
            P("dp", "tensor"),
            P("dp", "tensor"),
            P("tensor", "dp"),
            P("dp"),
            P("dp"),
            P("dp"),
            P("dp"),
        ),
        check_vma=False,
    )
```

```python
import functools
import math

import jax
import jax.numpy as jnp
from jax import lax
from jax.experimental import pallas as pl
from jax.experimental.pallas import tpu as pltpu
from jax.sharding import PartitionSpec as P

HEADS = 8
KV = 4
HD = 256
ROW_LEN = 128
LANE = 128


EPS = 1e-06
CAP = 50.0
THETA = 10000.0

f32 = jnp.float32
bf16 = jnp.bfloat16


def rms_scale(field, gain):
    inverse = lax.rsqrt(jnp.mean(field * field, axis=-1, keepdims=True) + EPS)
    return field * inverse * gain


def rms_back(field, gain, grad):
    inverse = lax.rsqrt(jnp.mean(field * field, axis=-1, keepdims=True) + EPS)
    unit = field * inverse
    d_gain = jnp.sum(grad * unit, axis=0)
    scaled = grad * gain
    d_field = inverse * (scaled - unit * jnp.mean(scaled * unit, axis=-1, keepdims=True))
    return d_field, d_gain


def geglu(gate, upward):
    return jax.nn.gelu(gate, approximate=True) * upward


def rotate(field, cosine, sine):
    half = field.shape[-1] // 2
    first = field[..., :half]
    second = field[..., half:]
    return jnp.concatenate(
        [first * cosine - second * sine, second * cosine + first * sine], axis=-1
    )


def make_angles(positions, head_size):
    half = head_size // 2
    freqs = THETA ** (-(jnp.arange(half).astype(f32) * 2.0) / head_size)
    return positions.astype(f32)[:, None, None] * freqs[None, None, :]


def row_mask(segments, rows, length):
    seg_rows = segments.reshape(rows, length)
    same = seg_rows[:, :, None] == seg_rows[:, None, :]
    index = jnp.arange(length)
    causal = index[:, None] >= index[None, :]
    return jnp.logical_and(same, causal[None])


def dot(left, right):
    return jnp.dot(left, right, preferred_element_type=f32)


def contract_rows(left, right):
    return lax.dot_general(left, right, (((0,), (0,)), ((), ())), preferred_element_type=f32)


def contract_cols(left, right):
    return lax.dot_general(left, right, (((1,), (1,)), ((), ())), preferred_element_type=f32)


class Grid:
    def __init__(self, mesh):
        self.dp = mesh.shape["dp"]
        self.tensor = mesh.shape["tensor"]
        self.depth = 4 if self.dp % 4 == 0 else (2 if self.dp % 2 == 0 else 1)
        self.width = self.dp // self.depth

    def here(self):
        index = lax.axis_index("dp")
        self.deep = index // self.width
        self.wide = lax.rem(index, self.width)
        self.rank = lax.axis_index("tensor")

    def shift(self, value, step):
        pairs = [
            (z * self.width + y, ((z + step) % self.depth) * self.width + y)
            for z in range(self.depth)
            for y in range(self.width)
        ]
        return lax.ppermute(value, "dp", pairs)

    def swap_wide(self, value, bit):
        pairs = [
            (z * self.width + y, z * self.width + (y ^ bit))
            for z in range(self.depth)
            for y in range(self.width)
        ]
        return lax.ppermute(value, "dp", pairs)

    def swap_rank(self, value, bit):
        return lax.ppermute(value, "tensor", [(q, q ^ bit) for q in range(self.tensor)])

    def wide_bits(self):
        return [1 << b for b in range(self.width.bit_length() - 1)]

    def rank_bits(self):
        return [1 << b for b in range(self.tensor.bit_length() - 1)]

    def reduce_width(self, full):
        rows, columns = full.shape[0] // self.dp, full.shape[1]
        held = full.reshape(self.depth, self.width, rows, columns)
        for bit in reversed(self.wide_bits()):
            held = held.reshape(self.depth, 2, bit, rows, columns)
            mine = lax.rem(self.wide // bit, 2)
            other = lax.dynamic_index_in_dim(held, 1 - mine, 1, keepdims=False)
            own = lax.dynamic_index_in_dim(held, mine, 1, keepdims=False)
            held = own + self.swap_wide(other, bit)
        return held.reshape(self.depth, rows, columns)

    def pick(self, held, step):
        to = lax.rem(self.deep + step, self.depth)
        return lax.dynamic_index_in_dim(held, to, 0, keepdims=False)

    def scatter_rows(self, full):
        held = self.reduce_width(full)
        total = self.pick(held, 0).astype(f32)
        for step in range(1, self.depth):
            total = total + self.shift(self.pick(held, step), step).astype(f32)
        return total

    def return_blocks(self, full):
        held = self.reduce_width(full)
        out = jnp.zeros_like(held)
        for step in range(self.depth):
            part = self.pick(held, step)
            part = part if step == 0 else self.shift(part, step)
            source = lax.rem(self.deep + self.depth - step, self.depth)
            out = lax.dynamic_update_slice(out, part[None], (source, 0, 0))
        return out

    def spread_rank(self, block):
        x, c = self.rank // 2, lax.rem(self.rank, 2)
        n, d = block.shape
        out = jnp.zeros((2, 2, n, d), block.dtype)
        for far_c in range(2):
            for far_x in range(2):
                part = block
                if far_x:
                    part = across
                if far_c:
                    part = self.swap_rank(part, 1)
                elif not far_x:
                    across = self.swap_rank(block, 2)
                out = lax.dynamic_update_slice(
                    out, part[None, None], (jnp.bitwise_xor(c, far_c), jnp.bitwise_xor(x, far_x), 0, 0)
                )
        return out.reshape(4 * n, d)

    def reduce_rank(self, full):
        x, c = self.rank // 2, lax.rem(self.rank, 2)
        held = full.reshape(2, 2, full.shape[0] // 4, full.shape[1])
        for at, bit in ((c, 1), (x, 2)):
            own = lax.dynamic_index_in_dim(held, at, 0, keepdims=False)
            other = lax.dynamic_index_in_dim(held, 1 - at, 0, keepdims=False)
            held = own + self.swap_rank(other, bit)
        return held


MESH = pl.DeviceIdType.MESH


class Spot:
    def __init__(self, grid):
        self.depth, self.width = grid.depth, grid.width
        self.dp = lax.axis_index("dp")
        self.q = lax.axis_index("tensor")
        self.z, self.y = self.dp // self.width, self.dp % self.width
        self.x, self.c = self.q // 2, self.q % 2
        self.at_x = (self.dp, (1 - self.x) * 2 + self.c)
        self.at_c = (self.dp, self.x * 2 + 1 - self.c)
        self.at_up = (self.dp + self.width, self.q)
        self.at_dn = (self.dp - self.width, self.q)
        self.low, self.high = self.z > 0, self.z < self.depth - 1

    def order(self, i):
        z = self.z
        near = z + 1 - 2 * (z % 2)
        middle = 2 - z // 2
        far = 3 * (1 - z // 2)
        return jnp.where(i == 0, z, jnp.where(i == 1, near, jnp.where(i == 2, middle, far)))

    def at_depth(self, z):
        return (z * self.width + self.y, self.q)

    def at_wide(self, over):
        return (self.z * self.width + (self.y + over) % self.width, self.q)


def remote(src, dst, put, got, device):
    return pltpu.make_async_remote_copy(
        src_ref=src, dst_ref=dst, send_sem=put, recv_sem=got, device_id=device, device_id_type=MESH
    )


def signal(semaphore, device):
    pl.semaphore_signal(semaphore, inc=1, device_id=device, device_id_type=MESH)


class Trade:
    def __init__(self, spot, buf, part, acc, c_in, x_in, z_in, sems):
        self.spot, self.buf, self.part, self.acc = spot, buf, part, acc
        self.c_in, self.x_in, self.z_in = c_in, x_in, z_in
        (self.z_up, self.z_dn, self.z_got, self.x_put, self.x_got, self.c_put, self.c_got,
         self.rc_put, self.rc_got, self.rx_put, self.rx_got, self.rz_put, self.ru_got, self.rd_got) = sems

    @staticmethod
    def semaphores(depth):
        dma = pltpu.SemaphoreType.DMA
        return [dma((depth,))] * 5 + [dma((depth, 2))] * 2 + [dma((depth,))] * 7

    @staticmethod
    def buffers(depth, n, d):
        return [
            pltpu.VMEM((depth, 2, 2, n, d), bf16),
            pltpu.VMEM((depth, 2, n, d), bf16),
            pltpu.VMEM((depth, n, d), bf16),
            pltpu.VMEM((depth + 1, n, d), bf16),
        ]

    def hop_up(self, g):
        s = self.spot
        return remote(self.buf.at[g, s.c, s.x], self.buf.at[g, s.c, s.x], self.z_up.at[g], self.z_got.at[g], s.at_up)

    def hop_dn(self, g):
        s = self.spot
        return remote(self.buf.at[g, s.c, s.x], self.buf.at[g, s.c, s.x], self.z_dn.at[g], self.z_got.at[g], s.at_dn)

    def hop_x(self, g):
        s = self.spot
        return remote(self.buf.at[g, s.c, s.x], self.buf.at[g, s.c, s.x], self.x_put.at[g], self.x_got.at[g], s.at_x)

    def hop_c(self, g, far):
        s = self.spot
        xx = (1 - s.x) if far else s.x
        return remote(
            self.buf.at[g, s.c, xx], self.buf.at[g, s.c, xx], self.c_put.at[g, int(far)], self.c_got.at[g, int(far)], s.at_c
        )

    def got(self, sem, ref):
        remote(ref, ref, sem, sem, self.spot.at_x).wait_recv()

    def pass_on(self, g):
        s = self.spot

        @pl.when(jnp.logical_and(g <= s.z, s.high))
        def _():
            self.hop_up(g).start()

        @pl.when(jnp.logical_and(g >= s.z, s.low))
        def _():
            self.hop_dn(g).start()

        self.hop_x(g).start()
        self.hop_c(g, False).start()

    def take_z(self, g):
        s = self.spot
        self.got(self.z_got.at[g], self.buf.at[g, s.c, s.x])
        self.pass_on(g)

    def take_rank(self, g):
        s = self.spot
        self.got(self.x_got.at[g], self.buf.at[g, s.c, 1 - s.x])
        self.hop_c(g, True).start()
        self.got(self.c_got.at[g, 0], self.buf.at[g, 1 - s.c, s.x])
        self.got(self.c_got.at[g, 1], self.buf.at[g, 1 - s.c, 1 - s.x])

    def back_c(self, g):
        s = self.spot
        return remote(self.part.at[g, 1 - s.c], self.c_in.at[g], self.rc_put.at[g], self.rc_got.at[g], s.at_c)

    def back_x(self, g):
        s = self.spot
        return remote(self.part.at[g, s.c, 1 - s.x], self.x_in.at[g], self.rx_put.at[g], self.rx_got.at[g], s.at_x)

    def back_up(self, g):
        s = self.spot
        return remote(self.part.at[g, s.c, s.x], self.z_in.at[g], self.rz_put.at[g], self.ru_got.at[g], s.at_up)

    def back_dn(self, g):
        s = self.spot
        slot = jnp.where(g == s.z - 1, s.depth, g)
        return remote(self.part.at[g, s.c, s.x], self.z_in.at[slot], self.rz_put.at[g], self.rd_got.at[g], s.at_dn)

    def add_c(self, g):
        s, part, c_in = self.spot, self.part, self.c_in
        self.got(self.rc_got.at[g], c_in.at[g])
        part[g, s.c, 1 - s.x] = (part[g, s.c, 1 - s.x].astype(f32) + c_in[g, 1 - s.x].astype(f32)).astype(bf16)
        self.back_x(g).start()
        part[g, s.c, s.x] = (part[g, s.c, s.x].astype(f32) + c_in[g, s.x].astype(f32)).astype(bf16)

    def add_xz(self, g):
        s, part, acc = self.spot, self.part, self.acc
        self.got(self.rx_got.at[g], self.x_in.at[g])
        acc[...] = part[g, s.c, s.x].astype(f32) + self.x_in[g].astype(f32)

        @pl.when(jnp.logical_and(g >= s.z, s.low))
        def _():
            self.got(self.ru_got.at[g], self.z_in.at[g])
            acc[...] += self.z_in[g].astype(f32)

        @pl.when(jnp.logical_and(g <= s.z, s.high))
        def _():
            slot = jnp.where(g == s.z, s.depth, g)
            self.got(self.rd_got.at[g], self.z_in.at[slot])
            acc[...] += self.z_in[slot].astype(f32)

        @pl.when(g > s.z)
        def _():
            part[g, s.c, s.x] = acc[...].astype(bf16)
            self.back_up(g).start()

        @pl.when(g < s.z)
        def _():
            part[g, s.c, s.x] = acc[...].astype(bf16)
            self.back_dn(g).start()

    def settle(self):
        s = self.spot

        @pl.loop(0, s.depth)
        def _(g):
            @pl.when(jnp.logical_and(g <= s.z, s.high))
            def _():
                self.hop_up(g).wait_send()

            @pl.when(jnp.logical_and(g >= s.z, s.low))
            def _():
                self.hop_dn(g).wait_send()

            self.hop_x(g).wait_send()
            self.hop_c(g, False).wait_send()
            self.hop_c(g, True).wait_send()
            self.back_c(g).wait_send()
            self.back_x(g).wait_send()

            @pl.when(g > s.z)
            def _():
                self.back_up(g).wait_send()

            @pl.when(g < s.z)
            def _():
                self.back_dn(g).wait_send()


def put_part(part, g, left, right, n, d):
    @pl.loop(0, d // 256)
    def _(t):
        at = pl.multiple_of(t * 256, 256)
        value = lax.dot_general(left[g], right[pl.ds(at, 256), :], (((1,), (1,)), ((), ())), preferred_element_type=f32)
        part[g, :, :, :, pl.ds(at, 256)] = value.astype(bf16).reshape(2, 2, n, 256)


def forward_group(g, buf, gu, mid, w_gu, share):
    n, d = buf.shape[3:]
    main = share // 256 * 256
    tokens = lambda: buf[g].reshape(4 * n, d)

    def save(lo, hi, gate, upward):
        inner = math.sqrt(2.0 / math.pi) * (gate + 0.044715 * gate * gate * gate)
        mid[g, :, lo:hi] = (0.5 * gate * (1.0 + jnp.tanh(inner)) * upward).astype(bf16)

    for lo in range(0, main, 256):
        hi = lo + 256
        gate = jnp.dot(tokens(), w_gu[:, lo:hi], preferred_element_type=f32)
        upward = jnp.dot(tokens(), w_gu[:, main + lo : main + hi], preferred_element_type=f32)
        gu[g, :, lo:hi] = gate.astype(bf16)
        gu[g, :, main + lo : main + hi] = upward.astype(bf16)
        save(lo, hi, gate, upward)
    if main < share:
        rest = share - main
        both = jnp.dot(tokens(), w_gu[:, 2 * main :], preferred_element_type=f32)
        gu[g, :, 2 * main :] = both.astype(bf16)
        save(main, share, both[:, :rest], both[:, rest:])


def backward_group(g, buf, gu, mid, part, w_gu, w_dn, share):
    n, d = buf.shape[3:]
    main = share // 256 * 256
    tokens = lambda: buf[g].reshape(4 * n, d)

    def pull(lo, hi, gate_at, up_at):
        grad = jnp.dot(tokens(), w_dn[:, lo:hi], preferred_element_type=f32)
        gate = gu[g, :, gate_at : gate_at + hi - lo].astype(f32)
        upward = gu[g, :, up_at : up_at + hi - lo].astype(f32)
        factor = math.sqrt(2.0 / math.pi)
        square = gate * gate
        curve = jnp.tanh(factor * gate * (1.0 + 0.044715 * square))
        half = 0.5 * (1.0 + curve)
        slope = half + 0.5 * gate * (1.0 - curve * curve) * factor * (1.0 + 3.0 * 0.044715 * square)
        mid[g, :, gate_at : gate_at + hi - lo] = (grad * upward * slope).astype(bf16)
        mid[g, :, up_at : up_at + hi - lo] = (grad * gate * half).astype(bf16)

    for lo in range(0, main, 256):
        pull(lo, lo + 256, lo, main + lo)
    if main < share:
        pull(main, share, 2 * main, main + share)
    put_part(part, g, mid, w_gu, n, d)


def forward_kernel(grid, inputs, w_attn, wide_blocks, slim_blocks, gains, cosine, sine, mask, heads, kv_heads):
    depth, width, dp_n = grid.depth, grid.width, grid.dp
    count, d = inputs.shape
    n = count // 4
    shard, a_cols = w_attn.shape
    q_cols, k_cols = heads * HD, kv_heads * HD
    qkv_cols = q_cols + 2 * k_cols
    share = slim_blocks.shape[2]
    group = heads // kv_heads
    align = math.gcd(shard, 16)
    parts = ((0, qkv_cols), (qkv_cols, q_cols))
    scale = 1.0 / math.sqrt(HD)
    others = width - 1

    def kernel(
        x_ref, wa_ref, blk_wide, blk_slim, gain_ref, cos_ref, sin_ref, mask_ref,
        wa_all, wide_all, slim_all, normed_out, qkv_out, att_out, branch_out, hidden_out, gains_out,
        all_out, gu_out, mid_out, ffw_out,
        buf, c_in, x_in, z_in, gain_in, ca_in, xa_in, acc, hid, full_gain, w_a, w_gu, w_dn,
        g_put, g_got, a_up, a_dn, a_got, ay_put, ay_got, f_put, f_got, fy_put, fy_got,
        la_sem, lf_sem, in_sem, o_sem, g_sem, ra_put, ra_got, *sems,
    ):
        s = Spot(grid)
        z, y, x, c = s.z, s.y, s.x, s.c

        def got(sem, ref):
            remote(ref, ref, sem, sem, s.at_x).wait_recv()

        def row(g, yy):
            return pl.multiple_of((g * width + yy) * shard, align)

        barrier = pltpu.get_barrier_semaphore()
        for k in range(1, dp_n):
            signal(barrier, ((s.dp + k) % dp_n, s.q))
        signal(barrier, s.at_x)
        signal(barrier, s.at_c)
        pl.semaphore_wait(barrier, dp_n + 1)

        def a_at(g, yy, k):
            return wa_all.at[g * width + yy, :, pl.ds(parts[k][0], parts[k][1])]

        def a_src(g, k, own):
            return wa_ref.at[:, pl.ds(parts[k][0], parts[k][1])] if own else a_at(g, y, k)

        def a_hop(g, k, own, up):
            return remote(
                a_src(g, k, own), a_at(g, y, k), (a_up if up else a_dn).at[g, k], a_got.at[g, k], s.at_up if up else s.at_dn
            )

        def a_wide(g, k, own, over):
            return remote(a_src(g, k, own), a_at(g, y, k), ay_put.at[g, k, over - 1], ay_got.at[g, k, over - 1], s.at_wide(over))

        def a_pass(g, k, own):
            @pl.when(jnp.logical_and(g <= z, s.high))
            def _():
                a_hop(g, k, own, True).start()

            @pl.when(jnp.logical_and(g >= z, s.low))
            def _():
                a_hop(g, k, own, False).start()

            for over in range(1, width):
                a_wide(g, k, own, over).start()

        def f_at(g, yy, k):
            return (wide_all, slim_all)[k].at[g * width + yy]

        def f_own(g, k):
            return (blk_wide, blk_slim)[k].at[g]

        def f_hop(to, k):
            return remote(f_own(to, k), f_at(z, y, k), f_put.at[to, k], f_got.at[z, k], s.at_depth(to))

        def f_wide(g, own, over, k):
            source = f_own(z, k) if own else f_at(g, y, k)
            return remote(source, f_at(g, y, k), fy_put.at[g, over - 1, k], fy_got.at[g, over - 1, k], s.at_wide(over))

        ends = jnp.logical_or(z == 0, z == depth - 1)
        inner = jnp.logical_not(ends)

        def f_hops(i, k):
            @pl.when(ends)
            def _():
                for j in {1: (1,), 3: (2, 3)}.get(i, ()):
                    f_hop(s.order(j), k).start()

            @pl.when(inner)
            def _():
                for j in {3: (2, 3, 1)}.get(i, ()):
                    f_hop(s.order(j), k).start()

        for k in range(1, dp_n):
            remote(gain_ref, gain_in.at[s.dp], g_put.at[k - 1], g_got.at[k - 1], ((s.dp + k) % dp_n, s.q)).start()
        for k in range(2):
            a_pass(z, k, True)

        def attention(x_v, normed_v, qkv_v, att_v, part_a, cos_v, sin_v, mask_v):
            own_gain = pltpu.make_async_copy(gain_ref, gain_in.at[s.dp], in_sem.at[4])
            fills = [
                pltpu.make_async_copy(x_ref, x_v, in_sem.at[0]),
                pltpu.make_async_copy(cos_ref, cos_v, in_sem.at[1]),
                pltpu.make_async_copy(sin_ref, sin_v, in_sem.at[2]),
                pltpu.make_async_copy(mask_ref, mask_v, in_sem.at[3]),
                own_gain,
            ]
            for fill in fills:
                fill.start()

            def load(g, yy, k, own, slot):
                return pltpu.make_async_copy(
                    a_src(g, k, True) if own else a_at(g, yy, k),
                    w_a.at[pl.ds(row(g, yy), shard), pl.ds(parts[k][0], parts[k][1])],
                    la_sem.at[slot, k],
                )

            for k in range(2):
                load(z, y, k, True, 0).start()

            for k in range(1, dp_n):
                remote(
                    gain_in.at[0], gain_in.at[(s.dp + dp_n - k) % dp_n], g_put.at[k - 1], g_got.at[k - 1], s.at_x
                ).wait_recv()
            for fill in fills:
                fill.wait()
            whole = jnp.zeros((8, d), f32)
            for p in range(dp_n):
                one = gain_in[p].astype(f32)[:8]
                one = jnp.concatenate([one, jnp.zeros((8, d - one.shape[1]), f32)], axis=1)
                whole = whole + (pltpu.roll(one, p * shard, 1) if p else one)
            full_gain[...] = whole
            pltpu.make_async_copy(full_gain, gains_out, o_sem.at[0]).start()

            @pl.loop(0, count // 32)
            def _(i):
                at = pl.ds(pl.multiple_of(i * 32, 32), 32)
                value = x_v[at, :].astype(f32)
                inverse = lax.rsqrt(jnp.mean(value * value, axis=-1, keepdims=True) + EPS)
                normed_v[at, :] = (value * inverse * full_gain[0:1, :]).astype(bf16)

            pltpu.make_async_copy(normed_v, normed_out, o_sem.at[1]).start()

            for i in range(1, depth):
                g = s.order(i)
                for k in range(2):
                    got(a_got.at[g, k], a_at(g, y, k))
                    a_pass(g, k, False)
                    load(g, y, k, False, i * width).start()
                f_hops(i, 0)
            for over in range(1, width):
                f_wide(z, True, over, 0).start()
            for k in range(2):
                for i in range(depth):
                    g = s.order(i)
                    for over in range(1, width):
                        yy = (y + width - over) % width
                        got(ay_got.at[g, k, over - 1], a_at(g, yy, k))
                        load(g, yy, k, False, i * width + over).start()
                for i in range(depth):
                    g = s.order(i)
                    for over in range(width):
                        load(g, (y + width - over) % width, k, i + over == 0, i * width + over).wait()
                if k:
                    continue
                for h in range(heads + 2 * kv_heads):
                    value = jnp.dot(normed_v[...], w_a[:, h * HD : (h + 1) * HD], preferred_element_type=f32)
                    if h < heads + kv_heads:
                        half = HD // 2
                        first, second = value[:, :half], value[:, half:]
                        low = first * cos_v[...] - second * sin_v[...]
                        high = second * cos_v[...] + first * sin_v[...]
                        if h < heads:
                            low, high = low * scale, high * scale
                        qkv_v[:, h * HD : h * HD + half] = low.astype(bf16)
                        qkv_v[:, h * HD + half : (h + 1) * HD] = high.astype(bf16)
                    else:
                        qkv_v[:, h * HD : (h + 1) * HD] = value.astype(bf16)
                pltpu.make_async_copy(qkv_v, qkv_out, o_sem.at[2]).start()

                @pl.loop(0, count // ROW_LEN)
                def _(r):
                    at = pl.ds(pl.multiple_of(r * ROW_LEN, ROW_LEN), ROW_LEN)
                    allowed = mask_v[at, :] > 0.5
                    for h in range(heads):
                        kv = heads + h // group
                        scores = lax.dot_general(
                            qkv_v[at, h * HD : (h + 1) * HD],
                            qkv_v[at, kv * HD : (kv + 1) * HD],
                            (((1,), (1,)), ((), ())),
                            preferred_element_type=f32,
                        )
                        expo = jnp.where(allowed, jnp.exp(CAP * jnp.tanh(scores / CAP)), 0.0)
                        probs = (expo / jnp.sum(expo, axis=-1, keepdims=True)).astype(bf16)
                        kv = kv + kv_heads
                        value = jnp.dot(probs, qkv_v[at, kv * HD : (kv + 1) * HD], preferred_element_type=f32)
                        att_v[at, h * HD : (h + 1) * HD] = value.astype(bf16)

                pltpu.make_async_copy(att_v, att_out, o_sem.at[3]).start()

            @pl.loop(0, d // 256)
            def _(t):
                at = pl.multiple_of(t * 256, 256)
                value = lax.dot_general(
                    att_v[...], w_a[pl.ds(at, 256), qkv_cols:], (((1,), (1,)), ((), ())), preferred_element_type=f32
                )
                part_a[:, :, :, pl.ds(at, 256)] = value.astype(bf16).reshape(2, 2, n, 256)

            own_rows = pltpu.make_async_copy(
                w_a.at[pl.ds(row(z, y), shard)], wa_all.at[s.dp], o_sem.at[4]
            )
            own_rows.start()
            to_c = remote(part_a.at[1 - c], ca_in, ra_put.at[0], ra_got.at[0], s.at_c)
            to_c.start()
            to_c.wait_recv()
            part_a[c, 1 - x] = (part_a[c, 1 - x].astype(f32) + ca_in[1 - x].astype(f32)).astype(bf16)
            to_x = remote(part_a.at[c, 1 - x], xa_in, ra_put.at[1], ra_got.at[1], s.at_x)
            to_x.start()
            acc[...] = part_a[c, x].astype(f32) + ca_in[x].astype(f32)
            to_x.wait_recv()

            @pl.loop(0, n // 16)
            def _(i):
                at = pl.ds(pl.multiple_of(i * 16, 16), 16)
                branch = acc[at, :] + xa_in[at, :].astype(f32)
                acc[at, :] = branch
                inverse = lax.rsqrt(jnp.mean(branch * branch, axis=-1, keepdims=True) + EPS)
                mine = pl.ds(pl.multiple_of((c * 2 + x) * n + i * 16, 16), 16)
                hidden = x_v[mine, :].astype(f32) + branch * inverse * full_gain[1:2, :]
                hid[at, :] = hidden
                inverse = lax.rsqrt(jnp.mean(hidden * hidden, axis=-1, keepdims=True) + EPS)
                buf[z, c, x, at, :] = (hidden * inverse * full_gain[2:3, :]).astype(bf16)

            to_c.wait_send()
            to_x.wait_send()
            pltpu.make_async_copy(full_gain, gains_out, o_sem.at[0]).wait()
            pltpu.make_async_copy(normed_v, normed_out, o_sem.at[1]).wait()
            pltpu.make_async_copy(qkv_v, qkv_out, o_sem.at[2]).wait()
            pltpu.make_async_copy(att_v, att_out, o_sem.at[3]).wait()
            own_rows.wait()

        pl.run_scoped(
            attention,
            pltpu.VMEM((count, d), bf16),
            pltpu.VMEM((count, d), bf16),
            pltpu.VMEM((count, qkv_cols), bf16),
            pltpu.VMEM((count, q_cols), bf16),
            pltpu.VMEM((2, 2, n, d), bf16),
            pltpu.VMEM((count, HD // 2), f32),
            pltpu.VMEM((count, HD // 2), f32),
            pltpu.VMEM((count, ROW_LEN), f32),
        )

        def ffn(part, gu, mid, tot):
            trade = Trade(s, buf, part, tot, c_in, x_in, z_in, sems)
            trade.pass_on(z)
            saved = [
                pltpu.make_async_copy(acc, branch_out, o_sem.at[0]),
                pltpu.make_async_copy(hid, hidden_out, o_sem.at[1]),
            ]
            for save in saved:
                save.start()

            def load(g, yy, own, slot, k):
                source = f_own(z, k) if own else f_at(g, yy, k)
                return pltpu.make_async_copy(source, (w_gu, w_dn)[k].at[pl.ds(row(g, yy), shard)], lf_sem.at[slot, k])

            for k in range(2):
                load(z, y, True, 0, k).start()

            def f_take(i, k):
                g = s.order(i)
                got(f_got.at[g, k], f_at(g, y, k))
                for over in range(1, width):
                    f_wide(g, False, over, k).start()
                load(g, y, False, i * width, k).start()

            def f_rest(k):
                for i in range(depth):
                    g = s.order(i)
                    for over in range(1, width):
                        yy = (y + width - over) % width
                        got(fy_got.at[g, over - 1, k], f_at(g, yy, k))
                        load(g, yy, False, i * width + over, k).start()
                for i in range(depth):
                    for over in range(width):
                        load(s.order(i), (y + width - over) % width, i + over == 0, i * width + over, k).wait()

            def gather(i):
                trade.take_rank(s.order(i))
                pltpu.make_async_copy(buf.at[s.order(i)], all_out.at[s.order(i)], g_sem.at[i, 0]).start()

            for i in range(1, depth):
                f_take(i, 0)
            for over in range(1, width):
                f_wide(z, True, over, 1).start()
            for i in range(1, depth):
                trade.take_z(s.order(i))
                f_hops(i, 1)
                gather(i - 1)
            gather(depth - 1)
            f_rest(0)

            def keep(g):
                return (
                    pltpu.make_async_copy(gu.at[g], gu_out.at[g], g_sem.at[g, 1]),
                    pltpu.make_async_copy(mid.at[g], mid_out.at[g], g_sem.at[g, 2]),
                )

            @pl.loop(0, depth)
            def _(i):
                @pl.when(i > 0)
                def _():
                    f_take(i, 1)

                g = s.order(depth - 1 - i)
                forward_group(g, buf, gu, mid, w_gu, share)
                for copy in keep(g):
                    copy.start()

            f_rest(1)
            at = pl.ds(row(z, y), shard)
            own_rows = [
                pltpu.make_async_copy((w_gu, w_dn)[k].at[at], f_at(z, y, k), o_sem.at[2 + k]) for k in range(2)
            ]
            for copy in own_rows:
                copy.start()

            @pl.loop(0, depth)
            def _(i):
                g = s.order(depth - 1 - i)
                put_part(part, g, mid, w_dn, n, d)
                trade.back_c(g).start()
                trade.add_c(g)

                @pl.when(jnp.logical_and(i == 1, ends))
                def _():
                    trade.add_xz(s.order(depth - 1))

            @pl.when(inner)
            def _():
                trade.add_xz(s.order(depth - 1))

            for i in reversed(range(depth - 1)):
                trade.add_xz(s.order(i))

            last = pltpu.make_async_copy(tot, ffw_out, o_sem.at[4])
            last.start()
            trade.settle()
            for i in range(depth):
                g = s.order(i)
                pltpu.make_async_copy(buf.at[g], all_out.at[g], g_sem.at[i, 0]).wait()
                for copy in keep(g):
                    copy.wait()
            for copy in saved + own_rows:
                copy.wait()
            last.wait()

        pl.run_scoped(
            ffn,
            pltpu.VMEM((depth, 2, 2, n, d), bf16),
            pltpu.VMEM((depth, count, 2 * share), bf16),
            pltpu.VMEM((depth, count, share), bf16),
            pltpu.VMEM((n, d), f32),
        )

        for k in range(1, dp_n):
            remote(gain_ref, gain_in.at[s.dp], g_put.at[k - 1], g_got.at[k - 1], ((s.dp + k) % dp_n, s.q)).wait_send()
        for i in range(depth):
            g = s.order(i)
            for k in range(2):

                @pl.when(jnp.logical_and(g <= z, s.high))
                def _():
                    a_hop(g, k, i == 0, True).wait_send()

                @pl.when(jnp.logical_and(g >= z, s.low))
                def _():
                    a_hop(g, k, i == 0, False).wait_send()

                for over in range(1, width):
                    a_wide(g, k, i == 0, over).wait_send()
            for k in range(2):
                for over in range(1, width):
                    f_wide(g, i == 0, over, k).wait_send()
                if i:
                    f_hop(g, k).wait_send()

    shape = jax.ShapeDtypeStruct
    outs = (
        shape((dp_n, shard, a_cols), bf16),
        shape((dp_n, shard, 2 * share), bf16),
        shape((dp_n, shard, share), bf16),
        shape((count, d), bf16),
        shape((count, qkv_cols), bf16),
        shape((count, q_cols), bf16),
        shape((n, d), f32),
        shape((n, d), f32),
        shape((8, d), f32),
        shape((depth, 2, 2, n, d), bf16),
        shape((depth, count, 2 * share), bf16),
        shape((depth, count, share), bf16),
        shape((n, d), f32),
    )
    operands = (inputs, w_attn, wide_blocks, slim_blocks, gains, cosine, sine, mask)
    anywhere = pl.BlockSpec(memory_space=pl.ANY)
    dma = pltpu.SemaphoreType.DMA
    return pl.pallas_call(
        kernel,
        out_shape=outs,
        in_specs=[anywhere] * len(operands),
        out_specs=tuple([anywhere] * len(outs)),
        scratch_shapes=Trade.buffers(depth, n, d)
        + [
            pltpu.VMEM((dp_n,) + gains.shape, bf16),
            pltpu.VMEM((2, n, d), bf16),
            pltpu.VMEM((n, d), bf16),
            pltpu.VMEM((n, d), f32),
            pltpu.VMEM((n, d), f32),
            pltpu.VMEM((8, d), f32),
            pltpu.VMEM((d, a_cols), bf16),
            pltpu.VMEM((d, 2 * share), bf16),
            pltpu.VMEM((d, share), bf16),
            dma((dp_n - 1,)),
            dma((dp_n - 1,)),
            dma((depth, 2)),
            dma((depth, 2)),
            dma((depth, 2)),
            dma((depth, 2, others)),
            dma((depth, 2, others)),
            dma((depth, 2)),
            dma((depth, 2)),
            dma((depth, others, 2)),
            dma((depth, others, 2)),
            dma((dp_n, 2)),
            dma((dp_n, 2)),
            dma((5,)),
            dma((5,)),
            dma((depth, 3)),
            dma((2,)),
            dma((2,)),
        ]
        + Trade.semaphores(depth),
        compiler_params=pltpu.CompilerParams(collective_id=1, has_side_effects=True, vmem_limit_bytes=66_000_000),
        name="forward",
    )(*operands)


def backward_kernel(grid, first, weights, saves, heads, kv_heads, sizes):
    depth, width, dp_n = grid.depth, grid.width, grid.dp
    n, d = first[0].shape
    count = 4 * n
    a_cols = weights[0].shape[1]
    shard = weights[1].shape[1]
    share = weights[2].shape[2]
    q_cols, k_cols = heads * HD, kv_heads * HD
    qkv_cols = q_cols + 2 * k_cols
    group = heads // kv_heads
    align = math.gcd(shard, 16)
    others = width - 1
    scale = 1.0 / math.sqrt(HD)
    half = d // 2
    strip = 3 * LANE
    lanes = shard + -shard % LANE
    f_cols = ((0, 2 * share), (2 * share, share))
    main = share // 256 * 256
    f_parts = ((0, 2 * main), (2 * share, main))
    if main < share:
        f_parts = f_parts + ((2 * main, 2 * (share - main)), (2 * share + main, share - main))
    assert min(sizes) >= main

    def kernel(
        ffw_ref, hid_ref, att_branch_ref, cot_ref, x_ref, gain_ref,
        wa_ref, wide_ref, slim_ref, gu_ref, tok_ref, mix_ref, normed_ref, qkv_ref, att_ref, cos_ref, sin_ref, mask_ref,
        out_all, gin_all, f_out, a_out, yf, ya, az, gains_out,
        buf, c_in, x_in, z_in, w_gu, w_dn, g_attn, acc, dbr, own_out, gain_v, gain_acc,
        gain_put, gain_got, gain_x, gain_c,
        in_sem, w_sem, s_sem, o_sem, t_put, t_got, fy_put, fy_got, fz_put, fz_got, ay_put, ay_got, az_put, au_got, ad_got,
        gg_put, gg_got, gt_put, gt_got, ra_put, ra_got, *sems,
    ):
        s = Spot(grid)
        z, y, x, c = s.z, s.y, s.x, s.c
        mine = pl.multiple_of((c * 2 + x) * n, n)

        def got(sem, ref):
            remote(ref, ref, sem, sem, s.at_x).wait_recv()

        def row(g, yy):
            return pl.ds(pl.multiple_of((g * width + yy) * shard, align), shard)

        def copy(src, dst, sem):
            return pltpu.make_async_copy(src, dst, sem)

        loads = []
        for p in range(dp_n):
            at = pl.ds(p * shard, shard)
            for k, (source, where) in enumerate(((wide_ref, w_gu), (slim_ref, w_dn))):
                loads.append(copy(source.at[p], where.at[at], w_sem.at[p, k]))

        barrier = pltpu.get_barrier_semaphore()
        for k in range(1, dp_n):
            signal(barrier, ((s.dp + k) % dp_n, s.q))
        signal(barrier, s.at_x)
        signal(barrier, s.at_c)

        def norm_back(field, gain, grad, slot):
            inverse = lax.rsqrt(jnp.mean(field * field, axis=-1, keepdims=True) + EPS)
            unit = field * inverse
            terms = grad * unit
            gain_acc[slot] += terms[:8] + terms[8:]
            scaled = grad * gain
            return inverse * (scaled - unit * jnp.mean(scaled * unit, axis=-1, keepdims=True))

        def rows16(i):
            return pl.ds(pl.multiple_of(i * 16, 16), 16)

        gain_acc[...] = jnp.zeros_like(gain_acc)

        def open_up(field_v, hid_v, cot_v):
            fills = [
                copy(gain_ref, gain_v, in_sem.at[0]),
                copy(ffw_ref, field_v, in_sem.at[1]),
                copy(hid_ref, hid_v, in_sem.at[2]),
                copy(cot_ref.at[pl.ds(mine, n)], cot_v, in_sem.at[3]),
            ]
            for fill in fills:
                fill.start()
            for load in loads:
                load.start()
            for fill in fills:
                fill.wait()

            @pl.loop(0, n // 16)
            def _(i):
                at = rows16(i)
                field, grad = field_v[at, :], cot_v[at, :].astype(f32)
                inverse = lax.rsqrt(jnp.mean(field * field, axis=-1, keepdims=True) + EPS)
                own_out[at, :] = (hid_v[at, :] + field * inverse * gain_v[3:4, :]).astype(bf16)
                buf[z, c, x, at, :] = norm_back(field, gain_v[3:4, :], grad, 3).astype(bf16)

        pl.run_scoped(open_up, pltpu.VMEM((n, d), f32), pltpu.VMEM((n, d), f32), pltpu.VMEM((n, d), bf16))
        pl.semaphore_wait(barrier, dp_n + 1)

        def f_wide(g, over, k):
            yy = (y + over) % width
            return remote(
                (w_gu, w_dn)[k].at[row(g, yy)],
                yf.at[over - 1, g, :, pl.ds(f_cols[k][0], f_cols[k][1])],
                fy_put.at[g, over - 1, k], fy_got.at[g, over - 1, k], s.at_wide(over),
            )

        def full(g):
            return functools.reduce(jnp.logical_or, [g == k for k in range(depth) if sizes[k] > main] or [g < 0])

        def f_deep(g, slot, stage, p):
            cols = pl.ds(f_parts[p][0], f_parts[p][1])
            return remote(stage.at[slot, :, cols], f_out.at[z, :, cols], fz_put.at[g, p], fz_got.at[z, p], s.at_depth(g))

        def f_deeps(do):
            for p in (0, 1):
                do(p)
            if len(f_parts) > 2:

                @pl.when(full(z))
                def _():
                    for p in (2, 3):
                        do(p)

        def a_wide(g, over):
            yy = (y + over) % width
            return remote(
                g_attn.at[row(g, yy)], ya.at[over - 1, g], ay_put.at[g, over - 1], ay_got.at[g, over - 1], s.at_wide(over)
            )

        def a_up(g, slot, stage):
            return remote(stage.at[slot, :, pl.ds(0, a_cols)], az.at[g], az_put.at[g], au_got.at[g], s.at_up)

        def a_dn(g, slot, stage):
            to = jnp.where(g == z - 1, depth, g)
            return remote(stage.at[slot, :, pl.ds(0, a_cols)], az.at[to], az_put.at[g], ad_got.at[g], s.at_dn)

        def a_left(g, slot, stage):
            @pl.when(g > z)
            def _():
                a_up(g, slot, stage).wait_send()

            @pl.when(g < z)
            def _():
                a_dn(g, slot, stage).wait_send()

        def f_sum(i, stage):
            g = s.order(i)
            slot = i % 2
            if i + 2 < depth:
                f_deeps(lambda p: f_deep(s.order(i + 2), slot, stage, p).wait_send())
            own = [
                copy(where.at[row(g, y)], stage.at[slot, :, pl.ds(f_cols[k][0], f_cols[k][1])], s_sem.at[k])
                for k, where in enumerate((w_gu, w_dn))
            ]
            for part_copy in own:
                part_copy.start()
            for over in range(1, width):
                for k in range(2):
                    got(fy_got.at[g, over - 1, k], yf.at[over - 1, g, :, pl.ds(f_cols[k][0], f_cols[k][1])])
                bring = copy(yf.at[over - 1, g], stage.at[2], s_sem.at[2])
                bring.start()
                bring.wait()
                if over == 1:
                    for part_copy in own:
                        part_copy.wait()
                stage[slot] = (stage[slot].astype(f32) + stage[2].astype(f32)).astype(bf16)
            if width == 1:
                for part_copy in own:
                    part_copy.wait()
            if i:
                f_deeps(lambda p: f_deep(g, slot, stage, p).start())
            else:
                copy(stage.at[slot], f_out.at[z], o_sem.at[0]).start()

        def a_sum(i, stage):
            g = s.order(i)
            slot = i % 2
            narrow = pl.ds(0, a_cols)
            if i + 2 < depth:
                a_left(s.order(i + 2), slot, stage)
            own = copy(g_attn.at[row(g, y)], stage.at[slot, :, narrow], s_sem.at[0])
            own.start()

            def add(source):
                bring = copy(source, stage.at[2, :, narrow], s_sem.at[2])
                bring.start()
                bring.wait()
                total = stage[slot, :, :a_cols].astype(f32) + stage[2, :, :a_cols].astype(f32)
                stage[slot, :, :a_cols] = total.astype(bf16)

            for over in range(1, width):
                got(ay_got.at[g, over - 1], ya.at[over - 1, g])
                if over == 1:
                    own.wait()
                add(ya.at[over - 1, g])
            if width == 1:
                own.wait()

            @pl.when(jnp.logical_and(g >= z, s.low))
            def _():
                got(au_got.at[g], az.at[g])
                add(az.at[g])

            @pl.when(jnp.logical_and(g <= z, s.high))
            def _():
                where = jnp.where(g == z, depth, g)
                got(ad_got.at[g], az.at[where])
                add(az.at[where])

            @pl.when(g > z)
            def _():
                a_up(g, slot, stage).start()

            @pl.when(g < z)
            def _():
                a_dn(g, slot, stage).start()

            if i == 0:
                copy(stage.at[slot, :, narrow], a_out, o_sem.at[1]).start()

        def ffn(part, mid, mix, strips):
            trade = Trade(s, buf, part, acc, c_in, x_in, z_in, sems)
            trade.pass_on(z)
            first_loads = loads + [copy(gu_ref, mid, in_sem.at[0])]
            first_loads[-1].start()
            mix_load = copy(mix_ref, mix, in_sem.at[1])
            mix_load.start()

            @pl.loop(1, depth + 1)
            def _(i):
                @pl.when(i < depth)
                def _():
                    trade.take_z(s.order(i))

                g = s.order(i - 1)
                trade.take_rank(g)

                @pl.when(i == 1)
                def _():
                    for load in first_loads:
                        load.wait()

                backward_group(g, buf, mid, mid, part, w_gu, w_dn, share)
                trade.back_c(g).start()

            n_strip = half // strip
            assert 2 * strip >= d // depth and n_strip > 2

            away = 1 - z // 2

            def strip_at(j):
                side = jnp.where(j < n_strip, away, 1 - away)
                return pl.multiple_of(side * half + j % n_strip * strip, strip)

            def bring(j):
                return copy(tok_ref.at[:, :, pl.ds(strip_at(j), strip)], strips.at[j % 2], in_sem.at[2 + j % 2])

            def weight_grads(j):
                bring(j).wait()
                rows = pl.ds(strip_at(j), strip)

                def product(left, right, where, cols):
                    where[rows, cols] = lax.dot_general(
                        left, right, (((0,), (0,)), ((), ())), preferred_element_type=f32
                    ).astype(bf16)

                @pl.loop(0, 2 * share // 256)
                def _(t):
                    cols = pl.ds(pl.multiple_of(t * 256, 256), 256)
                    left = strips[j % 2].reshape(depth * count, strip)
                    product(left, mid[:, :, cols].reshape(depth * count, 256), w_gu, cols)

                @pl.when(j + 2 < 2 * n_strip)
                def _():
                    bring(j + 2).start()

                for lo in range(0, share, 256):
                    hi = min(lo + 256, share)
                    left = buf[:, :, :, :, rows].reshape(depth * count, strip)
                    right = mix[:, :, lo:hi].reshape(depth * count, hi - lo)
                    product(left, right, w_dn, slice(lo, hi))

            def send_wide(g):
                for over in range(1, width):
                    for k in range(2):
                        f_wide(g, over, k).start()

            ends = jnp.logical_or(z == 0, z == depth - 1)
            inner = jnp.logical_not(ends)
            for j in range(2):
                bring(j).start()
            mix_load.wait()
            for i in reversed(range(depth)):
                trade.add_c(s.order(i))

            @pl.loop(0, 2 * n_strip)
            def _(j):
                weight_grads(j)

                @pl.when(jnp.logical_and(j == n_strip - 2, ends))
                def _():
                    trade.add_xz(s.order(3))

                @pl.when(jnp.logical_or(j == 1, j == n_strip - 1))
                def _():
                    send_wide(2 * away + jnp.where(j == 1, 0, 1))

                @pl.when(jnp.logical_and(j == n_strip, ends))
                def _():
                    trade.add_xz(s.order(2))

                @pl.when(jnp.logical_and(j == n_strip + 1, inner))
                def _():
                    trade.add_xz(s.order(3))

            send_wide(s.order(1))
            send_wide(z)

            @pl.when(inner)
            def _():
                trade.add_xz(s.order(2))

            trade.add_xz(s.order(1))
            trade.add_xz(z)
            trade.settle()

        pl.run_scoped(
            ffn,
            pltpu.VMEM((depth, 2, 2, n, d), bf16),
            pltpu.VMEM((depth, count, 2 * share), bf16),
            pltpu.VMEM((depth, count, share), bf16),
            pltpu.VMEM((2, depth, count, strip), bf16),
        )

        def hop_x(where, src, kind):
            return remote(src, where.at[c, x], t_put.at[kind, 0], t_got.at[kind, 0], s.at_x)

        def hop_c(where, src, kind):
            return remote(src, where.at[c, x], t_put.at[kind, 1], t_got.at[kind, 1], s.at_c)

        def hop_far(where, kind):
            return remote(where.at[c, 1 - x], where.at[c, 1 - x], t_put.at[kind, 2], t_got.at[kind, 2], s.at_c)

        def spread(where, src, kind):
            hop_x(where, src, kind).start()
            hop_c(where, src, kind).start()

        def spread_on(where, kind):
            got(t_got.at[kind, 0], where.at[c, 1 - x])
            hop_far(where, kind).start()

        def spread_end(where, kind):
            got(t_got.at[kind, 1], where.at[1 - c, x])
            got(t_got.at[kind, 2], where.at[1 - c, 1 - x])

        def attention(stage, w_a, normed_v, qkv_v, att_v, d_att, d_qkv, part_a, cos_v, sin_v, mask_v, field_v, other_v, cot_v):
            own_x = copy(x_ref.at[pl.ds(mine, n)], cot_v.at[1], in_sem.at[4])
            fills = [
                copy(hid_ref, field_v, in_sem.at[0]),
                copy(att_branch_ref, other_v, in_sem.at[1]),
                copy(cot_ref.at[pl.ds(mine, n)], cot_v.at[0], in_sem.at[2]),
            ]
            later = [
                copy(wa_ref, w_a, w_sem.at[0, 0]),
                copy(att_ref, att_v, w_sem.at[0, 1]),
                copy(qkv_ref, qkv_v, w_sem.at[1, 0]),
                copy(normed_ref, normed_v, w_sem.at[1, 1]),
                copy(cos_ref, cos_v, in_sem.at[5]),
                copy(sin_ref, sin_v, in_sem.at[6]),
                copy(mask_ref, mask_v, in_sem.at[7]),
                own_x,
            ]
            for fill in fills + later:
                fill.start()
            for fill in fills:
                fill.wait()

            @pl.loop(0, n // 16)
            def _(i):
                at = rows16(i)
                d_hidden = cot_v[0, at, :].astype(f32) + norm_back(field_v[at, :], gain_v[2:3, :], acc[at, :], 2)
                acc[at, :] = d_hidden
                dbr[c, x, at, :] = norm_back(other_v[at, :], gain_v[1:2, :], d_hidden, 1).astype(bf16)

            spread(dbr, dbr.at[c, x], 0)
            spread(out_all, own_out, 1)
            copy(own_out, out_all.at[c, x], o_sem.at[2]).start()
            for fill in later:
                fill.wait()
            spread_on(dbr, 0)
            f_sum(2, stage)
            spread_end(dbr, 0)

            for lo in range(0, q_cols, HD):
                value = jnp.dot(
                    dbr[...].reshape(count, d), w_a[:, qkv_cols + lo : qkv_cols + lo + HD], preferred_element_type=f32
                )
                d_att[:, lo : lo + HD] = value.astype(bf16)

            def turn(value, factor, at):
                low, high = value[:, : HD // 2], value[:, HD // 2 :]
                cosine, sine = cos_v[at, :], sin_v[at, :]
                return (low * cosine + high * sine) * factor, (high * cosine - low * sine) * factor

            def contract(left, right, dims):
                return lax.dot_general(left, right, ((dims[0], dims[1]), ((), ())), preferred_element_type=f32)

            @pl.loop(0, count // ROW_LEN)
            def _(r):
                at = pl.ds(pl.multiple_of(r * ROW_LEN, ROW_LEN), ROW_LEN)
                allowed = mask_v[at, :] > 0.5
                for kv in range(kv_heads):
                    k_at, v_at = q_cols + kv * HD, q_cols + k_cols + kv * HD
                    key, val = qkv_v[at, k_at : k_at + HD], qkv_v[at, v_at : v_at + HD]
                    d_key = jnp.zeros((ROW_LEN, HD), f32)
                    d_val = jnp.zeros((ROW_LEN, HD), f32)
                    for h in range(kv * group, (kv + 1) * group):
                        query = qkv_v[at, h * HD : (h + 1) * HD]
                        grad = d_att[at, h * HD : (h + 1) * HD]
                        bent = jnp.tanh(contract(query, key, ((1,), (1,))) / CAP)
                        expo = jnp.where(allowed, jnp.exp(CAP * bent), 0.0)
                        soft = expo / jnp.sum(expo, axis=-1, keepdims=True)
                        d_val = d_val + contract(soft.astype(bf16), grad, ((0,), (0,)))
                        d_probs = contract(grad, val, ((1,), (1,)))
                        d_soft = soft * (d_probs - jnp.sum(soft * d_probs, axis=-1, keepdims=True))
                        d_cap = (d_soft * (1.0 - bent * bent)).astype(bf16)
                        d_key = d_key + contract(d_cap, query, ((0,), (0,)))
                        low, high = turn(contract(d_cap, key, ((1,), (0,))), scale, at)
                        d_qkv[at, h * HD : h * HD + HD // 2] = low.astype(bf16)
                        d_qkv[at, h * HD + HD // 2 : (h + 1) * HD] = high.astype(bf16)
                    low, high = turn(d_key, 1.0, at)
                    d_qkv[at, k_at : k_at + HD // 2] = low.astype(bf16)
                    d_qkv[at, k_at + HD // 2 : k_at + HD] = high.astype(bf16)
                    d_qkv[at, v_at : v_at + HD] = d_val.astype(bf16)

            def attn_grads(side):
                at = pl.multiple_of(side * half, LANE)
                rows = pl.ds(at, half)
                for lo in range(0, qkv_cols, 256):
                    value = contract(normed_v[:, rows], d_qkv[:, lo : lo + 256], ((0,), (0,)))
                    g_attn[rows, lo : lo + 256] = value.astype(bf16)
                for lo in range(0, q_cols, 256):
                    value = contract(dbr[:, :, :, rows].reshape(count, half), att_v[:, lo : lo + 256], ((0,), (0,)))
                    g_attn[rows, qkv_cols + lo : qkv_cols + lo + 256] = value.astype(bf16)

            away = 1 - z // 2
            attn_grads(away)
            for i in (3, 2):
                for over in range(1, width):
                    a_wide(s.order(i), over).start()
            attn_grads(1 - away)
            for i in (1, 0):
                for over in range(1, width):
                    a_wide(s.order(i), over).start()

            @pl.loop(0, d // 256)
            def _(t):
                at = pl.multiple_of(t * 256, 256)
                value = lax.dot_general(
                    d_qkv[...], w_a[pl.ds(at, 256), :qkv_cols], (((1,), (1,)), ((), ())), preferred_element_type=f32
                )
                part_a[:, :, :, pl.ds(at, 256)] = value.astype(bf16).reshape(2, 2, n, 256)

            to_c = remote(part_a.at[1 - c], c_in.at[0], ra_put.at[0], ra_got.at[0], s.at_c)
            to_c.start()
            to_c.wait_recv()
            part_a[c, 1 - x] = (part_a[c, 1 - x].astype(f32) + c_in[0, 1 - x].astype(f32)).astype(bf16)
            to_x = remote(part_a.at[c, 1 - x], x_in.at[0], ra_put.at[1], ra_got.at[1], s.at_x)
            to_x.start()
            field_v[...] = part_a[c, x].astype(f32) + c_in[0, x].astype(f32)
            f_sum(1, stage)
            spread_on(out_all, 1)
            to_x.wait_recv()
            hop_x(out_all, own_out, 1).wait_send()
            hop_c(out_all, own_out, 1).wait_send()
            copy(own_out, out_all.at[c, x], o_sem.at[2]).wait()

            @pl.loop(0, n // 16)
            def _(i):
                at = rows16(i)
                grad = field_v[at, :] + x_in[0, at, :].astype(f32)
                d_source = norm_back(cot_v[1, at, :].astype(f32), gain_v[0:1, :], grad, 0)
                own_out[at, :] = (acc[at, :] + d_source).astype(bf16)

            to_c.wait_send()
            to_x.wait_send()
            spread(gin_all, own_out, 2)
            copy(own_out, gin_all.at[c, x], o_sem.at[3]).start()

        def finish(stage):
            f_sum(3, stage)
            pl.run_scoped(
                functools.partial(attention, stage),
                pltpu.VMEM((d, a_cols), bf16),
                pltpu.VMEM((count, d), bf16),
                pltpu.VMEM((count, qkv_cols), bf16),
                pltpu.VMEM((count, q_cols), bf16),
                pltpu.VMEM((count, q_cols), bf16),
                pltpu.VMEM((count, qkv_cols), bf16),
                pltpu.VMEM((2, 2, n, d), bf16),
                pltpu.VMEM((count, HD // 2), f32),
                pltpu.VMEM((count, HD // 2), f32),
                pltpu.VMEM((count, ROW_LEN), f32),
                pltpu.VMEM((n, d), f32),
                pltpu.VMEM((n, d), f32),
                pltpu.VMEM((2, n, d), bf16),
            )

            for k in range(4):
                gain_v[k : k + 1, :] = jnp.sum(gain_acc[k], axis=0, keepdims=True)
            whole = gain_v[...]
            for p in range(dp_n):
                turned = pltpu.roll(whole, (d - p * shard) % d, 1) if p else whole
                gain_put[p] = turned[:, :lanes]

            def gain_hop(k):
                to = (s.dp + k) % dp_n
                return remote(gain_put.at[to], gain_got.at[s.dp], gg_put.at[k - 1], gg_got.at[k - 1], (to, s.q))

            for k in range(1, dp_n):
                gain_hop(k).start()
            spread_on(gin_all, 2)
            f_sum(0, stage)

            f_deeps(lambda p: f_deep(s.order(1), 1, stage, p).wait_send())
            copy(stage.at[0], f_out.at[z], o_sem.at[0]).wait()
            for i in reversed(range(1, depth)):
                a_sum(i, stage)
            for k in range(1, dp_n):
                got(gg_got.at[k - 1], gain_got.at[(s.dp + dp_n - k) % dp_n])
            total = gain_put[s.dp]
            for k in range(1, dp_n):
                total = total + gain_got[(s.dp + dp_n - k) % dp_n]
            gain_x[0] = total
            across = remote(gain_x.at[0], gain_x.at[1], gt_put.at[0], gt_got.at[0], s.at_x)
            across.start()
            a_sum(0, stage)
            across.wait_recv()
            gain_c[0] = gain_x[0] + gain_x[1]
            beside = remote(gain_c.at[0], gain_c.at[1], gt_put.at[1], gt_got.at[1], s.at_c)
            beside.start()
            beside.wait_recv()
            gain_c[2] = gain_c[0] + gain_c[1]
            copy(gain_c.at[2], gains_out, o_sem.at[4]).start()

            spread_end(out_all, 1)
            spread_end(gin_all, 2)
            for i in range(1, depth):
                g = s.order(i)
                for p in (0, 1):
                    got(fz_got.at[g, p], f_out.at[g, :, pl.ds(f_parts[p][0], f_parts[p][1])])
                if len(f_parts) > 2:

                    @pl.when(full(g))
                    def _():
                        for p in (2, 3):
                            got(fz_got.at[g, p], f_out.at[g, :, pl.ds(f_parts[p][0], f_parts[p][1])])

            for i in range(depth):
                g = s.order(i)
                for over in range(1, width):
                    for k in range(2):
                        f_wide(g, over, k).wait_send()
                    a_wide(g, over).wait_send()
            a_left(s.order(1), 1, stage)
            for kind, where, src in ((0, dbr, dbr.at[c, x]), (1, out_all, own_out), (2, gin_all, own_out)):
                if kind != 1:
                    hop_x(where, src, kind).wait_send()
                    hop_c(where, src, kind).wait_send()
                hop_far(where, kind).wait_send()
            for k in range(1, dp_n):
                gain_hop(k).wait_send()
            across.wait_send()
            beside.wait_send()
            copy(stage.at[0, :, pl.ds(0, a_cols)], a_out, o_sem.at[1]).wait()
            copy(own_out, gin_all.at[c, x], o_sem.at[3]).wait()
            copy(gain_c.at[2], gains_out, o_sem.at[4]).wait()

        pl.run_scoped(finish, pltpu.VMEM((3, shard, 3 * share), bf16))

    shape = jax.ShapeDtypeStruct
    outs = (
        shape((2, 2, n, d), bf16),
        shape((2, 2, n, d), bf16),
        shape((depth, shard, 3 * share), bf16),
        shape((shard, a_cols), bf16),
        shape((max(others, 1), depth, shard, 3 * share), bf16),
        shape((max(others, 1), depth, shard, a_cols), bf16),
        shape((depth + 1, shard, a_cols), bf16),
        shape((8, lanes), f32),
    )
    operands = tuple(first) + tuple(weights) + tuple(saves)
    anywhere = pl.BlockSpec(memory_space=pl.ANY)
    dma = pltpu.SemaphoreType.DMA
    return pl.pallas_call(
        kernel,
        out_shape=outs,
        in_specs=[anywhere] * len(operands),
        out_specs=tuple([anywhere] * len(outs)),
        scratch_shapes=Trade.buffers(depth, n, d)
        + [
            pltpu.VMEM((d, 2 * share), bf16),
            pltpu.VMEM((d, share), bf16),
            pltpu.VMEM((d, a_cols), bf16),
            pltpu.VMEM((n, d), f32),
            pltpu.VMEM((2, 2, n, d), bf16),
            pltpu.VMEM((n, d), bf16),
            pltpu.VMEM((8, d), f32),
            pltpu.VMEM((4, 8, d), f32),
            pltpu.VMEM((dp_n, 8, lanes), f32),
            pltpu.VMEM((dp_n, 8, lanes), f32),
            pltpu.VMEM((2, 8, lanes), f32),
            pltpu.VMEM((3, 8, lanes), f32),
            dma((8,)),
            dma((dp_n, 2)),
            dma((3,)),
            dma((5,)),
            dma((3, 3)),
            dma((3, 3)),
            dma((depth, max(others, 1), 2)),
            dma((depth, max(others, 1), 2)),
            dma((depth, 4)),
            dma((depth, 4)),
            dma((depth, max(others, 1))),
            dma((depth, max(others, 1))),
            dma((depth,)),
            dma((depth,)),
            dma((depth,)),
            dma((dp_n - 1,)),
            dma((dp_n - 1,)),
            dma((2,)),
            dma((2,)),
            dma((2,)),
            dma((2,)),
        ]
        + Trade.semaphores(depth),
        compiler_params=pltpu.CompilerParams(collective_id=2, has_side_effects=True, vmem_limit_bytes=67_043_328),
        name="backward",
    )(*operands)


def unit_cuts(units, parts):
    tiles = units // LANE
    edges = [(tiles * k + parts - 1) // parts for k in range(parts + 1)]
    starts = [e * LANE for e in edges[:-1]]
    sizes = [(b - a) * LANE for a, b in zip(edges[:-1], edges[1:])]
    return starts, sizes, max(sizes)


def cut_units(block, cuts):
    starts, sizes, share = cuts
    return jnp.stack(
        [
            jnp.pad(block[:, a : a + n], ((0, 0), (0, share - n))) if n < share else block[:, a : a + n]
            for a, n in zip(starts, sizes)
        ]
    )


def join_units(blocks, cuts):
    starts, sizes, share = cuts
    return jnp.concatenate([blocks[k, :, :n] for k, n in enumerate(sizes)], axis=1)


def make_body(grid):
    def body(
        inputs,
        cotangent,
        segments,
        positions,
        w_query,
        w_key,
        w_value,
        w_output,
        w_gate,
        w_up,
        w_down,
        gain_attn,
        gain_post_attn,
        gain_ffw,
        gain_post_ffw,
    ):
        grid.here()
        count, width = inputs.shape
        shard = w_query.shape[0]
        group = HEADS // KV
        local_kv = w_key.shape[1] // HD
        local_heads = local_kv * group
        q_cols, k_cols = w_query.shape[1], w_key.shape[1]
        scale = 1.0 / math.sqrt(HD)
        part = count // grid.tensor
        rows = count // ROW_LEN
        cuts = unit_cuts(w_gate.shape[1], grid.depth)
        share = cuts[2]
        main = share // 256 * 256

        gains = 0.0
        line = lax.broadcasted_iota(jnp.int32, (16, shard + -shard % LANE), 0)
        for k, gain in enumerate((gain_attn, gain_post_attn, gain_ffw, gain_post_ffw)):
            gains = gains + jnp.where(line == k, jnp.pad(gain, (0, -shard % LANE)).astype(f32), 0.0)
        gains = gains.astype(bf16)
        angles = make_angles(positions, HD)[:, 0]
        cosine, sine = jnp.cos(angles), jnp.sin(angles)
        mask = row_mask(segments, rows, ROW_LEN).astype(f32).reshape(count, ROW_LEN)
        cut_gate, cut_up = cut_units(w_gate, cuts), cut_units(w_up, cuts)
        wide_blocks = jnp.concatenate(
            [cut_gate[:, :, :main], cut_up[:, :, :main], cut_gate[:, :, main:], cut_up[:, :, main:]], axis=2
        )
        slim_blocks = cut_units(w_down.T, cuts)
        w_attn = jnp.concatenate([w_query, w_key, w_value, w_output.T], axis=1)
        (full_attn, full_wide, full_slim, normed, qkv, attended, branch_attn, hidden, full_gains,
         all_normed, saved, mixed, branch_ffw) = forward_kernel(
            grid, inputs, w_attn, wide_blocks, slim_blocks, gains, cosine, sine,
            mask, local_heads, local_kv,
        )
        full_attn = full_attn.reshape(width, full_attn.shape[2])
        out_all, gin_all, blocks_ffn, grad_attn, _, _, _, d_gains = backward_kernel(
            grid,
            (branch_ffw, hidden, branch_attn, cotangent, inputs, full_gains),
            (full_attn, full_wide, full_slim),
            (saved, all_normed.reshape(grid.depth, count, width), mixed, normed, qkv, attended, cosine, sine, mask),
            local_heads, local_kv, cuts[1],
        )
        gate, upward = [], []
        for k, size in enumerate(cuts[1]):
            low, rest = min(size, main), max(size - main, 0)
            gate.append(blocks_ffn[k, :, :low])
            upward.append(blocks_ffn[k, :, main : main + low])
            if rest:
                gate.append(blocks_ffn[k, :, 2 * main : 2 * main + rest])
                upward.append(blocks_ffn[k, :, main + share : main + share + rest])
        grad_gate = jnp.concatenate(gate, axis=1).astype(f32)
        grad_up = jnp.concatenate(upward, axis=1).astype(f32)
        grad_down = join_units(blocks_ffn[:, :, 2 * share :], cuts).T.astype(f32)
        qkv_cols = q_cols + 2 * k_cols

        return (
            out_all.reshape(count, width),
            gin_all.reshape(count, width),
            grad_attn[:, :q_cols].astype(f32),
            grad_attn[:, q_cols : q_cols + k_cols].astype(f32),
            grad_attn[:, q_cols + k_cols : qkv_cols].astype(f32),
            grad_attn[:, qkv_cols:].T.astype(f32),
            grad_gate,
            grad_up,
            grad_down,
            d_gains[0, :shard],
            d_gains[1, :shard],
            d_gains[2, :shard],
            d_gains[3, :shard],
        )

    return body


def solution(mesh):
    placed = (
        P("dp", None),
        P("dp", None),
        P("dp"),
        P("dp"),
        P("dp", "tensor"),
        P("dp", "tensor"),
        P("dp", "tensor"),
        P("tensor", "dp"),
        P("dp", "tensor"),
        P("dp", "tensor"),
        P("tensor", "dp"),
        P("dp"),
        P("dp"),
        P("dp"),
        P("dp"),
    )
    return jax.shard_map(
        make_body(Grid(mesh)),
        mesh=mesh,
        in_specs=placed,
        out_specs=(
            P("dp", None),
            P("dp", None),
            P("dp", "tensor"),
            P("dp", "tensor"),
            P("dp", "tensor"),
            P("tensor", "dp"),
            P("dp", "tensor"),
            P("dp", "tensor"),
            P("tensor", "dp"),
            P("dp"),
            P("dp"),
            P("dp"),
            P("dp"),
        ),
        check_vma=False,
    )
```
